32 devices in a mesh: rows: 4 (over z), ty: 4 (over x, core), tx: 2 (over y).
Axes of the slice: x: 2, y: 2, z: 4, core: 2. Of those that a mesh axis runs over, the one named last changes fastest.
Arguments:
- latent: bfloat16 [12, 32, 32, 16], P('rows', 'ty', 'tx'), may hold values from -6 to 6
- skip_input: bfloat16 [12, 32, 32, 768], P('rows', 'ty', 'tx'), may hold values from -6 to 6
- segment_ids: int32 [12, 32, 32], P('rows'), may hold values from 0 to 2, as said below
- embed_weight: bfloat16 [768, 16], replicated, may hold values from -1.5 to 1.5
- embed_bias: bfloat16 [768], replicated, may hold values from -1.75 to 1.75
- skip_weight: bfloat16 [1536, 768], replicated, may hold values from -0.15625 to 0.15625
- skip_bias: bfloat16 [768], replicated, may hold values from -1.75 to 1.75
- norm1_gain: bfloat16 [768], replicated, may hold values from 0.5 to 1.5
- norm1_bias: bfloat16 [768], replicated, may hold values from -1.75 to 1.75
- qkv_weight: bfloat16 [768, 2304], replicated, may hold values from -0.21875 to 0.21875
- proj_weight: bfloat16 [768, 768], replicated, may hold values from -0.875 to 0.875
- proj_bias: bfloat16 [768], replicated, may hold values from -1.75 to 1.75
- norm2_gain: bfloat16 [768], replicated, may hold values from 0.5 to 1.5
- norm2_bias: bfloat16 [768], replicated, may hold values from -1.75 to 1.75
- fc1_weight: bfloat16 [768, 3072], replicated, may hold values from -0.21875 to 0.21875
- fc1_bias: bfloat16 [3072], replicated, may hold values from -1.75 to 1.75
- fc2_weight: bfloat16 [3072, 768], replicated, may hold values from -0.109375 to 0.109375
- fc2_bias: bfloat16 [768], replicated, may hold values from -1.75 to 1.75
- conv_weight: bfloat16 [768, 144], replicated, may hold values from -0.125 to 0.125
- cotangent: bfloat16 [12, 32, 32, 16], P('rows', 'ty', 'tx'), may hold values from -6 to 6
Outputs:
- output: bfloat16 [12, 32, 32, 16], P('rows', 'ty', 'tx')
- skip_input_grad: bfloat16 [12, 32, 32, 768], P('rows', 'ty', 'tx')
- embed_weight_grad: float32 [768, 16], P('rows')
- embed_bias_grad: float32 [768], P('rows')
- skip_weight_grad: float32 [1536, 768], P('rows')
- skip_bias_grad: float32 [768], P('rows')
- norm1_gain_grad: float32 [768], P('rows')
- norm1_bias_grad: float32 [768], P('rows')
- qkv_weight_grad: float32 [768, 2304], P('rows')
- proj_weight_grad: float32 [768, 768], P('rows')
- proj_bias_grad: float32 [768], P('rows')
- norm2_gain_grad: float32 [768], P('rows')
- norm2_bias_grad: float32 [768], P('rows')
- fc1_weight_grad: float32 [768, 3072], P('rows')
- fc1_bias_grad: float32 [3072], P('rows')
- fc2_weight_grad: float32 [3072, 768], P('rows')
- fc2_bias_grad: float32 [768], P('rows')
- conv_weight_grad: float32 [768, 144], P('rows')
The draws below stay inside these ranges and needn't reach their ends.
Inputs may be any that keep to these rules, and one draw needn't show every extreme that they name: `segment_ids`: each row's 32 x 32 grid is cut into three rectangular images: id 0 fills every grid row up to a left width, ids 1 and 2 fill the remaining columns above and below a top height; the width and the height are drawn for each row among the multiples of 4 from 8 to 24.
All inputs are finite; a program needn't handle non-finite values.
Results may differ from the reference program's by a relative error of at most 0.014.
Values may be sent and summed in bfloat16 or wider, within the bound.
A program may use at most 256 MiB of HBM per device.

```python
import jax
import jax.numpy as jnp
from jax import lax

D = 768
HEADS = 12
HEAD = 64
FF = 3072
PATCH = 16
GRID = 32
ROWS = 12


def draw_segment_ids(key, part):
    width_key, height_key = jax.random.split(key)
    step_unit = GRID // 8
    left_width = step_unit * jax.random.randint(width_key, (ROWS, 1, 1), 2, 7)
    top_height = step_unit * jax.random.randint(height_key, (ROWS, 1, 1), 2, 7)
    across_index = jnp.arange(GRID, dtype=jnp.int32)[None, None, :]
    down_index = jnp.arange(GRID, dtype=jnp.int32)[None, :, None]
    return jnp.where(across_index < left_width, 0, jnp.where(down_index < top_height, 1, 2)).astype(jnp.int32)


def level_of(stream_key, shape, cuts, low, top_value):
    gain = 1.0
    for position, parts in cuts:
        steps = jax.random.uniform(jax.random.fold_in(jax.random.fold_in(stream_key, 6), position), (parts,), jnp.float32, low / len(cuts), top_value / len(cuts))
        gain = gain * jnp.repeat(jnp.exp(steps), shape[position] // parts).reshape((-1,) + (1,) * (len(shape) - 1 - position))
    return gain


def noise(key, shape, scale, reach, cuts=(), kind=jnp.bfloat16):
    entries = jax.random.normal(key, shape, jnp.float32) * scale
    if len(cuts) > 0:
        entries = level_of(key, shape, cuts, -0.22, 0.18) * entries
    return jnp.clip(entries, min=-reach, max=reach).astype(kind)


def setup_inputs(seed: int = 0) -> dict:
    key_list = jax.random.split(jax.random.key(seed), 21)
    return {
        "latent": noise(key_list[0], (ROWS, GRID, GRID, PATCH), 1.0, 6.0, ((0, 4), (1, 4), (2, 2))),
        "skip_input": noise(key_list[1], (ROWS, GRID, GRID, D), 1.0, 6.0, ((0, 4), (1, 4), (2, 2))),
        "segment_ids": draw_segment_ids(jax.random.fold_in(key_list[20], 71), 0),
        "embed_weight": noise(key_list[3], (D, PATCH), PATCH ** -0.5, 1.5),
        "embed_bias": noise(key_list[4], (D,), 0.3, 1.75),
        "skip_weight": noise(key_list[5], (2 * D, D), (2 * D) ** -0.5, 0.15625),
        "skip_bias": noise(key_list[6], (D,), 0.3, 1.75),
        "norm1_gain": jnp.clip(1.0 + 0.1 * jax.random.normal(key_list[7], (D,), jnp.float32), 0.5, 1.5).astype(jnp.bfloat16),
        "norm1_bias": noise(key_list[8], (D,), 0.3, 1.75),
        "qkv_weight": noise(key_list[9], (D, 3 * D), D ** -0.5, 0.21875),
        "proj_weight": noise(key_list[10], (D, D), (D // 16) ** -0.5, 0.875),
        "proj_bias": noise(key_list[11], (D,), 0.3, 1.75),
        "norm2_gain": jnp.clip(1.0 + 0.1 * jax.random.normal(key_list[12], (D,), jnp.float32), 0.5, 1.5).astype(jnp.bfloat16),
        "norm2_bias": noise(key_list[13], (D,), 0.3, 1.75),
        "fc1_weight": noise(key_list[14], (D, FF), D ** -0.5, 0.21875),
        "fc1_bias": noise(key_list[15], (FF,), 0.3, 1.75),
        "fc2_weight": noise(key_list[16], (FF, D), FF ** -0.5, 0.109375),
        "fc2_bias": noise(key_list[17], (D,), 0.3, 1.75),
        "conv_weight": noise(key_list[18], (D, 9 * PATCH), (3 * D) ** -0.5, 0.125),
        "cotangent": noise(key_list[19], (ROWS, GRID, GRID, PATCH), 1.0, 6.0, ((0, 4), (1, 4), (2, 2))),
    }


@jax.custom_vjp
def low(v):
    return lax.optimization_barrier(v.astype(jnp.bfloat16)).astype(jnp.float32)

@jax.custom_vjp
def low_back(v):
    return v

def low_keep(v):
    return (low(v), None)

def low_pass(kept, grad):
    return (grad,)

def back_keep(v):
    return (v, None)

def back_low(kept, grad):
    return (low(grad),)
low.defvjp(low_keep, low_pass)
low_back.defvjp(back_keep, back_low)
norm_eps = 1e-05
masked_score = -1e+30
highest = lax.Precision.HIGHEST

def product(former, latter, pattern):
    return jnp.einsum(pattern, former, latter, precision=highest)

def layer_norm(values, norm_gain, norm_bias):
    average = lax.optimization_barrier(jnp.mean(values, axis=-1, keepdims=True))
    centred = values - average
    variance = lax.optimization_barrier(jnp.mean(centred * centred, axis=-1, keepdims=True))
    return centred * lax.rsqrt(variance + norm_eps) * norm_gain + norm_bias

def row_forward(weight_list, latent_row, skip_row, segment_row):
    embed_weight, embed_bias, skip_weight, skip_bias, norm1_gain, norm1_bias, qkv_weight, proj_weight, proj_bias, norm2_gain, norm2_bias, fc1_weight, fc1_bias, fc2_weight, fc2_bias, conv_weight = weight_list
    tokens = latent_row.reshape(GRID * GRID, PATCH)
    embedded = low_back(product(tokens, embed_weight, 'tc,dc->td')) + embed_bias
    joined = jnp.concatenate([low(embedded), skip_row.reshape(GRID * GRID, D)], axis=1)
    stream = low_back(product(joined, skip_weight, 'tj,jd->td')) + skip_bias
    normed = low(layer_norm(stream, norm1_gain, norm1_bias))
    projected = low_back(low(product(normed, qkv_weight, 'td,de->te')))
    queries = projected[:, :D].reshape(GRID * GRID, HEADS, HEAD)
    row_keys = projected[:, D:2 * D].reshape(GRID * GRID, HEADS, HEAD)
    values = projected[:, 2 * D:].reshape(GRID * GRID, HEADS, HEAD)
    flat_ids = segment_row.reshape(GRID * GRID)
    allowed = flat_ids[:, None] == flat_ids[None, :]
    scores = low_back(product(queries, row_keys, 'qhd,khd->hqk') * HEAD ** (-0.5))
    attention_weights = jax.nn.softmax(jnp.where(allowed[None], scores, masked_score), axis=-1)
    attended = product(low(attention_weights), values, 'hqk,khd->qhd').reshape(GRID * GRID, D)
    attended = low_back(low(attended))
    stream_mid = stream + low_back(product(attended, proj_weight, 'td,de->te')) + proj_bias
    normed_mid = low(layer_norm(stream_mid, norm2_gain, norm2_bias))
    hidden = low_back(product(normed_mid, fc1_weight, 'td,df->tf')) + fc1_bias
    activated = low(jax.nn.gelu(hidden, approximate=False))
    stream_out = stream_mid + low_back(product(activated, fc2_weight, 'tf,fd->td')) + fc2_bias
    conv_in = jnp.pad(low(stream_out).reshape(GRID, GRID, D), ((1, 1), (1, 1), (0, 0)))
    padded_ids = jnp.pad(segment_row, 1, constant_values=-1)
    result = jnp.zeros((GRID, GRID, PATCH), jnp.float32)
    offset_index = 0
    for down_step in (-1, 0, 1):
        for side_step in (-1, 0, 1):
            window = conv_in[1 + down_step:1 + down_step + GRID, 1 + side_step:1 + side_step + GRID, :]
            same = padded_ids[1 + down_step:1 + down_step + GRID, 1 + side_step:1 + side_step + GRID] == segment_row
            tap_weight = conv_weight[:, offset_index * PATCH:(offset_index + 1) * PATCH]
            result = result + jnp.where(same[:, :, None], product(window, tap_weight, 'yxc,ck->yxk'), 0.0)
            offset_index = offset_index + 1
    return result

def reference(latent, skip_input, segment_ids, embed_weight, embed_bias, skip_weight, skip_bias, norm1_gain, norm1_bias, qkv_weight, proj_weight, proj_bias, norm2_gain, norm2_bias, fc1_weight, fc1_bias, fc2_weight, fc2_bias, conv_weight, cotangent):
    weights = tuple((weight_array.astype(jnp.float32) for weight_array in (embed_weight, embed_bias, skip_weight, skip_bias, norm1_gain, norm1_bias, qkv_weight, proj_weight, proj_bias, norm2_gain, norm2_bias, fc1_weight, fc1_bias, fc2_weight, fc2_bias, conv_weight)))

    def one_row(totals, row_inputs):
        latent_row, skip_row, segment_row, cotangent_row = row_inputs

        def forward(weight_list, skip_value):
            return row_forward(weight_list, latent_row.astype(jnp.float32), skip_value, segment_row)
        result, pullback = jax.vjp(forward, weights, skip_row.astype(jnp.float32))
        weight_grads, skip_grad = pullback(cotangent_row.astype(jnp.float32))
        totals = jax.tree.map(jnp.add, totals, weight_grads)
        return (totals, (result.astype(jnp.bfloat16), skip_grad.astype(jnp.bfloat16)))
    zero_grads = jax.tree.map(jnp.zeros_like, weights)
    totals, (output, skip_input_grad) = lax.scan(one_row, zero_grads, (latent, skip_input, segment_ids, cotangent))
    return (output, skip_input_grad, totals[0], totals[1], totals[2], totals[3], totals[4], totals[5], totals[6], totals[7], totals[8], totals[9], totals[10], totals[11], totals[12], totals[13], totals[14], totals[15])
```

```python
import functools

import jax
import jax.numpy as jnp
from jax import lax
from jax.experimental import pallas as pl
from jax.experimental.pallas import tpu as pltpu
from jax.sharding import PartitionSpec as P

HEADS = 12
MESH = pl.DeviceIdType.MESH


norm_eps = 1e-05
masked_score = -1e30


def with_halo(x, sides, width):
    for axis, dim in sides:
        peers, length = (lax.axis_size(axis), x.shape[dim])
        up = [(i, (i + 1) % peers) for i in range(peers - 1)]
        down = [(j, i) for i, j in up]
        last = lax.slice_in_dim(x, length - width, length, axis=dim)
        first = lax.slice_in_dim(x, 0, width, axis=dim)
        before = lax.ppermute(last, axis, up)
        after = lax.ppermute(first, axis, down)
        x = jnp.concatenate([before, x, after], axis=dim)
    return x


def layer_norm(values, norm_gain, norm_bias):
    average = jnp.mean(values, axis=-1, keepdims=True)
    centred = values - average
    variance = jnp.mean(centred * centred, axis=-1, keepdims=True)
    return centred * lax.rsqrt(variance + norm_eps) * norm_gain + norm_bias


def gelu_exact(values):
    return jax.nn.gelu(values, approximate=False)


def product(former, latter, pattern):
    return jnp.einsum(pattern, former, latter, preferred_element_type=jnp.float32)


def add_rows(target, first, second, rows):
    step = 16

    def body(i, carry):
        at = pl.ds(pl.multiple_of(i * step, step), step)
        target[at, :] = first[at, :] + second[at, :]
        return carry

    lax.fori_loop(0, rows // step, body, 0)


def grad_reduce_kernel(shapes, *refs):
    count = len(shapes)
    grads = refs[:count]
    outs = refs[count : 2 * count]
    rest = refs[2 * count :]
    own, got, half, quarter, final = [rest[i * count : (i + 1) * count] for i in range(5)]
    local_sem, send_sem, recv_sem = rest[5 * count :]
    z, ty, y = lax.axis_index("rows"), lax.axis_index("ty"), lax.axis_index("tx")
    core, x = lax.rem(ty, 2), ty // 2
    peer_core = (z, x * 2 + 1 - core, y)
    peer_x = (z, (1 - x) * 2 + core, y)
    peer_y = (z, ty, 1 - y)
    peer_xy = (z, (1 - x) * 2 + core, 1 - y)
    peers_z = [(lax.rem(z + k, 4), ty, y) for k in (1, 2, 3)]
    barrier = pltpu.get_barrier_semaphore()
    everyone = [peer_core, peer_x, peer_y, peer_xy] + peers_z
    for peer in everyone:
        pl.semaphore_signal(barrier, inc=1, device_id=peer, device_id_type=MESH)
    pl.semaphore_wait(barrier, len(everyone))

    def send(w, slot, source, target, peer):
        return pltpu.make_async_remote_copy(
            src_ref=source,
            dst_ref=target,
            send_sem=send_sem.at[w, slot],
            recv_sem=recv_sem.at[w, slot],
            device_id=peer,
            device_id_type=MESH,
        )

    def columns(w, which):
        width = shapes[w][2] // 2
        return pl.ds(pl.multiple_of(which * width, 128), width)

    def rows(start, size):
        return pl.ds(pl.multiple_of(start, 16), size)

    def place(w, block):
        depth = shapes[w][1]
        later = block // 2
        major = x + later * (y - x)
        minor = y + later * (x - y)
        return rows(major * (depth // 2) + minor * (depth // 4), depth // 4)

    pending = [{} for _ in shapes]

    def begin(w):
        swap = send(w, 0, grads[w].at[:, :, columns(w, 1 - core)], got[w], peer_core)
        swap.start()
        mine = pltpu.make_async_copy(grads[w].at[:, :, columns(w, core)], own[w], local_sem.at[w, 0])
        mine.start()
        pending[w].update(swap=swap, mine=mine)

    def stage_core(w):
        depth = shapes[w][1]
        pending[w]["mine"].wait()
        pending[w]["swap"].wait()
        for block in range(4):
            add_rows(own[w].at[block], own[w].at[block], got[w].at[block], depth)
        first = send(w, 1, own[w].at[0:2, rows((1 - x) * (depth // 2), depth // 2)], half[w].at[0:2], peer_x)
        second = send(w, 2, own[w].at[2:4, rows((1 - y) * (depth // 2), depth // 2)], half[w].at[2:4], peer_y)
        first.start()
        second.start()
        pending[w].update(half=(first, second))

    def stage_half(w):
        depth = shapes[w][1]
        for copy in pending[w]["half"]:
            copy.wait()
        for block in range(4):
            side = x if block < 2 else y
            kept = own[w].at[block, rows(side * (depth // 2), depth // 2)]
            add_rows(kept, kept, half[w].at[block], depth // 2)
        first = send(w, 3, own[w].at[0:2, rows(x * (depth // 2) + (1 - y) * (depth // 4), depth // 4)], quarter[w].at[0:2], peer_y)
        second = send(w, 4, own[w].at[2:4, rows(y * (depth // 2) + (1 - x) * (depth // 4), depth // 4)], quarter[w].at[2:4], peer_x)
        first.start()
        second.start()
        pending[w].update(quarter=(first, second))

    def stage_quarter(w):
        depth = shapes[w][1]
        for copy in pending[w]["quarter"]:
            copy.wait()
        for block in range(4):
            kept = own[w].at[block, place(w, block // 2 * 2)]
            add_rows(kept, kept, quarter[w].at[block], depth // 4)
        copies = []
        for k, peer in enumerate(peers_z):
            block = peer[0]
            copy = send(w, 5 + k, own[w].at[block, place(w, block)], final[w].at[k], peer)
            copy.start()
            copies.append(copy)
        pending[w].update(final=copies)

    def stage_final(w):
        depth = shapes[w][1]
        for copy in pending[w]["final"]:
            copy.wait()
        kept = own[w].at[z, place(w, z)]
        total = final[w].at[0]

        def body(i, carry):
            at = pl.ds(pl.multiple_of(i * 16, 16), 16)
            parts = [ref[at, :].astype(jnp.float32) for ref in (kept, total, final[w].at[1], final[w].at[2])]
            total[at, :] = (parts[0] + parts[1] + (parts[2] + parts[3])).astype(jnp.bfloat16)
            return carry

        lax.fori_loop(0, depth // 64, body, 0)
        target = outs[w].at[place(w, z), columns(w, core)]
        copies = []
        for k, peer in enumerate((peer_x, peer_y, peer_xy)):
            copy = send(w, 8 + k, total, target, peer)
            copy.start()
            copies.append(copy)
        keep = pltpu.make_async_copy(total, target, local_sem.at[w, 1])
        keep.start()
        pending[w].update(gather=copies, keep=keep)

    def stage_gather(w):
        for copy in pending[w]["gather"]:
            copy.wait()
        pending[w]["keep"].wait()
        strip = outs[w].at[:, columns(w, core)]
        copy = send(w, 11, strip, strip, peer_core)
        copy.start()
        pending[w].update(strip=copy)

    def stage_strip(w):
        pending[w]["strip"].wait()

    for w in range(count):
        begin(w)
    stages = [stage_core, stage_half, stage_quarter, stage_final, stage_gather, stage_strip]
    for tick in range(count + len(stages) - 1):
        for depth_index in reversed(range(len(stages))):
            w = tick - depth_index
            if 0 <= w < count:
                stages[depth_index](w)


def grad_reduce(grads):
    shapes = tuple(entry.shape for entry in grads)
    count = len(shapes)
    low = jnp.bfloat16
    scratch = (
        [pltpu.VMEM((s[0], s[1], s[2] // 2), low) for s in shapes]
        + [pltpu.VMEM((s[0], s[1], s[2] // 2), low) for s in shapes]
        + [pltpu.VMEM((s[0], s[1] // 2, s[2] // 2), low) for s in shapes]
        + [pltpu.VMEM((s[0], s[1] // 4, s[2] // 2), low) for s in shapes]
        + [pltpu.VMEM((3, s[1] // 4, s[2] // 2), low) for s in shapes]
        + [
            pltpu.SemaphoreType.DMA((count, 2)),
            pltpu.SemaphoreType.DMA((count, 12)),
            pltpu.SemaphoreType.DMA((count, 12)),
        ]
    )
    return pl.pallas_call(
        functools.partial(grad_reduce_kernel, shapes),
        out_shape=[jax.ShapeDtypeStruct(s[1:], low) for s in shapes],
        in_specs=[pl.BlockSpec(memory_space=pl.ANY)] * count,
        out_specs=[pl.BlockSpec(memory_space=pl.ANY)] * count,
        scratch_shapes=scratch,
        compiler_params=pltpu.CompilerParams(collective_id=3, has_side_effects=True, vmem_limit_bytes=56 * 1024 * 1024),
        name="grad_reduce",
    )(*grads)


def sum_by_table(local_grads):
    band_count, column_count = lax.axis_size("ty"), lax.axis_size("tx")
    group_count = lax.axis_size("rows")
    tile_count = band_count * column_count
    table = jnp.concatenate([entry.reshape(group_count, -1) for entry in local_grads], axis=1)
    column_total = table.shape[1]
    padded_columns = -(-column_total // tile_count) * tile_count
    piece_width = padded_columns // tile_count
    table = table.reshape(group_count, tile_count, piece_width)
    shares = lax.psum_scatter(
        table.reshape(group_count * tile_count, piece_width),
        ("rows", "ty", "tx"),
        scatter_dimension=0,
        tiled=True,
    )
    summed = (
        lax.all_gather(shares.astype(jnp.bfloat16), ("ty", "tx"), axis=0, tiled=True)
        .astype(shares.dtype)
        .reshape(-1)
    )
    totals = []
    start_at = 0
    for entry in local_grads:
        length = entry.size // group_count
        shard_shape = (entry.shape[0] // group_count,) + entry.shape[1:]
        totals.append(summed[start_at : start_at + length].reshape(shard_shape))
        start_at = start_at + length
    return tuple(totals)


def sum_grads(local_grads):
    if (lax.axis_size("rows"), lax.axis_size("ty"), lax.axis_size("tx")) != (4, 4, 2):
        return sum_by_table(local_grads)
    low = jnp.bfloat16
    groups = 4
    blocks = [entry.reshape((groups, -1) + entry.shape[1:]) for entry in local_grads]
    wide = [k for k, entry in enumerate(local_grads) if entry.ndim == 2 and entry.shape[1] % 256 == 0]
    thin = [k for k, entry in enumerate(local_grads) if entry.ndim == 2 and k not in wide]
    flat = [k for k, entry in enumerate(local_grads) if entry.ndim == 1]
    thin_part = jnp.concatenate([blocks[k].astype(low) for k in thin], axis=2)
    thin_width = thin_part.shape[2]
    thin_part = jnp.pad(thin_part, ((0, 0), (0, 0), (0, -thin_width % 256)))
    flat_part = jnp.concatenate([blocks[k].astype(low) for k in flat], axis=1)
    flat_size = flat_part.shape[1]
    flat_part = jnp.pad(flat_part, ((0, 0), (0, -flat_size % (64 * 256))))
    flat_part = flat_part.reshape(groups, -1, 256)
    order = sorted(wide, key=lambda k: local_grads[k].size)
    order = order[:1] + order[1:][::-1]
    summed = grad_reduce([blocks[k].astype(low) for k in order] + [thin_part, flat_part])
    totals = {k: part.astype(jnp.float32) for k, part in zip(order, summed)}
    start_at = 0
    for k in thin:
        width = local_grads[k].shape[1]
        totals[k] = summed[-2][:, start_at : start_at + width].astype(jnp.float32)
        start_at = start_at + width
    line = summed[-1].reshape(-1)
    start_at = 0
    for k in flat:
        length = blocks[k].shape[1]
        totals[k] = line[start_at : start_at + length].astype(jnp.float32)
        start_at = start_at + length
    return tuple(totals[k] for k in range(len(local_grads)))


def shards(
    latent,
    skip_input,
    segment_ids,
    embed_weight,
    embed_bias,
    skip_weight,
    skip_bias,
    norm1_gain,
    norm1_bias,
    qkv_weight,
    proj_weight,
    proj_bias,
    norm2_gain,
    norm2_bias,
    fc1_weight,
    fc1_bias,
    fc2_weight,
    fc2_bias,
    conv_weight,
    cotangent,
):
    row_count, tile_height, tile_width, model_width = skip_input.shape
    patch_width = latent.shape[3]
    grid_side = segment_ids.shape[1]
    tile_tokens = tile_height * tile_width
    token_count = row_count * tile_tokens
    row_tokens = grid_side * grid_side
    head_count = HEADS
    head_size = model_width // head_count
    score_scale = head_size ** (-0.5)
    band_count = lax.axis_size("ty")
    column_count = lax.axis_size("tx")
    band_index = lax.axis_index("ty")
    column_index = lax.axis_index("tx")
    padded_ids = jnp.pad(segment_ids, ((0, 0), (1, 1), (1, 1)), constant_values=-1)
    window_ids = lax.dynamic_slice(
        padded_ids,
        (jnp.int32(0), band_index * tile_height, column_index * tile_width),
        (row_count, tile_height + 2, tile_width + 2),
    )
    own_ids = window_ids[:, 1:-1, 1:-1]
    shifts = [(down_step, side_step) for down_step in (-1, 0, 1) for side_step in (-1, 0, 1)]
    same_place = jnp.stack(
        [
            window_ids[
                :,
                1 + down_step : 1 + down_step + tile_height,
                1 + side_step : 1 + side_step + tile_width,
            ]
            == own_ids
            for down_step, side_step in shifts
        ],
        axis=-1,
    )
    key_ids = segment_ids.reshape(row_count, band_count, tile_height, column_count, tile_width)
    key_ids = key_ids.transpose(0, 1, 3, 2, 4).reshape(row_count, row_tokens)
    own_flat = own_ids.reshape(row_count, tile_tokens)
    allowed = own_flat[:, None, :, None] == key_ids[:, None, None, :]
    flat_latent = latent.reshape(token_count, patch_width)
    flat_skip = skip_input.reshape(token_count, model_width)
    embedded = product(flat_latent, embed_weight, "tc,dc->td") + embed_bias.astype(jnp.float32)
    joined = jnp.concatenate([embedded.astype(jnp.bfloat16), flat_skip], axis=1)
    stream = product(joined, skip_weight, "tj,jd->td") + skip_bias.astype(jnp.float32)
    normed, norm1_back = jax.vjp(
        layer_norm, stream, norm1_gain.astype(jnp.float32), norm1_bias.astype(jnp.float32)
    )
    normed_low = normed.astype(jnp.bfloat16)
    projected = product(normed_low, qkv_weight, "td,de->te").astype(jnp.bfloat16)
    queries = projected[:, :model_width].reshape(row_count, tile_tokens, head_count, head_size)
    local_pairs = projected[:, model_width:].reshape(row_count, tile_tokens, 2 * model_width)
    row_pairs = lax.all_gather(local_pairs, ("ty", "tx"), axis=1, tiled=True)
    row_keys = row_pairs[:, :, :model_width].reshape(row_count, row_tokens, head_count, head_size)
    values = row_pairs[:, :, model_width:].reshape(row_count, row_tokens, head_count, head_size)

    def masked_scores():
        raw_scores = product(queries, row_keys, "rqhd,rkhd->rhqk") * score_scale
        return jnp.where(allowed, raw_scores, masked_score)

    scores = masked_scores()
    row_peak = jnp.max(scores, axis=-1, keepdims=True)
    exponents = jnp.exp(scores - row_peak)
    row_total = jnp.sum(exponents, axis=-1, keepdims=True)
    attention_weights = exponents / row_total
    log_total = row_peak + jnp.log(row_total)
    attended = product(attention_weights.astype(jnp.bfloat16), values, "rhqk,rkhd->rqhd")
    attended = attended.astype(jnp.bfloat16).reshape(token_count, model_width)
    stream_mid = (
        stream + product(attended, proj_weight, "td,de->te") + proj_bias.astype(jnp.float32)
    )
    normed_mid, norm2_back = jax.vjp(
        layer_norm, stream_mid, norm2_gain.astype(jnp.float32), norm2_bias.astype(jnp.float32)
    )
    normed_mid_low = normed_mid.astype(jnp.bfloat16)
    hidden = product(normed_mid_low, fc1_weight, "td,df->tf") + fc1_bias.astype(jnp.float32)
    activated, gelu_back = jax.vjp(gelu_exact, hidden)
    active_low = activated.astype(jnp.bfloat16)
    stream_out = (
        stream_mid + product(active_low, fc2_weight, "tf,fd->td") + fc2_bias.astype(jnp.float32)
    )
    conv_in = stream_out.astype(jnp.bfloat16).reshape(
        row_count, tile_height, tile_width, model_width
    )
    rimmed = with_halo(conv_in, (("ty", 1), ("tx", 2)), 1)
    tap_values = product(rimmed, conv_weight, "ryxc,ck->ryxk")
    conv_sum = jnp.zeros((row_count, tile_height, tile_width, patch_width), jnp.float32)
    for offset_index, (down_step, side_step) in enumerate(shifts):
        window = tap_values[
            :,
            1 + down_step : 1 + down_step + tile_height,
            1 + side_step : 1 + side_step + tile_width,
            offset_index * patch_width : (offset_index + 1) * patch_width,
        ]
        conv_sum = conv_sum + jnp.where(
            same_place[..., offset_index : offset_index + 1], window, 0.0
        )
    output = conv_sum.astype(jnp.bfloat16)
    rim_cotangent = with_halo(cotangent, (("ty", 1), ("tx", 2)), 1)
    spread_parts = []
    for offset_index, (down_step, side_step) in enumerate(shifts):
        mirror = 8 - offset_index
        window = rim_cotangent[
            :,
            1 - down_step : 1 - down_step + tile_height,
            1 - side_step : 1 - side_step + tile_width,
            :,
        ]
        spread_parts.append(jnp.where(same_place[..., mirror : mirror + 1], window, 0.0))
    spread = jnp.concatenate(spread_parts, axis=-1)
    out_grad = product(spread, conv_weight, "ryxk,ck->ryxc").reshape(token_count, model_width)
    conv_weight_grad = product(conv_in, spread, "ryxc,ryxk->ck")
    out_low = out_grad.astype(jnp.bfloat16)
    fc2_bias_grad = jnp.sum(out_grad, axis=0)
    fc2_weight_grad = product(active_low, out_low, "tf,td->fd")
    active_grad = product(out_low, fc2_weight, "td,fd->tf")
    (hidden_grad,) = gelu_back(active_grad)
    fc1_bias_grad = jnp.sum(hidden_grad, axis=0)
    hidden_low = hidden_grad.astype(jnp.bfloat16)
    fc1_weight_grad = product(normed_mid_low, hidden_low, "td,tf->df")
    normed_mid_grad = product(hidden_low, fc1_weight, "tf,df->td")
    mid_part, norm2_gain_grad, norm2_bias_grad = norm2_back(normed_mid_grad)
    mid_grad = out_grad + mid_part
    mid_low = mid_grad.astype(jnp.bfloat16)
    proj_bias_grad = jnp.sum(mid_grad, axis=0)
    proj_weight_grad = product(attended, mid_low, "td,te->de")
    attended_grad = product(mid_low, proj_weight, "te,de->td").astype(jnp.bfloat16)
    attended_grad = attended_grad.reshape(row_count, tile_tokens, head_count, head_size)
    weights_again = jnp.exp(masked_scores() - log_total)
    weights_grad = product(attended_grad, values, "rqhd,rkhd->rhqk")
    weighted_sum = jnp.sum(weights_again * weights_grad, axis=-1, keepdims=True)
    score_grad = (weights_again * (weights_grad - weighted_sum)).astype(jnp.bfloat16)
    query_grad = product(score_grad, row_keys, "rhqk,rkhd->rqhd") * score_scale
    value_grad = product(weights_again.astype(jnp.bfloat16), attended_grad, "rhqk,rqhd->rkhd")
    key_grad = product(score_grad, queries, "rhqk,rqhd->rkhd") * score_scale
    pair_terms = jnp.concatenate(
        [
            key_grad.reshape(row_count, row_tokens, model_width),
            value_grad.reshape(row_count, row_tokens, model_width),
        ],
        axis=2,
    )
    own_pairs = lax.psum_scatter(
        pair_terms.astype(jnp.bfloat16), ("ty", "tx"), scatter_dimension=1, tiled=True
    ).astype(jnp.float32)
    projected_grad = jnp.concatenate(
        [
            query_grad.reshape(token_count, model_width),
            own_pairs.reshape(token_count, 2 * model_width),
        ],
        axis=1,
    )
    projected_grad = projected_grad.astype(jnp.bfloat16)
    qkv_weight_grad = product(normed_low, projected_grad, "td,te->de")
    normed_grad = product(projected_grad, qkv_weight, "te,de->td")
    stream_part, norm1_gain_grad, norm1_bias_grad = norm1_back(normed_grad)
    stream_grad = mid_grad + stream_part
    stream_low = stream_grad.astype(jnp.bfloat16)
    skip_bias_grad = jnp.sum(stream_grad, axis=0)
    skip_weight_grad = product(joined, stream_low, "tj,td->jd")
    joined_grad = product(stream_low, skip_weight, "td,jd->tj")
    skip_input_grad = joined_grad[:, model_width:].astype(jnp.bfloat16)
    skip_input_grad = skip_input_grad.reshape(row_count, tile_height, tile_width, model_width)
    embedded_grad = joined_grad[:, :model_width]
    embed_bias_grad = jnp.sum(embedded_grad, axis=0)
    embed_weight_grad = product(embedded_grad.astype(jnp.bfloat16), flat_latent, "td,tc->dc")
    local_grads = (
        embed_weight_grad,
        embed_bias_grad,
        skip_weight_grad,
        skip_bias_grad,
        norm1_gain_grad,
        norm1_bias_grad,
        qkv_weight_grad,
        proj_weight_grad,
        proj_bias_grad,
        norm2_gain_grad,
        norm2_bias_grad,
        fc1_weight_grad,
        fc1_bias_grad,
        fc2_weight_grad,
        fc2_bias_grad,
        conv_weight_grad,
    )
    return (output, skip_input_grad) + sum_grads(local_grads)


def solution(mesh):
    return jax.shard_map(
        shards,
        mesh=mesh,
        in_specs=(
            P("rows", "ty", "tx", None),
            P("rows", "ty", "tx", None),
            P("rows", None, None),
            P(),
            P(),
            P(),
            P(),
            P(),
            P(),
            P(),
            P(),
            P(),
            P(),
            P(),
            P(),
            P(),
            P(),
            P(),
            P(),
            P("rows", "ty", "tx", None),
        ),
        out_specs=(
            P("rows", "ty", "tx", None),
            P("rows", "ty", "tx", None),
            P("rows", None),
            P("rows"),
            P("rows", None),
            P("rows"),
            P("rows"),
            P("rows"),
            P("rows", None),
            P("rows", None),
            P("rows"),
            P("rows"),
            P("rows"),
            P("rows", None),
            P("rows"),
            P("rows", None),
            P("rows"),
            P("rows", None),
        ),
        check_vma=False,
    )
```

```python
import functools

import jax
import jax.numpy as jnp
from jax import lax
from jax.experimental import pallas as pl
from jax.experimental.pallas import tpu as pltpu
from jax.sharding import PartitionSpec as P

HEADS = 12
MESH = pl.DeviceIdType.MESH


norm_eps = 1e-05
masked_score = -1e30


def with_halo(x, sides, width):
    for axis, dim in sides:
        peers, length = (lax.axis_size(axis), x.shape[dim])
        up = [(i, (i + 1) % peers) for i in range(peers - 1)]
        down = [(j, i) for i, j in up]
        last = lax.slice_in_dim(x, length - width, length, axis=dim)
        first = lax.slice_in_dim(x, 0, width, axis=dim)
        before = lax.ppermute(last, axis, up)
        after = lax.ppermute(first, axis, down)
        x = jnp.concatenate([before, x, after], axis=dim)
    return x


def layer_norm(values, norm_gain, norm_bias):
    average = jnp.mean(values, axis=-1, keepdims=True)
    centred = values - average
    variance = jnp.mean(centred * centred, axis=-1, keepdims=True)
    return centred * lax.rsqrt(variance + norm_eps) * norm_gain + norm_bias


def gelu_exact(values):
    return jax.nn.gelu(values, approximate=False)


def product(former, latter, pattern):
    return jnp.einsum(pattern, former, latter, preferred_element_type=jnp.float32)


def add_rows(target, first, second, rows):
    step = 16

    def body(i, carry):
        at = pl.ds(pl.multiple_of(i * step, step), step)
        target[at, :] = first[at, :] + second[at, :]
        return carry

    lax.fori_loop(0, rows // step, body, 0)


def grad_reduce_kernel(shapes, *refs):
    count = len(shapes)
    grads = refs[:count]
    outs = refs[count : 2 * count]
    rest = refs[2 * count :]
    own, got, half, quarter, final = [rest[i * count : (i + 1) * count] for i in range(5)]
    local_sem, send_sem, recv_sem = rest[5 * count :]
    z, ty, y = lax.axis_index("rows"), lax.axis_index("ty"), lax.axis_index("tx")
    core, x = lax.rem(ty, 2), ty // 2
    peer_core = (z, x * 2 + 1 - core, y)
    peer_x = (z, (1 - x) * 2 + core, y)
    peer_y = (z, ty, 1 - y)
    peer_xy = (z, (1 - x) * 2 + core, 1 - y)
    peers_z = [(lax.rem(z + k, 4), ty, y) for k in (1, 2, 3)]
    barrier = pltpu.get_barrier_semaphore()
    everyone = [peer_core, peer_x, peer_y, peer_xy] + peers_z
    for peer in everyone:
        pl.semaphore_signal(barrier, inc=1, device_id=peer, device_id_type=MESH)
    pl.semaphore_wait(barrier, len(everyone))

    def send(w, slot, source, target, peer):
        return pltpu.make_async_remote_copy(
            src_ref=source,
            dst_ref=target,
            send_sem=send_sem.at[w, slot],
            recv_sem=recv_sem.at[w, slot],
            device_id=peer,
            device_id_type=MESH,
        )

    def columns(w, which):
        width = shapes[w][2] // 2
        return pl.ds(pl.multiple_of(which * width, 128), width)

    def rows(start, size):
        return pl.ds(pl.multiple_of(start, 16), size)

    def place(w, block):
        depth = shapes[w][1]
        later = block // 2
        major = x + later * (y - x)
        minor = y + later * (x - y)
        return rows(major * (depth // 2) + minor * (depth // 4), depth // 4)

    pending = [{} for _ in shapes]

    def begin(w):
        swap = send(w, 0, grads[w].at[:, :, columns(w, 1 - core)], got[w], peer_core)
        swap.start()
        mine = pltpu.make_async_copy(grads[w].at[:, :, columns(w, core)], own[w], local_sem.at[w, 0])
        mine.start()
        pending[w].update(swap=swap, mine=mine)

    def stage_core(w):
        depth = shapes[w][1]
        pending[w]["mine"].wait()
        pending[w]["swap"].wait()
        for block in range(4):
            add_rows(own[w].at[block], own[w].at[block], got[w].at[block], depth)
        first = send(w, 1, own[w].at[0:2, rows((1 - x) * (depth // 2), depth // 2)], half[w].at[0:2], peer_x)
        second = send(w, 2, own[w].at[2:4, rows((1 - y) * (depth // 2), depth // 2)], half[w].at[2:4], peer_y)
        first.start()
        second.start()
        pending[w].update(half=(first, second))

    def stage_half(w):
        depth = shapes[w][1]
        for copy in pending[w]["half"]:
            copy.wait()
        for block in range(4):
            side = x if block < 2 else y
            kept = own[w].at[block, rows(side * (depth // 2), depth // 2)]
            add_rows(kept, kept, half[w].at[block], depth // 2)
        first = send(w, 3, own[w].at[0:2, rows(x * (depth // 2) + (1 - y) * (depth // 4), depth // 4)], quarter[w].at[0:2], peer_y)
        second = send(w, 4, own[w].at[2:4, rows(y * (depth // 2) + (1 - x) * (depth // 4), depth // 4)], quarter[w].at[2:4], peer_x)
        first.start()
        second.start()
        pending[w].update(quarter=(first, second))

    def stage_quarter(w):
        depth = shapes[w][1]
        for copy in pending[w]["quarter"]:
            copy.wait()
        for block in range(4):
            kept = own[w].at[block, place(w, block // 2 * 2)]
            add_rows(kept, kept, quarter[w].at[block], depth // 4)
        copies = []
        for k, peer in enumerate(peers_z):
            block = peer[0]
            copy = send(w, 5 + k, own[w].at[block, place(w, block)], final[w].at[k], peer)
            copy.start()
            copies.append(copy)
        pending[w].update(final=copies)

    def stage_final(w):
        depth = shapes[w][1]
        for copy in pending[w]["final"]:
            copy.wait()
        kept = own[w].at[z, place(w, z)]
        total = final[w].at[0]

        def body(i, carry):
            at = pl.ds(pl.multiple_of(i * 16, 16), 16)
            parts = [ref[at, :].astype(jnp.float32) for ref in (kept, total, final[w].at[1], final[w].at[2])]
            total[at, :] = (parts[0] + parts[1] + (parts[2] + parts[3])).astype(jnp.bfloat16)
            return carry

        lax.fori_loop(0, depth // 64, body, 0)
        target = outs[w].at[place(w, z), columns(w, core)]
        copies = []
        for k, peer in enumerate((peer_x, peer_y, peer_xy)):
            copy = send(w, 8 + k, total, target, peer)
            copy.start()
            copies.append(copy)
        keep = pltpu.make_async_copy(total, target, local_sem.at[w, 1])
        keep.start()
        pending[w].update(gather=copies, keep=keep)

    def stage_gather(w):
        for copy in pending[w]["gather"]:
            copy.wait()
        pending[w]["keep"].wait()
        strip = outs[w].at[:, columns(w, core)]
        copy = send(w, 11, strip, strip, peer_core)
        copy.start()
        pending[w].update(strip=copy)

    def stage_strip(w):
        pending[w]["strip"].wait()

    for w in range(count):
        begin(w)
    stages = [stage_core, stage_half, stage_quarter, stage_final, stage_gather, stage_strip]
    for tick in range(count + len(stages) - 1):
        for depth_index in reversed(range(len(stages))):
            w = tick - depth_index
            if 0 <= w < count:
                stages[depth_index](w)


def grad_reduce(grads):
    shapes = tuple(entry.shape for entry in grads)
    count = len(shapes)
    low = jnp.bfloat16
    scratch = (
        [pltpu.VMEM((s[0], s[1], s[2] // 2), low) for s in shapes]
        + [pltpu.VMEM((s[0], s[1], s[2] // 2), low) for s in shapes]
        + [pltpu.VMEM((s[0], s[1] // 2, s[2] // 2), low) for s in shapes]
        + [pltpu.VMEM((s[0], s[1] // 4, s[2] // 2), low) for s in shapes]
        + [pltpu.VMEM((3, s[1] // 4, s[2] // 2), low) for s in shapes]
        + [
            pltpu.SemaphoreType.DMA((count, 2)),
            pltpu.SemaphoreType.DMA((count, 12)),
            pltpu.SemaphoreType.DMA((count, 12)),
        ]
    )
    return pl.pallas_call(
        functools.partial(grad_reduce_kernel, shapes),
        out_shape=[jax.ShapeDtypeStruct(s[1:], low) for s in shapes],
        in_specs=[pl.BlockSpec(memory_space=pl.ANY)] * count,
        out_specs=[pl.BlockSpec(memory_space=pl.ANY)] * count,
        scratch_shapes=scratch,
        compiler_params=pltpu.CompilerParams(collective_id=3, has_side_effects=True, vmem_limit_bytes=56 * 1024 * 1024),
        name="grad_reduce",
    )(*grads)


def plane_peers():
    z, ty, y = lax.axis_index("rows"), lax.axis_index("ty"), lax.axis_index("tx")
    core, x = lax.rem(ty, 2), ty // 2
    here = x * 2 + core
    across = (1 - x) * 2 + core
    tiles = {
        "own": here * 2 + y,
        "x": across * 2 + y,
        "y": here * 2 + 1 - y,
        "xy": across * 2 + 1 - y,
    }
    peers = {
        "core": (z, x * 2 + 1 - core, y),
        "x": (z, across, y),
        "y": (z, here, 1 - y),
    }
    return tiles, peers


def greet(peers):
    barrier = pltpu.get_barrier_semaphore()
    for peer in peers:
        pl.semaphore_signal(barrier, inc=1, device_id=peer, device_id_type=MESH)
    pl.semaphore_wait(barrier, len(peers))


def fill_mask(mask_ref, cuts_ref, row, tile_height, tile_width):
    ty, tx = lax.axis_index("ty"), lax.axis_index("tx")
    columns = lax.axis_size("tx")
    tokens = tile_height * tile_width
    left_width = cuts_ref[row, 0]
    top_height = cuts_ref[row, 1]

    def image_of(down, across):
        return jnp.where(across < left_width, 0, jnp.where(down < top_height, 1, 2))

    lane = lax.broadcasted_iota(jnp.int32, (tokens, tokens), 1)
    step = lax.broadcasted_iota(jnp.int32, (tokens, tokens), 0)
    mine = image_of(
        ty * tile_height + lane // tile_width, tx * tile_width + lane % tile_width
    )
    for tile in range(mask_ref.shape[0] // tokens):
        theirs = image_of(
            tile // columns * tile_height + step // tile_width,
            tile % columns * tile_width + step % tile_width,
        )
        mask_ref[tile * tokens : (tile + 1) * tokens, :] = jnp.where(
            mine == theirs, 0.0, -1e30
        )


def two_heads(pair, scale):
    lane = lax.broadcasted_iota(jnp.int32, pair.shape, 1)
    wide = pair.astype(jnp.float32) * scale
    first = jnp.where(lane < pair.shape[1] // 2, wide, 0.0)
    return jnp.concatenate([first, wide - first], axis=0).astype(jnp.bfloat16)


def mm(former, latter, axis_former, axis_latter):
    return lax.dot_general(
        former,
        latter,
        (((axis_former,), (axis_latter,)), ((), ())),
        preferred_element_type=jnp.float32,
    )


def own_blocks(both):
    head, tokens = both.shape[0] // 2, both.shape[1] // 2
    return jnp.concatenate([both[:head, :tokens], both[head:, tokens:]], axis=0)


def attend_kernel(
    tile_height, tile_width, cuts, query, pairs, out, lse, all_out, held, scores, mask, local_sem, send_sem, recv_sem
):
    row_count, tokens, width = query.shape
    tile_count = held.shape[1]
    pair_count = width // 128
    tiles, peers = plane_peers()
    own = tiles["own"]
    greet(list(peers.values()))

    def send(row, slot, source, target, peer):
        copy = pltpu.make_async_remote_copy(
            src_ref=source,
            dst_ref=target,
            send_sem=send_sem.at[row, slot],
            recv_sem=recv_sem.at[row, slot],
            device_id=peer,
            device_id_type=MESH,
        )
        copy.start()
        return copy

    flights = [{} for _ in range(row_count)]

    def begin(row):
        here = held.at[row, own]
        source = pairs.at[row]
        flights[row]["x"] = send(row, 0, source, here, peers["x"])
        flights[row]["y"] = send(row, 1, source, here, peers["y"])
        flights[row]["core"] = send(row, 2, source, here, peers["core"])
        keep = pltpu.make_async_copy(source, here, local_sem.at[row, 0])
        keep.start()
        flights[row]["keep"] = keep

    def forward(row):
        flights[row]["y"].wait_recv()
        key_half = held.at[row, tiles["y"], :, pl.ds(0, width)]
        flights[row]["far_x"] = send(row, 3, key_half, key_half, peers["x"])
        flights[row]["x"].wait_recv()
        value_half = held.at[row, tiles["x"], :, pl.ds(width, width)]
        flights[row]["far_y"] = send(row, 4, value_half, value_half, peers["y"])
        for slot, name in ((5, "x"), (6, "y")):
            tile = held.at[row, tiles[name]]
            flights[row]["core_" + name] = send(row, slot, tile, tile, peers["core"])

    def finish(row):
        flights[row]["far_x"].wait_recv()
        flights[row]["far_y"].wait_recv()
        tile = held.at[row, tiles["xy"]]
        last = send(row, 7, tile, tile, peers["core"])
        flights[row]["keep"].wait()
        for name in ("core", "core_x", "core_y"):
            flights[row][name].wait_recv()
        last.wait_recv()
        for name in ("x", "y", "core", "far_x", "far_y", "core_x", "core_y"):
            flights[row][name].wait_send()
        last.wait_send()
        keep = pltpu.make_async_copy(held.at[row], all_out.at[row], local_sem.at[row, 1])
        keep.start()
        flights[row]["out"] = keep

    chunk = 2

    def compute(row):
        fill_mask(mask, cuts, row, tile_height, tile_width)

        def one_pair(p, carry):
            at = pl.ds(pl.multiple_of(p * 128, 128), 128)
            at_value = pl.ds(pl.multiple_of(width + p * 128, 128), 128)
            both = two_heads(query[row, :, at], 0.125)
            peak = None
            for c in range(tile_count // chunk):
                span = slice(c * chunk * tokens, (c + 1) * chunk * tokens)
                keys = held[row, c * chunk : (c + 1) * chunk, :, at].reshape(chunk * tokens, 128)
                extra = mask[span, :]
                part = mm(keys, both, 1, 1) + jnp.concatenate([extra, extra], axis=1)
                scores[span, :] = part
                top = jnp.max(part, axis=0, keepdims=True)
                peak = top if peak is None else jnp.maximum(peak, top)
            total = jnp.zeros_like(peak)
            summed = jnp.zeros((128, 2 * tokens), jnp.float32)
            for c in range(tile_count // chunk):
                span = slice(c * chunk * tokens, (c + 1) * chunk * tokens)
                values = held[row, c * chunk : (c + 1) * chunk, :, at_value].reshape(chunk * tokens, 128)
                part = jnp.exp(scores[span, :] - peak)
                total = total + jnp.sum(part, axis=0, keepdims=True)
                summed = summed + mm(values, part.astype(jnp.bfloat16), 0, 0)
            blocks = own_blocks(summed / total)
            out[row, :, at] = jnp.transpose(blocks).astype(jnp.bfloat16)
            lse[row, p] = peak + jnp.log(total)
            return carry

        lax.fori_loop(0, pair_count, one_pair, 0)

    begin(0)
    if row_count > 1:
        begin(1)
    forward(0)
    for row in range(row_count):
        if row + 2 < row_count:
            begin(row + 2)
        if row + 1 < row_count:
            forward(row + 1)
        finish(row)
        compute(row)
    for row in range(row_count):
        flights[row]["out"].wait()


def attend(cuts, query, pairs, tile_height, tile_width):
    row_count, tokens, width = query.shape
    tile_count = lax.axis_size("ty") * lax.axis_size("tx")
    pair_count = width // 128
    low = jnp.bfloat16
    vmem = pl.BlockSpec(memory_space=pltpu.VMEM)
    return pl.pallas_call(
        functools.partial(attend_kernel, tile_height, tile_width),
        out_shape=[
            jax.ShapeDtypeStruct((row_count, tokens, width), low),
            jax.ShapeDtypeStruct((row_count, pair_count, 1, 2 * tokens), jnp.float32),
            jax.ShapeDtypeStruct((row_count, tile_count, tokens, 2 * width), low),
        ],
        in_specs=[pl.BlockSpec(memory_space=pltpu.SMEM), vmem, pl.BlockSpec(memory_space=pl.ANY)],
        out_specs=[vmem, vmem, pl.BlockSpec(memory_space=pl.ANY)],
        scratch_shapes=[
            pltpu.VMEM((row_count, tile_count, tokens, 2 * width), low),
            pltpu.VMEM((tile_count * tokens, 2 * tokens), jnp.float32),
            pltpu.VMEM((tile_count * tokens, tokens), jnp.float32),
            pltpu.SemaphoreType.DMA((row_count, 2)),
            pltpu.SemaphoreType.DMA((row_count, 8)),
            pltpu.SemaphoreType.DMA((row_count, 8)),
        ],
        compiler_params=pltpu.CompilerParams(
            collective_id=1, has_side_effects=True, vmem_limit_bytes=40 * 1024 * 1024
        ),
        name="attend",
    )(cuts, query, pairs)


def attend_back_kernel(
    tile_height, tile_width, cuts, query, attended, grad, lse, all_pairs, out,
    held, terms, core_terms, side_terms, mask, deltas, load_sem, send_sem, recv_sem
):
    row_count, tokens, width = query.shape
    tile_count = held.shape[1]
    pair_count = width // 128
    tiles, peers = plane_peers()
    low = jnp.bfloat16
    loads = []
    for row in range(row_count):
        load = pltpu.make_async_copy(all_pairs.at[row], held.at[row], load_sem.at[row])
        load.start()
        loads.append(load)
    greet(list(peers.values()))
    z, ty, y = lax.axis_index("rows"), lax.axis_index("ty"), lax.axis_index("tx")
    core = lax.rem(ty, 2)
    chunk = 2

    def send(row, slot, source, target, peer):
        copy = pltpu.make_async_remote_copy(
            src_ref=source,
            dst_ref=target,
            send_sem=send_sem.at[row, slot],
            recv_sem=recv_sem.at[row, slot],
            device_id=peer,
            device_id_type=MESH,
        )
        copy.start()
        return copy

    def compute(row):
        loads[row].wait()
        fill_mask(mask, cuts, row, tile_height, tile_width)

        def one_pair(p, carry):
            at = pl.ds(pl.multiple_of(p * 128, 128), 128)
            at_value = pl.ds(pl.multiple_of(width + p * 128, 128), 128)
            grad_pair = grad[row, :, at]
            both = two_heads(query[row, :, at], 0.125)
            both_grad = two_heads(grad_pair, 1.0)
            inner = jnp.transpose(grad_pair.astype(jnp.float32) * attended[row, :, at].astype(jnp.float32))
            half = inner.shape[0] // 2
            delta = jnp.concatenate(
                [jnp.sum(inner[:half], axis=0, keepdims=True), jnp.sum(inner[half:], axis=0, keepdims=True)], axis=1
            )
            level = lse[row, p]
            query_part = jnp.zeros((128, 2 * tokens), jnp.float32)
            for c in range(tile_count // chunk):
                span = slice(c * chunk * tokens, (c + 1) * chunk * tokens)
                some = slice(c * chunk, (c + 1) * chunk)
                keys = held[row, some, :, at].reshape(chunk * tokens, 128)
                values = held[row, some, :, at_value].reshape(chunk * tokens, 128)
                extra = mask[span, :]
                weights = jnp.exp(mm(keys, both, 1, 1) + jnp.concatenate([extra, extra], axis=1) - level)
                score_grad = (weights * (mm(values, both_grad, 1, 1) - delta)).astype(low)
                value_part = mm(weights.astype(low), both_grad, 1, 0)
                key_part = mm(score_grad, both, 1, 0)
                query_part = query_part + mm(keys, score_grad, 0, 0)
                terms[row, some, :, at] = key_part.astype(low).reshape(chunk, tokens, 128)
                terms[row, some, :, at_value] = value_part.astype(low).reshape(chunk, tokens, 128)
            blocks = own_blocks(query_part) * 0.125
            out[row, :, at] = jnp.transpose(blocks).astype(low)
            return carry

        lax.fori_loop(0, pair_count, one_pair, 0)

    flights = [{} for _ in range(row_count)]
    names = ("own", "x", "y", "xy")
    key_at, value_at = pl.ds(0, width), pl.ds(width, width)

    def begin(row):
        copies = []
        other = 2 - 4 * core
        for k, name in enumerate(names):
            copies.append(send(row, k, terms.at[row, tiles[name] + other], core_terms.at[row, k], peers["core"]))
        flights[row]["core"] = copies

    def add(target, source, row_total):
        def body(i, carry):
            at = pl.ds(pl.multiple_of(i * 16, 16), 16)
            target[at, :] = target[at, :] + source[at, :]
            return carry

        lax.fori_loop(0, row_total // 16, body, 0)

    def spread(row):
        for k in (3, 1, 2, 0):
            flights[row]["core"][k].wait()
            add(terms.at[row, tiles[names[k]]], core_terms.at[row, k], tokens)
            if k == 3:
                far = terms.at[row, tiles["xy"]]
                flights[row]["far_x"] = send(row, 4, far.at[:, key_at], side_terms.at[row, 0], peers["x"])
                flights[row]["far_y"] = send(row, 5, far.at[:, value_at], side_terms.at[row, 1], peers["y"])
            if k == 1:
                near = terms.at[row, tiles["x"]]
                flights[row]["near_x"] = send(row, 6, near.at[:, key_at], side_terms.at[row, 2], peers["x"])
            if k == 2:
                near = terms.at[row, tiles["y"]]
                flights[row]["near_y"] = send(row, 7, near.at[:, value_at], side_terms.at[row, 3], peers["y"])

    def pass_on(row):
        flights[row]["far_x"].wait()
        near = terms.at[row, tiles["y"], :, key_at]
        add(near, side_terms.at[row, 0], tokens)
        flights[row]["last_y"] = send(row, 8, near, side_terms.at[row, 4], peers["y"])
        flights[row]["far_y"].wait()
        near = terms.at[row, tiles["x"], :, value_at]
        add(near, side_terms.at[row, 1], tokens)
        flights[row]["last_x"] = send(row, 9, near, side_terms.at[row, 5], peers["x"])

    def close(row):
        for name in ("near_x", "near_y", "last_x", "last_y"):
            flights[row][name].wait()
        mine = terms.at[row, tiles["own"]]

        def body(i, carry):
            at = pl.ds(pl.multiple_of(i * 16, 16), 16)
            for start, first, second in ((0, 2, 4), (width, 3, 5)):
                total = mine[at, start : start + width].astype(jnp.float32)
                total = total + side_terms[row, first, at, :].astype(jnp.float32)
                total = total + side_terms[row, second, at, :].astype(jnp.float32)
                out[row, at, width + start : 2 * width + start] = total.astype(low)
            return carry

        lax.fori_loop(0, tokens // 16, body, 0)

    for row in range(row_count):
        compute(row)
        begin(row)
        if row > 0:
            spread(row - 1)
        if row > 1:
            pass_on(row - 2)
    spread(row_count - 1)
    for row in range(max(row_count - 2, 0), row_count):
        pass_on(row)
    for row in range(row_count):
        close(row)


def attend_back(cuts, query, attended, grad, lse, all_pairs, tile_height, tile_width):
    row_count, tokens, width = query.shape
    tile_count = all_pairs.shape[1]
    low = jnp.bfloat16
    vmem = pl.BlockSpec(memory_space=pltpu.VMEM)
    return pl.pallas_call(
        functools.partial(attend_back_kernel, tile_height, tile_width),
        out_shape=jax.ShapeDtypeStruct((row_count, tokens, 3 * width), low),
        in_specs=[pl.BlockSpec(memory_space=pltpu.SMEM)] + [vmem] * 4 + [pl.BlockSpec(memory_space=pl.ANY)],
        out_specs=vmem,
        scratch_shapes=[
            pltpu.VMEM((row_count, tile_count, tokens, 2 * width), low),
            pltpu.VMEM((row_count, tile_count, tokens, 2 * width), low),
            pltpu.VMEM((row_count, 4, tokens, 2 * width), low),
            pltpu.VMEM((row_count, 6, tokens, width), low),
            pltpu.VMEM((tile_count * tokens, tokens), jnp.float32),
            pltpu.VMEM((8, 2 * tokens), jnp.float32),
            pltpu.SemaphoreType.DMA((row_count,)),
            pltpu.SemaphoreType.DMA((row_count, 10)),
            pltpu.SemaphoreType.DMA((row_count, 10)),
        ],
        compiler_params=pltpu.CompilerParams(
            collective_id=2, has_side_effects=True, vmem_limit_bytes=50 * 1024 * 1024
        ),
        name="attend_back",
    )(cuts, query, attended, grad, lse, all_pairs)


def sum_by_table(local_grads):
    band_count, column_count = lax.axis_size("ty"), lax.axis_size("tx")
    group_count = lax.axis_size("rows")
    tile_count = band_count * column_count
    table = jnp.concatenate([entry.reshape(group_count, -1) for entry in local_grads], axis=1)
    column_total = table.shape[1]
    padded_columns = -(-column_total // tile_count) * tile_count
    piece_width = padded_columns // tile_count
    table = table.reshape(group_count, tile_count, piece_width)
    shares = lax.psum_scatter(
        table.reshape(group_count * tile_count, piece_width),
        ("rows", "ty", "tx"),
        scatter_dimension=0,
        tiled=True,
    )
    summed = (
        lax.all_gather(shares.astype(jnp.bfloat16), ("ty", "tx"), axis=0, tiled=True)
        .astype(shares.dtype)
        .reshape(-1)
    )
    totals = []
    start_at = 0
    for entry in local_grads:
        length = entry.size // group_count
        shard_shape = (entry.shape[0] // group_count,) + entry.shape[1:]
        totals.append(summed[start_at : start_at + length].reshape(shard_shape))
        start_at = start_at + length
    return tuple(totals)


def sum_grads(local_grads):
    if (lax.axis_size("rows"), lax.axis_size("ty"), lax.axis_size("tx")) != (4, 4, 2):
        return sum_by_table(local_grads)
    low = jnp.bfloat16
    groups = 4
    blocks = [entry.reshape((groups, -1) + entry.shape[1:]) for entry in local_grads]
    wide = [k for k, entry in enumerate(local_grads) if entry.ndim == 2 and entry.shape[1] % 256 == 0]
    thin = [k for k, entry in enumerate(local_grads) if entry.ndim == 2 and k not in wide]
    flat = [k for k, entry in enumerate(local_grads) if entry.ndim == 1]
    thin_part = jnp.concatenate([blocks[k].astype(low) for k in thin], axis=2)
    thin_width = thin_part.shape[2]
    thin_part = jnp.pad(thin_part, ((0, 0), (0, 0), (0, -thin_width % 256)))
    flat_part = jnp.concatenate([blocks[k].astype(low) for k in flat], axis=1)
    flat_size = flat_part.shape[1]
    flat_part = jnp.pad(flat_part, ((0, 0), (0, -flat_size % (64 * 256))))
    flat_part = flat_part.reshape(groups, -1, 256)
    order = sorted(wide, key=lambda k: local_grads[k].size)
    order = order[:1] + order[1:][::-1]
    summed = grad_reduce([blocks[k].astype(low) for k in order] + [thin_part, flat_part])
    totals = {k: part.astype(jnp.float32) for k, part in zip(order, summed)}
    start_at = 0
    for k in thin:
        width = local_grads[k].shape[1]
        totals[k] = summed[-2][:, start_at : start_at + width].astype(jnp.float32)
        start_at = start_at + width
    line = summed[-1].reshape(-1)
    start_at = 0
    for k in flat:
        length = blocks[k].shape[1]
        totals[k] = line[start_at : start_at + length].astype(jnp.float32)
        start_at = start_at + length
    return tuple(totals[k] for k in range(len(local_grads)))


def shards(
    latent,
    skip_input,
    segment_ids,
    embed_weight,
    embed_bias,
    skip_weight,
    skip_bias,
    norm1_gain,
    norm1_bias,
    qkv_weight,
    proj_weight,
    proj_bias,
    norm2_gain,
    norm2_bias,
    fc1_weight,
    fc1_bias,
    fc2_weight,
    fc2_bias,
    conv_weight,
    cotangent,
):
    row_count, tile_height, tile_width, model_width = skip_input.shape
    patch_width = latent.shape[3]
    tile_tokens = tile_height * tile_width
    token_count = row_count * tile_tokens
    band_index = lax.axis_index("ty")
    column_index = lax.axis_index("tx")
    padded_ids = jnp.pad(segment_ids, ((0, 0), (1, 1), (1, 1)), constant_values=-1)
    window_ids = lax.dynamic_slice(
        padded_ids,
        (jnp.int32(0), band_index * tile_height, column_index * tile_width),
        (row_count, tile_height + 2, tile_width + 2),
    )
    own_ids = window_ids[:, 1:-1, 1:-1]
    shifts = [(down_step, side_step) for down_step in (-1, 0, 1) for side_step in (-1, 0, 1)]
    same_place = jnp.stack(
        [
            window_ids[
                :,
                1 + down_step : 1 + down_step + tile_height,
                1 + side_step : 1 + side_step + tile_width,
            ]
            == own_ids
            for down_step, side_step in shifts
        ],
        axis=-1,
    )
    cuts = jnp.stack(
        [jnp.sum(segment_ids[:, 0, :] == 0, axis=1), jnp.sum(segment_ids[:, :, -1] == 1, axis=1)],
        axis=1,
    ).astype(jnp.int32)
    flat_latent = latent.reshape(token_count, patch_width)
    flat_skip = skip_input.reshape(token_count, model_width)
    embedded = product(flat_latent, embed_weight, "tc,dc->td") + embed_bias.astype(jnp.float32)
    joined = jnp.concatenate([embedded.astype(jnp.bfloat16), flat_skip], axis=1)
    stream = product(joined, skip_weight, "tj,jd->td") + skip_bias.astype(jnp.float32)
    normed, norm1_back = jax.vjp(
        layer_norm, stream, norm1_gain.astype(jnp.float32), norm1_bias.astype(jnp.float32)
    )
    normed_low = normed.astype(jnp.bfloat16)
    projected = product(normed_low, qkv_weight, "td,de->te").astype(jnp.bfloat16)
    queries = projected[:, :model_width].reshape(row_count, tile_tokens, model_width)
    local_pairs = projected[:, model_width:].reshape(row_count, tile_tokens, 2 * model_width)
    attended, log_total, row_pairs = attend(cuts, queries, local_pairs, tile_height, tile_width)
    attended_tiles = attended
    attended = attended.reshape(token_count, model_width)
    stream_mid = (
        stream + product(attended, proj_weight, "td,de->te") + proj_bias.astype(jnp.float32)
    )
    normed_mid, norm2_back = jax.vjp(
        layer_norm, stream_mid, norm2_gain.astype(jnp.float32), norm2_bias.astype(jnp.float32)
    )
    normed_mid_low = normed_mid.astype(jnp.bfloat16)
    hidden = product(normed_mid_low, fc1_weight, "td,df->tf") + fc1_bias.astype(jnp.float32)
    activated, gelu_back = jax.vjp(gelu_exact, hidden)
    active_low = activated.astype(jnp.bfloat16)
    stream_out = (
        stream_mid + product(active_low, fc2_weight, "tf,fd->td") + fc2_bias.astype(jnp.float32)
    )
    conv_in = stream_out.astype(jnp.bfloat16).reshape(
        row_count, tile_height, tile_width, model_width
    )
    rimmed = with_halo(conv_in, (("ty", 1), ("tx", 2)), 1)
    tap_values = product(rimmed, conv_weight, "ryxc,ck->ryxk")
    conv_sum = jnp.zeros((row_count, tile_height, tile_width, patch_width), jnp.float32)
    for offset_index, (down_step, side_step) in enumerate(shifts):
        window = tap_values[
            :,
            1 + down_step : 1 + down_step + tile_height,
            1 + side_step : 1 + side_step + tile_width,
            offset_index * patch_width : (offset_index + 1) * patch_width,
        ]
        conv_sum = conv_sum + jnp.where(
            same_place[..., offset_index : offset_index + 1], window, 0.0
        )
    output = conv_sum.astype(jnp.bfloat16)
    rim_cotangent = with_halo(cotangent, (("ty", 1), ("tx", 2)), 1)
    spread_parts = []
    for offset_index, (down_step, side_step) in enumerate(shifts):
        mirror = 8 - offset_index
        window = rim_cotangent[
            :,
            1 - down_step : 1 - down_step + tile_height,
            1 - side_step : 1 - side_step + tile_width,
            :,
        ]
        spread_parts.append(jnp.where(same_place[..., mirror : mirror + 1], window, 0.0))
    spread = jnp.concatenate(spread_parts, axis=-1)
    out_grad = product(spread, conv_weight, "ryxk,ck->ryxc").reshape(token_count, model_width)
    conv_weight_grad = product(conv_in, spread, "ryxc,ryxk->ck")
    out_low = out_grad.astype(jnp.bfloat16)
    fc2_bias_grad = jnp.sum(out_grad, axis=0)
    fc2_weight_grad = product(active_low, out_low, "tf,td->fd")
    active_grad = product(out_low, fc2_weight, "td,fd->tf")
    (hidden_grad,) = gelu_back(active_grad)
    fc1_bias_grad = jnp.sum(hidden_grad, axis=0)
    hidden_low = hidden_grad.astype(jnp.bfloat16)
    fc1_weight_grad = product(normed_mid_low, hidden_low, "td,tf->df")
    normed_mid_grad = product(hidden_low, fc1_weight, "tf,df->td")
    mid_part, norm2_gain_grad, norm2_bias_grad = norm2_back(normed_mid_grad)
    mid_grad = out_grad + mid_part
    mid_low = mid_grad.astype(jnp.bfloat16)
    proj_bias_grad = jnp.sum(mid_grad, axis=0)
    proj_weight_grad = product(attended, mid_low, "td,te->de")
    attended_grad = product(mid_low, proj_weight, "te,de->td").astype(jnp.bfloat16)
    projected_grad = attend_back(
        cuts,
        queries,
        attended_tiles,
        attended_grad.reshape(row_count, tile_tokens, model_width),
        log_total,
        row_pairs,
        tile_height,
        tile_width,
    ).reshape(token_count, 3 * model_width)
    qkv_weight_grad = product(normed_low, projected_grad, "td,te->de")
    normed_grad = product(projected_grad, qkv_weight, "te,de->td")
    stream_part, norm1_gain_grad, norm1_bias_grad = norm1_back(normed_grad)
    stream_grad = mid_grad + stream_part
    stream_low = stream_grad.astype(jnp.bfloat16)
    skip_bias_grad = jnp.sum(stream_grad, axis=0)
    skip_weight_grad = product(joined, stream_low, "tj,td->jd")
    joined_grad = product(stream_low, skip_weight, "td,jd->tj")
    skip_input_grad = joined_grad[:, model_width:].astype(jnp.bfloat16)
    skip_input_grad = skip_input_grad.reshape(row_count, tile_height, tile_width, model_width)
    embedded_grad = joined_grad[:, :model_width]
    embed_bias_grad = jnp.sum(embedded_grad, axis=0)
    embed_weight_grad = product(embedded_grad.astype(jnp.bfloat16), flat_latent, "td,tc->dc")
    local_grads = (
        embed_weight_grad,
        embed_bias_grad,
        skip_weight_grad,
        skip_bias_grad,
        norm1_gain_grad,
        norm1_bias_grad,
        qkv_weight_grad,
        proj_weight_grad,
        proj_bias_grad,
        norm2_gain_grad,
        norm2_bias_grad,
        fc1_weight_grad,
        fc1_bias_grad,
        fc2_weight_grad,
        fc2_bias_grad,
        conv_weight_grad,
    )
    return (output, skip_input_grad) + sum_grads(local_grads)


def solution(mesh):
    return jax.shard_map(
        shards,
        mesh=mesh,
        in_specs=(
            P("rows", "ty", "tx", None),
            P("rows", "ty", "tx", None),
            P("rows", None, None),
            P(),
            P(),
            P(),
            P(),
            P(),
            P(),
            P(),
            P(),
            P(),
            P(),
            P(),
            P(),
            P(),
            P(),
            P(),
            P(),
            P("rows", "ty", "tx", None),
        ),
        out_specs=(
            P("rows", "ty", "tx", None),
            P("rows", "ty", "tx", None),
            P("rows", None),
            P("rows"),
            P("rows", None),
            P("rows"),
            P("rows"),
            P("rows"),
            P("rows", None),
            P("rows", None),
            P("rows"),
            P("rows"),
            P("rows"),
            P("rows", None),
            P("rows"),
            P("rows", None),
            P("rows"),
            P("rows", None),
        ),
        check_vma=False,
    )
```

```python
import functools

import jax
import jax.numpy as jnp
from jax import lax
from jax.experimental import pallas as pl
from jax.experimental.pallas import tpu as pltpu
from jax.sharding import PartitionSpec as P

MESH = pl.DeviceIdType.MESH
norm_eps = 1e-05


def cell_of(token, tile, tile_height, tile_width, columns):
    down = tile // columns * tile_height + token // tile_width
    across = tile % columns * tile_width + token % tile_width
    return down, across


def fill_shift(shift_ref, tile_height, tile_width):
    tokens = tile_height * tile_width
    bands, columns = lax.axis_size("ty"), lax.axis_size("tx")
    own = lax.axis_index("ty") * columns + lax.axis_index("tx")
    lane = lax.broadcasted_iota(jnp.int32, (8, tokens), 1)
    down, across = cell_of(lane, own, tile_height, tile_width, columns)
    step = lax.broadcasted_iota(jnp.int32, (shift_ref.shape[0], tokens), 0)
    for p in range(9):
        i, j = down - (p // 3 - 1), across - (p % 3 - 1)
        inside = (i >= 0) & (i < bands * tile_height) & (j >= 0) & (j < columns * tile_width)
        tile = i // tile_height * columns + j // tile_width
        place = tile * tokens + i % tile_height * tile_width + j % tile_width
        place = jnp.where(inside, place, -1)[0:1]
        chosen = jnp.where(step == place, 1.0, 0.0)
        shift_ref[:, p * tokens : (p + 1) * tokens] = chosen.astype(jnp.bfloat16)


def same_image(cuts_ref, row, p, tile_height, tile_width):
    tokens = tile_height * tile_width
    columns = lax.axis_size("tx")
    own = lax.axis_index("ty") * columns + lax.axis_index("tx")
    lane = lax.broadcasted_iota(jnp.int32, (8, tokens), 1)
    down, across = cell_of(lane, own, tile_height, tile_width, columns)
    left_width, top_height = cuts_ref[row, 0], cuts_ref[row, 1]

    def image_of(i, j):
        return jnp.where(j < left_width, 0, jnp.where(i < top_height, 1, 2))

    there = image_of(down - (p // 3 - 1), across - (p % 3 - 1))
    return jnp.where(image_of(down, across) == there, 1.0, 0.0)[0:1]


def mm(former, latter, axis_former, axis_latter):
    return lax.dot_general(
        former,
        latter,
        (((axis_former,), (axis_latter,)), ((), ())),
        preferred_element_type=jnp.float32,
    )


def normalised(values):
    average = jnp.mean(values, axis=1, keepdims=True)
    centred = values - average
    rate = lax.rsqrt(jnp.mean(centred * centred, axis=1, keepdims=True) + norm_eps)
    return centred * rate, rate


def norm_back(incoming, unit, rate, gain):
    scaled = incoming * gain
    first = jnp.mean(scaled, axis=1, keepdims=True)
    second = jnp.mean(scaled * unit, axis=1, keepdims=True)
    return (scaled - first - unit * second) * rate


def down_sum(values):
    return jnp.sum(values, axis=0, keepdims=True)


def front_kernel(latent, skip, embed_weight, skip_weight, qkv_weight, vectors, embedded, stream, normed, query, pairs):
    width = skip.shape[1]
    row_count, tokens = query.shape[0], query.shape[1]
    for row in range(row_count):
        at = slice(row * tokens, (row + 1) * tokens)
        entered = (mm(latent[at, :], embed_weight[...], 1, 1) + vectors[0:1]).astype(jnp.bfloat16)
        embedded[at, :] = entered
        total = mm(entered, skip_weight[:width], 1, 0) + mm(skip[at, :], skip_weight[width:], 1, 0) + vectors[1:2]
        stream[at, :] = total
        unit, rate = normalised(total)
        low = (unit * vectors[2:3] + vectors[3:4]).astype(jnp.bfloat16)
        normed[at, :] = low
        query[row] = mm(low, qkv_weight[:, :width], 1, 0).astype(jnp.bfloat16)
        pairs[row] = mm(low, qkv_weight[:, width:], 1, 0).astype(jnp.bfloat16)


def front(latent, skip, embed_weight, skip_weight, qkv_weight, vectors, row_count):
    token_count, width = skip.shape
    tokens = token_count // row_count
    low = jnp.bfloat16
    return pl.pallas_call(
        front_kernel,
        out_shape=[
            jax.ShapeDtypeStruct((token_count, width), low),
            jax.ShapeDtypeStruct((token_count, width), jnp.float32),
            jax.ShapeDtypeStruct((token_count, width), low),
            jax.ShapeDtypeStruct((row_count, tokens, width), low),
            jax.ShapeDtypeStruct((row_count, tokens, 2 * width), low),
        ],
        compiler_params=pltpu.CompilerParams(vmem_limit_bytes=32 * 1024 * 1024),
        name="front",
    )(latent, skip, embed_weight, skip_weight, qkv_weight, vectors)


def erf_of(values):
    x = jnp.clip(values, -4.0, 4.0)
    square = x * x
    upper = square * -2.72614225801306e-10 + 2.77068142495902e-08
    for term in (-2.10102402082508e-06, -5.69250639462346e-05, -7.34990630326855e-04, -2.95459980854025e-03, -1.60960333262415e-02):
        upper = upper * square + term
    lower = square * -1.45660718464996e-05 + -2.13374055278905e-04
    for term in (-1.68282697438203e-03, -7.37332916720468e-03, -1.42647390514189e-02):
        lower = lower * square + term
    return x * upper / lower


def middle_kernel(
    tile_height, tile_width,
    cuts, attended, stream, cot_tiles, proj_weight, conv_turned, vectors, hidden_bias, fc1_weight, fc2_weight,
    fc1_grad, fc2_grad, hidden_bias_grad, proj_grad, attended_grad, mid_grad, conv_in, spread, vector_grads,
    middle, normed, out_grad, out_low, forward_sum, backward_sum, shift,
):
    step = pl.program_id(0)
    row_count, tokens = cot_tiles.shape[1], cot_tiles.shape[3]
    token_count = row_count * tokens
    low = jnp.bfloat16
    parts = [slice(k * tokens, (k + 1) * tokens) for k in range(row_count)]

    @pl.when(step == 0)
    def _():
        fill_shift(shift, tile_height, tile_width)
        tile_count = cot_tiles.shape[0]
        patch = cot_tiles.shape[2]
        turned = jnp.concatenate(
            [cot_tiles[t].reshape(row_count * patch, tokens) for t in range(tile_count)], axis=1
        )
        moved = mm(turned, shift[...], 1, 0)
        for row in range(row_count):
            for p in range(9):
                piece = moved[row * patch : (row + 1) * patch, p * tokens : (p + 1) * tokens]
                piece = piece * same_image(cuts, row, p, tile_height, tile_width)
                spread[p * patch : (p + 1) * patch, parts[row]] = piece.astype(low)
        total = jnp.zeros((1, stream.shape[1]), jnp.float32)
        for at in parts:
            grad = mm(spread[:, at], conv_turned[...], 0, 0)
            out_grad[at, :] = grad
            out_low[at, :] = grad.astype(low)
            total = total + down_sum(grad)
            value = stream[at, :] + mm(attended[at, :], proj_weight[...], 1, 0) + vectors[4:5]
            middle[at, :] = value
            unit, rate = normalised(value)
            normed[at, :] = (unit * vectors[5:6] + vectors[6:7]).astype(low)
        vector_grads[7:8] = total
        forward_sum[...] = jnp.zeros_like(forward_sum)
        backward_sum[...] = jnp.zeros_like(backward_sum)

    bias_grad = jnp.zeros((1, fc1_weight.shape[1]), jnp.float32)
    actives, hidden_lows = [], []
    for at in parts:
        hidden = mm(normed[at, :], fc1_weight[...], 1, 0) + hidden_bias[0]
        active_grad = mm(out_low[at, :], fc2_weight[...], 1, 1)
        share = 0.5 + 0.5 * erf_of(hidden * 0.7071067811865476)
        density = jnp.exp(hidden * hidden * -0.5) * 0.3989422804014327
        active = (hidden * share).astype(low)
        hidden_grad = active_grad * (share + hidden * density)
        bias_grad = bias_grad + down_sum(hidden_grad)
        hidden_low = hidden_grad.astype(low)
        forward_sum[at, :] = forward_sum[at, :] + mm(active, fc2_weight[...], 1, 0)
        backward_sum[at, :] = backward_sum[at, :] + mm(hidden_low, fc1_weight[...], 1, 1)
        actives.append(active)
        hidden_lows.append(hidden_low)
    hidden_bias_grad[0] = bias_grad
    fc2_grad[...] = mm(jnp.concatenate(actives, axis=0), out_low[...], 0, 0).astype(low)
    fc1_grad[...] = mm(normed[...], jnp.concatenate(hidden_lows, axis=0), 0, 0).astype(low)

    @pl.when(step == pl.num_programs(0) - 1)
    def _():
        width = stream.shape[1]
        gain_sum = jnp.zeros((1, width), jnp.float32)
        bias_sum = jnp.zeros((1, width), jnp.float32)
        mid_sum = jnp.zeros((1, width), jnp.float32)
        lows = []
        for at in parts:
            unit, rate = normalised(middle[at, :])
            conv_in[at, :] = (middle[at, :] + forward_sum[at, :] + vectors[7:8]).astype(low)
            incoming = backward_sum[at, :]
            gain_sum = gain_sum + down_sum(incoming * unit)
            bias_sum = bias_sum + down_sum(incoming)
            grad = out_grad[at, :] + norm_back(incoming, unit, rate, vectors[5:6])
            mid_grad[at, :] = grad
            mid_sum = mid_sum + down_sum(grad)
            mid_low = grad.astype(low)
            lows.append(mid_low)
            attended_grad[at, :] = mm(mid_low, proj_weight[...], 1, 1).astype(low)
        proj_grad[...] = mm(attended[...], jnp.concatenate(lows, axis=0), 0, 0).astype(low)
        vector_grads[4:5] = mid_sum
        vector_grads[5:6] = gain_sum
        vector_grads[6:7] = bias_sum


def middle(cuts, attended, stream, cot_tiles, proj_weight, conv_turned, vectors, hidden_bias, fc1_weight, fc2_weight, tile_height, tile_width):
    token_count, width = stream.shape
    hidden_width = fc1_weight.shape[1]
    block = 512
    steps = hidden_width // block
    low = jnp.bfloat16
    vmem = pl.BlockSpec(memory_space=pltpu.VMEM)
    tile_count, tokens = cot_tiles.shape[0], cot_tiles.shape[3]
    taps = conv_turned.shape[0]
    return pl.pallas_call(
        functools.partial(middle_kernel, tile_height, tile_width),
        grid=(steps,),
        out_shape=[
            jax.ShapeDtypeStruct((width, hidden_width), low),
            jax.ShapeDtypeStruct((hidden_width, width), low),
            jax.ShapeDtypeStruct((steps, 1, block), jnp.float32),
            jax.ShapeDtypeStruct((width, width), low),
            jax.ShapeDtypeStruct((token_count, width), low),
            jax.ShapeDtypeStruct((token_count, width), jnp.float32),
            jax.ShapeDtypeStruct((token_count, width), low),
            jax.ShapeDtypeStruct((taps, token_count), low),
            jax.ShapeDtypeStruct((8, width), jnp.float32),
        ],
        in_specs=[pl.BlockSpec(memory_space=pltpu.SMEM)]
        + [vmem] * 6
        + [
            pl.BlockSpec((1, 1, block), lambda k: (k, 0, 0)),
            pl.BlockSpec((width, block), lambda k: (0, k)),
            pl.BlockSpec((block, width), lambda k: (k, 0)),
        ],
        out_specs=[
            pl.BlockSpec((width, block), lambda k: (0, k)),
            pl.BlockSpec((block, width), lambda k: (k, 0)),
            pl.BlockSpec((1, 1, block), lambda k: (k, 0, 0)),
        ]
        + [vmem] * 6,
        scratch_shapes=[
            pltpu.VMEM((token_count, width), jnp.float32),
            pltpu.VMEM((token_count, width), low),
            pltpu.VMEM((token_count, width), jnp.float32),
            pltpu.VMEM((token_count, width), low),
            pltpu.VMEM((token_count, width), jnp.float32),
            pltpu.VMEM((token_count, width), jnp.float32),
            pltpu.VMEM((tile_count * tokens, 9 * tokens), low),
        ],
        compiler_params=pltpu.CompilerParams(vmem_limit_bytes=40 * 1024 * 1024),
        name="middle",
    )(cuts, attended, stream, cot_tiles, proj_weight, conv_turned, vectors, hidden_bias, fc1_weight, fc2_weight)


def rear_kernel(
    projected_grad, qkv_weight, normed, stream, mid_grad, embedded, skip, latent, skip_weight, vectors,
    middle_grads, hidden_bias_grad, conv_grad, qkv_grad, skip_grad, skip_input_grad, thin, flat, stream_low,
):
    token_count, width = stream.shape
    low = jnp.bfloat16
    tokens = 128
    parts = [slice(k * tokens, (k + 1) * tokens) for k in range(token_count // tokens)]
    zero = jnp.zeros((1, width), jnp.float32)
    gain_sum, bias_sum, stream_sum, embed_sum = zero, zero, zero, zero
    for at in parts:
        incoming = mm(projected_grad[at, :], qkv_weight[...], 1, 1)
        unit, rate = normalised(stream[at, :])
        gain_sum = gain_sum + down_sum(incoming * unit)
        bias_sum = bias_sum + down_sum(incoming)
        grad = mid_grad[at, :] + norm_back(incoming, unit, rate, vectors[2:3])
        stream_sum = stream_sum + down_sum(grad)
        stream_low[at, :] = grad.astype(low)
    embed_lows = []
    for at in parts:
        embed_grad = mm(stream_low[at, :], skip_weight[:width], 1, 1)
        embed_sum = embed_sum + down_sum(embed_grad)
        embed_lows.append(embed_grad.astype(low))
        skip_input_grad[at, :] = mm(stream_low[at, :], skip_weight[width:], 1, 1).astype(low)
    qkv_grad[...] = mm(normed[...], projected_grad[...], 0, 0).astype(low)
    skip_grad[:width] = mm(embedded[...], stream_low[...], 0, 0).astype(low)
    skip_grad[width:] = mm(skip[...], stream_low[...], 0, 0).astype(low)
    embed_weight_grad = mm(jnp.concatenate(embed_lows, axis=0), latent[...], 0, 0)
    thin[:, :128] = conv_grad[:, :128].astype(low)
    rest = jnp.zeros((width, 128 - 2 * 16), jnp.float32)
    thin[:, 128:] = jnp.concatenate([conv_grad[:, 128:144], embed_weight_grad, rest], axis=1).astype(low)
    rows = [embed_sum, stream_sum, gain_sum, bias_sum] + [middle_grads[k : k + 1] for k in range(4, 8)]
    stack = jnp.concatenate(rows, axis=0)
    share = width // 4
    for block in range(4):
        own = stack[:, block * share : (block + 1) * share]
        own = jnp.concatenate([own, jnp.zeros((8, 256 - share), jnp.float32)], axis=1)
        line = hidden_bias_grad[block : block + 1]
        pieces = [line[:, k * 256 : (k + 1) * 256] for k in range(width // 256)]
        body = jnp.concatenate([own] + pieces + [jnp.zeros((8 - len(pieces), 256), jnp.float32)], axis=0)
        flat[block, 0:16] = body.astype(low)
        flat[block, 16:64] = jnp.zeros((48, 256), low)


def rear(projected_grad, qkv_weight, normed, stream, mid_grad, embedded, skip, latent, skip_weight, vectors, middle_grads, hidden_bias_grad, conv_grad):
    token_count, width = stream.shape
    low = jnp.bfloat16
    return pl.pallas_call(
        rear_kernel,
        out_shape=[
            jax.ShapeDtypeStruct((width, 3 * width), low),
            jax.ShapeDtypeStruct((2 * width, width), low),
            jax.ShapeDtypeStruct((token_count, width), low),
            jax.ShapeDtypeStruct((width, 256), low),
            jax.ShapeDtypeStruct((4, 64, 256), low),
        ],
        scratch_shapes=[pltpu.VMEM((token_count, width), low)],
        compiler_params=pltpu.CompilerParams(vmem_limit_bytes=40 * 1024 * 1024),
        name="rear",
    )(projected_grad, qkv_weight, normed, stream, mid_grad, embedded, skip, latent, skip_weight, vectors, middle_grads, hidden_bias_grad, conv_grad)


def plane_peers():
    z, ty, y = lax.axis_index("rows"), lax.axis_index("ty"), lax.axis_index("tx")
    core, x = lax.rem(ty, 2), ty // 2
    here = x * 2 + core
    across = (1 - x) * 2 + core
    tiles = {
        "own": here * 2 + y,
        "x": across * 2 + y,
        "y": here * 2 + 1 - y,
        "xy": across * 2 + 1 - y,
    }
    peers = {
        "core": (z, x * 2 + 1 - core, y),
        "x": (z, across, y),
        "y": (z, here, 1 - y),
    }
    return tiles, peers


def plane_peer(k):
    z, ty, y = lax.axis_index("rows"), lax.axis_index("ty"), lax.axis_index("tx")
    x, core = ty // 2, lax.rem(ty, 2)
    flip_x, flip_core, flip_y = k // 4, k // 2 % 2, k % 2
    x = x + flip_x - 2 * flip_x * x
    core = core + flip_core - 2 * flip_core * core
    y = y + flip_y - 2 * flip_y * y
    return (z, x * 2 + core, y), (x * 2 + core) * 2 + y


def greet(peers):
    barrier = pltpu.get_barrier_semaphore()
    for peer in peers:
        pl.semaphore_signal(barrier, inc=1, device_id=peer, device_id_type=MESH)
    pl.semaphore_wait(barrier, len(peers))


def fill_mask(mask_ref, cuts_ref, row, tile_height, tile_width):
    ty, tx = lax.axis_index("ty"), lax.axis_index("tx")
    columns = lax.axis_size("tx")
    tokens = tile_height * tile_width
    left_width = cuts_ref[row, 0]
    top_height = cuts_ref[row, 1]

    def image_of(down, across):
        return jnp.where(across < left_width, 0, jnp.where(down < top_height, 1, 2))

    lane = lax.broadcasted_iota(jnp.int32, (tokens, tokens), 1)
    step = lax.broadcasted_iota(jnp.int32, (tokens, tokens), 0)
    mine = image_of(
        ty * tile_height + lane // tile_width, tx * tile_width + lane % tile_width
    )
    for tile in range(mask_ref.shape[0] // tokens):
        theirs = image_of(
            tile // columns * tile_height + step // tile_width,
            tile % columns * tile_width + step % tile_width,
        )
        mask_ref[tile * tokens : (tile + 1) * tokens, :] = jnp.where(
            mine == theirs, 0.0, -1e30
        )


def two_heads(pair, scale):
    lane = lax.broadcasted_iota(jnp.int32, pair.shape, 1)
    wide = pair.astype(jnp.float32) * scale
    first = jnp.where(lane < pair.shape[1] // 2, wide, 0.0)
    return jnp.concatenate([first, wide - first], axis=0).astype(jnp.bfloat16)


def own_blocks(both):
    head, tokens = both.shape[0] // 2, both.shape[1] // 2
    return jnp.concatenate([both[:head, :tokens], both[head:, tokens:]], axis=0)


def attend_kernel(
    tile_height, tile_width, cuts, query, pairs, cot, out, lse, all_out, cot_out, held, scores, mask, local_sem, send_sem, recv_sem,
    cot_sem, cot_send_sem, cot_recv_sem
):
    row_count, tokens, width = query.shape
    tile_count = held.shape[1]
    pair_count = width // 128
    tiles, peers = plane_peers()
    own = tiles["own"]
    greet([plane_peer(k)[0] for k in range(1, tile_count)])
    cot_copies = [pltpu.make_async_copy(cot, cot_out.at[own], cot_sem.at[0])]
    for k in range(1, tile_count):
        cot_copies.append(
            pltpu.make_async_remote_copy(
                src_ref=cot,
                dst_ref=cot_out.at[own],
                send_sem=cot_send_sem.at[k],
                recv_sem=cot_recv_sem.at[k],
                device_id=plane_peer(k)[0],
                device_id_type=MESH,
            )
        )

    def send(row, slot, source, target, peer):
        copy = pltpu.make_async_remote_copy(
            src_ref=source,
            dst_ref=target,
            send_sem=send_sem.at[row, slot],
            recv_sem=recv_sem.at[row, slot],
            device_id=peer,
            device_id_type=MESH,
        )
        copy.start()
        return copy

    flights = [{} for _ in range(row_count)]

    def begin(row):
        here = held.at[row, own]
        source = pairs.at[row]
        flights[row]["x"] = send(row, 0, source, here, peers["x"])
        flights[row]["y"] = send(row, 1, source, here, peers["y"])
        flights[row]["core"] = send(row, 2, source, here, peers["core"])
        keep = pltpu.make_async_copy(source, here, local_sem.at[row, 0])
        keep.start()
        flights[row]["keep"] = keep

    def forward(row):
        flights[row]["y"].wait_recv()
        key_half = held.at[row, tiles["y"], :, pl.ds(0, width)]
        flights[row]["far_x"] = send(row, 3, key_half, key_half, peers["x"])
        flights[row]["x"].wait_recv()
        value_half = held.at[row, tiles["x"], :, pl.ds(width, width)]
        flights[row]["far_y"] = send(row, 4, value_half, value_half, peers["y"])
        for slot, name in ((5, "x"), (6, "y")):
            tile = held.at[row, tiles[name]]
            flights[row]["core_" + name] = send(row, slot, tile, tile, peers["core"])

    def finish(row):
        flights[row]["far_x"].wait_recv()
        flights[row]["far_y"].wait_recv()
        tile = held.at[row, tiles["xy"]]
        last = send(row, 7, tile, tile, peers["core"])
        flights[row]["keep"].wait()
        for name in ("core", "core_x", "core_y"):
            flights[row][name].wait_recv()
        last.wait_recv()
        for name in ("x", "y", "core", "far_x", "far_y", "core_x", "core_y"):
            flights[row][name].wait_send()
        last.wait_send()
        keep = pltpu.make_async_copy(held.at[row], all_out.at[row], local_sem.at[row, 1])
        keep.start()
        flights[row]["out"] = keep

    chunk = 2

    def compute(row):
        fill_mask(mask, cuts, row, tile_height, tile_width)

        def one_pair(p, carry):
            at = pl.ds(pl.multiple_of(p * 128, 128), 128)
            at_value = pl.ds(pl.multiple_of(width + p * 128, 128), 128)
            both = two_heads(query[row, :, at], 0.125)
            peak = None
            for c in range(tile_count // chunk):
                span = slice(c * chunk * tokens, (c + 1) * chunk * tokens)
                keys = held[row, c * chunk : (c + 1) * chunk, :, at].reshape(chunk * tokens, 128)
                extra = mask[span, :]
                part = mm(keys, both, 1, 1) + jnp.concatenate([extra, extra], axis=1)
                scores[span, :] = part
                top = jnp.max(part, axis=0, keepdims=True)
                peak = top if peak is None else jnp.maximum(peak, top)
            total = jnp.zeros_like(peak)
            summed = jnp.zeros((128, 2 * tokens), jnp.float32)
            for c in range(tile_count // chunk):
                span = slice(c * chunk * tokens, (c + 1) * chunk * tokens)
                values = held[row, c * chunk : (c + 1) * chunk, :, at_value].reshape(chunk * tokens, 128)
                part = jnp.exp(scores[span, :] - peak)
                total = total + jnp.sum(part, axis=0, keepdims=True)
                summed = summed + mm(values, part.astype(jnp.bfloat16), 0, 0)
            blocks = own_blocks(summed / total)
            out[row, :, at] = jnp.transpose(blocks).astype(jnp.bfloat16)
            lse[row, p] = peak + jnp.log(total)
            return carry

        lax.fori_loop(0, pair_count, one_pair, 0)

    begin(0)
    if row_count > 1:
        begin(1)
    for copy in cot_copies:
        copy.start()
    forward(0)
    for row in range(row_count):
        if row + 2 < row_count:
            begin(row + 2)
        if row + 1 < row_count:
            forward(row + 1)
        finish(row)
        compute(row)
    for row in range(row_count):
        flights[row]["out"].wait()
    for copy in cot_copies:
        copy.wait()


def attend(cuts, query, pairs, cot, tile_height, tile_width):
    row_count, tokens, width = query.shape
    tile_count = lax.axis_size("ty") * lax.axis_size("tx")
    pair_count = width // 128
    low = jnp.bfloat16
    vmem = pl.BlockSpec(memory_space=pltpu.VMEM)
    return pl.pallas_call(
        functools.partial(attend_kernel, tile_height, tile_width),
        out_shape=[
            jax.ShapeDtypeStruct((row_count, tokens, width), low),
            jax.ShapeDtypeStruct((row_count, pair_count, 1, 2 * tokens), jnp.float32),
            jax.ShapeDtypeStruct((row_count, tile_count, tokens, 2 * width), low),
            jax.ShapeDtypeStruct((tile_count,) + cot.shape, low),
        ],
        in_specs=[pl.BlockSpec(memory_space=pltpu.SMEM), vmem] + [pl.BlockSpec(memory_space=pl.ANY)] * 2,
        out_specs=[vmem, vmem] + [pl.BlockSpec(memory_space=pl.ANY)] * 2,
        scratch_shapes=[
            pltpu.VMEM((row_count, tile_count, tokens, 2 * width), low),
            pltpu.VMEM((tile_count * tokens, 2 * tokens), jnp.float32),
            pltpu.VMEM((tile_count * tokens, tokens), jnp.float32),
            pltpu.SemaphoreType.DMA((row_count, 2)),
            pltpu.SemaphoreType.DMA((row_count, 8)),
            pltpu.SemaphoreType.DMA((row_count, 8)),
            pltpu.SemaphoreType.DMA((1,)),
            pltpu.SemaphoreType.DMA((tile_count,)),
            pltpu.SemaphoreType.DMA((tile_count,)),
        ],
        compiler_params=pltpu.CompilerParams(
            collective_id=1, has_side_effects=True, vmem_limit_bytes=40 * 1024 * 1024
        ),
        name="attend",
    )(cuts, query, pairs, cot)


def attend_back_kernel(
    tile_height, tile_width, cuts, query, attended, grad, lse, conv_in, conv_turned, spread, all_pairs,
    out, conv_grad, conv_out, held, terms, core_terms, side_terms, mask, shift, taps, part, part_got,
    load_sem, send_sem, recv_sem, part_send_sem, part_recv_sem
):
    row_count, tokens, width = query.shape
    tile_count = held.shape[1]
    pair_count = width // 128
    tiles, peers = plane_peers()
    low = jnp.bfloat16
    loads = []
    for row in range(row_count):
        load = pltpu.make_async_copy(all_pairs.at[row], held.at[row], load_sem.at[row])
        load.start()
        loads.append(load)
    greet([plane_peer(k)[0] for k in range(1, tile_count)])
    core = lax.rem(lax.axis_index("ty"), 2)
    chunk = 2

    def send(row, slot, source, target, peer):
        copy = pltpu.make_async_remote_copy(
            src_ref=source,
            dst_ref=target,
            send_sem=send_sem.at[row, slot],
            recv_sem=recv_sem.at[row, slot],
            device_id=peer,
            device_id_type=MESH,
        )
        copy.start()
        return copy

    def compute(row):
        loads[row].wait()
        fill_mask(mask, cuts, row, tile_height, tile_width)

        def one_pair(p, carry):
            at = pl.ds(pl.multiple_of(p * 128, 128), 128)
            at_value = pl.ds(pl.multiple_of(width + p * 128, 128), 128)
            grad_pair = grad[row, :, at]
            both = two_heads(query[row, :, at], 0.125)
            both_grad = two_heads(grad_pair, 1.0)
            inner = jnp.transpose(grad_pair.astype(jnp.float32) * attended[row, :, at].astype(jnp.float32))
            half = inner.shape[0] // 2
            delta = jnp.concatenate(
                [jnp.sum(inner[:half], axis=0, keepdims=True), jnp.sum(inner[half:], axis=0, keepdims=True)], axis=1
            )
            level = lse[row, p]
            query_part = jnp.zeros((128, 2 * tokens), jnp.float32)
            for c in range(tile_count // chunk):
                span = slice(c * chunk * tokens, (c + 1) * chunk * tokens)
                some = slice(c * chunk, (c + 1) * chunk)
                keys = held[row, some, :, at].reshape(chunk * tokens, 128)
                values = held[row, some, :, at_value].reshape(chunk * tokens, 128)
                extra = mask[span, :]
                weights = jnp.exp(mm(keys, both, 1, 1) + jnp.concatenate([extra, extra], axis=1) - level)
                score_grad = (weights * (mm(values, both_grad, 1, 1) - delta)).astype(low)
                value_part = mm(weights.astype(low), both_grad, 1, 0)
                key_part = mm(score_grad, both, 1, 0)
                query_part = query_part + mm(keys, score_grad, 0, 0)
                terms[row, some, :, at] = key_part.astype(low).reshape(chunk, tokens, 128)
                terms[row, some, :, at_value] = value_part.astype(low).reshape(chunk, tokens, 128)
            blocks = own_blocks(query_part) * 0.125
            out[row, :, at] = jnp.transpose(blocks).astype(low)
            return carry

        lax.fori_loop(0, pair_count, one_pair, 0)

    flights = [{} for _ in range(row_count)]
    names = ("own", "x", "y", "xy")
    key_at, value_at = pl.ds(0, width), pl.ds(width, width)

    def begin(row):
        copies = []
        other = 2 - 4 * core
        for k, name in enumerate(names):
            copies.append(send(row, k, terms.at[row, tiles[name] + other], core_terms.at[row, k], peers["core"]))
        flights[row]["core"] = copies

    def add(target, source, row_total):
        def body(i, carry):
            at = pl.ds(pl.multiple_of(i * 16, 16), 16)
            target[at, :] = target[at, :] + source[at, :]
            return carry

        lax.fori_loop(0, row_total // 16, body, 0)

    def scatter(row):
        for k in (3, 1, 2, 0):
            flights[row]["core"][k].wait()
            add(terms.at[row, tiles[names[k]]], core_terms.at[row, k], tokens)
            if k == 3:
                far = terms.at[row, tiles["xy"]]
                flights[row]["far_x"] = send(row, 4, far.at[:, key_at], side_terms.at[row, 0], peers["x"])
                flights[row]["far_y"] = send(row, 5, far.at[:, value_at], side_terms.at[row, 1], peers["y"])
            if k == 1:
                near = terms.at[row, tiles["x"]]
                flights[row]["near_x"] = send(row, 6, near.at[:, key_at], side_terms.at[row, 2], peers["x"])
            if k == 2:
                near = terms.at[row, tiles["y"]]
                flights[row]["near_y"] = send(row, 7, near.at[:, value_at], side_terms.at[row, 3], peers["y"])

    def pass_on(row):
        flights[row]["far_x"].wait()
        near = terms.at[row, tiles["y"], :, key_at]
        add(near, side_terms.at[row, 0], tokens)
        flights[row]["last_y"] = send(row, 8, near, side_terms.at[row, 4], peers["y"])
        flights[row]["far_y"].wait()
        near = terms.at[row, tiles["x"], :, value_at]
        add(near, side_terms.at[row, 1], tokens)
        flights[row]["last_x"] = send(row, 9, near, side_terms.at[row, 5], peers["x"])

    def close(row):
        for name in ("near_x", "near_y", "last_x", "last_y"):
            flights[row][name].wait()
        mine = terms.at[row, tiles["own"]]

        def body(i, carry):
            at = pl.ds(pl.multiple_of(i * 16, 16), 16)
            for start, first, second in ((0, 2, 4), (width, 3, 5)):
                total = mine[at, start : start + width].astype(jnp.float32)
                total = total + side_terms[row, first, at, :].astype(jnp.float32)
                total = total + side_terms[row, second, at, :].astype(jnp.float32)
                out[row, at, width + start : 2 * width + start] = total.astype(low)
            return carry

        lax.fori_loop(0, tokens // 16, body, 0)

    part_copies = []

    def convolve():
        fill_shift(shift, tile_height, tile_width)
        patch = part.shape[2]
        taps[...] = mm(conv_turned[...], conv_in[...], 1, 1)
        rows = []
        for row in range(row_count):
            pieces = []
            for p in range(9):
                piece = taps[p * patch : (p + 1) * patch, row * tokens : (row + 1) * tokens]
                pieces.append(piece * same_image(cuts, row, p, tile_height, tile_width))
            rows.append(jnp.concatenate(pieces, axis=1))
        whole = jnp.concatenate(rows, axis=0)
        coarse = whole.astype(low)
        fine = (whole - coarse.astype(jnp.float32)).astype(low)
        moved = mm(coarse, shift[...], 1, 1) + mm(fine, shift[...], 1, 1)
        for tile in range(tile_count):
            part[tile] = moved[:, tile * tokens : (tile + 1) * tokens].reshape(row_count, patch, tokens)
        for k in range(1, tile_count):
            peer, tile = plane_peer(k)
            copy = pltpu.make_async_remote_copy(
                src_ref=part.at[tile],
                dst_ref=part_got.at[k],
                send_sem=part_send_sem.at[k],
                recv_sem=part_recv_sem.at[k],
                device_id=peer,
                device_id_type=MESH,
            )
            copy.start()
            part_copies.append(copy)
        conv_grad[...] = mm(conv_in[...], spread[...], 0, 1)

    def collect():
        total = part[tiles["own"]]
        for k, copy in enumerate(part_copies):
            copy.wait()
            total = total + part_got[k + 1]
        conv_out[...] = total.astype(low)

    for row in range(row_count):
        compute(row)
        begin(row)
        if row > 0:
            scatter(row - 1)
        if row > 1:
            pass_on(row - 2)
    scatter(row_count - 1)
    convolve()
    for row in range(max(row_count - 2, 0), row_count):
        pass_on(row)
    for row in range(row_count):
        close(row)
    collect()


def attend_back(cuts, query, attended, grad, lse, conv_in, conv_turned, spread, all_pairs, tile_height, tile_width):
    row_count, tokens, width = query.shape
    tile_count = all_pairs.shape[1]
    taps = conv_turned.shape[0]
    low = jnp.bfloat16
    vmem = pl.BlockSpec(memory_space=pltpu.VMEM)
    return pl.pallas_call(
        functools.partial(attend_back_kernel, tile_height, tile_width),
        out_shape=[
            jax.ShapeDtypeStruct((row_count, tokens, 3 * width), low),
            jax.ShapeDtypeStruct((width, taps), jnp.float32),
            jax.ShapeDtypeStruct((row_count, taps // 9, tokens), low),
        ],
        in_specs=[pl.BlockSpec(memory_space=pltpu.SMEM)] + [vmem] * 7 + [pl.BlockSpec(memory_space=pl.ANY)],
        out_specs=[vmem] * 3,
        scratch_shapes=[
            pltpu.VMEM((row_count, tile_count, tokens, 2 * width), low),
            pltpu.VMEM((row_count, tile_count, tokens, 2 * width), low),
            pltpu.VMEM((row_count, 4, tokens, 2 * width), low),
            pltpu.VMEM((row_count, 6, tokens, width), low),
            pltpu.VMEM((tile_count * tokens, tokens), jnp.float32),
            pltpu.VMEM((tile_count * tokens, 9 * tokens), low),
            pltpu.VMEM((taps, row_count * tokens), jnp.float32),
            pltpu.VMEM((tile_count, row_count, taps // 9, tokens), jnp.float32),
            pltpu.VMEM((tile_count, row_count, taps // 9, tokens), jnp.float32),
            pltpu.SemaphoreType.DMA((row_count,)),
            pltpu.SemaphoreType.DMA((row_count, 10)),
            pltpu.SemaphoreType.DMA((row_count, 10)),
            pltpu.SemaphoreType.DMA((tile_count,)),
            pltpu.SemaphoreType.DMA((tile_count,)),
        ],
        compiler_params=pltpu.CompilerParams(
            collective_id=2, has_side_effects=True, vmem_limit_bytes=50 * 1024 * 1024
        ),
        name="attend_back",
    )(cuts, query, attended, grad, lse, conv_in, conv_turned, spread, all_pairs)


def add_rows(target, first, second, rows):
    step = 16

    def body(i, carry):
        at = pl.ds(pl.multiple_of(i * step, step), step)
        target[at, :] = first[at, :] + second[at, :]
        return carry

    lax.fori_loop(0, rows // step, body, 0)


def grad_reduce_kernel(shapes, *refs):
    count = len(shapes)
    grads = refs[:count]
    outs = refs[count : 2 * count]
    rest = refs[2 * count :]
    own, got, half, quarter, final = [rest[i * count : (i + 1) * count] for i in range(5)]
    local_sem, send_sem, recv_sem = rest[5 * count :]
    z, ty, y = lax.axis_index("rows"), lax.axis_index("ty"), lax.axis_index("tx")
    core, x = lax.rem(ty, 2), ty // 2
    peer_core = (z, x * 2 + 1 - core, y)
    peer_x = (z, (1 - x) * 2 + core, y)
    peer_y = (z, ty, 1 - y)
    peer_xy = (z, (1 - x) * 2 + core, 1 - y)
    peers_z = [(lax.rem(z + k, 4), ty, y) for k in (1, 2, 3)]
    barrier = pltpu.get_barrier_semaphore()
    everyone = [peer_core, peer_x, peer_y, peer_xy] + peers_z
    for peer in everyone:
        pl.semaphore_signal(barrier, inc=1, device_id=peer, device_id_type=MESH)
    pl.semaphore_wait(barrier, len(everyone))

    def send(w, slot, source, target, peer):
        return pltpu.make_async_remote_copy(
            src_ref=source,
            dst_ref=target,
            send_sem=send_sem.at[w, slot],
            recv_sem=recv_sem.at[w, slot],
            device_id=peer,
            device_id_type=MESH,
        )

    def columns(w, which):
        width = shapes[w][2] // 2
        return pl.ds(pl.multiple_of(which * width, 128), width)

    def rows(start, size):
        return pl.ds(pl.multiple_of(start, 16), size)

    def place(w, block):
        depth = shapes[w][1]
        later = block // 2
        major = x + later * (y - x)
        minor = y + later * (x - y)
        return rows(major * (depth // 2) + minor * (depth // 4), depth // 4)

    pending = [{} for _ in shapes]

    def begin(w):
        swap = send(w, 0, grads[w].at[:, :, columns(w, 1 - core)], got[w], peer_core)
        swap.start()
        mine = pltpu.make_async_copy(grads[w].at[:, :, columns(w, core)], own[w], local_sem.at[w, 0])
        mine.start()
        pending[w].update(swap=swap, mine=mine)

    def stage_core(w):
        depth = shapes[w][1]
        pending[w]["mine"].wait()
        pending[w]["swap"].wait()
        for block in range(4):
            add_rows(own[w].at[block], own[w].at[block], got[w].at[block], depth)
        first = send(w, 1, own[w].at[0:2, rows((1 - x) * (depth // 2), depth // 2)], half[w].at[0:2], peer_x)
        second = send(w, 2, own[w].at[2:4, rows((1 - y) * (depth // 2), depth // 2)], half[w].at[2:4], peer_y)
        first.start()
        second.start()
        pending[w].update(half=(first, second))

    def stage_half(w):
        depth = shapes[w][1]
        for copy in pending[w]["half"]:
            copy.wait()
        for block in range(4):
            side = x if block < 2 else y
            kept = own[w].at[block, rows(side * (depth // 2), depth // 2)]
            add_rows(kept, kept, half[w].at[block], depth // 2)
        first = send(w, 3, own[w].at[0:2, rows(x * (depth // 2) + (1 - y) * (depth // 4), depth // 4)], quarter[w].at[0:2], peer_y)
        second = send(w, 4, own[w].at[2:4, rows(y * (depth // 2) + (1 - x) * (depth // 4), depth // 4)], quarter[w].at[2:4], peer_x)
        first.start()
        second.start()
        pending[w].update(quarter=(first, second))

    def stage_quarter(w):
        depth = shapes[w][1]
        for copy in pending[w]["quarter"]:
            copy.wait()
        for block in range(4):
            kept = own[w].at[block, place(w, block // 2 * 2)]
            add_rows(kept, kept, quarter[w].at[block], depth // 4)
        copies = []
        for k, peer in enumerate(peers_z):
            block = peer[0]
            copy = send(w, 5 + k, own[w].at[block, place(w, block)], final[w].at[k], peer)
            copy.start()
            copies.append(copy)
        pending[w].update(final=copies)

    def stage_final(w):
        depth = shapes[w][1]
        for copy in pending[w]["final"]:
            copy.wait()
        kept = own[w].at[z, place(w, z)]
        total = final[w].at[0]

        def body(i, carry):
            at = pl.ds(pl.multiple_of(i * 16, 16), 16)
            parts = [ref[at, :].astype(jnp.float32) for ref in (kept, total, final[w].at[1], final[w].at[2])]
            total[at, :] = (parts[0] + parts[1] + (parts[2] + parts[3])).astype(jnp.bfloat16)
            return carry

        lax.fori_loop(0, depth // 64, body, 0)
        target = outs[w].at[place(w, z), columns(w, core)]
        copies = []
        for k, peer in enumerate((peer_x, peer_y, peer_xy)):
            copy = send(w, 8 + k, total, target, peer)
            copy.start()
            copies.append(copy)
        keep = pltpu.make_async_copy(total, target, local_sem.at[w, 1])
        keep.start()
        pending[w].update(gather=copies, keep=keep)

    def stage_gather(w):
        for copy in pending[w]["gather"]:
            copy.wait()
        pending[w]["keep"].wait()
        strip = outs[w].at[:, columns(w, core)]
        copy = send(w, 11, strip, strip, peer_core)
        copy.start()
        pending[w].update(strip=copy)

    def stage_strip(w):
        pending[w]["strip"].wait()

    for w in range(count):
        begin(w)
    stages = [stage_core, stage_half, stage_quarter, stage_final, stage_gather, stage_strip]
    for tick in range(count + len(stages) - 1):
        for depth_index in reversed(range(len(stages))):
            w = tick - depth_index
            if 0 <= w < count:
                stages[depth_index](w)


def grad_reduce(grads):
    shapes = tuple(entry.shape for entry in grads)
    count = len(shapes)
    low = jnp.bfloat16
    scratch = (
        [pltpu.VMEM((s[0], s[1], s[2] // 2), low) for s in shapes]
        + [pltpu.VMEM((s[0], s[1], s[2] // 2), low) for s in shapes]
        + [pltpu.VMEM((s[0], s[1] // 2, s[2] // 2), low) for s in shapes]
        + [pltpu.VMEM((s[0], s[1] // 4, s[2] // 2), low) for s in shapes]
        + [pltpu.VMEM((3, s[1] // 4, s[2] // 2), low) for s in shapes]
        + [
            pltpu.SemaphoreType.DMA((count, 2)),
            pltpu.SemaphoreType.DMA((count, 12)),
            pltpu.SemaphoreType.DMA((count, 12)),
        ]
    )
    return pl.pallas_call(
        functools.partial(grad_reduce_kernel, shapes),
        out_shape=[jax.ShapeDtypeStruct(s[1:], low) for s in shapes],
        in_specs=[pl.BlockSpec(memory_space=pl.ANY)] * count,
        out_specs=[pl.BlockSpec(memory_space=pl.ANY)] * count,
        scratch_shapes=scratch,
        compiler_params=pltpu.CompilerParams(collective_id=3, has_side_effects=True, vmem_limit_bytes=56 * 1024 * 1024),
        name="grad_reduce",
    )(*grads)


def sum_by_table(local_grads):
    band_count, column_count = lax.axis_size("ty"), lax.axis_size("tx")
    group_count = lax.axis_size("rows")
    tile_count = band_count * column_count
    table = jnp.concatenate([entry.reshape(group_count, -1) for entry in local_grads], axis=1)
    column_total = table.shape[1]
    padded_columns = -(-column_total // tile_count) * tile_count
    piece_width = padded_columns // tile_count
    table = table.reshape(group_count, tile_count, piece_width)
    shares = lax.psum_scatter(
        table.reshape(group_count * tile_count, piece_width),
        ("rows", "ty", "tx"),
        scatter_dimension=0,
        tiled=True,
    )
    summed = (
        lax.all_gather(shares.astype(jnp.bfloat16), ("ty", "tx"), axis=0, tiled=True)
        .astype(shares.dtype)
        .reshape(-1)
    )
    totals = []
    start_at = 0
    for entry in local_grads:
        length = entry.size // group_count
        shard_shape = (entry.shape[0] // group_count,) + entry.shape[1:]
        totals.append(summed[start_at : start_at + length].reshape(shard_shape))
        start_at = start_at + length
    return tuple(totals)


def shards(
    latent,
    skip_input,
    segment_ids,
    embed_weight,
    embed_bias,
    skip_weight,
    skip_bias,
    norm1_gain,
    norm1_bias,
    qkv_weight,
    proj_weight,
    proj_bias,
    norm2_gain,
    norm2_bias,
    fc1_weight,
    fc1_bias,
    fc2_weight,
    fc2_bias,
    conv_weight,
    cotangent,
):
    row_count, tile_height, tile_width, width = skip_input.shape
    patch = latent.shape[3]
    tokens = tile_height * tile_width
    token_count = row_count * tokens
    low = jnp.bfloat16
    wide = jnp.float32
    cuts = jnp.stack(
        [jnp.sum(segment_ids[:, 0, :] == 0, axis=1), jnp.sum(segment_ids[:, :, -1] == 1, axis=1)],
        axis=1,
    ).astype(jnp.int32)
    vectors = jnp.stack(
        [embed_bias, skip_bias, norm1_gain, norm1_bias, proj_bias, norm2_gain, norm2_bias, fc2_bias]
    ).astype(wide)
    hidden_bias = fc1_bias.astype(wide).reshape(-1, 1, 512)
    conv_turned = conv_weight.T
    cot = cotangent.reshape(row_count, tokens, patch).transpose(0, 2, 1)
    flat_latent = latent.reshape(token_count, patch)
    flat_skip = skip_input.reshape(token_count, width)
    embedded, stream, normed, query, pairs = front(
        flat_latent, flat_skip, embed_weight, skip_weight, qkv_weight, vectors, row_count
    )
    attended, log_total, row_pairs, cot_tiles = attend(cuts, query, pairs, cot, tile_height, tile_width)
    (
        fc1_grad, fc2_grad, hidden_bias_grad, proj_grad, attended_grad, mid_grad, conv_in, spread, middle_grads
    ) = middle(
        cuts, attended.reshape(token_count, width), stream, cot_tiles, proj_weight, conv_turned, vectors,
        hidden_bias, fc1_weight, fc2_weight, tile_height, tile_width,
    )
    projected_grad, conv_grad, conv_out = attend_back(
        cuts, query, attended, attended_grad.reshape(row_count, tokens, width), log_total,
        conv_in, conv_turned, spread, row_pairs, tile_height, tile_width,
    )
    qkv_grad, skip_grad, skip_input_grad, thin, flat = rear(
        projected_grad.reshape(token_count, 3 * width), qkv_weight, normed, stream, mid_grad, embedded, flat_skip,
        flat_latent, skip_weight, vectors, middle_grads, hidden_bias_grad.reshape(4, -1), conv_grad,
    )
    output = conv_out.transpose(0, 2, 1).reshape(row_count, tile_height, tile_width, patch)
    skip_input_grad = skip_input_grad.reshape(row_count, tile_height, tile_width, width)
    taps = 9 * patch
    share = width // 4
    mesh_shape = (lax.axis_size("rows"), lax.axis_size("ty"), lax.axis_size("tx"))
    if mesh_shape == (4, 4, 2):
        local = [proj_grad, fc1_grad, fc2_grad, qkv_grad, skip_grad, thin]
        summed = grad_reduce([entry.reshape(4, -1, entry.shape[1]) for entry in local] + [flat])
        proj_total, fc1_total, fc2_total, qkv_total, skip_total = [entry.astype(wide) for entry in summed[:5]]
        conv_total = summed[5][:, :taps].astype(wide)
        embed_total = summed[5][:, taps : taps + patch].astype(wide)
        line = [summed[6][k, :share].astype(wide) for k in range(8)]
        fc1_line = summed[6][8:11].reshape(-1).astype(wide)
        return (
            output, skip_input_grad, embed_total, line[0], skip_total, line[1], line[2], line[3], qkv_total,
            proj_total, line[4], line[5], line[6], fc1_total, fc1_line, fc2_total, line[7], conv_total,
        )
    line = [flat[:, k, :share].reshape(-1) for k in range(8)]
    fc1_line = flat[:, 8:11].reshape(-1)
    local_grads = [
        thin[:, taps : taps + patch], line[0], skip_grad, line[1], line[2], line[3], qkv_grad, proj_grad, line[4],
        line[5], line[6], fc1_grad, fc1_line, fc2_grad, line[7], thin[:, :taps],
    ]
    return (output, skip_input_grad) + sum_by_table([entry.astype(wide) for entry in local_grads])


def solution(mesh):
    return jax.shard_map(
        shards,
        mesh=mesh,
        in_specs=(
            P("rows", "ty", "tx", None),
            P("rows", "ty", "tx", None),
            P("rows", None, None),
            P(),
            P(),
            P(),
            P(),
            P(),
            P(),
            P(),
            P(),
            P(),
            P(),
            P(),
            P(),
            P(),
            P(),
            P(),
            P(),
            P("rows", "ty", "tx", None),
        ),
        out_specs=(
            P("rows", "ty", "tx", None),
            P("rows", "ty", "tx", None),
            P("rows", None),
            P("rows"),
            P("rows", None),
            P("rows"),
            P("rows"),
            P("rows"),
            P("rows", None),
            P("rows", None),
            P("rows"),
            P("rows"),
            P("rows"),
            P("rows", None),
            P("rows"),
            P("rows", None),
            P("rows"),
            P("rows", None),
        ),
        check_vma=False,
    )
```

```python
import functools

import jax
import jax.numpy as jnp
from jax import lax
from jax.experimental import pallas as pl
from jax.experimental.pallas import tpu as pltpu
from jax.sharding import PartitionSpec as P

MESH = pl.DeviceIdType.MESH
norm_eps = 1e-05


def cell_of(token, tile, tile_height, tile_width, columns):
    down = tile // columns * tile_height + token // tile_width
    across = tile % columns * tile_width + token % tile_width
    return down, across


def fill_shift(shift_ref, tile_height, tile_width):
    tokens = tile_height * tile_width
    bands, columns = lax.axis_size("ty"), lax.axis_size("tx")
    own = lax.axis_index("ty") * columns + lax.axis_index("tx")
    lane = lax.broadcasted_iota(jnp.int32, (8, tokens), 1)
    down, across = cell_of(lane, own, tile_height, tile_width, columns)
    step = lax.broadcasted_iota(jnp.int32, (shift_ref.shape[0], tokens), 0)
    for p in range(9):
        i, j = down - (p // 3 - 1), across - (p % 3 - 1)
        inside = (i >= 0) & (i < bands * tile_height) & (j >= 0) & (j < columns * tile_width)
        tile = i // tile_height * columns + j // tile_width
        place = tile * tokens + i % tile_height * tile_width + j % tile_width
        place = jnp.where(inside, place, -1)[0:1]
        chosen = jnp.where(step == place, 1.0, 0.0)
        shift_ref[:, p * tokens : (p + 1) * tokens] = chosen.astype(jnp.bfloat16)


def same_image(cuts_ref, row, p, tile_height, tile_width):
    tokens = tile_height * tile_width
    columns = lax.axis_size("tx")
    own = lax.axis_index("ty") * columns + lax.axis_index("tx")
    lane = lax.broadcasted_iota(jnp.int32, (8, tokens), 1)
    down, across = cell_of(lane, own, tile_height, tile_width, columns)
    left_width, top_height = cuts_ref[row, 0], cuts_ref[row, 1]

    def image_of(i, j):
        return jnp.where(j < left_width, 0, jnp.where(i < top_height, 1, 2))

    there = image_of(down - (p // 3 - 1), across - (p % 3 - 1))
    return jnp.where(image_of(down, across) == there, 1.0, 0.0)[0:1]


def mm(former, latter, axis_former, axis_latter):
    return lax.dot_general(
        former,
        latter,
        (((axis_former,), (axis_latter,)), ((), ())),
        preferred_element_type=jnp.float32,
    )


def normalised(values):
    average = jnp.mean(values, axis=1, keepdims=True)
    centred = values - average
    rate = lax.rsqrt(jnp.mean(centred * centred, axis=1, keepdims=True) + norm_eps)
    return centred * rate, rate


def norm_back(incoming, unit, rate, gain):
    scaled = incoming * gain
    first = jnp.mean(scaled, axis=1, keepdims=True)
    second = jnp.mean(scaled * unit, axis=1, keepdims=True)
    return (scaled - first - unit * second) * rate


def down_sum(values):
    return jnp.sum(values, axis=0, keepdims=True)


def front_kernel(latent, skip, embed_weight, skip_weight, qkv_weight, vectors, embedded, stream, normed, query, pairs):
    width = skip.shape[1]
    row_count, tokens = query.shape[0], query.shape[1]
    for row in range(row_count):
        at = slice(row * tokens, (row + 1) * tokens)
        entered = (mm(latent[at, :], embed_weight[...], 1, 1) + vectors[0:1]).astype(jnp.bfloat16)
        embedded[at, :] = entered
        total = mm(entered, skip_weight[:width], 1, 0) + mm(skip[at, :], skip_weight[width:], 1, 0) + vectors[1:2]
        stream[at, :] = total
        unit, rate = normalised(total)
        low = (unit * vectors[2:3] + vectors[3:4]).astype(jnp.bfloat16)
        normed[at, :] = low
        query[row] = mm(low, qkv_weight[:, :width], 1, 0).astype(jnp.bfloat16)
        pairs[row] = mm(low, qkv_weight[:, width:], 1, 0).astype(jnp.bfloat16)


def front(latent, skip, embed_weight, skip_weight, qkv_weight, vectors, row_count):
    token_count, width = skip.shape
    tokens = token_count // row_count
    low = jnp.bfloat16
    return pl.pallas_call(
        front_kernel,
        out_shape=[
            jax.ShapeDtypeStruct((token_count, width), low),
            jax.ShapeDtypeStruct((token_count, width), jnp.float32),
            jax.ShapeDtypeStruct((token_count, width), low),
            jax.ShapeDtypeStruct((row_count, tokens, width), low),
            jax.ShapeDtypeStruct((row_count, tokens, 2 * width), low),
        ],
        compiler_params=pltpu.CompilerParams(vmem_limit_bytes=32 * 1024 * 1024),
        name="front",
    )(latent, skip, embed_weight, skip_weight, qkv_weight, vectors)


def erf_of(values):
    x = jnp.clip(values, -4.0, 4.0)
    square = x * x
    upper = square * -2.72614225801306e-10 + 2.77068142495902e-08
    for term in (-2.10102402082508e-06, -5.69250639462346e-05, -7.34990630326855e-04, -2.95459980854025e-03, -1.60960333262415e-02):
        upper = upper * square + term
    lower = square * -1.45660718464996e-05 + -2.13374055278905e-04
    for term in (-1.68282697438203e-03, -7.37332916720468e-03, -1.42647390514189e-02):
        lower = lower * square + term
    return x * upper / lower


def middle_kernel(
    tile_height, tile_width,
    cuts, attended, stream, cot_tiles, proj_weight, conv_turned, vectors, hidden_bias, fc1_weight, fc2_weight,
    fc1_grad, fc2_grad, hidden_bias_grad, proj_grad, attended_grad, mid_grad, conv_in, spread, vector_grads,
    middle, normed, out_grad, out_low, forward_sum, backward_sum, shift,
):
    step = pl.program_id(0)
    row_count, tokens = cot_tiles.shape[1], cot_tiles.shape[3]
    token_count = row_count * tokens
    low = jnp.bfloat16
    parts = [slice(k * tokens, (k + 1) * tokens) for k in range(row_count)]

    @pl.when(step == 0)
    def _():
        fill_shift(shift, tile_height, tile_width)
        tile_count = cot_tiles.shape[0]
        patch = cot_tiles.shape[2]
        turned = jnp.concatenate(
            [cot_tiles[t].reshape(row_count * patch, tokens) for t in range(tile_count)], axis=1
        )
        moved = mm(turned, shift[...], 1, 0)
        for row in range(row_count):
            for p in range(9):
                piece = moved[row * patch : (row + 1) * patch, p * tokens : (p + 1) * tokens]
                piece = piece * same_image(cuts, row, p, tile_height, tile_width)
                spread[p * patch : (p + 1) * patch, parts[row]] = piece.astype(low)
        total = jnp.zeros((1, stream.shape[1]), jnp.float32)
        for at in parts:
            grad = mm(spread[:, at], conv_turned[...], 0, 0)
            out_grad[at, :] = grad
            out_low[at, :] = grad.astype(low)
            total = total + down_sum(grad)
            value = stream[at, :] + mm(attended[at, :], proj_weight[...], 1, 0) + vectors[4:5]
            middle[at, :] = value
            unit, rate = normalised(value)
            normed[at, :] = (unit * vectors[5:6] + vectors[6:7]).astype(low)
        vector_grads[7:8] = total
        forward_sum[...] = jnp.zeros_like(forward_sum)
        backward_sum[...] = jnp.zeros_like(backward_sum)

    bias_grad = jnp.zeros((1, fc1_weight.shape[1]), jnp.float32)
    actives, hidden_lows = [], []
    for at in parts:
        hidden = mm(normed[at, :], fc1_weight[...], 1, 0) + hidden_bias[0]
        active_grad = mm(out_low[at, :], fc2_weight[...], 1, 1)
        share = 0.5 + 0.5 * erf_of(hidden * 0.7071067811865476)
        density = jnp.exp(hidden * hidden * -0.5) * 0.3989422804014327
        active = (hidden * share).astype(low)
        hidden_grad = active_grad * (share + hidden * density)
        bias_grad = bias_grad + down_sum(hidden_grad)
        hidden_low = hidden_grad.astype(low)
        forward_sum[at, :] = forward_sum[at, :] + mm(active, fc2_weight[...], 1, 0)
        backward_sum[at, :] = backward_sum[at, :] + mm(hidden_low, fc1_weight[...], 1, 1)
        actives.append(active)
        hidden_lows.append(hidden_low)
    hidden_bias_grad[0] = bias_grad
    fc2_grad[...] = mm(jnp.concatenate(actives, axis=0), out_low[...], 0, 0).astype(low)
    fc1_grad[...] = mm(normed[...], jnp.concatenate(hidden_lows, axis=0), 0, 0).astype(low)

    @pl.when(step == pl.num_programs(0) - 1)
    def _():
        width = stream.shape[1]
        gain_sum = jnp.zeros((1, width), jnp.float32)
        bias_sum = jnp.zeros((1, width), jnp.float32)
        mid_sum = jnp.zeros((1, width), jnp.float32)
        lows = []
        for at in parts:
            unit, rate = normalised(middle[at, :])
            conv_in[at, :] = (middle[at, :] + forward_sum[at, :] + vectors[7:8]).astype(low)
            incoming = backward_sum[at, :]
            gain_sum = gain_sum + down_sum(incoming * unit)
            bias_sum = bias_sum + down_sum(incoming)
            grad = out_grad[at, :] + norm_back(incoming, unit, rate, vectors[5:6])
            mid_grad[at, :] = grad
            mid_sum = mid_sum + down_sum(grad)
            mid_low = grad.astype(low)
            lows.append(mid_low)
            attended_grad[at, :] = mm(mid_low, proj_weight[...], 1, 1).astype(low)
        proj_grad[...] = mm(attended[...], jnp.concatenate(lows, axis=0), 0, 0).astype(low)
        vector_grads[4:5] = mid_sum
        vector_grads[5:6] = gain_sum
        vector_grads[6:7] = bias_sum


def middle(cuts, attended, stream, cot_tiles, proj_weight, conv_turned, vectors, hidden_bias, fc1_weight, fc2_weight, tile_height, tile_width):
    token_count, width = stream.shape
    hidden_width = fc1_weight.shape[1]
    block = 512
    steps = hidden_width // block
    low = jnp.bfloat16
    vmem = pl.BlockSpec(memory_space=pltpu.VMEM)
    tile_count, tokens = cot_tiles.shape[0], cot_tiles.shape[3]
    taps = conv_turned.shape[0]
    return pl.pallas_call(
        functools.partial(middle_kernel, tile_height, tile_width),
        grid=(steps,),
        out_shape=[
            jax.ShapeDtypeStruct((width, hidden_width), low),
            jax.ShapeDtypeStruct((hidden_width, width), low),
            jax.ShapeDtypeStruct((steps, 1, block), jnp.float32),
            jax.ShapeDtypeStruct((width, width), low),
            jax.ShapeDtypeStruct((token_count, width), low),
            jax.ShapeDtypeStruct((token_count, width), jnp.float32),
            jax.ShapeDtypeStruct((token_count, width), low),
            jax.ShapeDtypeStruct((taps, token_count), low),
            jax.ShapeDtypeStruct((8, width), jnp.float32),
        ],
        in_specs=[pl.BlockSpec(memory_space=pltpu.SMEM)]
        + [vmem] * 6
        + [
            pl.BlockSpec((1, 1, block), lambda k: (k, 0, 0)),
            pl.BlockSpec((width, block), lambda k: (0, k)),
            pl.BlockSpec((block, width), lambda k: (k, 0)),
        ],
        out_specs=[
            pl.BlockSpec((width, block), lambda k: (0, k)),
            pl.BlockSpec((block, width), lambda k: (k, 0)),
            pl.BlockSpec((1, 1, block), lambda k: (k, 0, 0)),
        ]
        + [vmem] * 6,
        scratch_shapes=[
            pltpu.VMEM((token_count, width), jnp.float32),
            pltpu.VMEM((token_count, width), low),
            pltpu.VMEM((token_count, width), jnp.float32),
            pltpu.VMEM((token_count, width), low),
            pltpu.VMEM((token_count, width), jnp.float32),
            pltpu.VMEM((token_count, width), jnp.float32),
            pltpu.VMEM((tile_count * tokens, 9 * tokens), low),
        ],
        compiler_params=pltpu.CompilerParams(vmem_limit_bytes=40 * 1024 * 1024),
        name="middle",
    )(cuts, attended, stream, cot_tiles, proj_weight, conv_turned, vectors, hidden_bias, fc1_weight, fc2_weight)


def rear_kernel(
    starts, reduces, projected_in, qkv_in, normed_in, stream_in, mid_in, embedded_in, skip_in, skip_weight_in,
    latent, vectors, middle_grads, hidden_bias_grad, conv_grad, *refs
):
    count = len(starts)
    resumed, refs = refs[:count], refs[count:]
    skip_input_grad, refs = refs[0], refs[1:]
    if reduces:
        sums, refs = refs[: count + 4], refs[count + 4 :]
        peers = chip_peers()
    qkv_grad, skip_grad, thin, flat, refs = *refs[:4], refs[4:]
    projected_grad, qkv_weight, normed, stream, mid_grad, embedded, skip, skip_weight, stream_low, load_sem = refs[:10]
    sources = (projected_in, normed_in, qkv_in, stream_in, mid_in, embedded_in, skip_in, skip_weight_in)
    targets = (projected_grad, normed, qkv_weight, stream, mid_grad, embedded, skip, skip_weight)
    loads = [pltpu.make_async_copy(a, b, load_sem.at[k]) for k, (a, b) in enumerate(zip(sources, targets))]
    for load in loads[:3]:
        load.start()
    later, news = [], []
    if reduces:
        items = make_reducers(
            starts + ("plane",) * 4, resumed + (qkv_grad, skip_grad, thin, flat), sums, refs[10:]
        )
        later, news = items[:count], items[count:]
        greet([peers[name] for name in ("core", "x", "y", "xy")] + peers["z"])
    for item in later:
        item.begin()
    for load in loads[3:]:
        load.start()
    for item in later:
        item.stages.pop(0)()
    token_count, width = stream.shape
    low = jnp.bfloat16
    tokens = 128
    parts = [slice(k * tokens, (k + 1) * tokens) for k in range(token_count // tokens)]
    zero = jnp.zeros((1, width), jnp.float32)
    gain_sum, bias_sum, stream_sum, embed_sum = zero, zero, zero, zero
    loads[0].wait()
    loads[1].wait()
    blocks, depth = qkv_grad.shape[0], qkv_grad.shape[1]
    for k in range(3):
        at = slice(k * width, (k + 1) * width)
        qkv_grad[:, :, at] = mm(normed[...], projected_grad[:, at], 0, 0).astype(low).reshape(blocks, depth, width)

    def open_up(which):
        for item in news[which]:
            item.begin()

    def step_on(group):
        for item in group:
            if item.stages:
                item.stages.pop(0)()

    open_up(slice(0, 1))
    for load in loads[2:5]:
        load.wait()
    for at in parts:
        incoming = mm(projected_grad[at, :], qkv_weight[...], 1, 1)
        unit, rate = normalised(stream[at, :])
        gain_sum = gain_sum + down_sum(incoming * unit)
        bias_sum = bias_sum + down_sum(incoming)
        grad = mid_grad[at, :] + norm_back(incoming, unit, rate, vectors[2:3])
        stream_sum = stream_sum + down_sum(grad)
        stream_low[at, :] = grad.astype(low)
    step_on(news[0:1])
    loads[5].wait()
    loads[6].wait()
    skip_grad[0:2] = mm(embedded[...], stream_low[...], 0, 0).astype(low).reshape(2, width // 2, width)
    skip_grad[2:4] = mm(skip[...], stream_low[...], 0, 0).astype(low).reshape(2, width // 2, width)
    open_up(slice(1, 2))
    loads[7].wait()
    embed_lows = []
    for at in parts:
        embed_grad = mm(stream_low[at, :], skip_weight[:width], 1, 1)
        embed_sum = embed_sum + down_sum(embed_grad)
        embed_lows.append(embed_grad.astype(low))
    embed_weight_grad = mm(jnp.concatenate(embed_lows, axis=0), latent[...], 0, 0)
    step_on(news[1:2])
    rest = jnp.zeros((width, 128 - 2 * 16), jnp.float32)
    thin[:, :, :128] = conv_grad[:, :128].astype(low).reshape(4, width // 4, 128)
    edge = jnp.concatenate([conv_grad[:, 128:144], embed_weight_grad, rest], axis=1)
    thin[:, :, 128:] = edge.astype(low).reshape(4, width // 4, 128)
    rows = [embed_sum, stream_sum, gain_sum, bias_sum] + [middle_grads[k : k + 1] for k in range(4, 8)]
    stack = jnp.concatenate(rows, axis=0)
    share = width // 4
    for block in range(4):
        own = stack[:, block * share : (block + 1) * share]
        own = jnp.concatenate([own, jnp.zeros((8, 256 - share), jnp.float32)], axis=1)
        line = hidden_bias_grad[block : block + 1]
        pieces = [line[:, k * 256 : (k + 1) * 256] for k in range(width // 256)]
        body = jnp.concatenate([own] + pieces + [jnp.zeros((8 - len(pieces), 256), jnp.float32)], axis=0)
        flat[block, 0:16] = body.astype(low)
        flat[block, 16:64] = jnp.zeros((48, 256), low)
    open_up(slice(2, 4))
    step_on(later)
    step_on(news[0:1])
    for at in parts:
        skip_input_grad[at, :] = mm(stream_low[at, :], skip_weight[width:], 1, 1).astype(low)
    step_on(news[2:4])
    while any(item.stages for item in later + news):
        step_on(later)
        step_on(news)


def rear(projected_grad, qkv_weight, normed, stream, mid_grad, embedded, skip, skip_weight, latent, vectors, middle_grads, hidden_bias_grad, conv_grad, resumed, reduces):
    token_count, width = stream.shape
    low = jnp.bfloat16
    starts = tuple(start for start, _, _ in resumed)
    sizes = [(width // 4, 3 * width), (width // 2, width), (width // 4, 256), (64, 256)]
    totals = [shape for _, _, shape in resumed] + sizes
    vmem, anywhere = pl.BlockSpec(memory_space=pltpu.VMEM), pl.BlockSpec(memory_space=pl.ANY)
    big = [projected_grad, qkv_weight, normed, stream, mid_grad, embedded, skip, skip_weight]
    out_shape = [jax.ShapeDtypeStruct((token_count, width), low)]
    out_specs = [vmem]
    scratch = []
    if reduces:
        out_shape += [jax.ShapeDtypeStruct(shape, low) for shape in totals]
        out_specs += [anywhere] * len(totals)
        scratch += [pltpu.VMEM((4,) + shape, low) for shape in sizes]
        params = pltpu.CompilerParams(collective_id=3, has_side_effects=True, vmem_limit_bytes=56 * 1024 * 1024)
    else:
        out_shape += [jax.ShapeDtypeStruct((4,) + shape, low) for shape in sizes]
        out_specs += [vmem] * len(sizes)
        params = pltpu.CompilerParams(vmem_limit_bytes=48 * 1024 * 1024)
    scratch += [pltpu.VMEM(entry.shape, entry.dtype) for entry in big]
    scratch += [pltpu.VMEM((token_count, width), low), pltpu.SemaphoreType.DMA((len(big),))]
    if reduces:
        scratch += reducer_scratch(starts + ("plane",) * 4, totals)
    return pl.pallas_call(
        functools.partial(rear_kernel, starts, reduces),
        out_shape=out_shape,
        in_specs=[anywhere] * len(big) + [vmem] * 5 + [anywhere] * len(starts),
        out_specs=out_specs,
        scratch_shapes=scratch,
        compiler_params=params,
        name="rear",
    )(*big, latent, vectors, middle_grads, hidden_bias_grad, conv_grad, *[entry for _, entry, _ in resumed])


def plane_peers():
    z, ty, y = lax.axis_index("rows"), lax.axis_index("ty"), lax.axis_index("tx")
    core, x = lax.rem(ty, 2), ty // 2
    here = x * 2 + core
    across = (1 - x) * 2 + core
    tiles = {
        "own": here * 2 + y,
        "x": across * 2 + y,
        "y": here * 2 + 1 - y,
        "xy": across * 2 + 1 - y,
    }
    peers = {
        "core": (z, x * 2 + 1 - core, y),
        "x": (z, across, y),
        "y": (z, here, 1 - y),
    }
    return tiles, peers


def plane_peer(k):
    z, ty, y = lax.axis_index("rows"), lax.axis_index("ty"), lax.axis_index("tx")
    x, core = ty // 2, lax.rem(ty, 2)
    flip_x, flip_core, flip_y = k // 4, k // 2 % 2, k % 2
    x = x + flip_x - 2 * flip_x * x
    core = core + flip_core - 2 * flip_core * core
    y = y + flip_y - 2 * flip_y * y
    return (z, x * 2 + core, y), (x * 2 + core) * 2 + y


def greet(peers):
    barrier = pltpu.get_barrier_semaphore()
    for peer in peers:
        pl.semaphore_signal(barrier, inc=1, device_id=peer, device_id_type=MESH)
    pl.semaphore_wait(barrier, len(peers))


def fill_mask(mask_ref, cuts_ref, row, tile_height, tile_width):
    ty, tx = lax.axis_index("ty"), lax.axis_index("tx")
    columns = lax.axis_size("tx")
    tokens = tile_height * tile_width
    left_width = cuts_ref[row, 0]
    top_height = cuts_ref[row, 1]

    def image_of(down, across):
        return jnp.where(across < left_width, 0, jnp.where(down < top_height, 1, 2))

    lane = lax.broadcasted_iota(jnp.int32, (tokens, tokens), 1)
    step = lax.broadcasted_iota(jnp.int32, (tokens, tokens), 0)
    mine = image_of(
        ty * tile_height + lane // tile_width, tx * tile_width + lane % tile_width
    )
    for tile in range(mask_ref.shape[0] // tokens):
        theirs = image_of(
            tile // columns * tile_height + step // tile_width,
            tile % columns * tile_width + step % tile_width,
        )
        mask_ref[tile * tokens : (tile + 1) * tokens, :] = jnp.where(
            mine == theirs, 0.0, -1e30
        )


def two_heads(pair, scale):
    lane = lax.broadcasted_iota(jnp.int32, pair.shape, 1)
    wide = pair.astype(jnp.float32) * scale
    first = jnp.where(lane < pair.shape[1] // 2, wide, 0.0)
    return jnp.concatenate([first, wide - first], axis=0).astype(jnp.bfloat16)


def own_blocks(both):
    head, tokens = both.shape[0] // 2, both.shape[1] // 2
    return jnp.concatenate([both[:head, :tokens], both[head:, tokens:]], axis=0)


def attend_kernel(
    tile_height, tile_width, cuts, query, pairs, cot, out, lse, all_out, cot_out, held, scores, mask, local_sem, send_sem, recv_sem,
    cot_sem, cot_send_sem, cot_recv_sem
):
    row_count, tokens, width = query.shape
    tile_count = held.shape[1]
    pair_count = width // 128
    tiles, peers = plane_peers()
    own = tiles["own"]
    greet([plane_peer(k)[0] for k in range(1, tile_count)])
    cot_copies = [pltpu.make_async_copy(cot, cot_out.at[own], cot_sem.at[0])]
    for k in range(1, tile_count):
        cot_copies.append(
            pltpu.make_async_remote_copy(
                src_ref=cot,
                dst_ref=cot_out.at[own],
                send_sem=cot_send_sem.at[k],
                recv_sem=cot_recv_sem.at[k],
                device_id=plane_peer(k)[0],
                device_id_type=MESH,
            )
        )

    def send(row, slot, source, target, peer):
        copy = pltpu.make_async_remote_copy(
            src_ref=source,
            dst_ref=target,
            send_sem=send_sem.at[row, slot],
            recv_sem=recv_sem.at[row, slot],
            device_id=peer,
            device_id_type=MESH,
        )
        copy.start()
        return copy

    flights = [{} for _ in range(row_count)]

    def begin(row):
        here = held.at[row, own]
        source = pairs.at[row]
        flights[row]["x"] = send(row, 0, source, here, peers["x"])
        flights[row]["y"] = send(row, 1, source, here, peers["y"])
        flights[row]["core"] = send(row, 2, source, here, peers["core"])
        keep = pltpu.make_async_copy(source, here, local_sem.at[row, 0])
        keep.start()
        flights[row]["keep"] = keep

    def forward(row):
        flights[row]["y"].wait_recv()
        key_half = held.at[row, tiles["y"], :, pl.ds(0, width)]
        flights[row]["far_x"] = send(row, 3, key_half, key_half, peers["x"])
        flights[row]["x"].wait_recv()
        value_half = held.at[row, tiles["x"], :, pl.ds(width, width)]
        flights[row]["far_y"] = send(row, 4, value_half, value_half, peers["y"])
        for slot, name in ((5, "x"), (6, "y")):
            tile = held.at[row, tiles[name]]
            flights[row]["core_" + name] = send(row, slot, tile, tile, peers["core"])

    def finish(row):
        flights[row]["far_x"].wait_recv()
        flights[row]["far_y"].wait_recv()
        tile = held.at[row, tiles["xy"]]
        last = send(row, 7, tile, tile, peers["core"])
        flights[row]["keep"].wait()
        for name in ("core", "core_x", "core_y"):
            flights[row][name].wait_recv()
        last.wait_recv()
        for name in ("x", "y", "core", "far_x", "far_y", "core_x", "core_y"):
            flights[row][name].wait_send()
        last.wait_send()
        keep = pltpu.make_async_copy(held.at[row], all_out.at[row], local_sem.at[row, 1])
        keep.start()
        flights[row]["out"] = keep

    chunk = 2

    def compute(row):
        fill_mask(mask, cuts, row, tile_height, tile_width)

        def one_pair(p, carry):
            at = pl.ds(pl.multiple_of(p * 128, 128), 128)
            at_value = pl.ds(pl.multiple_of(width + p * 128, 128), 128)
            both = two_heads(query[row, :, at], 0.125)
            peak = None
            for c in range(tile_count // chunk):
                span = slice(c * chunk * tokens, (c + 1) * chunk * tokens)
                keys = held[row, c * chunk : (c + 1) * chunk, :, at].reshape(chunk * tokens, 128)
                extra = mask[span, :]
                part = mm(keys, both, 1, 1) + jnp.concatenate([extra, extra], axis=1)
                scores[span, :] = part
                top = jnp.max(part, axis=0, keepdims=True)
                peak = top if peak is None else jnp.maximum(peak, top)
            total = jnp.zeros_like(peak)
            summed = jnp.zeros((128, 2 * tokens), jnp.float32)
            for c in range(tile_count // chunk):
                span = slice(c * chunk * tokens, (c + 1) * chunk * tokens)
                values = held[row, c * chunk : (c + 1) * chunk, :, at_value].reshape(chunk * tokens, 128)
                part = jnp.exp(scores[span, :] - peak)
                total = total + jnp.sum(part, axis=0, keepdims=True)
                summed = summed + mm(values, part.astype(jnp.bfloat16), 0, 0)
            blocks = own_blocks(summed / total)
            out[row, :, at] = jnp.transpose(blocks).astype(jnp.bfloat16)
            lse[row, p] = peak + jnp.log(total)
            return carry

        lax.fori_loop(0, pair_count, one_pair, 0, unroll=3)

    begin(0)
    if row_count > 1:
        begin(1)
    for copy in cot_copies:
        copy.start()
    forward(0)
    for row in range(row_count):
        if row + 2 < row_count:
            begin(row + 2)
        if row + 1 < row_count:
            forward(row + 1)
        finish(row)
        compute(row)
    for row in range(row_count):
        flights[row]["out"].wait()
    for copy in cot_copies:
        copy.wait()


def attend(cuts, query, pairs, cot, tile_height, tile_width):
    row_count, tokens, width = query.shape
    tile_count = lax.axis_size("ty") * lax.axis_size("tx")
    pair_count = width // 128
    low = jnp.bfloat16
    vmem = pl.BlockSpec(memory_space=pltpu.VMEM)
    return pl.pallas_call(
        functools.partial(attend_kernel, tile_height, tile_width),
        out_shape=[
            jax.ShapeDtypeStruct((row_count, tokens, width), low),
            jax.ShapeDtypeStruct((row_count, pair_count, 1, 2 * tokens), jnp.float32),
            jax.ShapeDtypeStruct((row_count, tile_count, tokens, 2 * width), low),
            jax.ShapeDtypeStruct((tile_count,) + cot.shape, low),
        ],
        in_specs=[pl.BlockSpec(memory_space=pltpu.SMEM), vmem] + [pl.BlockSpec(memory_space=pl.ANY)] * 2,
        out_specs=[vmem, vmem] + [pl.BlockSpec(memory_space=pl.ANY)] * 2,
        scratch_shapes=[
            pltpu.VMEM((row_count, tile_count, tokens, 2 * width), low),
            pltpu.VMEM((tile_count * tokens, 2 * tokens), jnp.float32),
            pltpu.VMEM((tile_count * tokens, tokens), jnp.float32),
            pltpu.SemaphoreType.DMA((row_count, 2)),
            pltpu.SemaphoreType.DMA((row_count, 8)),
            pltpu.SemaphoreType.DMA((row_count, 8)),
            pltpu.SemaphoreType.DMA((1,)),
            pltpu.SemaphoreType.DMA((tile_count,)),
            pltpu.SemaphoreType.DMA((tile_count,)),
        ],
        compiler_params=pltpu.CompilerParams(
            collective_id=1, has_side_effects=True, vmem_limit_bytes=40 * 1024 * 1024
        ),
        name="attend",
    )(cuts, query, pairs, cot)


def attend_back_kernel(
    tile_height, tile_width, starts, cuts, query_in, attended_in, grad_in, lse_in, conv_in, conv_turned, spread, all_pairs, *refs
):
    count = len(starts)
    grads, refs = refs[:count], refs[count:]
    (out, conv_grad, conv_out), saved, refs = refs[:3], refs[3 : 3 + count], refs[3 + count :]
    query, attended, grad, lse, row_sem = refs[:5]
    refs = refs[5:]
    held, terms, core_terms, side_terms, mask, shift, taps, part, part_got = refs[:9]
    load_sem, send_sem, recv_sem, part_send_sem, part_recv_sem = refs[9:14]
    items = make_reducers(starts, grads, saved, refs[14:]) if count else []
    firsts = [item for item in items if item.start == "z"]
    planes = [item for item in items if item.start == "plane"]

    row_count, tokens, width = query.shape
    tile_count = held.shape[1]
    pair_count = width // 128
    tiles, peers = plane_peers()
    low = jnp.bfloat16
    loads = []
    for row in range(row_count):
        load = pltpu.make_async_copy(all_pairs.at[row], held.at[row], load_sem.at[row])
        load.start()
        loads.append([load])
        for k, (source, target) in enumerate(((query_in, query), (attended_in, attended), (grad_in, grad), (lse_in, lse))):
            load = pltpu.make_async_copy(source.at[row], target.at[row], row_sem.at[row, k])
            load.start()
            loads[-1].append(load)
    greet([plane_peer(k)[0] for k in range(1, tile_count)] + (chip_peers()["z"] if count else []))
    core = lax.rem(lax.axis_index("ty"), 2)
    chunk = 2

    def send(row, slot, source, target, peer):
        copy = pltpu.make_async_remote_copy(
            src_ref=source,
            dst_ref=target,
            send_sem=send_sem.at[row, slot],
            recv_sem=recv_sem.at[row, slot],
            device_id=peer,
            device_id_type=MESH,
        )
        copy.start()
        return copy

    def compute(row):
        for load in loads[row]:
            load.wait()
        fill_mask(mask, cuts, row, tile_height, tile_width)

        def one_pair(p, carry):
            at = pl.ds(pl.multiple_of(p * 128, 128), 128)
            at_value = pl.ds(pl.multiple_of(width + p * 128, 128), 128)
            grad_pair = grad[row, :, at]
            both = two_heads(query[row, :, at], 0.125)
            both_grad = two_heads(grad_pair, 1.0)
            inner = jnp.transpose(grad_pair.astype(jnp.float32) * attended[row, :, at].astype(jnp.float32))
            half = inner.shape[0] // 2
            delta = jnp.concatenate(
                [jnp.sum(inner[:half], axis=0, keepdims=True), jnp.sum(inner[half:], axis=0, keepdims=True)], axis=1
            )
            level = lse[row, p]
            query_part = jnp.zeros((128, 2 * tokens), jnp.float32)
            for c in range(tile_count // chunk):
                span = slice(c * chunk * tokens, (c + 1) * chunk * tokens)
                some = slice(c * chunk, (c + 1) * chunk)
                keys = held[row, some, :, at].reshape(chunk * tokens, 128)
                values = held[row, some, :, at_value].reshape(chunk * tokens, 128)
                extra = mask[span, :]
                weights = jnp.exp(mm(keys, both, 1, 1) + jnp.concatenate([extra, extra], axis=1) - level)
                score_grad = (weights * (mm(values, both_grad, 1, 1) - delta)).astype(low)
                value_part = mm(weights.astype(low), both_grad, 1, 0)
                key_part = mm(score_grad, both, 1, 0)
                query_part = query_part + mm(keys, score_grad, 0, 0)
                terms[row, some, :, at] = key_part.astype(low).reshape(chunk, tokens, 128)
                terms[row, some, :, at_value] = value_part.astype(low).reshape(chunk, tokens, 128)
            blocks = own_blocks(query_part) * 0.125
            out[row, :, at] = jnp.transpose(blocks).astype(low)
            return carry

        lax.fori_loop(0, pair_count, one_pair, 0, unroll=3)

    flights = [{} for _ in range(row_count)]
    names = ("own", "x", "y", "xy")
    key_at, value_at = pl.ds(0, width), pl.ds(width, width)

    def begin(row):
        copies = []
        other = 2 - 4 * core
        for k, name in enumerate(names):
            copies.append(send(row, k, terms.at[row, tiles[name] + other], core_terms.at[row, k], peers["core"]))
        flights[row]["core"] = copies

    def add(target, source, row_total):
        def body(i, carry):
            at = pl.ds(pl.multiple_of(i * 16, 16), 16)
            target[at, :] = target[at, :] + source[at, :]
            return carry

        lax.fori_loop(0, row_total // 16, body, 0)

    def scatter(row):
        for k in (3, 1, 2, 0):
            flights[row]["core"][k].wait()
            add(terms.at[row, tiles[names[k]]], core_terms.at[row, k], tokens)
            if k == 3:
                far = terms.at[row, tiles["xy"]]
                flights[row]["far_x"] = send(row, 4, far.at[:, key_at], side_terms.at[row, 0], peers["x"])
                flights[row]["far_y"] = send(row, 5, far.at[:, value_at], side_terms.at[row, 1], peers["y"])
            if k == 1:
                near = terms.at[row, tiles["x"]]
                flights[row]["near_x"] = send(row, 6, near.at[:, key_at], side_terms.at[row, 2], peers["x"])
            if k == 2:
                near = terms.at[row, tiles["y"]]
                flights[row]["near_y"] = send(row, 7, near.at[:, value_at], side_terms.at[row, 3], peers["y"])

    def pass_on(row):
        flights[row]["far_x"].wait()
        near = terms.at[row, tiles["y"], :, key_at]
        add(near, side_terms.at[row, 0], tokens)
        flights[row]["last_y"] = send(row, 8, near, side_terms.at[row, 4], peers["y"])
        flights[row]["far_y"].wait()
        near = terms.at[row, tiles["x"], :, value_at]
        add(near, side_terms.at[row, 1], tokens)
        flights[row]["last_x"] = send(row, 9, near, side_terms.at[row, 5], peers["x"])

    def close(row):
        for name in ("near_x", "near_y", "last_x", "last_y"):
            flights[row][name].wait()
        mine = terms.at[row, tiles["own"]]

        def body(i, carry):
            at = pl.ds(pl.multiple_of(i * 16, 16), 16)
            for start, first, second in ((0, 2, 4), (width, 3, 5)):
                total = mine[at, start : start + width].astype(jnp.float32)
                total = total + side_terms[row, first, at, :].astype(jnp.float32)
                total = total + side_terms[row, second, at, :].astype(jnp.float32)
                out[row, at, width + start : 2 * width + start] = total.astype(low)
            return carry

        lax.fori_loop(0, tokens // 16, body, 0)

    part_copies = []

    def convolve():
        fill_shift(shift, tile_height, tile_width)
        patch = part.shape[2]
        taps[...] = mm(conv_turned[...], conv_in[...], 1, 1)
        rows = []
        for row in range(row_count):
            pieces = []
            for p in range(9):
                piece = taps[p * patch : (p + 1) * patch, row * tokens : (row + 1) * tokens]
                pieces.append(piece * same_image(cuts, row, p, tile_height, tile_width))
            rows.append(jnp.concatenate(pieces, axis=1))
        whole = jnp.concatenate(rows, axis=0)
        coarse = whole.astype(low)
        fine = (whole - coarse.astype(jnp.float32)).astype(low)
        moved = mm(coarse, shift[...], 1, 1) + mm(fine, shift[...], 1, 1)
        for tile in range(tile_count):
            part[tile] = moved[:, tile * tokens : (tile + 1) * tokens].reshape(row_count, patch, tokens)
        for k in range(1, tile_count):
            peer, tile = plane_peer(k)
            copy = pltpu.make_async_remote_copy(
                src_ref=part.at[tile],
                dst_ref=part_got.at[k],
                send_sem=part_send_sem.at[k],
                recv_sem=part_recv_sem.at[k],
                device_id=peer,
                device_id_type=MESH,
            )
            copy.start()
            part_copies.append(copy)
        conv_grad[...] = mm(conv_in[...], spread[...], 0, 1)

    def collect():
        total = part[tiles["own"]]
        for k, copy in enumerate(part_copies):
            copy.wait()
            total = total + part_got[k + 1]
        conv_out[...] = total.astype(low)

    def advance(group, stage):
        for item in group:
            item.stages[stage]()

    for item in items:
        item.begin()
    advance(items[:2], 0)
    for row in range(row_count):
        compute(row)
        begin(row)
        if row == 0:
            advance(items[2:], 0)
        if row > 1:
            pass_on(row - 2)
        if row > 0:
            scatter(row - 1)
            if row < 3:
                advance(planes, row)
    scatter(row_count - 1)
    if row_count > 1:
        pass_on(row_count - 2)
    convolve()
    pass_on(row_count - 1)
    for stage in range(min(row_count, 3), 3):
        advance(planes, stage)
    for row in range(row_count):
        close(row)
    collect()
    advance(planes, 3)
    advance(firsts, 1)
    for item in items:
        item.save()
    for item in items:
        item.land("save")


def attend_back(cuts, query, attended, grad, lse, conv_in, conv_turned, spread, all_pairs, grads, tile_height, tile_width):
    row_count, tokens, width = query.shape
    starts = tuple(start for start, _ in grads)
    grads = [entry for _, entry in grads]
    count = len(starts)
    shapes = [entry.shape[1:] for entry in grads]
    saves = [(r if start == "z" else r // 4, c // 2) for start, (r, c) in zip(starts, shapes)]
    tile_count = all_pairs.shape[1]
    taps = conv_turned.shape[0]
    low = jnp.bfloat16
    vmem = pl.BlockSpec(memory_space=pltpu.VMEM)
    return pl.pallas_call(
        functools.partial(attend_back_kernel, tile_height, tile_width, starts),
        out_shape=[
            jax.ShapeDtypeStruct((row_count, tokens, 3 * width), low),
            jax.ShapeDtypeStruct((width, taps), jnp.float32),
            jax.ShapeDtypeStruct((row_count, taps // 9, tokens), low),
        ]
        + [jax.ShapeDtypeStruct(s, low) for s in saves],
        in_specs=[pl.BlockSpec(memory_space=pltpu.SMEM)]
        + [pl.BlockSpec(memory_space=pl.ANY)] * 4
        + [vmem] * 3
        + [pl.BlockSpec(memory_space=pl.ANY)] * (1 + count),
        out_specs=[vmem] * 3 + [pl.BlockSpec(memory_space=pl.ANY)] * count,
        scratch_shapes=[
            pltpu.VMEM(query.shape, low),
            pltpu.VMEM(attended.shape, low),
            pltpu.VMEM(grad.shape, low),
            pltpu.VMEM(lse.shape, jnp.float32),
            pltpu.SemaphoreType.DMA((row_count, 4)),
            pltpu.VMEM((row_count, tile_count, tokens, 2 * width), low),
            pltpu.VMEM((row_count, tile_count, tokens, 2 * width), low),
            pltpu.VMEM((row_count, 4, tokens, 2 * width), low),
            pltpu.VMEM((row_count, 6, tokens, width), low),
            pltpu.VMEM((tile_count * tokens, tokens), jnp.float32),
            pltpu.VMEM((tile_count * tokens, 9 * tokens), low),
            pltpu.VMEM((taps, row_count * tokens), jnp.float32),
            pltpu.VMEM((tile_count, row_count, taps // 9, tokens), jnp.float32),
            pltpu.VMEM((tile_count, row_count, taps // 9, tokens), jnp.float32),
            pltpu.SemaphoreType.DMA((row_count,)),
            pltpu.SemaphoreType.DMA((row_count, 10)),
            pltpu.SemaphoreType.DMA((row_count, 10)),
            pltpu.SemaphoreType.DMA((tile_count,)),
            pltpu.SemaphoreType.DMA((tile_count,)),
        ]
        + (reducer_scratch(starts, shapes) if count else []),
        compiler_params=pltpu.CompilerParams(
            collective_id=2, has_side_effects=True, vmem_limit_bytes=60 * 1024 * 1024
        ),
        name="attend_back",
    )(cuts, query, attended, grad, lse, conv_in, conv_turned, spread, all_pairs, *grads)


def add_rows(target, first, second, rows):
    def body(i, carry):
        at = pl.ds(pl.multiple_of(i * 16, 16), 16)
        target[at, :] = first[at, :] + second[at, :]
        return carry

    lax.fori_loop(0, rows // 16, body, 0)


def add_four(target, others, rows):
    def body(i, carry):
        at = pl.ds(pl.multiple_of(i * 16, 16), 16)
        total = target[at, :].astype(jnp.float32) + others[0, at, :].astype(jnp.float32)
        total = total + (others[1, at, :].astype(jnp.float32) + others[2, at, :].astype(jnp.float32))
        target[at, :] = total.astype(jnp.bfloat16)
        return carry

    lax.fori_loop(0, rows // 16, body, 0)


def chip_peers():
    z, ty, y = lax.axis_index("rows"), lax.axis_index("ty"), lax.axis_index("tx")
    core, x = lax.rem(ty, 2), ty // 2
    across = (1 - x) * 2 + core
    return {
        "core": (z, x * 2 + 1 - core, y),
        "x": (z, across, y),
        "y": (z, ty, 1 - y),
        "xy": (z, across, 1 - y),
        "z": [(lax.rem(z + k, 4), ty, y) for k in (1, 2, 3)],
    }


class Reducer:
    def __init__(self, start, grad, out, buffers, sems, w):
        self.start, self.grad, self.out, self.buffers, self.w = start, grad, out, buffers, w
        self.local_sem, self.send_sem, self.recv_sem = sems
        self.z, ty, self.y = lax.axis_index("rows"), lax.axis_index("ty"), lax.axis_index("tx")
        self.core, self.x = lax.rem(ty, 2), ty // 2
        self.peers = chip_peers()
        self.flying = {}
        self.own = buffers[0]
        if start in ("plane", "z"):
            self.got, self.half, self.quarter, self.final = buffers[1:]
            self.depth, self.width = grad.shape[1], grad.shape[2] // 2
        else:
            self.depth, self.width = out.shape[0], out.shape[1] // 2
        if start == "block":
            self.half, self.quarter = buffers[1:]
        late = [self.begin_late, self.add_half_late, self.add_quarter_late, self.pass_strip, self.end]
        self.stages = {
            "plane": [self.add_core, self.add_half, self.add_quarter, self.sum_z, self.gather_piece, self.pass_strip, self.end],
            "z": [self.add_core, self.sum_z_first] + late,
            "block": late,
            "piece": [self.gather_piece, self.pass_strip, self.end],
        }[start]

    def part(self, at):
        if self.start == "block":
            return self.own.at[at]
        return self.own.at[self.z, at]

    def send(self, slot, source, target, peer):
        copy = pltpu.make_async_remote_copy(
            src_ref=source,
            dst_ref=target,
            send_sem=self.send_sem.at[self.w, slot],
            recv_sem=self.recv_sem.at[self.w, slot],
            device_id=peer,
            device_id_type=MESH,
        )
        copy.start()
        return copy

    def keep(self, slot, source, target):
        copy = pltpu.make_async_copy(source, target, self.local_sem.at[self.w, slot])
        copy.start()
        return copy

    def land(self, name):
        for copy in self.flying.pop(name):
            copy.wait()

    def columns(self, which):
        return pl.ds(pl.multiple_of(which * self.width, 128), self.width)

    def rows(self, start, size):
        return pl.ds(pl.multiple_of(start, 16), size)

    def place(self, block):
        later = block // 2
        major = self.x + later * (self.y - self.x)
        minor = self.y + later * (self.x - self.y)
        return self.rows(major * (self.depth // 2) + minor * (self.depth // 4), self.depth // 4)

    def begin(self):
        if self.start in ("block", "piece"):
            self.flying["load"] = [self.keep(0, self.grad, self.own)]
            return
        swap = self.send(0, self.grad.at[:, :, self.columns(1 - self.core)], self.got, self.peers["core"])
        mine = self.keep(0, self.grad.at[:, :, self.columns(self.core)], self.own)
        self.flying["core"] = [swap, mine]

    def add_core(self):
        self.land("core")
        for block in range(4):
            add_rows(self.own.at[block], self.own.at[block], self.got.at[block], self.depth)
        if self.start == "z":
            self.flying["z"] = [
                self.send(5 + k, self.own.at[peer[0]], self.final.at[k], peer) for k, peer in enumerate(self.peers["z"])
            ]
            return
        part = self.depth // 2
        first = self.send(1, self.own.at[0:2, self.rows((1 - self.x) * part, part)], self.half.at[0:2], self.peers["x"])
        second = self.send(2, self.own.at[2:4, self.rows((1 - self.y) * part, part)], self.half.at[2:4], self.peers["y"])
        self.flying["half"] = [first, second]

    def add_half(self):
        self.land("half")
        part, less = self.depth // 2, self.depth // 4
        for block in range(4):
            side = self.x if block < 2 else self.y
            kept = self.own.at[block, self.rows(side * part, part)]
            add_rows(kept, kept, self.half.at[block], part)
        first = self.own.at[0:2, self.rows(self.x * part + (1 - self.y) * less, less)]
        second = self.own.at[2:4, self.rows(self.y * part + (1 - self.x) * less, less)]
        self.flying["quarter"] = [
            self.send(3, first, self.quarter.at[0:2], self.peers["y"]),
            self.send(4, second, self.quarter.at[2:4], self.peers["x"]),
        ]

    def add_quarter(self):
        self.land("quarter")
        for block in range(4):
            kept = self.own.at[block, self.place(block // 2 * 2)]
            add_rows(kept, kept, self.quarter.at[block], self.depth // 4)
        self.flying["z"] = [
            self.send(5 + k, self.own.at[peer[0], self.place(peer[0])], self.final.at[k], peer)
            for k, peer in enumerate(self.peers["z"])
        ]

    def gather(self, pieces, sources):
        copies = []
        for n, (at, source) in enumerate(zip(pieces, sources)):
            target = self.out.at[at, self.columns(self.core)]
            for k, name in enumerate(("x", "y", "xy")):
                copies.append(self.send(8 + 3 * n + k, source, target, self.peers[name]))
            copies.append(self.keep(1 + n, source, target))
        self.flying["gather"] = copies

    def sum_z(self):
        self.land("z")
        add_four(self.own.at[self.z, self.place(self.z)], self.final, self.depth // 4)

    def gather_piece(self):
        if self.start == "piece":
            self.land("load")
            self.gather([self.place(self.z)], [self.own])
        else:
            self.gather([self.place(self.z)], [self.own.at[self.z, self.place(self.z)]])

    def sum_z_first(self):
        self.land("z")
        add_four(self.own.at[self.z], self.final, self.depth)

    def save(self):
        source = self.own.at[self.z] if self.start == "z" else self.own.at[self.z, self.place(self.z)]
        self.flying["save"] = [self.keep(1, source, self.out)]

    def begin_late(self):
        if self.start == "block":
            self.land("load")
        half, less = self.depth // 2, self.depth // 4
        self.flying["half"] = [
            self.send(1, self.part(self.rows((1 - self.x) * less, less)), self.half.at[0], self.peers["x"]),
            self.send(2, self.part(self.rows(half + (1 - self.y) * less, less)), self.half.at[1], self.peers["y"]),
        ]

    def add_half_late(self):
        self.land("half")
        half, less, least = self.depth // 2, self.depth // 4, self.depth // 8
        for n, start in enumerate((self.x * less, half + self.y * less)):
            kept = self.part(self.rows(start, less))
            add_rows(kept, kept, self.half.at[n], less)
        first = self.part(self.rows(self.x * less + (1 - self.y) * least, least))
        second = self.part(self.rows(half + self.y * less + (1 - self.x) * least, least))
        self.flying["quarter"] = [
            self.send(3, first, self.quarter.at[0], self.peers["y"]),
            self.send(4, second, self.quarter.at[1], self.peers["x"]),
        ]

    def add_quarter_late(self):
        self.land("quarter")
        half, less, least = self.depth // 2, self.depth // 4, self.depth // 8
        pieces = [self.rows(self.x * less + self.y * least, least), self.rows(half + self.y * less + self.x * least, least)]
        for n, at in enumerate(pieces):
            add_rows(self.part(at), self.part(at), self.quarter.at[n], least)
        self.gather(pieces, [self.part(at) for at in pieces])

    def pass_strip(self):
        self.land("gather")
        strip = self.out.at[:, self.columns(self.core)]
        self.flying["strip"] = [self.send(14, strip, strip, self.peers["core"])]

    def end(self):
        self.land("strip")


def reducer_scratch(starts, shapes):
    buffers = []
    for start, (depth, width) in zip(starts, shapes):
        half = width // 2
        sizes = {
            "plane": [(4, depth, half)] * 2 + [(4, depth // 2, half), (4, depth // 4, half), (3, depth // 4, half)],
            "z": [(4, depth, half)] * 2 + [(2, depth // 4, half), (2, depth // 8, half), (3, depth, half)],
            "block": [(depth, half), (2, depth // 4, half), (2, depth // 8, half)],
            "piece": [(depth // 4, half)],
        }[start]
        buffers += [pltpu.VMEM(size, jnp.bfloat16) for size in sizes]
    count = len(starts)
    return buffers + [
        pltpu.SemaphoreType.DMA((count, 3)),
        pltpu.SemaphoreType.DMA((count, 15)),
        pltpu.SemaphoreType.DMA((count, 15)),
    ]


def make_reducers(starts, grads, outs, scratch):
    items, at = [], 0
    for w, (start, grad, out) in enumerate(zip(starts, grads, outs)):
        size = {"plane": 5, "z": 5, "block": 3, "piece": 1}[start]
        items.append(Reducer(start, grad, out, scratch[at : at + size], scratch[-3:], w))
        at = at + size
    return items


def sum_by_table(local_grads):
    band_count, column_count = lax.axis_size("ty"), lax.axis_size("tx")
    group_count = lax.axis_size("rows")
    tile_count = band_count * column_count
    table = jnp.concatenate([entry.reshape(group_count, -1) for entry in local_grads], axis=1)
    column_total = table.shape[1]
    padded_columns = -(-column_total // tile_count) * tile_count
    piece_width = padded_columns // tile_count
    table = table.reshape(group_count, tile_count, piece_width)
    shares = lax.psum_scatter(
        table.reshape(group_count * tile_count, piece_width),
        ("rows", "ty", "tx"),
        scatter_dimension=0,
        tiled=True,
    )
    summed = (
        lax.all_gather(shares.astype(jnp.bfloat16), ("ty", "tx"), axis=0, tiled=True)
        .astype(shares.dtype)
        .reshape(-1)
    )
    totals = []
    start_at = 0
    for entry in local_grads:
        length = entry.size // group_count
        shard_shape = (entry.shape[0] // group_count,) + entry.shape[1:]
        totals.append(summed[start_at : start_at + length].reshape(shard_shape))
        start_at = start_at + length
    return tuple(totals)


def shards(
    latent,
    skip_input,
    segment_ids,
    embed_weight,
    embed_bias,
    skip_weight,
    skip_bias,
    norm1_gain,
    norm1_bias,
    qkv_weight,
    proj_weight,
    proj_bias,
    norm2_gain,
    norm2_bias,
    fc1_weight,
    fc1_bias,
    fc2_weight,
    fc2_bias,
    conv_weight,
    cotangent,
):
    row_count, tile_height, tile_width, width = skip_input.shape
    patch = latent.shape[3]
    tokens = tile_height * tile_width
    token_count = row_count * tokens
    low = jnp.bfloat16
    wide = jnp.float32
    cuts = jnp.stack(
        [jnp.sum(segment_ids[:, 0, :] == 0, axis=1), jnp.sum(segment_ids[:, :, -1] == 1, axis=1)],
        axis=1,
    ).astype(jnp.int32)
    vectors = jnp.stack(
        [embed_bias, skip_bias, norm1_gain, norm1_bias, proj_bias, norm2_gain, norm2_bias, fc2_bias]
    ).astype(wide)
    hidden_bias = fc1_bias.astype(wide).reshape(-1, 1, 512)
    conv_turned = conv_weight.T
    cot = cotangent.reshape(row_count, tokens, patch).transpose(0, 2, 1)
    flat_latent = latent.reshape(token_count, patch)
    flat_skip = skip_input.reshape(token_count, width)
    embedded, stream, normed, query, pairs = front(
        flat_latent, flat_skip, embed_weight, skip_weight, qkv_weight, vectors, row_count
    )
    attended, log_total, row_pairs, cot_tiles = attend(cuts, query, pairs, cot, tile_height, tile_width)
    (
        fc1_grad, fc2_grad, hidden_bias_grad, proj_grad, attended_grad, mid_grad, conv_in, spread, middle_grads
    ) = middle(
        cuts, attended.reshape(token_count, width), stream, cot_tiles, proj_weight, conv_turned, vectors,
        hidden_bias, fc1_weight, fc2_weight, tile_height, tile_width,
    )
    here = (lax.axis_size("rows"), lax.axis_size("ty"), lax.axis_size("tx")) == (4, 4, 2)

    def in_blocks(grads):
        return [entry.reshape(4, -1, entry.shape[1]) for entry in grads]

    early = [("plane", fc1_grad), ("z", fc2_grad), ("plane", proj_grad)] if here else []
    projected_grad, conv_grad, conv_out, *saved = attend_back(
        cuts, query, attended, attended_grad.reshape(row_count, tokens, width), log_total,
        conv_in, conv_turned, spread, row_pairs, list(zip([start for start, _ in early], in_blocks([g for _, g in early]))),
        tile_height, tile_width,
    )
    follow = {"plane": "piece", "z": "block"}
    resumed = [
        (follow[start], entry, (grad.shape[0] // 4, grad.shape[1])) for (start, grad), entry in zip(early, saved)
    ]
    skip_input_grad, *rest = rear(
        projected_grad.reshape(token_count, 3 * width), qkv_weight, normed, stream, mid_grad, embedded, flat_skip,
        skip_weight, flat_latent, vectors, middle_grads, hidden_bias_grad.reshape(4, -1), conv_grad, resumed, here,
    )
    output = conv_out.transpose(0, 2, 1).reshape(row_count, tile_height, tile_width, patch)
    skip_input_grad = skip_input_grad.reshape(row_count, tile_height, tile_width, width)
    taps = 9 * patch
    share = width // 4
    if here:
        fc1_total, fc2_total, proj_total, qkv_total, skip_total = [entry.astype(wide) for entry in rest[:5]]
        conv_total = rest[5][:, :taps].astype(wide)
        embed_total = rest[5][:, taps : taps + patch].astype(wide)
        line = [rest[6][k, :share].astype(wide) for k in range(8)]
        fc1_line = rest[6][8:11].reshape(-1).astype(wide)
        return (
            output, skip_input_grad, embed_total, line[0], skip_total, line[1], line[2], line[3], qkv_total,
            proj_total, line[4], line[5], line[6], fc1_total, fc1_line, fc2_total, line[7], conv_total,
        )
    qkv_grad, skip_grad, thin = [entry.reshape(-1, entry.shape[2]) for entry in rest[:3]]
    flat = rest[3]
    line = [flat[:, k, :share].reshape(-1) for k in range(8)]
    fc1_line = flat[:, 8:11].reshape(-1)
    local_grads = [
        thin[:, taps : taps + patch], line[0], skip_grad, line[1], line[2], line[3], qkv_grad, proj_grad, line[4],
        line[5], line[6], fc1_grad, fc1_line, fc2_grad, line[7], thin[:, :taps],
    ]
    return (output, skip_input_grad) + sum_by_table([entry.astype(wide) for entry in local_grads])


def solution(mesh):
    return jax.shard_map(
        shards,
        mesh=mesh,
        in_specs=(
            P("rows", "ty", "tx", None),
            P("rows", "ty", "tx", None),
            P("rows", None, None),
            P(),
            P(),
            P(),
            P(),
            P(),
            P(),
            P(),
            P(),
            P(),
            P(),
            P(),
            P(),
            P(),
            P(),
            P(),
            P(),
            P("rows", "ty", "tx", None),
        ),
        out_specs=(
            P("rows", "ty", "tx", None),
            P("rows", "ty", "tx", None),
            P("rows", None),
            P("rows"),
            P("rows", None),
            P("rows"),
            P("rows"),
            P("rows"),
            P("rows", None),
            P("rows", None),
            P("rows"),
            P("rows"),
            P("rows"),
            P("rows", None),
            P("rows"),
            P("rows", None),
            P("rows"),
            P("rows", None),
        ),
        check_vma=False,
    )
```

```python
import functools

import jax
import jax.numpy as jnp
from jax import lax
from jax.experimental import pallas as pl
from jax.experimental.pallas import tpu as pltpu
from jax.sharding import PartitionSpec as P

MESH = pl.DeviceIdType.MESH
norm_eps = 1e-05
full_vmem = 62 * 1024 * 1024


def cell_of(token, tile, tile_height, tile_width, columns):
    down = tile // columns * tile_height + token // tile_width
    across = tile % columns * tile_width + token % tile_width
    return down, across


def fill_shift(shift_ref, tile_height, tile_width):
    tokens = tile_height * tile_width
    bands, columns = lax.axis_size("ty"), lax.axis_size("tx")
    own = lax.axis_index("ty") * columns + lax.axis_index("tx")
    lane = lax.broadcasted_iota(jnp.int32, (8, tokens), 1)
    down, across = cell_of(lane, own, tile_height, tile_width, columns)
    step = lax.broadcasted_iota(jnp.int32, (shift_ref.shape[0], tokens), 0)
    for p in range(9):
        i, j = down - (p // 3 - 1), across - (p % 3 - 1)
        inside = (i >= 0) & (i < bands * tile_height) & (j >= 0) & (j < columns * tile_width)
        tile = i // tile_height * columns + j // tile_width
        place = tile * tokens + i % tile_height * tile_width + j % tile_width
        place = jnp.where(inside, place, -1)[0:1]
        chosen = jnp.where(step == place, 1.0, 0.0)
        shift_ref[:, p * tokens : (p + 1) * tokens] = chosen.astype(jnp.bfloat16)


def same_image(cuts_ref, row, p, tile_height, tile_width):
    tokens = tile_height * tile_width
    columns = lax.axis_size("tx")
    own = lax.axis_index("ty") * columns + lax.axis_index("tx")
    lane = lax.broadcasted_iota(jnp.int32, (8, tokens), 1)
    down, across = cell_of(lane, own, tile_height, tile_width, columns)
    left_width, top_height = cuts_ref[row, 0], cuts_ref[row, 1]

    def image_of(i, j):
        return jnp.where(j < left_width, 0, jnp.where(i < top_height, 1, 2))

    there = image_of(down - (p // 3 - 1), across - (p % 3 - 1))
    return jnp.where(image_of(down, across) == there, 1.0, 0.0)[0:1]


def mm(former, latter, axis_former, axis_latter):
    return lax.dot_general(
        former,
        latter,
        (((axis_former,), (axis_latter,)), ((), ())),
        preferred_element_type=jnp.float32,
    )


def normalised(values):
    average = jnp.mean(values, axis=1, keepdims=True)
    centred = values - average
    rate = lax.rsqrt(jnp.mean(centred * centred, axis=1, keepdims=True) + norm_eps)
    return centred * rate, rate


def norm_back(incoming, unit, rate, gain):
    scaled = incoming * gain
    first = jnp.mean(scaled, axis=1, keepdims=True)
    second = jnp.mean(scaled * unit, axis=1, keepdims=True)
    return (scaled - first - unit * second) * rate


def down_sum(values):
    return jnp.sum(values, axis=0, keepdims=True)


def front_kernel(
    segment_ids, latent, cotangent, embed_turned, *refs
):
    biases, fc1_bias, refs = refs[:8], refs[8], refs[9:]
    skip_in, skip_weight_in, qkv_in, embedded, stream, normed, query, pairs, cot, vectors, hidden_bias, cuts = refs[:12]
    skip, skip_weight, qkv_weight, load_sem = refs[12:]
    sources, targets = (skip_weight_in, skip_in, qkv_in), (skip_weight, skip, qkv_weight)
    loads = [pltpu.make_async_copy(a, b, load_sem.at[k]) for k, (a, b) in enumerate(zip(sources, targets))]
    for load in loads:
        load.start()
    for k, bias in enumerate(biases):
        vectors[k : k + 1] = bias[...].reshape(1, bias.shape[0]).astype(jnp.float32)
    line = fc1_bias[...].reshape(1, fc1_bias.shape[0]).astype(jnp.float32)
    block = hidden_bias.shape[2]
    for k in range(hidden_bias.shape[0]):
        hidden_bias[k] = line[:, k * block : (k + 1) * block]
    width = skip.shape[1]
    row_count, tokens = query.shape[0], query.shape[1]
    side = segment_ids.shape[1]
    for row in range(row_count):

        def count(k, carry):
            left, top = carry
            left = left + jnp.where(segment_ids[row, 0, k] == 0, 1, 0)
            top = top + jnp.where(segment_ids[row, k, side - 1] == 1, 1, 0)
            return left, top

        left, top = lax.fori_loop(0, side, count, (jnp.int32(0), jnp.int32(0)), unroll=8)
        cuts[row, 0] = left
        cuts[row, 1] = top
        at = slice(row * tokens, (row + 1) * tokens)
        cot[row] = jnp.transpose(cotangent[at, :].astype(jnp.float32)).astype(jnp.bfloat16)
        embedded[at, :] = (mm(latent[at, :], embed_turned[...], 1, 0) + vectors[0:1]).astype(jnp.bfloat16)
    loads[0].wait()
    loads[1].wait()
    for row in range(row_count):
        at = slice(row * tokens, (row + 1) * tokens)
        total = mm(embedded[at, :], skip_weight[:width], 1, 0) + mm(skip[at, :], skip_weight[width:], 1, 0) + vectors[1:2]
        stream[at, :] = total
        unit, rate = normalised(total)
        normed[at, :] = (unit * vectors[2:3] + vectors[3:4]).astype(jnp.bfloat16)
    loads[2].wait()
    for row in range(row_count):
        low = normed[row * tokens : (row + 1) * tokens, :]
        pairs[row] = mm(low, qkv_weight[:, width:], 1, 0).astype(jnp.bfloat16)
        query[row] = mm(low, qkv_weight[:, :width], 1, 0).astype(jnp.bfloat16)


def front(segment_ids, latent, cotangent, embed_turned, biases, fc1_bias, skip, skip_weight, qkv_weight, row_count):
    token_count, width = skip.shape
    tokens = token_count // row_count
    low, wide = jnp.bfloat16, jnp.float32
    smem, vmem = pl.BlockSpec(memory_space=pltpu.SMEM), pl.BlockSpec(memory_space=pltpu.VMEM)
    return pl.pallas_call(
        front_kernel,
        out_shape=[
            jax.ShapeDtypeStruct((token_count, width), low),
            jax.ShapeDtypeStruct((token_count, width), wide),
            jax.ShapeDtypeStruct((token_count, width), low),
            jax.ShapeDtypeStruct((row_count, tokens, width), low),
            jax.ShapeDtypeStruct((row_count, tokens, 2 * width), low),
            jax.ShapeDtypeStruct((row_count, cotangent.shape[1], tokens), low),
            jax.ShapeDtypeStruct((8, width), wide),
            jax.ShapeDtypeStruct((fc1_bias.shape[0] // 512, 1, 512), wide),
            jax.ShapeDtypeStruct((row_count, 2), jnp.int32),
        ],
        in_specs=[smem] + [vmem] * 12 + [pl.BlockSpec(memory_space=pl.ANY)] * 3,
        out_specs=[vmem] * 8 + [smem],
        scratch_shapes=[pltpu.VMEM(entry.shape, low) for entry in (skip, skip_weight, qkv_weight)]
        + [pltpu.SemaphoreType.DMA((3,))],
        compiler_params=pltpu.CompilerParams(vmem_limit_bytes=full_vmem),
        name="front",
    )(segment_ids, latent, cotangent, embed_turned, *biases, fc1_bias, skip, skip_weight, qkv_weight)


def erf_of(values):
    x = jnp.clip(values, -4.0, 4.0)
    square = x * x
    upper = square * -2.72614225801306e-10 + 2.77068142495902e-08
    for term in (-2.10102402082508e-06, -5.69250639462346e-05, -7.34990630326855e-04, -2.95459980854025e-03, -1.60960333262415e-02):
        upper = upper * square + term
    lower = square * -1.45660718464996e-05 + -2.13374055278905e-04
    for term in (-1.68282697438203e-03, -7.37332916720468e-03, -1.42647390514189e-02):
        lower = lower * square + term
    return x * upper / lower


def middle_kernel(
    tile_height, tile_width,
    cuts, attended, stream, cot_tiles, proj_weight, conv_turned, vectors, hidden_bias, fc1_weight, fc2_weight,
    fc1_grad, fc2_grad, hidden_bias_grad, proj_grad, attended_grad, mid_grad, conv_in, spread, vector_grads,
    middle, normed, out_grad, out_low, forward_sum, backward_sum, shift,
):
    step = pl.program_id(0)
    row_count, tokens = cot_tiles.shape[1], cot_tiles.shape[3]
    token_count = row_count * tokens
    low = jnp.bfloat16
    parts = [slice(k * tokens, (k + 1) * tokens) for k in range(row_count)]

    @pl.when(step == 0)
    def _():
        fill_shift(shift, tile_height, tile_width)
        tile_count = cot_tiles.shape[0]
        patch = cot_tiles.shape[2]
        turned = jnp.concatenate(
            [cot_tiles[t].reshape(row_count * patch, tokens) for t in range(tile_count)], axis=1
        )
        moved = mm(turned, shift[...], 1, 0)
        for row in range(row_count):
            for p in range(9):
                piece = moved[row * patch : (row + 1) * patch, p * tokens : (p + 1) * tokens]
                piece = piece * same_image(cuts, row, p, tile_height, tile_width)
                spread[p * patch : (p + 1) * patch, parts[row]] = piece.astype(low)
        total = jnp.zeros((1, stream.shape[1]), jnp.float32)
        for at in parts:
            grad = mm(spread[:, at], conv_turned[...], 0, 0)
            out_grad[at, :] = grad
            out_low[at, :] = grad.astype(low)
            total = total + down_sum(grad)
            value = stream[at, :] + mm(attended[at, :], proj_weight[...], 1, 0) + vectors[4:5]
            middle[at, :] = value
            unit, rate = normalised(value)
            normed[at, :] = (unit * vectors[5:6] + vectors[6:7]).astype(low)
        vector_grads[7:8] = total
        forward_sum[...] = jnp.zeros_like(forward_sum)
        backward_sum[...] = jnp.zeros_like(backward_sum)

    bias_grad = jnp.zeros((1, fc1_weight.shape[1]), jnp.float32)
    actives, hidden_lows = [], []
    for at in parts:
        hidden = mm(normed[at, :], fc1_weight[...], 1, 0) + hidden_bias[0]
        active_grad = mm(out_low[at, :], fc2_weight[...], 1, 1)
        share = 0.5 + 0.5 * erf_of(hidden * 0.7071067811865476)
        density = jnp.exp(hidden * hidden * -0.5) * 0.3989422804014327
        active = (hidden * share).astype(low)
        hidden_grad = active_grad * (share + hidden * density)
        bias_grad = bias_grad + down_sum(hidden_grad)
        hidden_low = hidden_grad.astype(low)
        forward_sum[at, :] = forward_sum[at, :] + mm(active, fc2_weight[...], 1, 0)
        backward_sum[at, :] = backward_sum[at, :] + mm(hidden_low, fc1_weight[...], 1, 1)
        actives.append(active)
        hidden_lows.append(hidden_low)
    hidden_bias_grad[0] = bias_grad
    fc2_grad[...] = mm(jnp.concatenate(actives, axis=0), out_low[...], 0, 0).astype(low)
    fc1_grad[...] = mm(normed[...], jnp.concatenate(hidden_lows, axis=0), 0, 0).astype(low)

    @pl.when(step == pl.num_programs(0) - 1)
    def _():
        width = stream.shape[1]
        gain_sum = jnp.zeros((1, width), jnp.float32)
        bias_sum = jnp.zeros((1, width), jnp.float32)
        mid_sum = jnp.zeros((1, width), jnp.float32)
        lows = []
        for at in parts:
            unit, rate = normalised(middle[at, :])
            conv_in[at, :] = (middle[at, :] + forward_sum[at, :] + vectors[7:8]).astype(low)
            incoming = backward_sum[at, :]
            gain_sum = gain_sum + down_sum(incoming * unit)
            bias_sum = bias_sum + down_sum(incoming)
            grad = out_grad[at, :] + norm_back(incoming, unit, rate, vectors[5:6])
            mid_grad[at, :] = grad
            mid_sum = mid_sum + down_sum(grad)
            mid_low = grad.astype(low)
            lows.append(mid_low)
            attended_grad[at, :] = mm(mid_low, proj_weight[...], 1, 1).astype(low)
        proj_grad[...] = mm(attended[...], jnp.concatenate(lows, axis=0), 0, 0).astype(low)
        vector_grads[4:5] = mid_sum
        vector_grads[5:6] = gain_sum
        vector_grads[6:7] = bias_sum


def middle(cuts, attended, stream, cot_tiles, proj_weight, conv_turned, vectors, hidden_bias, fc1_weight, fc2_weight, tile_height, tile_width):
    token_count, width = stream.shape
    hidden_width = fc1_weight.shape[1]
    block = 512
    steps = hidden_width // block
    low = jnp.bfloat16
    vmem = pl.BlockSpec(memory_space=pltpu.VMEM)
    tile_count, tokens = cot_tiles.shape[0], cot_tiles.shape[3]
    taps = conv_turned.shape[0]
    return pl.pallas_call(
        functools.partial(middle_kernel, tile_height, tile_width),
        grid=(steps,),
        out_shape=[
            jax.ShapeDtypeStruct((width, hidden_width), low),
            jax.ShapeDtypeStruct((hidden_width, width), low),
            jax.ShapeDtypeStruct((steps, 1, block), jnp.float32),
            jax.ShapeDtypeStruct((width, width), low),
            jax.ShapeDtypeStruct((token_count, width), low),
            jax.ShapeDtypeStruct((token_count, width), jnp.float32),
            jax.ShapeDtypeStruct((token_count, width), low),
            jax.ShapeDtypeStruct((taps, token_count), low),
            jax.ShapeDtypeStruct((8, width), jnp.float32),
        ],
        in_specs=[pl.BlockSpec(memory_space=pltpu.SMEM)]
        + [vmem] * 6
        + [
            pl.BlockSpec((1, 1, block), lambda k: (k, 0, 0)),
            pl.BlockSpec((width, block), lambda k: (0, k)),
            pl.BlockSpec((block, width), lambda k: (k, 0)),
        ],
        out_specs=[
            pl.BlockSpec((width, block), lambda k: (0, k)),
            pl.BlockSpec((block, width), lambda k: (k, 0)),
            pl.BlockSpec((1, 1, block), lambda k: (k, 0, 0)),
        ]
        + [vmem] * 6,
        scratch_shapes=[
            pltpu.VMEM((token_count, width), jnp.float32),
            pltpu.VMEM((token_count, width), low),
            pltpu.VMEM((token_count, width), jnp.float32),
            pltpu.VMEM((token_count, width), low),
            pltpu.VMEM((token_count, width), jnp.float32),
            pltpu.VMEM((token_count, width), jnp.float32),
            pltpu.VMEM((tile_count * tokens, 9 * tokens), low),
        ],
        compiler_params=pltpu.CompilerParams(vmem_limit_bytes=full_vmem),
        name="middle",
    )(cuts, attended, stream, cot_tiles, proj_weight, conv_turned, vectors, hidden_bias, fc1_weight, fc2_weight)


def rear_kernel(
    starts, reduces, projected_in, qkv_in, normed_in, stream_in, mid_in, embedded_in, skip_in, skip_weight_in,
    latent, vectors, middle_grads, hidden_bias_grad, conv_grad, *refs
):
    count = len(starts)
    resumed, refs = refs[:count], refs[count:]
    skip_input_grad, refs = refs[0], refs[1:]
    if reduces:
        sums, refs = refs[: count + 4], refs[count + 4 :]
        peers = chip_peers()
    qkv_grad, skip_grad, thin, flat, refs = *refs[:4], refs[4:]
    projected_grad, qkv_weight, normed, stream, mid_grad, embedded, skip, skip_weight, stream_low, load_sem = refs[:10]
    sources = (projected_in, normed_in, qkv_in, stream_in, mid_in, embedded_in, skip_in, skip_weight_in)
    targets = (projected_grad, normed, qkv_weight, stream, mid_grad, embedded, skip, skip_weight)
    loads = [pltpu.make_async_copy(a, b, load_sem.at[k]) for k, (a, b) in enumerate(zip(sources, targets))]
    for load in loads[:3]:
        load.start()
    later, news = [], []
    if reduces:
        items = make_reducers(
            starts + ("plane",) * 4, resumed + (qkv_grad, skip_grad, thin, flat), sums, refs[10:]
        )
        later, news = items[:count], items[count:]
        greet([peers[name] for name in ("core", "x", "y", "xy")] + peers["z"])
    for item in later:
        item.begin()
    for load in loads[3:]:
        load.start()
    for item in later:
        item.stages.pop(0)()
    token_count, width = stream.shape
    low = jnp.bfloat16
    tokens = 128
    parts = [slice(k * tokens, (k + 1) * tokens) for k in range(token_count // tokens)]
    zero = jnp.zeros((1, width), jnp.float32)
    gain_sum, bias_sum, stream_sum, embed_sum = zero, zero, zero, zero
    loads[0].wait()
    loads[1].wait()
    blocks, depth = qkv_grad.shape[0], qkv_grad.shape[1]
    for k in range(3):
        at = slice(k * width, (k + 1) * width)
        qkv_grad[:, :, at] = mm(normed[...], projected_grad[:, at], 0, 0).astype(low).reshape(blocks, depth, width)

    def open_up(which):
        for item in news[which]:
            item.begin()

    def step_on(group):
        for item in group:
            if item.stages:
                item.stages.pop(0)()

    open_up(slice(0, 1))
    for load in loads[2:5]:
        load.wait()
    for at in parts:
        incoming = mm(projected_grad[at, :], qkv_weight[...], 1, 1)
        unit, rate = normalised(stream[at, :])
        gain_sum = gain_sum + down_sum(incoming * unit)
        bias_sum = bias_sum + down_sum(incoming)
        grad = mid_grad[at, :] + norm_back(incoming, unit, rate, vectors[2:3])
        stream_sum = stream_sum + down_sum(grad)
        stream_low[at, :] = grad.astype(low)
    step_on(news[0:1])
    loads[5].wait()
    loads[6].wait()
    skip_grad[0:2] = mm(embedded[...], stream_low[...], 0, 0).astype(low).reshape(2, width // 2, width)
    skip_grad[2:4] = mm(skip[...], stream_low[...], 0, 0).astype(low).reshape(2, width // 2, width)
    open_up(slice(1, 2))
    loads[7].wait()
    embed_lows = []
    for at in parts:
        embed_grad = mm(stream_low[at, :], skip_weight[:width], 1, 1)
        embed_sum = embed_sum + down_sum(embed_grad)
        embed_lows.append(embed_grad.astype(low))
    embed_weight_grad = mm(jnp.concatenate(embed_lows, axis=0), latent[...], 0, 0)
    step_on(news[1:2])
    rest = jnp.zeros((width, 128 - 2 * 16), jnp.float32)
    thin[:, :, :128] = conv_grad[:, :128].astype(low).reshape(4, width // 4, 128)
    edge = jnp.concatenate([conv_grad[:, 128:144], embed_weight_grad, rest], axis=1)
    thin[:, :, 128:] = edge.astype(low).reshape(4, width // 4, 128)
    rows = [embed_sum, stream_sum, gain_sum, bias_sum] + [middle_grads[k : k + 1] for k in range(4, 8)]
    stack = jnp.concatenate(rows, axis=0)
    share = width // 4
    hidden_line = jnp.concatenate([hidden_bias_grad[k] for k in range(hidden_bias_grad.shape[0])], axis=1)
    for block in range(4):
        own = stack[:, block * share : (block + 1) * share]
        own = jnp.concatenate([own, jnp.zeros((8, 256 - share), jnp.float32)], axis=1)
        line = hidden_line[:, block * width : (block + 1) * width]
        pieces = [line[:, k * 256 : (k + 1) * 256] for k in range(width // 256)]
        body = jnp.concatenate([own] + pieces + [jnp.zeros((8 - len(pieces), 256), jnp.float32)], axis=0)
        flat[block, 0:16] = body.astype(low)
        flat[block, 16:64] = jnp.zeros((48, 256), low)
    open_up(slice(2, 4))
    step_on(later)
    step_on(news[0:1])
    for at in parts:
        skip_input_grad[at, :] = mm(stream_low[at, :], skip_weight[width:], 1, 1).astype(low)
    step_on(news[2:4])
    while any(item.stages for item in later + news):
        step_on(later)
        step_on(news)


def rear(projected_grad, qkv_weight, normed, stream, mid_grad, embedded, skip, skip_weight, latent, vectors, middle_grads, hidden_bias_grad, conv_grad, resumed, reduces):
    token_count, width = stream.shape
    low = jnp.bfloat16
    starts = tuple(start for start, _, _ in resumed)
    sizes = [(width // 4, 3 * width), (width // 2, width), (width // 4, 256), (64, 256)]
    totals = [shape for _, _, shape in resumed] + sizes
    vmem, anywhere = pl.BlockSpec(memory_space=pltpu.VMEM), pl.BlockSpec(memory_space=pl.ANY)
    big = [projected_grad, qkv_weight, normed, stream, mid_grad, embedded, skip, skip_weight]
    out_shape = [jax.ShapeDtypeStruct((token_count, width), low)]
    out_specs = [vmem]
    scratch = []
    if reduces:
        out_shape += [jax.ShapeDtypeStruct(shape, low) for shape in totals]
        out_specs += [anywhere] * len(totals)
        scratch += [pltpu.VMEM((4,) + shape, low) for shape in sizes]
        params = pltpu.CompilerParams(collective_id=3, has_side_effects=True, vmem_limit_bytes=full_vmem)
    else:
        out_shape += [jax.ShapeDtypeStruct((4,) + shape, low) for shape in sizes]
        out_specs += [vmem] * len(sizes)
        params = pltpu.CompilerParams(vmem_limit_bytes=full_vmem)
    scratch += [pltpu.VMEM(entry.shape, entry.dtype) for entry in big]
    scratch += [pltpu.VMEM((token_count, width), low), pltpu.SemaphoreType.DMA((len(big),))]
    if reduces:
        scratch += reducer_scratch(starts + ("plane",) * 4, totals)
    return pl.pallas_call(
        functools.partial(rear_kernel, starts, reduces),
        out_shape=out_shape,
        in_specs=[anywhere] * len(big) + [vmem] * 5 + [anywhere] * len(starts),
        out_specs=out_specs,
        scratch_shapes=scratch,
        compiler_params=params,
        name="rear",
    )(*big, latent, vectors, middle_grads, hidden_bias_grad, conv_grad, *[entry for _, entry, _ in resumed])


def finish_kernel(patch, *refs):
    sums, (thin, flat, conv_out) = refs[:5], refs[5:8]
    totals, (embed_turned, conv_turned), refs = refs[8:13], refs[13:15], refs[15:]
    lines, fc1_line, output, refs = refs[:8], refs[8], refs[9], refs[10:]
    lows, wides, load_sem, store_sem = refs[:5], refs[5:10], refs[10], refs[11]
    loads = [pltpu.make_async_copy(a, b, load_sem.at[k]) for k, (a, b) in enumerate(zip(sums, lows))]
    for load in loads:
        load.start()
    share = thin.shape[0]
    turned = jnp.transpose(thin[...].astype(jnp.float32))
    taps = 9 * patch
    conv_turned[...] = turned[:taps]
    embed_turned[...] = turned[taps : taps + patch]
    rows = flat[0:16, :].astype(jnp.float32)
    for k, line in enumerate(lines):
        line[...] = rows[k : k + 1, :share].reshape(share)
    fc1_line[...] = jnp.concatenate([rows[k : k + 1] for k in range(8, 11)], axis=1).reshape(fc1_line.shape[0])
    for row in range(output.shape[0]):
        output[row] = jnp.transpose(conv_out[row].astype(jnp.float32)).astype(jnp.bfloat16)
    stores = []
    for k, (low, wide) in enumerate(zip(lows, wides)):
        loads[k].wait()

        def body(i, carry):
            at = pl.ds(pl.multiple_of(i * 16, 16), 16)
            wide[at, :] = low[at, :].astype(jnp.float32)
            return carry

        lax.fori_loop(0, low.shape[0] // 16, body, 0, unroll=2)
        store = pltpu.make_async_copy(wide, totals[k], store_sem.at[k])
        store.start()
        stores.append(store)
    for store in stores:
        store.wait()


def finish(sums, thin, flat, conv_out):
    row_count, patch, tokens = conv_out.shape
    share = thin.shape[0]
    wide = jnp.float32
    vmem, anywhere = pl.BlockSpec(memory_space=pltpu.VMEM), pl.BlockSpec(memory_space=pl.ANY)
    return pl.pallas_call(
        functools.partial(finish_kernel, patch),
        out_shape=[jax.ShapeDtypeStruct(entry.shape, wide) for entry in sums]
        + [jax.ShapeDtypeStruct((patch, share), wide), jax.ShapeDtypeStruct((9 * patch, share), wide)]
        + [jax.ShapeDtypeStruct((share,), wide)] * 8
        + [jax.ShapeDtypeStruct((4 * share,), wide), jax.ShapeDtypeStruct((row_count, tokens, patch), jnp.bfloat16)],
        in_specs=[anywhere] * 5 + [vmem] * 3,
        out_specs=[anywhere] * 5 + [vmem] * 12,
        scratch_shapes=[pltpu.VMEM(entry.shape, jnp.bfloat16) for entry in sums]
        + [pltpu.VMEM(entry.shape, wide) for entry in sums]
        + [pltpu.SemaphoreType.DMA((5,)), pltpu.SemaphoreType.DMA((5,))],
        compiler_params=pltpu.CompilerParams(vmem_limit_bytes=full_vmem),
        name="finish",
    )(*sums, thin, flat, conv_out)


def plane_peers():
    z, ty, y = lax.axis_index("rows"), lax.axis_index("ty"), lax.axis_index("tx")
    core, x = lax.rem(ty, 2), ty // 2
    here = x * 2 + core
    across = (1 - x) * 2 + core
    tiles = {
        "own": here * 2 + y,
        "x": across * 2 + y,
        "y": here * 2 + 1 - y,
        "xy": across * 2 + 1 - y,
    }
    peers = {
        "core": (z, x * 2 + 1 - core, y),
        "x": (z, across, y),
        "y": (z, here, 1 - y),
    }
    return tiles, peers


def plane_peer(k):
    z, ty, y = lax.axis_index("rows"), lax.axis_index("ty"), lax.axis_index("tx")
    x, core = ty // 2, lax.rem(ty, 2)
    flip_x, flip_core, flip_y = k // 4, k // 2 % 2, k % 2
    x = x + flip_x - 2 * flip_x * x
    core = core + flip_core - 2 * flip_core * core
    y = y + flip_y - 2 * flip_y * y
    return (z, x * 2 + core, y), (x * 2 + core) * 2 + y


def greet(peers):
    barrier = pltpu.get_barrier_semaphore()
    for peer in peers:
        pl.semaphore_signal(barrier, inc=1, device_id=peer, device_id_type=MESH)
    pl.semaphore_wait(barrier, len(peers))


def fill_mask(mask_ref, cuts_ref, row, tile_height, tile_width):
    ty, tx = lax.axis_index("ty"), lax.axis_index("tx")
    columns = lax.axis_size("tx")
    tokens = tile_height * tile_width
    left_width = cuts_ref[row, 0]
    top_height = cuts_ref[row, 1]

    def image_of(down, across):
        return jnp.where(across < left_width, 0, jnp.where(down < top_height, 1, 2))

    lane = lax.broadcasted_iota(jnp.int32, (tokens, tokens), 1)
    step = lax.broadcasted_iota(jnp.int32, (tokens, tokens), 0)
    mine = image_of(
        ty * tile_height + lane // tile_width, tx * tile_width + lane % tile_width
    )
    for tile in range(mask_ref.shape[0] // tokens):
        theirs = image_of(
            tile // columns * tile_height + step // tile_width,
            tile % columns * tile_width + step % tile_width,
        )
        mask_ref[tile * tokens : (tile + 1) * tokens, :] = jnp.where(
            mine == theirs, 0.0, -1e30
        )


def two_heads(pair, scale):
    lane = lax.broadcasted_iota(jnp.int32, pair.shape, 1)
    wide = pair.astype(jnp.float32) * scale
    first = jnp.where(lane < pair.shape[1] // 2, wide, 0.0)
    return jnp.concatenate([first, wide - first], axis=0).astype(jnp.bfloat16)


def own_blocks(both):
    head, tokens = both.shape[0] // 2, both.shape[1] // 2
    return jnp.concatenate([both[:head, :tokens], both[head:, tokens:]], axis=0)


def attend_kernel(
    tile_height, tile_width, cuts, query, pairs, cot, out, lse, all_out, cot_out, held, scores, mask, local_sem, send_sem, recv_sem,
    cot_sem, cot_send_sem, cot_recv_sem
):
    row_count, tokens, width = query.shape
    tile_count = held.shape[1]
    pair_count = width // 128
    tiles, peers = plane_peers()
    own = tiles["own"]
    greet([plane_peer(k)[0] for k in range(1, tile_count)])
    cot_copies = [pltpu.make_async_copy(cot, cot_out.at[own], cot_sem.at[0])]
    for k in range(1, tile_count):
        cot_copies.append(
            pltpu.make_async_remote_copy(
                src_ref=cot,
                dst_ref=cot_out.at[own],
                send_sem=cot_send_sem.at[k],
                recv_sem=cot_recv_sem.at[k],
                device_id=plane_peer(k)[0],
                device_id_type=MESH,
            )
        )

    def send(row, slot, source, target, peer):
        copy = pltpu.make_async_remote_copy(
            src_ref=source,
            dst_ref=target,
            send_sem=send_sem.at[row, slot],
            recv_sem=recv_sem.at[row, slot],
            device_id=peer,
            device_id_type=MESH,
        )
        copy.start()
        return copy

    flights = [{} for _ in range(row_count)]

    def begin(row):
        here = held.at[row, own]
        source = pairs.at[row]
        flights[row]["x"] = send(row, 0, source, here, peers["x"])
        flights[row]["y"] = send(row, 1, source, here, peers["y"])
        flights[row]["core"] = send(row, 2, source, here, peers["core"])
        keep = pltpu.make_async_copy(source, here, local_sem.at[row, 0])
        keep.start()
        flights[row]["keep"] = keep

    def forward(row):
        flights[row]["y"].wait_recv()
        key_half = held.at[row, tiles["y"], :, pl.ds(0, width)]
        flights[row]["far_x"] = send(row, 3, key_half, key_half, peers["x"])
        flights[row]["x"].wait_recv()
        value_half = held.at[row, tiles["x"], :, pl.ds(width, width)]
        flights[row]["far_y"] = send(row, 4, value_half, value_half, peers["y"])
        for slot, name in ((5, "x"), (6, "y")):
            tile = held.at[row, tiles[name]]
            flights[row]["core_" + name] = send(row, slot, tile, tile, peers["core"])

    def finish(row):
        flights[row]["far_x"].wait_recv()
        flights[row]["far_y"].wait_recv()
        tile = held.at[row, tiles["xy"]]
        last = send(row, 7, tile, tile, peers["core"])
        flights[row]["keep"].wait()
        for name in ("core", "core_x", "core_y"):
            flights[row][name].wait_recv()
        last.wait_recv()
        for name in ("x", "y", "core", "far_x", "far_y", "core_x", "core_y"):
            flights[row][name].wait_send()
        last.wait_send()
        keep = pltpu.make_async_copy(held.at[row], all_out.at[row], local_sem.at[row, 1])
        keep.start()
        flights[row]["out"] = keep

    chunk = 2

    def compute(row):
        fill_mask(mask, cuts, row, tile_height, tile_width)

        def one_pair(p, carry):
            at = pl.ds(pl.multiple_of(p * 128, 128), 128)
            at_value = pl.ds(pl.multiple_of(width + p * 128, 128), 128)
            both = two_heads(query[row, :, at], 0.125)
            peak = None
            for c in range(tile_count // chunk):
                span = slice(c * chunk * tokens, (c + 1) * chunk * tokens)
                keys = held[row, c * chunk : (c + 1) * chunk, :, at].reshape(chunk * tokens, 128)
                extra = mask[span, :]
                part = mm(keys, both, 1, 1) + jnp.concatenate([extra, extra], axis=1)
                scores[span, :] = part
                top = jnp.max(part, axis=0, keepdims=True)
                peak = top if peak is None else jnp.maximum(peak, top)
            total = jnp.zeros_like(peak)
            summed = jnp.zeros((128, 2 * tokens), jnp.float32)
            for c in range(tile_count // chunk):
                span = slice(c * chunk * tokens, (c + 1) * chunk * tokens)
                values = held[row, c * chunk : (c + 1) * chunk, :, at_value].reshape(chunk * tokens, 128)
                part = jnp.exp(scores[span, :] - peak)
                total = total + jnp.sum(part, axis=0, keepdims=True)
                summed = summed + mm(values, part.astype(jnp.bfloat16), 0, 0)
            blocks = own_blocks(summed / total)
            out[row, :, at] = jnp.transpose(blocks).astype(jnp.bfloat16)
            lse[row, p] = peak + jnp.log(total)
            return carry

        lax.fori_loop(0, pair_count, one_pair, 0, unroll=3)

    begin(0)
    if row_count > 1:
        begin(1)
    for copy in cot_copies:
        copy.start()
    forward(0)
    for row in range(row_count):
        if row + 2 < row_count:
            begin(row + 2)
        if row + 1 < row_count:
            forward(row + 1)
        finish(row)
        compute(row)
    for row in range(row_count):
        flights[row]["out"].wait()
    for copy in cot_copies:
        copy.wait()


def attend(cuts, query, pairs, cot, tile_height, tile_width):
    row_count, tokens, width = query.shape
    tile_count = lax.axis_size("ty") * lax.axis_size("tx")
    pair_count = width // 128
    low = jnp.bfloat16
    vmem = pl.BlockSpec(memory_space=pltpu.VMEM)
    return pl.pallas_call(
        functools.partial(attend_kernel, tile_height, tile_width),
        out_shape=[
            jax.ShapeDtypeStruct((row_count, tokens, width), low),
            jax.ShapeDtypeStruct((row_count, pair_count, 1, 2 * tokens), jnp.float32),
            jax.ShapeDtypeStruct((row_count, tile_count, tokens, 2 * width), low),
            jax.ShapeDtypeStruct((tile_count,) + cot.shape, low),
        ],
        in_specs=[pl.BlockSpec(memory_space=pltpu.SMEM), vmem] + [pl.BlockSpec(memory_space=pl.ANY)] * 2,
        out_specs=[vmem, vmem] + [pl.BlockSpec(memory_space=pl.ANY)] * 2,
        scratch_shapes=[
            pltpu.VMEM((row_count, tile_count, tokens, 2 * width), low),
            pltpu.VMEM((tile_count * tokens, 2 * tokens), jnp.float32),
            pltpu.VMEM((tile_count * tokens, tokens), jnp.float32),
            pltpu.SemaphoreType.DMA((row_count, 2)),
            pltpu.SemaphoreType.DMA((row_count, 8)),
            pltpu.SemaphoreType.DMA((row_count, 8)),
            pltpu.SemaphoreType.DMA((1,)),
            pltpu.SemaphoreType.DMA((tile_count,)),
            pltpu.SemaphoreType.DMA((tile_count,)),
        ],
        compiler_params=pltpu.CompilerParams(
            collective_id=1, has_side_effects=True, vmem_limit_bytes=full_vmem
        ),
        name="attend",
    )(cuts, query, pairs, cot)


def attend_back_kernel(
    tile_height, tile_width, starts, cuts, query_in, attended_in, grad_in, lse_in, conv_in, conv_turned, spread, all_pairs, *refs
):
    count = len(starts)
    grads, refs = refs[:count], refs[count:]
    (out, conv_grad, conv_out), saved, refs = refs[:3], refs[3 : 3 + count], refs[3 + count :]
    query, attended, grad, lse, row_sem = refs[:5]
    refs = refs[5:]
    held, terms, core_terms, side_terms, mask, shift, taps, part, part_got = refs[:9]
    load_sem, send_sem, recv_sem, part_send_sem, part_recv_sem = refs[9:14]
    items = make_reducers(starts, grads, saved, refs[14:]) if count else []
    firsts = [item for item in items if item.start == "z"]
    planes = [item for item in items if item.start == "plane"]

    row_count, tokens, width = query.shape
    tile_count = held.shape[1]
    pair_count = width // 128
    tiles, peers = plane_peers()
    low = jnp.bfloat16
    loads = []
    for row in range(row_count):
        load = pltpu.make_async_copy(all_pairs.at[row], held.at[row], load_sem.at[row])
        load.start()
        loads.append([load])
        for k, (source, target) in enumerate(((query_in, query), (attended_in, attended), (grad_in, grad), (lse_in, lse))):
            load = pltpu.make_async_copy(source.at[row], target.at[row], row_sem.at[row, k])
            load.start()
            loads[-1].append(load)
    greet([plane_peer(k)[0] for k in range(1, tile_count)] + (chip_peers()["z"] if count else []))
    core = lax.rem(lax.axis_index("ty"), 2)
    chunk = 2

    def send(row, slot, source, target, peer):
        copy = pltpu.make_async_remote_copy(
            src_ref=source,
            dst_ref=target,
            send_sem=send_sem.at[row, slot],
            recv_sem=recv_sem.at[row, slot],
            device_id=peer,
            device_id_type=MESH,
        )
        copy.start()
        return copy

    def compute(row):
        for load in loads[row]:
            load.wait()
        fill_mask(mask, cuts, row, tile_height, tile_width)

        def one_pair(p, carry):
            at = pl.ds(pl.multiple_of(p * 128, 128), 128)
            at_value = pl.ds(pl.multiple_of(width + p * 128, 128), 128)
            grad_pair = grad[row, :, at]
            both = two_heads(query[row, :, at], 0.125)
            both_grad = two_heads(grad_pair, 1.0)
            inner = jnp.transpose(grad_pair.astype(jnp.float32) * attended[row, :, at].astype(jnp.float32))
            half = inner.shape[0] // 2
            delta = jnp.concatenate(
                [jnp.sum(inner[:half], axis=0, keepdims=True), jnp.sum(inner[half:], axis=0, keepdims=True)], axis=1
            )
            level = lse[row, p]
            query_part = jnp.zeros((128, 2 * tokens), jnp.float32)
            for c in range(tile_count // chunk):
                span = slice(c * chunk * tokens, (c + 1) * chunk * tokens)
                some = slice(c * chunk, (c + 1) * chunk)
                keys = held[row, some, :, at].reshape(chunk * tokens, 128)
                values = held[row, some, :, at_value].reshape(chunk * tokens, 128)
                extra = mask[span, :]
                weights = jnp.exp(mm(keys, both, 1, 1) + jnp.concatenate([extra, extra], axis=1) - level)
                score_grad = (weights * (mm(values, both_grad, 1, 1) - delta)).astype(low)
                value_part = mm(weights.astype(low), both_grad, 1, 0)
                key_part = mm(score_grad, both, 1, 0)
                query_part = query_part + mm(keys, score_grad, 0, 0)
                terms[row, some, :, at] = key_part.astype(low).reshape(chunk, tokens, 128)
                terms[row, some, :, at_value] = value_part.astype(low).reshape(chunk, tokens, 128)
            blocks = own_blocks(query_part) * 0.125
            out[row, :, at] = jnp.transpose(blocks).astype(low)
            return carry

        lax.fori_loop(0, pair_count, one_pair, 0, unroll=3)

    flights = [{} for _ in range(row_count)]
    names = ("own", "x", "y", "xy")
    key_at, value_at = pl.ds(0, width), pl.ds(width, width)

    def begin(row):
        copies = []
        other = 2 - 4 * core
        for k, name in enumerate(names):
            copies.append(send(row, k, terms.at[row, tiles[name] + other], core_terms.at[row, k], peers["core"]))
        flights[row]["core"] = copies

    def add(target, source, row_total):
        def body(i, carry):
            at = pl.ds(pl.multiple_of(i * 16, 16), 16)
            target[at, :] = target[at, :] + source[at, :]
            return carry

        lax.fori_loop(0, row_total // 16, body, 0)

    def scatter(row):
        for k in (3, 1, 2, 0):
            flights[row]["core"][k].wait()
            add(terms.at[row, tiles[names[k]]], core_terms.at[row, k], tokens)
            if k == 3:
                far = terms.at[row, tiles["xy"]]
                flights[row]["far_x"] = send(row, 4, far.at[:, key_at], side_terms.at[row, 0], peers["x"])
                flights[row]["far_y"] = send(row, 5, far.at[:, value_at], side_terms.at[row, 1], peers["y"])
            if k == 1:
                near = terms.at[row, tiles["x"]]
                flights[row]["near_x"] = send(row, 6, near.at[:, key_at], side_terms.at[row, 2], peers["x"])
            if k == 2:
                near = terms.at[row, tiles["y"]]
                flights[row]["near_y"] = send(row, 7, near.at[:, value_at], side_terms.at[row, 3], peers["y"])

    def pass_on(row):
        flights[row]["far_x"].wait()
        near = terms.at[row, tiles["y"], :, key_at]
        add(near, side_terms.at[row, 0], tokens)
        flights[row]["last_y"] = send(row, 8, near, side_terms.at[row, 4], peers["y"])
        flights[row]["far_y"].wait()
        near = terms.at[row, tiles["x"], :, value_at]
        add(near, side_terms.at[row, 1], tokens)
        flights[row]["last_x"] = send(row, 9, near, side_terms.at[row, 5], peers["x"])

    def close(row):
        for name in ("near_x", "near_y", "last_x", "last_y"):
            flights[row][name].wait()
        mine = terms.at[row, tiles["own"]]

        def body(i, carry):
            at = pl.ds(pl.multiple_of(i * 16, 16), 16)
            for start, first, second in ((0, 2, 4), (width, 3, 5)):
                total = mine[at, start : start + width].astype(jnp.float32)
                total = total + side_terms[row, first, at, :].astype(jnp.float32)
                total = total + side_terms[row, second, at, :].astype(jnp.float32)
                out[row, at, width + start : 2 * width + start] = total.astype(low)
            return carry

        lax.fori_loop(0, tokens // 16, body, 0)

    part_copies = []

    def convolve():
        fill_shift(shift, tile_height, tile_width)
        patch = part.shape[2]
        taps[...] = mm(conv_turned[...], conv_in[...], 1, 1)
        rows = []
        for row in range(row_count):
            pieces = []
            for p in range(9):
                piece = taps[p * patch : (p + 1) * patch, row * tokens : (row + 1) * tokens]
                pieces.append(piece * same_image(cuts, row, p, tile_height, tile_width))
            rows.append(jnp.concatenate(pieces, axis=1))
        whole = jnp.concatenate(rows, axis=0)
        coarse = whole.astype(low)
        fine = (whole - coarse.astype(jnp.float32)).astype(low)
        moved = mm(coarse, shift[...], 1, 1) + mm(fine, shift[...], 1, 1)
        for tile in range(tile_count):
            part[tile] = moved[:, tile * tokens : (tile + 1) * tokens].reshape(row_count, patch, tokens)
        for k in range(1, tile_count):
            peer, tile = plane_peer(k)
            copy = pltpu.make_async_remote_copy(
                src_ref=part.at[tile],
                dst_ref=part_got.at[k],
                send_sem=part_send_sem.at[k],
                recv_sem=part_recv_sem.at[k],
                device_id=peer,
                device_id_type=MESH,
            )
            copy.start()
            part_copies.append(copy)
        conv_grad[...] = mm(conv_in[...], spread[...], 0, 1)

    def collect():
        total = part[tiles["own"]]
        for k, copy in enumerate(part_copies):
            copy.wait()
            total = total + part_got[k + 1]
        conv_out[...] = total.astype(low)

    def advance(group, stage):
        for item in group:
            item.stages[stage]()

    for item in items:
        item.begin()
    advance(items[:2], 0)
    for row in range(row_count):
        compute(row)
        begin(row)
        if row == 0:
            advance(items[2:], 0)
        if row > 1:
            pass_on(row - 2)
        if row > 0:
            scatter(row - 1)
            if row < 3:
                advance(planes, row)
    scatter(row_count - 1)
    if row_count > 1:
        pass_on(row_count - 2)
    convolve()
    pass_on(row_count - 1)
    for stage in range(min(row_count, 3), 3):
        advance(planes, stage)
    for row in range(row_count):
        close(row)
    collect()
    advance(planes, 3)
    advance(firsts, 1)
    for item in items:
        item.save()
    for item in items:
        item.land("save")


def attend_back(cuts, query, attended, grad, lse, conv_in, conv_turned, spread, all_pairs, grads, tile_height, tile_width):
    row_count, tokens, width = query.shape
    starts = tuple(start for start, _ in grads)
    grads = [entry for _, entry in grads]
    count = len(starts)
    shapes = [entry.shape[1:] for entry in grads]
    saves = [(r if start == "z" else r // 4, c // 2) for start, (r, c) in zip(starts, shapes)]
    tile_count = all_pairs.shape[1]
    taps = conv_turned.shape[0]
    low = jnp.bfloat16
    vmem = pl.BlockSpec(memory_space=pltpu.VMEM)
    return pl.pallas_call(
        functools.partial(attend_back_kernel, tile_height, tile_width, starts),
        out_shape=[
            jax.ShapeDtypeStruct((row_count, tokens, 3 * width), low),
            jax.ShapeDtypeStruct((width, taps), jnp.float32),
            jax.ShapeDtypeStruct((row_count, taps // 9, tokens), low),
        ]
        + [jax.ShapeDtypeStruct(s, low) for s in saves],
        in_specs=[pl.BlockSpec(memory_space=pltpu.SMEM)]
        + [pl.BlockSpec(memory_space=pl.ANY)] * 4
        + [vmem] * 3
        + [pl.BlockSpec(memory_space=pl.ANY)] * (1 + count),
        out_specs=[vmem] * 3 + [pl.BlockSpec(memory_space=pl.ANY)] * count,
        scratch_shapes=[
            pltpu.VMEM(query.shape, low),
            pltpu.VMEM(attended.shape, low),
            pltpu.VMEM(grad.shape, low),
            pltpu.VMEM(lse.shape, jnp.float32),
            pltpu.SemaphoreType.DMA((row_count, 4)),
            pltpu.VMEM((row_count, tile_count, tokens, 2 * width), low),
            pltpu.VMEM((row_count, tile_count, tokens, 2 * width), low),
            pltpu.VMEM((row_count, 4, tokens, 2 * width), low),
            pltpu.VMEM((row_count, 6, tokens, width), low),
            pltpu.VMEM((tile_count * tokens, tokens), jnp.float32),
            pltpu.VMEM((tile_count * tokens, 9 * tokens), low),
            pltpu.VMEM((taps, row_count * tokens), jnp.float32),
            pltpu.VMEM((tile_count, row_count, taps // 9, tokens), jnp.float32),
            pltpu.VMEM((tile_count, row_count, taps // 9, tokens), jnp.float32),
            pltpu.SemaphoreType.DMA((row_count,)),
            pltpu.SemaphoreType.DMA((row_count, 10)),
            pltpu.SemaphoreType.DMA((row_count, 10)),
            pltpu.SemaphoreType.DMA((tile_count,)),
            pltpu.SemaphoreType.DMA((tile_count,)),
        ]
        + (reducer_scratch(starts, shapes) if count else []),
        compiler_params=pltpu.CompilerParams(
            collective_id=2, has_side_effects=True, vmem_limit_bytes=full_vmem
        ),
        name="attend_back",
    )(cuts, query, attended, grad, lse, conv_in, conv_turned, spread, all_pairs, *grads)


def add_rows(target, first, second, rows):
    def body(i, carry):
        at = pl.ds(pl.multiple_of(i * 16, 16), 16)
        target[at, :] = first[at, :] + second[at, :]
        return carry

    lax.fori_loop(0, rows // 16, body, 0)


def add_four(target, others, rows):
    def body(i, carry):
        at = pl.ds(pl.multiple_of(i * 16, 16), 16)
        total = target[at, :].astype(jnp.float32) + others[0, at, :].astype(jnp.float32)
        total = total + (others[1, at, :].astype(jnp.float32) + others[2, at, :].astype(jnp.float32))
        target[at, :] = total.astype(jnp.bfloat16)
        return carry

    lax.fori_loop(0, rows // 16, body, 0)


def chip_peers():
    z, ty, y = lax.axis_index("rows"), lax.axis_index("ty"), lax.axis_index("tx")
    core, x = lax.rem(ty, 2), ty // 2
    across = (1 - x) * 2 + core
    return {
        "core": (z, x * 2 + 1 - core, y),
        "x": (z, across, y),
        "y": (z, ty, 1 - y),
        "xy": (z, across, 1 - y),
        "z": [(lax.rem(z + k, 4), ty, y) for k in (1, 2, 3)],
    }


class Reducer:
    def __init__(self, start, grad, out, buffers, sems, w):
        self.start, self.grad, self.out, self.buffers, self.w = start, grad, out, buffers, w
        self.local_sem, self.send_sem, self.recv_sem = sems
        self.z, ty, self.y = lax.axis_index("rows"), lax.axis_index("ty"), lax.axis_index("tx")
        self.core, self.x = lax.rem(ty, 2), ty // 2
        self.peers = chip_peers()
        self.flying = {}
        self.own = buffers[0]
        if start in ("plane", "z"):
            self.got, self.half, self.quarter, self.final = buffers[1:]
            self.depth, self.width = grad.shape[1], grad.shape[2] // 2
        else:
            self.depth, self.width = out.shape[0], out.shape[1] // 2
        if start == "block":
            self.half, self.quarter = buffers[1:]
        late = [self.begin_late, self.add_half_late, self.add_quarter_late, self.pass_strip, self.end]
        self.stages = {
            "plane": [self.add_core, self.add_half, self.add_quarter, self.sum_z, self.gather_piece, self.pass_strip, self.end],
            "z": [self.add_core, self.sum_z_first] + late,
            "block": late,
            "piece": [self.gather_piece, self.pass_strip, self.end],
        }[start]

    def part(self, at):
        if self.start == "block":
            return self.own.at[at]
        return self.own.at[self.z, at]

    def send(self, slot, source, target, peer):
        copy = pltpu.make_async_remote_copy(
            src_ref=source,
            dst_ref=target,
            send_sem=self.send_sem.at[self.w, slot],
            recv_sem=self.recv_sem.at[self.w, slot],
            device_id=peer,
            device_id_type=MESH,
        )
        copy.start()
        return copy

    def keep(self, slot, source, target):
        copy = pltpu.make_async_copy(source, target, self.local_sem.at[self.w, slot])
        copy.start()
        return copy

    def land(self, name):
        for copy in self.flying.pop(name):
            copy.wait()

    def columns(self, which):
        return pl.ds(pl.multiple_of(which * self.width, 128), self.width)

    def rows(self, start, size):
        return pl.ds(pl.multiple_of(start, 16), size)

    def place(self, block):
        later = block // 2
        major = self.x + later * (self.y - self.x)
        minor = self.y + later * (self.x - self.y)
        return self.rows(major * (self.depth // 2) + minor * (self.depth // 4), self.depth // 4)

    def begin(self):
        if self.start in ("block", "piece"):
            self.flying["load"] = [self.keep(0, self.grad, self.own)]
            return
        swap = self.send(0, self.grad.at[:, :, self.columns(1 - self.core)], self.got, self.peers["core"])
        mine = self.keep(0, self.grad.at[:, :, self.columns(self.core)], self.own)
        self.flying["core"] = [swap, mine]

    def add_core(self):
        self.land("core")
        for block in range(4):
            add_rows(self.own.at[block], self.own.at[block], self.got.at[block], self.depth)
        if self.start == "z":
            self.flying["z"] = [
                self.send(5 + k, self.own.at[peer[0]], self.final.at[k], peer) for k, peer in enumerate(self.peers["z"])
            ]
            return
        part = self.depth // 2
        first = self.send(1, self.own.at[0:2, self.rows((1 - self.x) * part, part)], self.half.at[0:2], self.peers["x"])
        second = self.send(2, self.own.at[2:4, self.rows((1 - self.y) * part, part)], self.half.at[2:4], self.peers["y"])
        self.flying["half"] = [first, second]

    def add_half(self):
        self.land("half")
        part, less = self.depth // 2, self.depth // 4
        for block in range(4):
            side = self.x if block < 2 else self.y
            kept = self.own.at[block, self.rows(side * part, part)]
            add_rows(kept, kept, self.half.at[block], part)
        first = self.own.at[0:2, self.rows(self.x * part + (1 - self.y) * less, less)]
        second = self.own.at[2:4, self.rows(self.y * part + (1 - self.x) * less, less)]
        self.flying["quarter"] = [
            self.send(3, first, self.quarter.at[0:2], self.peers["y"]),
            self.send(4, second, self.quarter.at[2:4], self.peers["x"]),
        ]

    def add_quarter(self):
        self.land("quarter")
        for block in range(4):
            kept = self.own.at[block, self.place(block // 2 * 2)]
            add_rows(kept, kept, self.quarter.at[block], self.depth // 4)
        self.flying["z"] = [
            self.send(5 + k, self.own.at[peer[0], self.place(peer[0])], self.final.at[k], peer)
            for k, peer in enumerate(self.peers["z"])
        ]

    def gather(self, pieces, sources):
        copies = []
        for n, (at, source) in enumerate(zip(pieces, sources)):
            target = self.out.at[at, self.columns(self.core)]
            for k, name in enumerate(("x", "y", "xy")):
                copies.append(self.send(8 + 3 * n + k, source, target, self.peers[name]))
            copies.append(self.keep(1 + n, source, target))
        self.flying["gather"] = copies

    def sum_z(self):
        self.land("z")
        add_four(self.own.at[self.z, self.place(self.z)], self.final, self.depth // 4)

    def gather_piece(self):
        if self.start == "piece":
            self.land("load")
            self.gather([self.place(self.z)], [self.own])
        else:
            self.gather([self.place(self.z)], [self.own.at[self.z, self.place(self.z)]])

    def sum_z_first(self):
        self.land("z")
        add_four(self.own.at[self.z], self.final, self.depth)

    def save(self):
        source = self.own.at[self.z] if self.start == "z" else self.own.at[self.z, self.place(self.z)]
        self.flying["save"] = [self.keep(1, source, self.out)]

    def begin_late(self):
        if self.start == "block":
            self.land("load")
        half, less = self.depth // 2, self.depth // 4
        self.flying["half"] = [
            self.send(1, self.part(self.rows((1 - self.x) * less, less)), self.half.at[0], self.peers["x"]),
            self.send(2, self.part(self.rows(half + (1 - self.y) * less, less)), self.half.at[1], self.peers["y"]),
        ]

    def add_half_late(self):
        self.land("half")
        half, less, least = self.depth // 2, self.depth // 4, self.depth // 8
        for n, start in enumerate((self.x * less, half + self.y * less)):
            kept = self.part(self.rows(start, less))
            add_rows(kept, kept, self.half.at[n], less)
        first = self.part(self.rows(self.x * less + (1 - self.y) * least, least))
        second = self.part(self.rows(half + self.y * less + (1 - self.x) * least, least))
        self.flying["quarter"] = [
            self.send(3, first, self.quarter.at[0], self.peers["y"]),
            self.send(4, second, self.quarter.at[1], self.peers["x"]),
        ]

    def add_quarter_late(self):
        self.land("quarter")
        half, less, least = self.depth // 2, self.depth // 4, self.depth // 8
        pieces = [self.rows(self.x * less + self.y * least, least), self.rows(half + self.y * less + self.x * least, least)]
        for n, at in enumerate(pieces):
            add_rows(self.part(at), self.part(at), self.quarter.at[n], least)
        self.gather(pieces, [self.part(at) for at in pieces])

    def pass_strip(self):
        self.land("gather")
        strip = self.out.at[:, self.columns(self.core)]
        self.flying["strip"] = [self.send(14, strip, strip, self.peers["core"])]

    def end(self):
        self.land("strip")


def reducer_scratch(starts, shapes):
    buffers = []
    for start, (depth, width) in zip(starts, shapes):
        half = width // 2
        sizes = {
            "plane": [(4, depth, half)] * 2 + [(4, depth // 2, half), (4, depth // 4, half), (3, depth // 4, half)],
            "z": [(4, depth, half)] * 2 + [(2, depth // 4, half), (2, depth // 8, half), (3, depth, half)],
            "block": [(depth, half), (2, depth // 4, half), (2, depth // 8, half)],
            "piece": [(depth // 4, half)],
        }[start]
        buffers += [pltpu.VMEM(size, jnp.bfloat16) for size in sizes]
    count = len(starts)
    return buffers + [
        pltpu.SemaphoreType.DMA((count, 3)),
        pltpu.SemaphoreType.DMA((count, 15)),
        pltpu.SemaphoreType.DMA((count, 15)),
    ]


def make_reducers(starts, grads, outs, scratch):
    items, at = [], 0
    for w, (start, grad, out) in enumerate(zip(starts, grads, outs)):
        size = {"plane": 5, "z": 5, "block": 3, "piece": 1}[start]
        items.append(Reducer(start, grad, out, scratch[at : at + size], scratch[-3:], w))
        at = at + size
    return items


def sum_by_table(local_grads):
    band_count, column_count = lax.axis_size("ty"), lax.axis_size("tx")
    group_count = lax.axis_size("rows")
    tile_count = band_count * column_count
    table = jnp.concatenate([entry.reshape(group_count, -1) for entry in local_grads], axis=1)
    column_total = table.shape[1]
    padded_columns = -(-column_total // tile_count) * tile_count
    piece_width = padded_columns // tile_count
    table = table.reshape(group_count, tile_count, piece_width)
    shares = lax.psum_scatter(
        table.reshape(group_count * tile_count, piece_width),
        ("rows", "ty", "tx"),
        scatter_dimension=0,
        tiled=True,
    )
    summed = (
        lax.all_gather(shares.astype(jnp.bfloat16), ("ty", "tx"), axis=0, tiled=True)
        .astype(shares.dtype)
        .reshape(-1)
    )
    totals = []
    start_at = 0
    for entry in local_grads:
        length = entry.size // group_count
        shard_shape = (entry.shape[0] // group_count,) + entry.shape[1:]
        totals.append(summed[start_at : start_at + length].reshape(shard_shape))
        start_at = start_at + length
    return tuple(totals)


def shards(
    latent,
    skip_input,
    segment_ids,
    embed_weight,
    embed_bias,
    skip_weight,
    skip_bias,
    norm1_gain,
    norm1_bias,
    qkv_weight,
    proj_weight,
    proj_bias,
    norm2_gain,
    norm2_bias,
    fc1_weight,
    fc1_bias,
    fc2_weight,
    fc2_bias,
    conv_weight,
    cotangent,
):
    row_count, tile_height, tile_width, width = skip_input.shape
    patch = latent.shape[3]
    tokens = tile_height * tile_width
    token_count = row_count * tokens
    low = jnp.bfloat16
    wide = jnp.float32
    conv_turned = conv_weight.T
    flat_latent = latent.reshape(token_count, patch)
    flat_skip = skip_input.reshape(token_count, width)
    biases = (embed_bias, skip_bias, norm1_gain, norm1_bias, proj_bias, norm2_gain, norm2_bias, fc2_bias)
    embedded, stream, normed, query, pairs, cot, vectors, hidden_bias, cuts = front(
        segment_ids, flat_latent, cotangent.reshape(token_count, patch), embed_weight.T, biases, fc1_bias,
        flat_skip, skip_weight, qkv_weight, row_count,
    )
    attended, log_total, row_pairs, cot_tiles = attend(cuts, query, pairs, cot, tile_height, tile_width)
    (
        fc1_grad, fc2_grad, hidden_bias_grad, proj_grad, attended_grad, mid_grad, conv_in, spread, middle_grads
    ) = middle(
        cuts, attended.reshape(token_count, width), stream, cot_tiles, proj_weight, conv_turned, vectors,
        hidden_bias, fc1_weight, fc2_weight, tile_height, tile_width,
    )
    here = (lax.axis_size("rows"), lax.axis_size("ty"), lax.axis_size("tx")) == (4, 4, 2)

    def in_blocks(grads):
        return [entry.reshape(4, -1, entry.shape[1]) for entry in grads]

    early = [("plane", fc1_grad), ("z", fc2_grad), ("plane", proj_grad)] if here else []
    projected_grad, conv_grad, conv_out, *saved = attend_back(
        cuts, query, attended, attended_grad.reshape(row_count, tokens, width), log_total,
        conv_in, conv_turned, spread, row_pairs, list(zip([start for start, _ in early], in_blocks([g for _, g in early]))),
        tile_height, tile_width,
    )
    follow = {"plane": "piece", "z": "block"}
    resumed = [
        (follow[start], entry, (grad.shape[0] // 4, grad.shape[1])) for (start, grad), entry in zip(early, saved)
    ]
    skip_input_grad, *rest = rear(
        projected_grad.reshape(token_count, 3 * width), qkv_weight, normed, stream, mid_grad, embedded, flat_skip,
        skip_weight, flat_latent, vectors, middle_grads, hidden_bias_grad, conv_grad, resumed, here,
    )
    skip_input_grad = skip_input_grad.reshape(row_count, tile_height, tile_width, width)
    taps = 9 * patch
    share = width // 4
    if here:
        totals = finish(rest[:5], rest[5], rest[6], conv_out)
        fc1_total, fc2_total, proj_total, qkv_total, skip_total, embed_turned, conv_grad_turned = totals[:7]
        line, fc1_line = totals[7:15], totals[15]
        output = totals[16].reshape(row_count, tile_height, tile_width, patch)
        return (
            output, skip_input_grad, embed_turned.T, line[0], skip_total, line[1], line[2], line[3], qkv_total,
            proj_total, line[4], line[5], line[6], fc1_total, fc1_line, fc2_total, line[7], conv_grad_turned.T,
        )
    output = conv_out.transpose(0, 2, 1).reshape(row_count, tile_height, tile_width, patch)
    qkv_grad, skip_grad, thin = [entry.reshape(-1, entry.shape[2]) for entry in rest[:3]]
    flat = rest[3]
    line = [flat[:, k, :share].reshape(-1) for k in range(8)]
    fc1_line = flat[:, 8:11].reshape(-1)
    local_grads = [
        thin[:, taps : taps + patch], line[0], skip_grad, line[1], line[2], line[3], qkv_grad, proj_grad, line[4],
        line[5], line[6], fc1_grad, fc1_line, fc2_grad, line[7], thin[:, :taps],
    ]
    return (output, skip_input_grad) + sum_by_table([entry.astype(wide) for entry in local_grads])


def solution(mesh):
    return jax.shard_map(
        shards,
        mesh=mesh,
        in_specs=(
            P("rows", "ty", "tx", None),
            P("rows", "ty", "tx", None),
            P("rows", None, None),
            P(),
            P(),
            P(),
            P(),
            P(),
            P(),
            P(),
            P(),
            P(),
            P(),
            P(),
            P(),
            P(),
            P(),
            P(),
            P(),
            P("rows", "ty", "tx", None),
        ),
        out_specs=(
            P("rows", "ty", "tx", None),
            P("rows", "ty", "tx", None),
            P("rows", None),
            P("rows"),
            P("rows", None),
            P("rows"),
            P("rows"),
            P("rows"),
            P("rows", None),
            P("rows", None),
            P("rows"),
            P("rows"),
            P("rows"),
            P("rows", None),
            P("rows"),
            P("rows", None),
            P("rows"),
            P("rows", None),
        ),
        check_vma=False,
    )
```

```python
import functools

import jax
import jax.numpy as jnp
from jax import lax
from jax.experimental import pallas as pl
from jax.experimental.pallas import tpu as pltpu
from jax.sharding import PartitionSpec as P

MESH = pl.DeviceIdType.MESH
norm_eps = 1e-05
full_vmem = 62 * 1024 * 1024


def cell_of(token, tile, tile_height, tile_width, columns):
    down = tile // columns * tile_height + token // tile_width
    across = tile % columns * tile_width + token % tile_width
    return down, across


def fill_shift(shift_ref, tile_height, tile_width):
    tokens = tile_height * tile_width
    bands, columns = lax.axis_size("ty"), lax.axis_size("tx")
    own = lax.axis_index("ty") * columns + lax.axis_index("tx")
    lane = lax.broadcasted_iota(jnp.int32, (8, tokens), 1)
    down, across = cell_of(lane, own, tile_height, tile_width, columns)
    step = lax.broadcasted_iota(jnp.int32, (shift_ref.shape[0], tokens), 0)
    for p in range(9):
        i, j = down - (p // 3 - 1), across - (p % 3 - 1)
        inside = (i >= 0) & (i < bands * tile_height) & (j >= 0) & (j < columns * tile_width)
        tile = i // tile_height * columns + j // tile_width
        place = tile * tokens + i % tile_height * tile_width + j % tile_width
        place = jnp.where(inside, place, -1)[0:1]
        chosen = jnp.where(step == place, 1.0, 0.0)
        shift_ref[:, p * tokens : (p + 1) * tokens] = chosen.astype(jnp.bfloat16)


def same_image(cuts_ref, row, p, tile_height, tile_width):
    tokens = tile_height * tile_width
    columns = lax.axis_size("tx")
    own = lax.axis_index("ty") * columns + lax.axis_index("tx")
    lane = lax.broadcasted_iota(jnp.int32, (8, tokens), 1)
    down, across = cell_of(lane, own, tile_height, tile_width, columns)
    left_width, top_height = cuts_ref[row, 0], cuts_ref[row, 1]

    def image_of(i, j):
        return jnp.where(j < left_width, 0, jnp.where(i < top_height, 1, 2))

    there = image_of(down - (p // 3 - 1), across - (p % 3 - 1))
    return jnp.where(image_of(down, across) == there, 1.0, 0.0)[0:1]


def mm(former, latter, axis_former, axis_latter):
    return lax.dot_general(
        former,
        latter,
        (((axis_former,), (axis_latter,)), ((), ())),
        preferred_element_type=jnp.float32,
    )


def normalised(values):
    average = jnp.mean(values, axis=1, keepdims=True)
    centred = values - average
    rate = lax.rsqrt(jnp.mean(centred * centred, axis=1, keepdims=True) + norm_eps)
    return centred * rate, rate


def norm_back(incoming, unit, rate, gain):
    scaled = incoming * gain
    first = jnp.mean(scaled, axis=1, keepdims=True)
    second = jnp.mean(scaled * unit, axis=1, keepdims=True)
    return (scaled - first - unit * second) * rate


def down_sum(values):
    return jnp.sum(values, axis=0, keepdims=True)


def front_kernel(
    segment_ids, latent, cotangent, embed_turned, *refs
):
    biases, fc1_bias, refs = refs[:8], refs[8], refs[9:]
    skip_in, skip_weight_in, qkv_in, embedded, stream, normed, query, pairs, cot, vectors, hidden_bias, cuts = refs[:12]
    skip, skip_weight, qkv_weight, load_sem = refs[12:]
    sources, targets = (skip_weight_in, skip_in, qkv_in), (skip_weight, skip, qkv_weight)
    loads = [pltpu.make_async_copy(a, b, load_sem.at[k]) for k, (a, b) in enumerate(zip(sources, targets))]
    for load in loads:
        load.start()
    for k, bias in enumerate(biases):
        vectors[k : k + 1] = bias[...].reshape(1, bias.shape[0]).astype(jnp.float32)
    line = fc1_bias[...].reshape(1, fc1_bias.shape[0]).astype(jnp.float32)
    block = hidden_bias.shape[2]
    for k in range(hidden_bias.shape[0]):
        hidden_bias[k] = line[:, k * block : (k + 1) * block]
    width = skip.shape[1]
    row_count, tokens = query.shape[0], query.shape[1]
    side = segment_ids.shape[1]
    for row in range(row_count):

        def count(k, carry):
            left, top = carry
            left = left + jnp.where(segment_ids[row, 0, k] == 0, 1, 0)
            top = top + jnp.where(segment_ids[row, k, side - 1] == 1, 1, 0)
            return left, top

        left, top = lax.fori_loop(0, side, count, (jnp.int32(0), jnp.int32(0)), unroll=8)
        cuts[row, 0] = left
        cuts[row, 1] = top
        at = slice(row * tokens, (row + 1) * tokens)
        cot[row] = jnp.transpose(cotangent[at, :].astype(jnp.float32)).astype(jnp.bfloat16)
        embedded[at, :] = (mm(latent[at, :], embed_turned[...], 1, 0) + vectors[0:1]).astype(jnp.bfloat16)
    loads[0].wait()
    loads[1].wait()
    total = mm(embedded[...], skip_weight[:width], 1, 0) + mm(skip[...], skip_weight[width:], 1, 0) + vectors[1:2]
    stream[...] = total
    unit, rate = normalised(total)
    normed[...] = (unit * vectors[2:3] + vectors[3:4]).astype(jnp.bfloat16)
    loads[2].wait()
    pairs[...] = mm(normed[...], qkv_weight[:, width:], 1, 0).astype(jnp.bfloat16).reshape(pairs.shape)
    query[...] = mm(normed[...], qkv_weight[:, :width], 1, 0).astype(jnp.bfloat16).reshape(query.shape)


def front(segment_ids, latent, cotangent, embed_turned, biases, fc1_bias, skip, skip_weight, qkv_weight, row_count):
    token_count, width = skip.shape
    tokens = token_count // row_count
    low, wide = jnp.bfloat16, jnp.float32
    smem, vmem = pl.BlockSpec(memory_space=pltpu.SMEM), pl.BlockSpec(memory_space=pltpu.VMEM)
    return pl.pallas_call(
        front_kernel,
        out_shape=[
            jax.ShapeDtypeStruct((token_count, width), low),
            jax.ShapeDtypeStruct((token_count, width), wide),
            jax.ShapeDtypeStruct((token_count, width), low),
            jax.ShapeDtypeStruct((row_count, tokens, width), low),
            jax.ShapeDtypeStruct((row_count, tokens, 2 * width), low),
            jax.ShapeDtypeStruct((row_count, cotangent.shape[1], tokens), low),
            jax.ShapeDtypeStruct((8, width), wide),
            jax.ShapeDtypeStruct((fc1_bias.shape[0] // width, 1, width), wide),
            jax.ShapeDtypeStruct((row_count, 2), jnp.int32),
        ],
        in_specs=[smem] + [vmem] * 12 + [pl.BlockSpec(memory_space=pl.ANY)] * 3,
        out_specs=[vmem] * 8 + [smem],
        scratch_shapes=[pltpu.VMEM(entry.shape, low) for entry in (skip, skip_weight, qkv_weight)]
        + [pltpu.SemaphoreType.DMA((3,))],
        compiler_params=pltpu.CompilerParams(vmem_limit_bytes=full_vmem),
        name="front",
    )(segment_ids, latent, cotangent, embed_turned, *biases, fc1_bias, skip, skip_weight, qkv_weight)


def erf_of(values):
    x = jnp.clip(values, -4.0, 4.0)
    square = x * x
    upper = square * -2.72614225801306e-10 + 2.77068142495902e-08
    for term in (-2.10102402082508e-06, -5.69250639462346e-05, -7.34990630326855e-04, -2.95459980854025e-03, -1.60960333262415e-02):
        upper = upper * square + term
    lower = square * -1.45660718464996e-05 + -2.13374055278905e-04
    for term in (-1.68282697438203e-03, -7.37332916720468e-03, -1.42647390514189e-02):
        lower = lower * square + term
    return x * upper / lower


def middle_kernel(
    paired, attended, stream, out_grad, proj_weight, vectors, hidden_bias, active_grad, fc1_weight, fc2_weight,
    fc1_out, fc2_out, hidden_bias_grad, proj_grad, attended_grad, mid_grad, conv_in, vector_grads,
    middle, normed, out_low, forward_sum, backward_sum, grad1, grad2, *refs
):
    step = pl.program_id(0)
    last = fc2_out.shape[0] // fc2_weight.shape[0] - 1
    token_count, width = stream.shape
    block = fc1_weight.shape[1]
    low = jnp.bfloat16
    parts = [slice(0, token_count)]
    store_sem = refs[-1]
    if paired:
        got1, got2, total1, total2, send_sem, recv_sem = refs[:6]
        z, ty, y = lax.axis_index("rows"), lax.axis_index("ty"), lax.axis_index("tx")
        core = lax.rem(ty, 2)
        peer = (z, ty + 1 - 2 * core, y)

    def stores(k):
        slot = lax.rem(k, 2)
        first, second = (total1, total2) if paired else (grad1, grad2)
        across = first.shape[3]
        down = second.shape[1]
        return [
            pltpu.make_async_copy(
                first.at[slot], fc1_out.at[:, :, pl.ds(pl.multiple_of(k * across, 128), across)], store_sem.at[slot, 0]
            ),
            pltpu.make_async_copy(
                second.at[slot], fc2_out.at[pl.ds(pl.multiple_of(k * down, 16), down)], store_sem.at[slot, 1]
            ),
        ]

    def swaps(k):
        slot = lax.rem(k, 2)
        theirs1 = pl.ds(pl.multiple_of((1 - core) * (block // 2), 128), block // 2)
        theirs2 = pl.ds(pl.multiple_of((1 - core) * (width // 2), 128), width // 2)
        pairs = ((grad1.at[slot, :, :, theirs1], got1.at[k]), (grad2.at[slot, :, theirs2], got2.at[k]))
        return [
            pltpu.make_async_remote_copy(
                src_ref=source,
                dst_ref=target,
                send_sem=send_sem.at[k, n],
                recv_sem=recv_sem.at[k, n],
                device_id=peer,
                device_id_type=MESH,
            )
            for n, (source, target) in enumerate(pairs)
        ]

    def settle(k):
        slot = lax.rem(k, 2)
        if paired:
            for copy in swaps(k):
                copy.wait()

            @pl.when(k >= 2)
            def _():
                for copy in stores(k - 2):
                    copy.wait()

            mine1 = pl.ds(pl.multiple_of(core * (block // 2), 128), block // 2)
            mine2 = pl.ds(pl.multiple_of(core * (width // 2), 128), width // 2)
            total1[slot] = grad1[slot, :, :, mine1] + got1[k]
            total2[slot] = grad2[slot, :, mine2] + got2[k]
        for copy in stores(k):
            copy.start()

    @pl.when(step == 0)
    def _():
        if paired:
            greet([peer])
        total = jnp.zeros((1, width), jnp.float32)
        for at in parts:
            grad = out_grad[at, :]
            out_low[at, :] = grad.astype(low)
            total = total + down_sum(grad)
            value = stream[at, :] + mm(attended[at, :], proj_weight[...], 1, 0) + vectors[4:5]
            middle[at, :] = value
            unit, rate = normalised(value)
            normed[at, :] = (unit * vectors[5:6] + vectors[6:7]).astype(low)
        vector_grads[7:8] = total
        forward_sum[...] = jnp.zeros_like(forward_sum)
        backward_sum[...] = jnp.zeros_like(backward_sum)

    slot = lax.rem(step, 2)
    if not paired:

        @pl.when(step >= 2)
        def _():
            for copy in stores(step - 2):
                copy.wait()

    bias_grad = jnp.zeros((1, block), jnp.float32)
    actives, hidden_lows = [], []
    for at in parts:
        hidden = mm(normed[at, :], fc1_weight[...], 1, 0) + hidden_bias[0]
        share = 0.5 + 0.5 * erf_of(hidden * 0.7071067811865476)
        density = jnp.exp(hidden * hidden * -0.5) * 0.3989422804014327
        active = (hidden * share).astype(low)
        hidden_grad = active_grad[at, :].astype(jnp.float32) * (share + hidden * density)
        bias_grad = bias_grad + down_sum(hidden_grad)
        hidden_low = hidden_grad.astype(low)
        forward_sum[at, :] = forward_sum[at, :] + mm(active, fc2_weight[...], 1, 0)
        backward_sum[at, :] = backward_sum[at, :] + mm(hidden_low, fc1_weight[...], 1, 1)
        actives.append(active)
        hidden_lows.append(hidden_low)
    hidden_bias_grad[0] = bias_grad
    grad2[slot] = mm(jnp.concatenate(actives, axis=0), out_low[...], 0, 0).astype(low)
    grad1[slot] = mm(normed[...], jnp.concatenate(hidden_lows, axis=0), 0, 0).astype(low).reshape(grad1.shape[1:])
    if paired:
        for copy in swaps(step):
            copy.start()

        @pl.when(step > 0)
        def _():
            settle(step - 1)
    else:
        settle(step)

    @pl.when(step == last)
    def _():
        gain_sum = jnp.zeros((1, width), jnp.float32)
        bias_sum = jnp.zeros((1, width), jnp.float32)
        mid_sum = jnp.zeros((1, width), jnp.float32)
        lows = []
        for at in parts:
            unit, rate = normalised(middle[at, :])
            conv_in[at, :] = (middle[at, :] + forward_sum[at, :] + vectors[7:8]).astype(low)
            incoming = backward_sum[at, :]
            gain_sum = gain_sum + down_sum(incoming * unit)
            bias_sum = bias_sum + down_sum(incoming)
            grad = out_grad[at, :] + norm_back(incoming, unit, rate, vectors[5:6])
            mid_grad[at, :] = grad
            mid_sum = mid_sum + down_sum(grad)
            mid_low = grad.astype(low)
            lows.append(mid_low)
            attended_grad[at, :] = mm(mid_low, proj_weight[...], 1, 1).astype(low)
        proj_grad[...] = mm(attended[...], jnp.concatenate(lows, axis=0), 0, 0).astype(low)
        vector_grads[4:5] = mid_sum
        vector_grads[5:6] = gain_sum
        vector_grads[6:7] = bias_sum
        if paired:
            settle(step)
        for k in (last - 1, last):
            for copy in stores(k):
                copy.wait()


def middle(attended, stream, out_grad, active_grad, proj_weight, vectors, hidden_bias, fc1_weight, fc2_weight, paired):
    token_count, width = stream.shape
    hidden_width = fc1_weight.shape[1]
    steps, _, block = hidden_bias.shape
    low, wide = jnp.bfloat16, jnp.float32
    cut = 2 if paired else 1
    vmem, anywhere = pl.BlockSpec(memory_space=pltpu.VMEM), pl.BlockSpec(memory_space=pl.ANY)
    scratch = [
        pltpu.VMEM((token_count, width), wide),
        pltpu.VMEM((token_count, width), low),
        pltpu.VMEM((token_count, width), low),
        pltpu.VMEM((token_count, width), wide),
        pltpu.VMEM((token_count, width), wide),
        pltpu.VMEM((2, 4, width // 4, block), low),
        pltpu.VMEM((2, block, width), low),
    ]
    if paired:
        scratch += [
            pltpu.VMEM((steps, 4, width // 4, block // 2), low),
            pltpu.VMEM((steps, block, width // 2), low),
            pltpu.VMEM((2, 4, width // 4, block // 2), low),
            pltpu.VMEM((2, block, width // 2), low),
            pltpu.SemaphoreType.DMA((steps, 2)),
            pltpu.SemaphoreType.DMA((steps, 2)),
        ]
        params = pltpu.CompilerParams(collective_id=4, has_side_effects=True, vmem_limit_bytes=full_vmem)
    else:
        params = pltpu.CompilerParams(vmem_limit_bytes=full_vmem)
    return pl.pallas_call(
        functools.partial(middle_kernel, paired),
        grid=(steps,),
        out_shape=[
            jax.ShapeDtypeStruct((4, width // 4, hidden_width // cut), low),
            jax.ShapeDtypeStruct((hidden_width, width // cut), low),
            jax.ShapeDtypeStruct((steps, 1, block), wide),
            jax.ShapeDtypeStruct((width, width), low),
            jax.ShapeDtypeStruct((token_count, width), low),
            jax.ShapeDtypeStruct((token_count, width), wide),
            jax.ShapeDtypeStruct((token_count, width), low),
            jax.ShapeDtypeStruct((8, width), wide),
        ],
        in_specs=[vmem] * 5
        + [
            pl.BlockSpec((1, 1, block), lambda k: (k, 0, 0)),
            pl.BlockSpec((token_count, block), lambda k: (0, k)),
            pl.BlockSpec((width, block), lambda k: (0, k)),
            pl.BlockSpec((block, width), lambda k: (k, 0)),
        ],
        out_specs=[anywhere, anywhere, pl.BlockSpec((1, 1, block), lambda k: (k, 0, 0))] + [vmem] * 5,
        scratch_shapes=scratch + [pltpu.SemaphoreType.DMA((2, 2))],
        compiler_params=params,
        name="middle",
    )(attended, stream, out_grad, proj_weight, vectors, hidden_bias, active_grad, fc1_weight, fc2_weight)


def rear_kernel(
    kinds, reduces, projected_in, qkv_in, normed_in, stream_in, mid_in, embedded_in, skip_in, skip_weight_in,
    latent, vectors, middle_grads, hidden_bias_grad, conv_grad, *refs
):
    count = len(kinds)
    resumed, refs = refs[:count], refs[count:]
    skip_input_grad, refs = refs[0], refs[1:]
    if reduces:
        sums, refs = refs[: count + 4], refs[count + 4 :]
        peers = chip_peers()
    qkv_grad, skip_grad, thin, flat, refs = *refs[:4], refs[4:]
    projected_grad, qkv_weight, normed, stream, mid_grad, embedded, skip, skip_weight, stream_low, load_sem = refs[:10]
    sources = (projected_in, normed_in, qkv_in, stream_in, mid_in, embedded_in, skip_in, skip_weight_in)
    targets = (projected_grad, normed, qkv_weight, stream, mid_grad, embedded, skip, skip_weight)
    loads = [pltpu.make_async_copy(a, b, load_sem.at[k]) for k, (a, b) in enumerate(zip(sources, targets))]
    for load in loads[:3]:
        load.start()
    later, news = [], []
    if reduces:
        items = make_reducers(
            kinds + (("plane", False),) * 4, resumed + (qkv_grad, skip_grad, thin, flat), sums, refs[10:]
        )
        later, news = items[:count], items[count:]
        greet([peers[name] for name in ("core", "x", "y", "xy")] + peers["z"])
    for item in later:
        item.begin()
    for load in loads[3:]:
        load.start()
    for item in later:
        item.stages.pop(0)()
    token_count, width = stream.shape
    low = jnp.bfloat16
    parts = [slice(0, token_count)]
    zero = jnp.zeros((1, width), jnp.float32)
    gain_sum, bias_sum, stream_sum, embed_sum = zero, zero, zero, zero
    loads[0].wait()
    loads[1].wait()
    blocks, depth = qkv_grad.shape[0], qkv_grad.shape[1]
    for k in range(3):
        at = slice(k * width, (k + 1) * width)
        qkv_grad[:, :, at] = mm(normed[...], projected_grad[:, at], 0, 0).astype(low).reshape(blocks, depth, width)

    def open_up(which):
        for item in news[which]:
            item.begin()

    def step_on(group):
        for item in group:
            if item.stages:
                item.stages.pop(0)()

    open_up(slice(0, 1))
    for load in loads[2:5]:
        load.wait()
    for at in parts:
        incoming = mm(projected_grad[at, :], qkv_weight[...], 1, 1)
        unit, rate = normalised(stream[at, :])
        gain_sum = gain_sum + down_sum(incoming * unit)
        bias_sum = bias_sum + down_sum(incoming)
        grad = mid_grad[at, :] + norm_back(incoming, unit, rate, vectors[2:3])
        stream_sum = stream_sum + down_sum(grad)
        stream_low[at, :] = grad.astype(low)
    step_on(news[0:1])
    loads[5].wait()
    loads[6].wait()
    skip_grad[0:2] = mm(embedded[...], stream_low[...], 0, 0).astype(low).reshape(2, width // 2, width)
    skip_grad[2:4] = mm(skip[...], stream_low[...], 0, 0).astype(low).reshape(2, width // 2, width)
    open_up(slice(1, 2))
    loads[7].wait()
    embed_lows = []
    for at in parts:
        embed_grad = mm(stream_low[at, :], skip_weight[:width], 1, 1)
        embed_sum = embed_sum + down_sum(embed_grad)
        embed_lows.append(embed_grad.astype(low))
    embed_weight_grad = mm(jnp.concatenate(embed_lows, axis=0), latent[...], 0, 0)
    step_on(news[1:2])
    rest = jnp.zeros((width, 128 - 2 * 16), jnp.float32)
    thin[:, :, :128] = conv_grad[:, :128].astype(low).reshape(4, width // 4, 128)
    edge = jnp.concatenate([conv_grad[:, 128:144], embed_weight_grad, rest], axis=1)
    thin[:, :, 128:] = edge.astype(low).reshape(4, width // 4, 128)
    rows = [embed_sum, stream_sum, gain_sum, bias_sum] + [middle_grads[k : k + 1] for k in range(4, 8)]
    stack = jnp.concatenate(rows, axis=0)
    share = width // 4
    hidden_line = jnp.concatenate([hidden_bias_grad[k] for k in range(hidden_bias_grad.shape[0])], axis=1)
    for block in range(4):
        own = stack[:, block * share : (block + 1) * share]
        own = jnp.concatenate([own, jnp.zeros((8, 256 - share), jnp.float32)], axis=1)
        line = hidden_line[:, block * width : (block + 1) * width]
        pieces = [line[:, k * 256 : (k + 1) * 256] for k in range(width // 256)]
        body = jnp.concatenate([own] + pieces + [jnp.zeros((8 - len(pieces), 256), jnp.float32)], axis=0)
        flat[block, 0:16] = body.astype(low)
        flat[block, 16:64] = jnp.zeros((48, 256), low)
    open_up(slice(2, 4))
    step_on(later)
    step_on(news[0:1])
    for at in parts:
        skip_input_grad[at, :] = mm(stream_low[at, :], skip_weight[width:], 1, 1).astype(low)
    step_on(news[2:4])
    while any(item.stages for item in later + news):
        step_on(later)
        step_on(news)


def rear(projected_grad, qkv_weight, normed, stream, mid_grad, embedded, skip, skip_weight, latent, vectors, middle_grads, hidden_bias_grad, conv_grad, resumed, reduces):
    token_count, width = stream.shape
    low = jnp.bfloat16
    kinds = tuple((start, True) for start, _, _ in resumed)
    sizes = [(width // 4, 3 * width), (width // 2, width), (width // 4, 256), (64, 256)]
    totals = [shape for _, _, shape in resumed] + [(r, c // 2) for r, c in sizes]
    vmem, anywhere = pl.BlockSpec(memory_space=pltpu.VMEM), pl.BlockSpec(memory_space=pl.ANY)
    big = [projected_grad, qkv_weight, normed, stream, mid_grad, embedded, skip, skip_weight]
    out_shape = [jax.ShapeDtypeStruct((token_count, width), low)]
    out_specs = [vmem]
    scratch = []
    if reduces:
        out_shape += [jax.ShapeDtypeStruct((2,) + shape, low) for shape in totals]
        out_specs += [anywhere] * len(totals)
        scratch += [pltpu.VMEM((4,) + shape, low) for shape in sizes]
        params = pltpu.CompilerParams(collective_id=3, has_side_effects=True, vmem_limit_bytes=full_vmem)
    else:
        out_shape += [jax.ShapeDtypeStruct((4,) + shape, low) for shape in sizes]
        out_specs += [vmem] * len(sizes)
        params = pltpu.CompilerParams(vmem_limit_bytes=full_vmem)
    scratch += [pltpu.VMEM(entry.shape, entry.dtype) for entry in big]
    scratch += [pltpu.VMEM((token_count, width), low), pltpu.SemaphoreType.DMA((len(big),))]
    if reduces:
        scratch += reducer_scratch(kinds + (("plane", False),) * 4, totals)
    return pl.pallas_call(
        functools.partial(rear_kernel, kinds, reduces),
        out_shape=out_shape,
        in_specs=[anywhere] * len(big) + [vmem] * 5 + [anywhere] * len(kinds),
        out_specs=out_specs,
        scratch_shapes=scratch,
        compiler_params=params,
        name="rear",
    )(*big, latent, vectors, middle_grads, hidden_bias_grad, conv_grad, *[entry for _, entry, _ in resumed])


def finish_kernel(patch, *refs):
    sums, (thin, flat, conv_out) = refs[:5], refs[5:8]
    totals, (embed_turned, conv_turned), refs = refs[8:13], refs[13:15], refs[15:]
    lines, fc1_line, output, refs = refs[:8], refs[8], refs[9], refs[10:]
    lows, wides, load_sem, store_sem = refs[:5], refs[5:10], refs[10], refs[11]
    loads = [pltpu.make_async_copy(a, b, load_sem.at[k]) for k, (a, b) in enumerate(zip(sums, lows))]
    for load in loads:
        load.start()
    share = thin.shape[1]
    turned = jnp.transpose(jnp.concatenate([thin[0], thin[1]], axis=1).astype(jnp.float32))
    taps = 9 * patch
    conv_turned[...] = turned[:taps]
    embed_turned[...] = turned[taps : taps + patch]
    rows = jnp.concatenate([flat[0, 0:16, :], flat[1, 0:16, :]], axis=1).astype(jnp.float32)
    for k, line in enumerate(lines):
        line[...] = rows[k : k + 1, :share].reshape(share)
    fc1_line[...] = jnp.concatenate([rows[k : k + 1] for k in range(8, 11)], axis=1).reshape(fc1_line.shape[0])
    for row in range(output.shape[0]):
        output[row] = jnp.transpose(conv_out[row].astype(jnp.float32)).astype(jnp.bfloat16)
    stores = []
    for k, (low, wide) in enumerate(zip(lows, wides)):
        loads[k].wait()

        half = low.shape[2]
        piece = 384 if k == 0 else half

        def body(i, carry):
            at = pl.ds(pl.multiple_of(i * 16, 16), 16)
            for core in range(2):
                for n in range(half // piece):
                    start = (2 * n + core) * piece
                    wide[at, start : start + piece] = low[core, at, n * piece : (n + 1) * piece].astype(jnp.float32)
            return carry

        lax.fori_loop(0, low.shape[1] // 16, body, 0)
        store = pltpu.make_async_copy(wide, totals[k], store_sem.at[k])
        store.start()
        stores.append(store)
    for store in stores:
        store.wait()


def finish(sums, thin, flat, conv_out):
    row_count, patch, tokens = conv_out.shape
    share = thin.shape[1]
    wide = jnp.float32
    whole = [(entry.shape[1], 2 * entry.shape[2]) for entry in sums]
    vmem, anywhere = pl.BlockSpec(memory_space=pltpu.VMEM), pl.BlockSpec(memory_space=pl.ANY)
    return pl.pallas_call(
        functools.partial(finish_kernel, patch),
        out_shape=[jax.ShapeDtypeStruct(shape, wide) for shape in whole]
        + [jax.ShapeDtypeStruct((patch, share), wide), jax.ShapeDtypeStruct((9 * patch, share), wide)]
        + [jax.ShapeDtypeStruct((share,), wide)] * 8
        + [jax.ShapeDtypeStruct((4 * share,), wide), jax.ShapeDtypeStruct((row_count, tokens, patch), jnp.bfloat16)],
        in_specs=[anywhere] * 5 + [vmem] * 3,
        out_specs=[anywhere] * 5 + [vmem] * 12,
        scratch_shapes=[pltpu.VMEM(entry.shape, jnp.bfloat16) for entry in sums]
        + [pltpu.VMEM(shape, wide) for shape in whole]
        + [pltpu.SemaphoreType.DMA((5,)), pltpu.SemaphoreType.DMA((5,))],
        compiler_params=pltpu.CompilerParams(vmem_limit_bytes=full_vmem),
        name="finish",
    )(*sums, thin, flat, conv_out)


def plane_peers():
    z, ty, y = lax.axis_index("rows"), lax.axis_index("ty"), lax.axis_index("tx")
    core, x = lax.rem(ty, 2), ty // 2
    here = x * 2 + core
    across = (1 - x) * 2 + core
    tiles = {
        "own": here * 2 + y,
        "x": across * 2 + y,
        "y": here * 2 + 1 - y,
        "xy": across * 2 + 1 - y,
    }
    peers = {
        "core": (z, x * 2 + 1 - core, y),
        "x": (z, across, y),
        "y": (z, here, 1 - y),
    }
    return tiles, peers


def plane_peer(k):
    z, ty, y = lax.axis_index("rows"), lax.axis_index("ty"), lax.axis_index("tx")
    x, core = ty // 2, lax.rem(ty, 2)
    flip_x, flip_core, flip_y = k // 4, k // 2 % 2, k % 2
    x = x + flip_x - 2 * flip_x * x
    core = core + flip_core - 2 * flip_core * core
    y = y + flip_y - 2 * flip_y * y
    return (z, x * 2 + core, y), (x * 2 + core) * 2 + y


def greet(peers):
    barrier = pltpu.get_barrier_semaphore()
    for peer in peers:
        pl.semaphore_signal(barrier, inc=1, device_id=peer, device_id_type=MESH)
    pl.semaphore_wait(barrier, len(peers))


def fill_mask(mask_ref, cuts_ref, row, tile_height, tile_width):
    ty, tx = lax.axis_index("ty"), lax.axis_index("tx")
    columns = lax.axis_size("tx")
    tokens = tile_height * tile_width
    left_width = cuts_ref[row, 0]
    top_height = cuts_ref[row, 1]

    def image_of(down, across):
        return jnp.where(across < left_width, 0, jnp.where(down < top_height, 1, 2))

    lane = lax.broadcasted_iota(jnp.int32, (tokens, tokens), 1)
    step = lax.broadcasted_iota(jnp.int32, (tokens, tokens), 0)
    mine = image_of(
        ty * tile_height + lane // tile_width, tx * tile_width + lane % tile_width
    )
    for tile in range(mask_ref.shape[0] // tokens):
        theirs = image_of(
            tile // columns * tile_height + step // tile_width,
            tile % columns * tile_width + step % tile_width,
        )
        mask_ref[tile * tokens : (tile + 1) * tokens, :] = jnp.where(
            mine == theirs, 0.0, -1e30
        )


def two_heads(pair, scale):
    lane = lax.broadcasted_iota(jnp.int32, pair.shape, 1)
    wide = pair.astype(jnp.float32) * scale
    first = jnp.where(lane < pair.shape[1] // 2, wide, 0.0)
    return jnp.concatenate([first, wide - first], axis=0).astype(jnp.bfloat16)


def own_blocks(both):
    head, tokens = both.shape[0] // 2, both.shape[1] // 2
    return jnp.concatenate([both[:head, :tokens], both[head:, tokens:]], axis=0)


def attend_kernel(
    tile_height, tile_width, cuts, query, pairs, cot, conv_turned, fc2_in,
    out, lse, all_out, spread, out_grad_out, active_grad_out,
    cot_out, held, scores, mask, shift, fc2_weight, out_grad, active_grad, local_sem, send_sem, recv_sem,
    cot_sem, cot_send_sem, cot_recv_sem, side_sem
):
    row_count, tokens, width = query.shape
    tile_count = held.shape[1]
    pair_count = width // 128
    tiles, peers = plane_peers()
    own = tiles["own"]
    fc2_load = pltpu.make_async_copy(fc2_in, fc2_weight, side_sem.at[0])
    fc2_load.start()
    greet([plane_peer(k)[0] for k in range(1, tile_count)])
    cot_copies = [pltpu.make_async_copy(cot, cot_out.at[own], cot_sem.at[0])]
    for k in range(1, tile_count):
        cot_copies.append(
            pltpu.make_async_remote_copy(
                src_ref=cot,
                dst_ref=cot_out.at[own],
                send_sem=cot_send_sem.at[k],
                recv_sem=cot_recv_sem.at[k],
                device_id=plane_peer(k)[0],
                device_id_type=MESH,
            )
        )

    def send(row, slot, source, target, peer):
        copy = pltpu.make_async_remote_copy(
            src_ref=source,
            dst_ref=target,
            send_sem=send_sem.at[row, slot],
            recv_sem=recv_sem.at[row, slot],
            device_id=peer,
            device_id_type=MESH,
        )
        copy.start()
        return copy

    flights = [{} for _ in range(row_count)]

    def begin(row):
        here = held.at[row, own]
        source = pairs.at[row]
        flights[row]["x"] = send(row, 0, source, here, peers["x"])
        flights[row]["y"] = send(row, 1, source, here, peers["y"])
        flights[row]["core"] = send(row, 2, source, here, peers["core"])
        keep = pltpu.make_async_copy(source, here, local_sem.at[row, 0])
        keep.start()
        flights[row]["keep"] = keep

    def forward(row):
        flights[row]["y"].wait_recv()
        key_half = held.at[row, tiles["y"], :, pl.ds(0, width)]
        flights[row]["far_x"] = send(row, 3, key_half, key_half, peers["x"])
        flights[row]["x"].wait_recv()
        value_half = held.at[row, tiles["x"], :, pl.ds(width, width)]
        flights[row]["far_y"] = send(row, 4, value_half, value_half, peers["y"])
        for slot, name in ((5, "x"), (6, "y")):
            tile = held.at[row, tiles[name]]
            flights[row]["core_" + name] = send(row, slot, tile, tile, peers["core"])

    def gather_row(row):
        flights[row]["far_x"].wait_recv()
        flights[row]["far_y"].wait_recv()
        tile = held.at[row, tiles["xy"]]
        last = send(row, 7, tile, tile, peers["core"])
        flights[row]["keep"].wait()
        for name in ("core", "core_x", "core_y"):
            flights[row][name].wait_recv()
        last.wait_recv()
        for name in ("x", "y", "core", "far_x", "far_y", "core_x", "core_y"):
            flights[row][name].wait_send()
        last.wait_send()
        keep = pltpu.make_async_copy(held.at[row], all_out.at[row], local_sem.at[row, 1])
        keep.start()
        flights[row]["out"] = keep

    chunk = 2

    def compute(row):
        fill_mask(mask, cuts, row, tile_height, tile_width)

        def one_pair(p, carry):
            at = pl.ds(pl.multiple_of(p * 128, 128), 128)
            at_value = pl.ds(pl.multiple_of(width + p * 128, 128), 128)
            both = two_heads(query[row, :, at], 0.125)
            peak = None
            for c in range(tile_count // chunk):
                span = slice(c * chunk * tokens, (c + 1) * chunk * tokens)
                keys = held[row, c * chunk : (c + 1) * chunk, :, at].reshape(chunk * tokens, 128)
                extra = mask[span, :]
                part = mm(keys, both, 1, 1) + jnp.concatenate([extra, extra], axis=1)
                scores[span, :] = part
                top = jnp.max(part, axis=0, keepdims=True)
                peak = top if peak is None else jnp.maximum(peak, top)
            total = jnp.zeros_like(peak)
            summed = jnp.zeros((128, 2 * tokens), jnp.float32)
            for c in range(tile_count // chunk):
                span = slice(c * chunk * tokens, (c + 1) * chunk * tokens)
                values = held[row, c * chunk : (c + 1) * chunk, :, at_value].reshape(chunk * tokens, 128)
                part = jnp.exp(scores[span, :] - peak)
                total = total + jnp.sum(part, axis=0, keepdims=True)
                summed = summed + mm(values, part.astype(jnp.bfloat16), 0, 0)
            blocks = own_blocks(summed / total)
            out[row, :, at] = jnp.transpose(blocks).astype(jnp.bfloat16)
            lse[row, p] = peak + jnp.log(total)
            return carry

        lax.fori_loop(0, pair_count, one_pair, 0, unroll=2)

    side_copies = []
    parts = [slice(k * tokens, (k + 1) * tokens) for k in range(row_count)]

    def spread_out():
        patch = cot_out.shape[2]
        turned = jnp.concatenate(
            [cot_out[t].reshape(row_count * patch, tokens) for t in range(tile_count)], axis=1
        )
        moved = mm(turned, shift[...], 1, 0)
        for row in range(row_count):
            for p in range(9):
                piece = moved[row * patch : (row + 1) * patch, p * tokens : (p + 1) * tokens]
                piece = piece * same_image(cuts, row, p, tile_height, tile_width)
                spread[p * patch : (p + 1) * patch, parts[row]] = piece.astype(jnp.bfloat16)
        for at in parts:
            out_grad[at, :] = mm(spread[:, at], conv_turned[...], 0, 0)
        copy = pltpu.make_async_copy(out_grad, out_grad_out, side_sem.at[1])
        copy.start()
        side_copies.append(copy)

    def activate():
        for k in range(fc2_weight.shape[0] // width):
            span = slice(k * width, (k + 1) * width)
            low = out_grad[...].astype(jnp.bfloat16)
            active_grad[:, span] = mm(low, fc2_weight[span, :], 1, 1).astype(jnp.bfloat16)
        copy = pltpu.make_async_copy(active_grad, active_grad_out, side_sem.at[2])
        copy.start()
        side_copies.append(copy)

    begin(0)
    if row_count > 1:
        begin(1)
    for copy in cot_copies:
        copy.start()
    fill_shift(shift, tile_height, tile_width)
    forward(0)
    if row_count > 2:
        begin(2)
    for copy in cot_copies:
        copy.wait()
    spread_out()
    if row_count > 1:
        forward(1)
    fc2_load.wait()
    activate()
    for row in range(row_count):
        if row > 0 and row + 2 < row_count:
            begin(row + 2)
        if row > 0 and row + 1 < row_count:
            forward(row + 1)
        gather_row(row)
        compute(row)
    for row in range(row_count):
        flights[row]["out"].wait()
    for copy in side_copies:
        copy.wait()


def attend(cuts, query, pairs, cot, conv_turned, fc2_weight, tile_height, tile_width):
    row_count, tokens, width = query.shape
    tile_count = lax.axis_size("ty") * lax.axis_size("tx")
    pair_count = width // 128
    low = jnp.bfloat16
    vmem = pl.BlockSpec(memory_space=pltpu.VMEM)
    return pl.pallas_call(
        functools.partial(attend_kernel, tile_height, tile_width),
        out_shape=[
            jax.ShapeDtypeStruct((row_count, tokens, width), low),
            jax.ShapeDtypeStruct((row_count, pair_count, 1, 2 * tokens), jnp.float32),
            jax.ShapeDtypeStruct((row_count, tile_count, tokens, 2 * width), low),
            jax.ShapeDtypeStruct((conv_turned.shape[0], row_count * tokens), low),
            jax.ShapeDtypeStruct((row_count * tokens, width), jnp.float32),
            jax.ShapeDtypeStruct((row_count * tokens, fc2_weight.shape[0]), low),
        ],
        in_specs=[pl.BlockSpec(memory_space=pltpu.SMEM), vmem]
        + [pl.BlockSpec(memory_space=pl.ANY), vmem, vmem, pl.BlockSpec(memory_space=pl.ANY)],
        out_specs=[vmem, vmem, pl.BlockSpec(memory_space=pl.ANY), vmem] + [pl.BlockSpec(memory_space=pl.ANY)] * 2,
        scratch_shapes=[
            pltpu.VMEM((tile_count,) + cot.shape, low),
            pltpu.VMEM((row_count, tile_count, tokens, 2 * width), low),
            pltpu.VMEM((tile_count * tokens, 2 * tokens), jnp.float32),
            pltpu.VMEM((tile_count * tokens, tokens), jnp.float32),
            pltpu.VMEM((tile_count * tokens, 9 * tokens), low),
            pltpu.VMEM(fc2_weight.shape, low),
            pltpu.VMEM((row_count * tokens, width), jnp.float32),
            pltpu.VMEM((row_count * tokens, fc2_weight.shape[0]), low),
            pltpu.SemaphoreType.DMA((row_count, 2)),
            pltpu.SemaphoreType.DMA((row_count, 8)),
            pltpu.SemaphoreType.DMA((row_count, 8)),
            pltpu.SemaphoreType.DMA((1,)),
            pltpu.SemaphoreType.DMA((tile_count,)),
            pltpu.SemaphoreType.DMA((tile_count,)),
            pltpu.SemaphoreType.DMA((3,)),
        ],
        compiler_params=pltpu.CompilerParams(
            collective_id=1, has_side_effects=True, vmem_limit_bytes=full_vmem
        ),
        name="attend",
    )(cuts, query, pairs, cot, conv_turned, fc2_weight)


def attend_back_kernel(
    tile_height, tile_width, kinds, cuts, query_in, attended_in, grad_in, lse_in, conv_in, conv_turned, spread, all_pairs, *refs
):
    count = len(kinds)
    grads, refs = refs[:count], refs[count:]
    (out, conv_grad, conv_out), saved, refs = refs[:3], refs[3 : 3 + count], refs[3 + count :]
    query, attended, grad, lse, row_sem = refs[:5]
    refs = refs[5:]
    held, terms, core_terms, side_terms, mask, shift, taps, part, part_got = refs[:9]
    load_sem, send_sem, recv_sem, part_send_sem, part_recv_sem = refs[9:14]
    items = make_reducers(kinds, grads, saved, refs[14:]) if count else []
    firsts = [item for item in items if item.start == "z"]
    planes = [item for item in items if item.start == "plane"]

    row_count, tokens, width = query.shape
    tile_count = held.shape[1]
    pair_count = width // 128
    tiles, peers = plane_peers()
    low = jnp.bfloat16
    loads = []
    for row in range(row_count):
        load = pltpu.make_async_copy(all_pairs.at[row], held.at[row], load_sem.at[row])
        load.start()
        loads.append([load])
        for k, (source, target) in enumerate(((query_in, query), (attended_in, attended), (grad_in, grad), (lse_in, lse))):
            load = pltpu.make_async_copy(source.at[row], target.at[row], row_sem.at[row, k])
            load.start()
            loads[-1].append(load)
    greet([plane_peer(k)[0] for k in range(1, tile_count)] + (chip_peers()["z"] if count else []))
    core = lax.rem(lax.axis_index("ty"), 2)
    chunk = 2

    def send(row, slot, source, target, peer):
        copy = pltpu.make_async_remote_copy(
            src_ref=source,
            dst_ref=target,
            send_sem=send_sem.at[row, slot],
            recv_sem=recv_sem.at[row, slot],
            device_id=peer,
            device_id_type=MESH,
        )
        copy.start()
        return copy

    def compute(row):
        for load in loads[row]:
            load.wait()
        fill_mask(mask, cuts, row, tile_height, tile_width)

        def one_pair(p, carry):
            at = pl.ds(pl.multiple_of(p * 128, 128), 128)
            at_value = pl.ds(pl.multiple_of(width + p * 128, 128), 128)
            grad_pair = grad[row, :, at]
            both = two_heads(query[row, :, at], 0.125)
            both_grad = two_heads(grad_pair, 1.0)
            inner = jnp.transpose(grad_pair.astype(jnp.float32) * attended[row, :, at].astype(jnp.float32))
            half = inner.shape[0] // 2
            delta = jnp.concatenate(
                [jnp.sum(inner[:half], axis=0, keepdims=True), jnp.sum(inner[half:], axis=0, keepdims=True)], axis=1
            )
            level = lse[row, p]
            query_part = jnp.zeros((128, 2 * tokens), jnp.float32)
            for c in range(tile_count // chunk):
                span = slice(c * chunk * tokens, (c + 1) * chunk * tokens)
                some = slice(c * chunk, (c + 1) * chunk)
                keys = held[row, some, :, at].reshape(chunk * tokens, 128)
                values = held[row, some, :, at_value].reshape(chunk * tokens, 128)
                extra = mask[span, :]
                weights = jnp.exp(mm(keys, both, 1, 1) + jnp.concatenate([extra, extra], axis=1) - level)
                score_grad = (weights * (mm(values, both_grad, 1, 1) - delta)).astype(low)
                value_part = mm(weights.astype(low), both_grad, 1, 0)
                key_part = mm(score_grad, both, 1, 0)
                query_part = query_part + mm(keys, score_grad, 0, 0)
                terms[row, some, :, at] = key_part.astype(low).reshape(chunk, tokens, 128)
                terms[row, some, :, at_value] = value_part.astype(low).reshape(chunk, tokens, 128)
            blocks = own_blocks(query_part) * 0.125
            out[row, :, at] = jnp.transpose(blocks).astype(low)
            return carry

        lax.fori_loop(0, pair_count, one_pair, 0, unroll=2)

    flights = [{} for _ in range(row_count)]
    names = ("own", "x", "y", "xy")
    key_at, value_at = pl.ds(0, width), pl.ds(width, width)

    def begin(row):
        copies = []
        other = 2 - 4 * core
        for k, name in enumerate(names):
            copies.append(send(row, k, terms.at[row, tiles[name] + other], core_terms.at[row, k], peers["core"]))
        flights[row]["core"] = copies

    def add(target, source, row_total):
        def body(i, carry):
            at = pl.ds(pl.multiple_of(i * 16, 16), 16)
            target[at, :] = target[at, :] + source[at, :]
            return carry

        lax.fori_loop(0, row_total // 16, body, 0)

    def scatter(row):
        for k in (3, 1, 2, 0):
            flights[row]["core"][k].wait()
            add(terms.at[row, tiles[names[k]]], core_terms.at[row, k], tokens)
            if k == 3:
                far = terms.at[row, tiles["xy"]]
                flights[row]["far_x"] = send(row, 4, far.at[:, key_at], side_terms.at[row, 0], peers["x"])
                flights[row]["far_y"] = send(row, 5, far.at[:, value_at], side_terms.at[row, 1], peers["y"])
            if k == 1:
                near = terms.at[row, tiles["x"]]
                flights[row]["near_x"] = send(row, 6, near.at[:, key_at], side_terms.at[row, 2], peers["x"])
            if k == 2:
                near = terms.at[row, tiles["y"]]
                flights[row]["near_y"] = send(row, 7, near.at[:, value_at], side_terms.at[row, 3], peers["y"])

    def pass_on(row):
        flights[row]["far_x"].wait()
        near = terms.at[row, tiles["y"], :, key_at]
        add(near, side_terms.at[row, 0], tokens)
        flights[row]["last_y"] = send(row, 8, near, side_terms.at[row, 4], peers["y"])
        flights[row]["far_y"].wait()
        near = terms.at[row, tiles["x"], :, value_at]
        add(near, side_terms.at[row, 1], tokens)
        flights[row]["last_x"] = send(row, 9, near, side_terms.at[row, 5], peers["x"])

    def close(row):
        for name in ("near_x", "near_y", "last_x", "last_y"):
            flights[row][name].wait()
        mine = terms.at[row, tiles["own"]]

        def body(i, carry):
            at = pl.ds(pl.multiple_of(i * 16, 16), 16)
            for start, first, second in ((0, 2, 4), (width, 3, 5)):
                total = mine[at, start : start + width].astype(jnp.float32)
                total = total + side_terms[row, first, at, :].astype(jnp.float32)
                total = total + side_terms[row, second, at, :].astype(jnp.float32)
                out[row, at, width + start : 2 * width + start] = total.astype(low)
            return carry

        lax.fori_loop(0, tokens // 16, body, 0)

    part_copies = []

    def convolve():
        fill_shift(shift, tile_height, tile_width)
        patch = part.shape[2]
        taps[...] = mm(conv_turned[...], conv_in[...], 1, 1)
        rows = []
        for row in range(row_count):
            pieces = []
            for p in range(9):
                piece = taps[p * patch : (p + 1) * patch, row * tokens : (row + 1) * tokens]
                pieces.append(piece * same_image(cuts, row, p, tile_height, tile_width))
            rows.append(jnp.concatenate(pieces, axis=1))
        whole = jnp.concatenate(rows, axis=0)
        coarse = whole.astype(low)
        fine = (whole - coarse.astype(jnp.float32)).astype(low)
        moved = mm(coarse, shift[...], 1, 1) + mm(fine, shift[...], 1, 1)
        for tile in range(tile_count):
            part[tile] = moved[:, tile * tokens : (tile + 1) * tokens].reshape(row_count, patch, tokens)
        for k in range(1, tile_count):
            peer, tile = plane_peer(k)
            copy = pltpu.make_async_remote_copy(
                src_ref=part.at[tile],
                dst_ref=part_got.at[k],
                send_sem=part_send_sem.at[k],
                recv_sem=part_recv_sem.at[k],
                device_id=peer,
                device_id_type=MESH,
            )
            copy.start()
            part_copies.append(copy)
        conv_grad[...] = mm(conv_in[...], spread[...], 0, 1)

    def collect():
        total = part[tiles["own"]]
        for k, copy in enumerate(part_copies):
            copy.wait()
            total = total + part_got[k + 1]
        conv_out[...] = total.astype(low)

    def advance(group, stage):
        for item in group:
            item.stages[stage]()

    for item in items:
        item.begin()
    advance(items[:2], 0)
    for row in range(row_count):
        compute(row)
        begin(row)
        if row == 0:
            advance(items[2:], 0)
        if row > 1:
            pass_on(row - 2)
        if row > 0:
            scatter(row - 1)
            if row < 3:
                advance(planes, row)
    scatter(row_count - 1)
    if row_count > 1:
        pass_on(row_count - 2)
    convolve()
    pass_on(row_count - 1)
    for stage in range(min(row_count, 3), 3):
        advance(planes, stage)
    for row in range(row_count):
        close(row)
    collect()
    advance(planes, 3)
    advance(firsts, 1)
    for item in items:
        item.save()
    for item in items:
        item.land("save")


def attend_back(cuts, query, attended, grad, lse, conv_in, conv_turned, spread, all_pairs, grads, tile_height, tile_width):
    row_count, tokens, width = query.shape
    kinds = tuple((start, paired) for start, paired, _ in grads)
    grads = [entry for _, _, entry in grads]
    count = len(kinds)
    shapes = [(g.shape[1], g.shape[2] if paired else g.shape[2] // 2) for (_, paired), g in zip(kinds, grads)]
    saves = [(r if start == "z" else r // 4, c) for (start, _), (r, c) in zip(kinds, shapes)]
    tile_count = all_pairs.shape[1]
    taps = conv_turned.shape[0]
    low = jnp.bfloat16
    vmem = pl.BlockSpec(memory_space=pltpu.VMEM)
    return pl.pallas_call(
        functools.partial(attend_back_kernel, tile_height, tile_width, kinds),
        out_shape=[
            jax.ShapeDtypeStruct((row_count, tokens, 3 * width), low),
            jax.ShapeDtypeStruct((width, taps), jnp.float32),
            jax.ShapeDtypeStruct((row_count, taps // 9, tokens), low),
        ]
        + [jax.ShapeDtypeStruct(s, low) for s in saves],
        in_specs=[pl.BlockSpec(memory_space=pltpu.SMEM)]
        + [pl.BlockSpec(memory_space=pl.ANY)] * 4
        + [vmem] * 3
        + [pl.BlockSpec(memory_space=pl.ANY)] * (1 + count),
        out_specs=[vmem] * 3 + [pl.BlockSpec(memory_space=pl.ANY)] * count,
        scratch_shapes=[
            pltpu.VMEM(query.shape, low),
            pltpu.VMEM(attended.shape, low),
            pltpu.VMEM(grad.shape, low),
            pltpu.VMEM(lse.shape, jnp.float32),
            pltpu.SemaphoreType.DMA((row_count, 4)),
            pltpu.VMEM((row_count, tile_count, tokens, 2 * width), low),
            pltpu.VMEM((row_count, tile_count, tokens, 2 * width), low),
            pltpu.VMEM((row_count, 4, tokens, 2 * width), low),
            pltpu.VMEM((row_count, 6, tokens, width), low),
            pltpu.VMEM((tile_count * tokens, tokens), jnp.float32),
            pltpu.VMEM((tile_count * tokens, 9 * tokens), low),
            pltpu.VMEM((taps, row_count * tokens), jnp.float32),
            pltpu.VMEM((tile_count, row_count, taps // 9, tokens), jnp.float32),
            pltpu.VMEM((tile_count, row_count, taps // 9, tokens), jnp.float32),
            pltpu.SemaphoreType.DMA((row_count,)),
            pltpu.SemaphoreType.DMA((row_count, 10)),
            pltpu.SemaphoreType.DMA((row_count, 10)),
            pltpu.SemaphoreType.DMA((tile_count,)),
            pltpu.SemaphoreType.DMA((tile_count,)),
        ]
        + (reducer_scratch(kinds, shapes) if count else []),
        compiler_params=pltpu.CompilerParams(
            collective_id=2, has_side_effects=True, vmem_limit_bytes=full_vmem
        ),
        name="attend_back",
    )(cuts, query, attended, grad, lse, conv_in, conv_turned, spread, all_pairs, *grads)


def add_rows(target, first, second, rows):
    def body(i, carry):
        at = pl.ds(pl.multiple_of(i * 16, 16), 16)
        target[at, :] = first[at, :] + second[at, :]
        return carry

    lax.fori_loop(0, rows // 16, body, 0)


def add_four(target, others, rows):
    def body(i, carry):
        at = pl.ds(pl.multiple_of(i * 16, 16), 16)
        total = target[at, :].astype(jnp.float32) + others[0, at, :].astype(jnp.float32)
        total = total + (others[1, at, :].astype(jnp.float32) + others[2, at, :].astype(jnp.float32))
        target[at, :] = total.astype(jnp.bfloat16)
        return carry

    lax.fori_loop(0, rows // 16, body, 0)


def chip_peers():
    z, ty, y = lax.axis_index("rows"), lax.axis_index("ty"), lax.axis_index("tx")
    core, x = lax.rem(ty, 2), ty // 2
    across = (1 - x) * 2 + core
    return {
        "core": (z, x * 2 + 1 - core, y),
        "x": (z, across, y),
        "y": (z, ty, 1 - y),
        "xy": (z, across, 1 - y),
        "z": [(lax.rem(z + k, 4), ty, y) for k in (1, 2, 3)],
    }


class Reducer:
    def __init__(self, start, paired, grad, out, buffers, sems, w):
        self.start, self.paired, self.grad, self.out, self.w = start, paired, grad, out, w
        self.local_sem, self.send_sem, self.recv_sem = sems
        self.z, ty, self.y = lax.axis_index("rows"), lax.axis_index("ty"), lax.axis_index("tx")
        self.core, self.x = lax.rem(ty, 2), ty // 2
        self.peers = chip_peers()
        self.flying = {}
        self.own = buffers[0]
        if start in ("plane", "z"):
            self.half, self.quarter, self.final = buffers[1:4]
            self.got = None if paired else buffers[4]
            self.depth, self.width = grad.shape[1], grad.shape[2] if paired else grad.shape[2] // 2
        else:
            self.depth, self.width = out.shape[1], out.shape[2]
        if start == "block":
            self.half, self.quarter = buffers[1:]
        late = [self.begin_late, self.add_half_late, self.add_quarter_late, self.pass_strip, self.end]
        self.stages = {
            "plane": [self.add_core, self.add_half, self.add_quarter, self.sum_z, self.gather_piece, self.pass_strip, self.end],
            "z": [self.add_core, self.sum_z_first] + late,
            "block": late,
            "piece": [self.gather_piece, self.pass_strip, self.end],
        }[start]

    def part(self, at):
        if self.start == "block":
            return self.own.at[at]
        return self.own.at[self.z, at]

    def send(self, slot, source, target, peer):
        copy = pltpu.make_async_remote_copy(
            src_ref=source,
            dst_ref=target,
            send_sem=self.send_sem.at[self.w, slot],
            recv_sem=self.recv_sem.at[self.w, slot],
            device_id=peer,
            device_id_type=MESH,
        )
        copy.start()
        return copy

    def keep(self, slot, source, target):
        copy = pltpu.make_async_copy(source, target, self.local_sem.at[self.w, slot])
        copy.start()
        return copy

    def land(self, name):
        for copy in self.flying.pop(name):
            copy.wait()

    def columns(self, which):
        return pl.ds(pl.multiple_of(which * self.width, 128), self.width)

    def rows(self, start, size):
        return pl.ds(pl.multiple_of(start, 16), size)

    def place(self, block):
        later = block // 2
        major = self.x + later * (self.y - self.x)
        minor = self.y + later * (self.x - self.y)
        return self.rows(major * (self.depth // 2) + minor * (self.depth // 4), self.depth // 4)

    def begin(self):
        if self.start in ("block", "piece"):
            self.flying["load"] = [self.keep(0, self.grad, self.own)]
            return
        if self.paired:
            self.flying["core"] = [self.keep(0, self.grad, self.own)]
            return
        swap = self.send(0, self.grad.at[:, :, self.columns(1 - self.core)], self.got, self.peers["core"])
        mine = self.keep(0, self.grad.at[:, :, self.columns(self.core)], self.own)
        self.flying["core"] = [swap, mine]

    def add_core(self):
        self.land("core")
        if not self.paired:
            for block in range(4):
                add_rows(self.own.at[block], self.own.at[block], self.got.at[block], self.depth)
        if self.start == "z":
            self.flying["z"] = [
                self.send(5 + k, self.own.at[peer[0]], self.final.at[k], peer) for k, peer in enumerate(self.peers["z"])
            ]
            return
        part = self.depth // 2
        first = self.send(1, self.own.at[0:2, self.rows((1 - self.x) * part, part)], self.half.at[0:2], self.peers["x"])
        second = self.send(2, self.own.at[2:4, self.rows((1 - self.y) * part, part)], self.half.at[2:4], self.peers["y"])
        self.flying["half"] = [first, second]

    def add_half(self):
        self.land("half")
        part, less = self.depth // 2, self.depth // 4
        for block in range(4):
            side = self.x if block < 2 else self.y
            kept = self.own.at[block, self.rows(side * part, part)]
            add_rows(kept, kept, self.half.at[block], part)
        first = self.own.at[0:2, self.rows(self.x * part + (1 - self.y) * less, less)]
        second = self.own.at[2:4, self.rows(self.y * part + (1 - self.x) * less, less)]
        self.flying["quarter"] = [
            self.send(3, first, self.quarter.at[0:2], self.peers["y"]),
            self.send(4, second, self.quarter.at[2:4], self.peers["x"]),
        ]

    def add_quarter(self):
        self.land("quarter")
        for block in range(4):
            kept = self.own.at[block, self.place(block // 2 * 2)]
            add_rows(kept, kept, self.quarter.at[block], self.depth // 4)
        self.flying["z"] = [
            self.send(5 + k, self.own.at[peer[0], self.place(peer[0])], self.final.at[k], peer)
            for k, peer in enumerate(self.peers["z"])
        ]

    def gather(self, pieces, sources):
        copies = []
        for n, (at, source) in enumerate(zip(pieces, sources)):
            target = self.out.at[self.core, at]
            for k, name in enumerate(("x", "y", "xy")):
                copies.append(self.send(8 + 3 * n + k, source, target, self.peers[name]))
            copies.append(self.keep(1 + n, source, target))
        self.flying["gather"] = copies

    def sum_z(self):
        self.land("z")
        add_four(self.own.at[self.z, self.place(self.z)], self.final, self.depth // 4)

    def gather_piece(self):
        if self.start == "piece":
            self.land("load")
            self.gather([self.place(self.z)], [self.own])
        else:
            self.gather([self.place(self.z)], [self.own.at[self.z, self.place(self.z)]])

    def sum_z_first(self):
        self.land("z")
        add_four(self.own.at[self.z], self.final, self.depth)

    def save(self):
        source = self.own.at[self.z] if self.start == "z" else self.own.at[self.z, self.place(self.z)]
        self.flying["save"] = [self.keep(1, source, self.out)]

    def begin_late(self):
        if self.start == "block":
            self.land("load")
        half, less = self.depth // 2, self.depth // 4
        self.flying["half"] = [
            self.send(1, self.part(self.rows((1 - self.x) * less, less)), self.half.at[0], self.peers["x"]),
            self.send(2, self.part(self.rows(half + (1 - self.y) * less, less)), self.half.at[1], self.peers["y"]),
        ]

    def add_half_late(self):
        self.land("half")
        half, less, least = self.depth // 2, self.depth // 4, self.depth // 8
        for n, start in enumerate((self.x * less, half + self.y * less)):
            kept = self.part(self.rows(start, less))
            add_rows(kept, kept, self.half.at[n], less)
        first = self.part(self.rows(self.x * less + (1 - self.y) * least, least))
        second = self.part(self.rows(half + self.y * less + (1 - self.x) * least, least))
        self.flying["quarter"] = [
            self.send(3, first, self.quarter.at[0], self.peers["y"]),
            self.send(4, second, self.quarter.at[1], self.peers["x"]),
        ]

    def add_quarter_late(self):
        self.land("quarter")
        half, less, least = self.depth // 2, self.depth // 4, self.depth // 8
        pieces = [self.rows(self.x * less + self.y * least, least), self.rows(half + self.y * less + self.x * least, least)]
        for n, at in enumerate(pieces):
            add_rows(self.part(at), self.part(at), self.quarter.at[n], least)
        self.gather(pieces, [self.part(at) for at in pieces])

    def pass_strip(self):
        self.land("gather")
        strip = self.out.at[self.core]
        self.flying["strip"] = [self.send(14, strip, strip, self.peers["core"])]

    def end(self):
        self.land("strip")


def reducer_scratch(kinds, shapes):
    buffers = []
    for (start, paired), (depth, half) in zip(kinds, shapes):
        sizes = {
            "plane": [(4, depth, half), (4, depth // 2, half), (4, depth // 4, half), (3, depth // 4, half)],
            "z": [(4, depth, half), (2, depth // 4, half), (2, depth // 8, half), (3, depth, half)],
            "block": [(depth, half), (2, depth // 4, half), (2, depth // 8, half)],
            "piece": [(depth // 4, half)],
        }[start]
        if not paired:
            sizes.append((4, depth, half))
        buffers += [pltpu.VMEM(size, jnp.bfloat16) for size in sizes]
    count = len(kinds)
    return buffers + [
        pltpu.SemaphoreType.DMA((count, 3)),
        pltpu.SemaphoreType.DMA((count, 15)),
        pltpu.SemaphoreType.DMA((count, 15)),
    ]


def make_reducers(kinds, grads, outs, scratch):
    items, at = [], 0
    for w, ((start, paired), grad, out) in enumerate(zip(kinds, grads, outs)):
        size = {"plane": 4, "z": 4, "block": 3, "piece": 1}[start] + (0 if paired else 1)
        items.append(Reducer(start, paired, grad, out, scratch[at : at + size], scratch[-3:], w))
        at = at + size
    return items


def sum_by_table(local_grads):
    band_count, column_count = lax.axis_size("ty"), lax.axis_size("tx")
    group_count = lax.axis_size("rows")
    tile_count = band_count * column_count
    table = jnp.concatenate([entry.reshape(group_count, -1) for entry in local_grads], axis=1)
    column_total = table.shape[1]
    padded_columns = -(-column_total // tile_count) * tile_count
    piece_width = padded_columns // tile_count
    table = table.reshape(group_count, tile_count, piece_width)
    shares = lax.psum_scatter(
        table.reshape(group_count * tile_count, piece_width),
        ("rows", "ty", "tx"),
        scatter_dimension=0,
        tiled=True,
    )
    summed = (
        lax.all_gather(shares.astype(jnp.bfloat16), ("ty", "tx"), axis=0, tiled=True)
        .astype(shares.dtype)
        .reshape(-1)
    )
    totals = []
    start_at = 0
    for entry in local_grads:
        length = entry.size // group_count
        shard_shape = (entry.shape[0] // group_count,) + entry.shape[1:]
        totals.append(summed[start_at : start_at + length].reshape(shard_shape))
        start_at = start_at + length
    return tuple(totals)


def shards(
    latent,
    skip_input,
    segment_ids,
    embed_weight,
    embed_bias,
    skip_weight,
    skip_bias,
    norm1_gain,
    norm1_bias,
    qkv_weight,
    proj_weight,
    proj_bias,
    norm2_gain,
    norm2_bias,
    fc1_weight,
    fc1_bias,
    fc2_weight,
    fc2_bias,
    conv_weight,
    cotangent,
):
    row_count, tile_height, tile_width, width = skip_input.shape
    patch = latent.shape[3]
    tokens = tile_height * tile_width
    token_count = row_count * tokens
    low = jnp.bfloat16
    wide = jnp.float32
    conv_turned = conv_weight.T
    flat_latent = latent.reshape(token_count, patch)
    flat_skip = skip_input.reshape(token_count, width)
    biases = (embed_bias, skip_bias, norm1_gain, norm1_bias, proj_bias, norm2_gain, norm2_bias, fc2_bias)
    embedded, stream, normed, query, pairs, cot, vectors, hidden_bias, cuts = front(
        segment_ids, flat_latent, cotangent.reshape(token_count, patch), embed_weight.T, biases, fc1_bias,
        flat_skip, skip_weight, qkv_weight, row_count,
    )
    attended, log_total, row_pairs, spread, out_grad, active_grad = attend(
        cuts, query, pairs, cot, conv_turned, fc2_weight, tile_height, tile_width
    )
    here = (lax.axis_size("rows"), lax.axis_size("ty"), lax.axis_size("tx")) == (4, 4, 2)
    fc1_grad, fc2_grad, hidden_bias_grad, proj_grad, attended_grad, mid_grad, conv_in, middle_grads = middle(
        attended.reshape(token_count, width), stream, out_grad, active_grad, proj_weight, vectors, hidden_bias,
        fc1_weight, fc2_weight, here,
    )
    early = []
    if here:
        early = [
            ("plane", True, fc1_grad),
            ("z", True, fc2_grad.reshape(4, -1, width // 2)),
            ("plane", False, proj_grad.reshape(4, -1, width)),
        ]
    projected_grad, conv_grad, conv_out, *saved = attend_back(
        cuts, query, attended, attended_grad.reshape(row_count, tokens, width), log_total,
        conv_in, conv_turned, spread, row_pairs, early, tile_height, tile_width,
    )
    follow = {"plane": "piece", "z": "block"}
    resumed = [
        (follow[start], entry, (grad.shape[1], entry.shape[1])) for (start, _, grad), entry in zip(early, saved)
    ]
    skip_input_grad, *rest = rear(
        projected_grad.reshape(token_count, 3 * width), qkv_weight, normed, stream, mid_grad, embedded, flat_skip,
        skip_weight, flat_latent, vectors, middle_grads, hidden_bias_grad, conv_grad, resumed, here,
    )
    skip_input_grad = skip_input_grad.reshape(row_count, tile_height, tile_width, width)
    taps = 9 * patch
    share = width // 4
    if here:
        totals = finish(rest[:5], rest[5], rest[6], conv_out)
        fc1_total, fc2_total, proj_total, qkv_total, skip_total, embed_turned, conv_grad_turned = totals[:7]
        line, fc1_line = totals[7:15], totals[15]
        output = totals[16].reshape(row_count, tile_height, tile_width, patch)
        return (
            output, skip_input_grad, embed_turned.T, line[0], skip_total, line[1], line[2], line[3], qkv_total,
            proj_total, line[4], line[5], line[6], fc1_total, fc1_line, fc2_total, line[7], conv_grad_turned.T,
        )
    output = conv_out.transpose(0, 2, 1).reshape(row_count, tile_height, tile_width, patch)
    qkv_grad, skip_grad, thin = [entry.reshape(-1, entry.shape[2]) for entry in rest[:3]]
    flat = rest[3]
    fc1_grad = fc1_grad.reshape(width, -1)
    line = [flat[:, k, :share].reshape(-1) for k in range(8)]
    fc1_line = flat[:, 8:11].reshape(-1)
    local_grads = [
        thin[:, taps : taps + patch], line[0], skip_grad, line[1], line[2], line[3], qkv_grad, proj_grad, line[4],
        line[5], line[6], fc1_grad, fc1_line, fc2_grad, line[7], thin[:, :taps],
    ]
    return (output, skip_input_grad) + sum_by_table([entry.astype(wide) for entry in local_grads])


def solution(mesh):
    return jax.shard_map(
        shards,
        mesh=mesh,
        in_specs=(
            P("rows", "ty", "tx", None),
            P("rows", "ty", "tx", None),
            P("rows", None, None),
            P(),
            P(),
            P(),
            P(),
            P(),
            P(),
            P(),
            P(),
            P(),
            P(),
            P(),
            P(),
            P(),
            P(),
            P(),
            P(),
            P("rows", "ty", "tx", None),
        ),
        out_specs=(
            P("rows", "ty", "tx", None),
            P("rows", "ty", "tx", None),
            P("rows", None),
            P("rows"),
            P("rows", None),
            P("rows"),
            P("rows"),
            P("rows"),
            P("rows", None),
            P("rows", None),
            P("rows"),
            P("rows"),
            P("rows"),
            P("rows", None),
            P("rows"),
            P("rows", None),
            P("rows"),
            P("rows", None),
        ),
        check_vma=False,
    )
```

```python
import functools

import jax
import jax.numpy as jnp
from jax import lax
from jax.experimental import pallas as pl
from jax.experimental.pallas import tpu as pltpu
from jax.sharding import PartitionSpec as P

MESH = pl.DeviceIdType.MESH
norm_eps = 1e-05
full_vmem = 62 * 1024 * 1024


def cell_of(token, tile, tile_height, tile_width, columns):
    down = tile // columns * tile_height + token // tile_width
    across = tile % columns * tile_width + token % tile_width
    return down, across


def fill_shift(shift_ref, tile_height, tile_width):
    tokens = tile_height * tile_width
    bands, columns = lax.axis_size("ty"), lax.axis_size("tx")
    own = lax.axis_index("ty") * columns + lax.axis_index("tx")
    lane = lax.broadcasted_iota(jnp.int32, (8, tokens), 1)
    down, across = cell_of(lane, own, tile_height, tile_width, columns)
    step = lax.broadcasted_iota(jnp.int32, (shift_ref.shape[0], tokens), 0)
    for p in range(9):
        i, j = down - (p // 3 - 1), across - (p % 3 - 1)
        inside = (i >= 0) & (i < bands * tile_height) & (j >= 0) & (j < columns * tile_width)
        tile = i // tile_height * columns + j // tile_width
        place = tile * tokens + i % tile_height * tile_width + j % tile_width
        place = jnp.where(inside, place, -1)[0:1]
        chosen = jnp.where(step == place, 1.0, 0.0)
        shift_ref[:, p * tokens : (p + 1) * tokens] = chosen.astype(jnp.bfloat16)


def same_image(cuts_ref, row, p, tile_height, tile_width):
    tokens = tile_height * tile_width
    columns = lax.axis_size("tx")
    own = lax.axis_index("ty") * columns + lax.axis_index("tx")
    lane = lax.broadcasted_iota(jnp.int32, (8, tokens), 1)
    down, across = cell_of(lane, own, tile_height, tile_width, columns)
    left_width, top_height = cuts_ref[row, 0], cuts_ref[row, 1]

    def image_of(i, j):
        return jnp.where(j < left_width, 0, jnp.where(i < top_height, 1, 2))

    there = image_of(down - (p // 3 - 1), across - (p % 3 - 1))
    return jnp.where(image_of(down, across) == there, 1.0, 0.0)[0:1]


def mm(former, latter, axis_former, axis_latter):
    return lax.dot_general(
        former,
        latter,
        (((axis_former,), (axis_latter,)), ((), ())),
        preferred_element_type=jnp.float32,
    )


def normalised(values):
    average = jnp.mean(values, axis=1, keepdims=True)
    centred = values - average
    rate = lax.rsqrt(jnp.mean(centred * centred, axis=1, keepdims=True) + norm_eps)
    return centred * rate, rate


def norm_back(incoming, unit, rate, gain):
    scaled = incoming * gain
    first = jnp.mean(scaled, axis=1, keepdims=True)
    second = jnp.mean(scaled * unit, axis=1, keepdims=True)
    return (scaled - first - unit * second) * rate


def down_sum(values):
    return jnp.sum(values, axis=0, keepdims=True)


def front_kernel(
    segment_ids, latent, cotangent, embed_turned, *refs
):
    biases, fc1_bias, refs = refs[:8], refs[8], refs[9:]
    skip_in, skip_weight_in, qkv_in, embedded, stream, normed, query, pairs, cot, vectors, hidden_bias, cuts = refs[:12]
    skip, skip_weight, qkv_weight, load_sem = refs[12:]
    sources, targets = (skip_weight_in, skip_in, qkv_in), (skip_weight, skip, qkv_weight)
    loads = [pltpu.make_async_copy(a, b, load_sem.at[k]) for k, (a, b) in enumerate(zip(sources, targets))]
    for load in loads:
        load.start()
    for k, bias in enumerate(biases):
        vectors[k : k + 1] = bias[...].reshape(1, bias.shape[0]).astype(jnp.float32)
    line = fc1_bias[...].reshape(1, fc1_bias.shape[0]).astype(jnp.float32)
    block = hidden_bias.shape[2]
    for k in range(hidden_bias.shape[0]):
        hidden_bias[k] = line[:, k * block : (k + 1) * block]
    width = skip.shape[1]
    row_count, tokens = query.shape[1], query.shape[2]
    side = segment_ids.shape[1]
    for row in range(row_count):

        def count(k, carry):
            left, top = carry
            left = left + jnp.where(segment_ids[row, 0, k] == 0, 1, 0)
            top = top + jnp.where(segment_ids[row, k, side - 1] == 1, 1, 0)
            return left, top

        left, top = lax.fori_loop(0, side, count, (jnp.int32(0), jnp.int32(0)), unroll=8)
        cuts[row, 0] = left
        cuts[row, 1] = top
        at = slice(row * tokens, (row + 1) * tokens)
        cot[row] = jnp.transpose(cotangent[at, :].astype(jnp.float32)).astype(jnp.bfloat16)
        embedded[at, :] = (mm(latent[at, :], embed_turned[...], 1, 0) + vectors[0:1]).astype(jnp.bfloat16)
    loads[0].wait()
    loads[1].wait()
    total = mm(embedded[...], skip_weight[:width], 1, 0) + mm(skip[...], skip_weight[width:], 1, 0) + vectors[1:2]
    stream[...] = total
    unit, rate = normalised(total)
    normed[...] = (unit * vectors[2:3] + vectors[3:4]).astype(jnp.bfloat16)
    loads[2].wait()
    half = width // 2
    for k in range(3):
        piece = mm(normed[...], qkv_weight[:, k * width : (k + 1) * width], 1, 0).astype(jnp.bfloat16)
        for g in range(2):
            part = piece[:, g * half : (g + 1) * half].reshape(row_count, tokens, half)
            if k == 0:
                query[g] = part
            else:
                pairs[g, :, :, (k - 1) * half : k * half] = part


def front(segment_ids, latent, cotangent, embed_turned, biases, fc1_bias, skip, skip_weight, qkv_weight, row_count):
    token_count, width = skip.shape
    tokens = token_count // row_count
    low, wide = jnp.bfloat16, jnp.float32
    smem, vmem = pl.BlockSpec(memory_space=pltpu.SMEM), pl.BlockSpec(memory_space=pltpu.VMEM)
    return pl.pallas_call(
        front_kernel,
        out_shape=[
            jax.ShapeDtypeStruct((token_count, width), low),
            jax.ShapeDtypeStruct((token_count, width), wide),
            jax.ShapeDtypeStruct((token_count, width), low),
            jax.ShapeDtypeStruct((2, row_count, tokens, width // 2), low),
            jax.ShapeDtypeStruct((2, row_count, tokens, width), low),
            jax.ShapeDtypeStruct((row_count, cotangent.shape[1], tokens), low),
            jax.ShapeDtypeStruct((8, width), wide),
            jax.ShapeDtypeStruct((fc1_bias.shape[0] // width, 1, width), wide),
            jax.ShapeDtypeStruct((row_count, 2), jnp.int32),
        ],
        in_specs=[smem] + [vmem] * 12 + [pl.BlockSpec(memory_space=pl.ANY)] * 3,
        out_specs=[vmem] * 8 + [smem],
        scratch_shapes=[pltpu.VMEM(entry.shape, low) for entry in (skip, skip_weight, qkv_weight)]
        + [pltpu.SemaphoreType.DMA((3,))],
        compiler_params=pltpu.CompilerParams(vmem_limit_bytes=full_vmem),
        name="front",
    )(segment_ids, latent, cotangent, embed_turned, *biases, fc1_bias, skip, skip_weight, qkv_weight)


def erf_of(values):
    x = jnp.clip(values, -4.0, 4.0)
    square = x * x
    upper = square * -2.72614225801306e-10 + 2.77068142495902e-08
    for term in (-2.10102402082508e-06, -5.69250639462346e-05, -7.34990630326855e-04, -2.95459980854025e-03, -1.60960333262415e-02):
        upper = upper * square + term
    lower = square * -1.45660718464996e-05 + -2.13374055278905e-04
    for term in (-1.68282697438203e-03, -7.37332916720468e-03, -1.42647390514189e-02):
        lower = lower * square + term
    return x * upper / lower


def middle_kernel(
    paired, attended, stream, out_grad, proj_weight, vectors, hidden_bias, active_grad, fc1_weight, fc2_weight,
    fc1_out, fc2_out, hidden_bias_grad, proj_grad, attended_grad, mid_grad, conv_in, vector_grads,
    middle, normed, out_low, forward_sum, backward_sum, grad1, grad2, *refs
):
    step = pl.program_id(0)
    last = fc2_out.shape[0] // fc2_weight.shape[0] - 1
    token_count, width = stream.shape
    block = fc1_weight.shape[1]
    low = jnp.bfloat16
    parts = [slice(0, token_count)]
    store_sem = refs[-1]
    if paired:
        got1, got2, total1, total2, send_sem, recv_sem = refs[:6]
        z, ty, y = lax.axis_index("rows"), lax.axis_index("ty"), lax.axis_index("tx")
        core = lax.rem(ty, 2)
        peer = (z, ty + 1 - 2 * core, y)

    def stores(k):
        slot = lax.rem(k, 2)
        first, second = (total1, total2) if paired else (grad1, grad2)
        across = first.shape[3]
        down = second.shape[1]
        return [
            pltpu.make_async_copy(
                first.at[slot], fc1_out.at[:, :, pl.ds(pl.multiple_of(k * across, 128), across)], store_sem.at[slot, 0]
            ),
            pltpu.make_async_copy(
                second.at[slot], fc2_out.at[pl.ds(pl.multiple_of(k * down, 16), down)], store_sem.at[slot, 1]
            ),
        ]

    def swaps(k):
        slot = lax.rem(k, 2)
        theirs1 = pl.ds(pl.multiple_of((1 - core) * (block // 2), 128), block // 2)
        theirs2 = pl.ds(pl.multiple_of((1 - core) * (width // 2), 128), width // 2)
        pairs = ((grad1.at[slot, :, :, theirs1], got1.at[k]), (grad2.at[slot, :, theirs2], got2.at[k]))
        return [
            pltpu.make_async_remote_copy(
                src_ref=source,
                dst_ref=target,
                send_sem=send_sem.at[k, n],
                recv_sem=recv_sem.at[k, n],
                device_id=peer,
                device_id_type=MESH,
            )
            for n, (source, target) in enumerate(pairs)
        ]

    def settle(k):
        slot = lax.rem(k, 2)
        if paired:
            for copy in swaps(k):
                copy.wait()

            @pl.when(k >= 2)
            def _():
                for copy in stores(k - 2):
                    copy.wait()

            mine1 = pl.ds(pl.multiple_of(core * (block // 2), 128), block // 2)
            mine2 = pl.ds(pl.multiple_of(core * (width // 2), 128), width // 2)
            total1[slot] = grad1[slot, :, :, mine1] + got1[k]
            total2[slot] = grad2[slot, :, mine2] + got2[k]
        for copy in stores(k):
            copy.start()

    @pl.when(step == 0)
    def _():
        if paired:
            greet([peer])
        total = jnp.zeros((1, width), jnp.float32)
        for at in parts:
            grad = out_grad[at, :]
            out_low[at, :] = grad.astype(low)
            total = total + down_sum(grad)
            value = stream[at, :] + vectors[4:5]
            for k in range(2):
                value = value + mm(attended[k], proj_weight[k * width // 2 : (k + 1) * width // 2], 1, 0)
            middle[at, :] = value
            unit, rate = normalised(value)
            normed[at, :] = (unit * vectors[5:6] + vectors[6:7]).astype(low)
        vector_grads[7:8] = total
        forward_sum[...] = jnp.zeros_like(forward_sum)
        backward_sum[...] = jnp.zeros_like(backward_sum)

    slot = lax.rem(step, 2)
    if not paired:

        @pl.when(step >= 2)
        def _():
            for copy in stores(step - 2):
                copy.wait()

    bias_grad = jnp.zeros((1, block), jnp.float32)
    actives, hidden_lows = [], []
    for at in parts:
        hidden = mm(normed[at, :], fc1_weight[...], 1, 0) + hidden_bias[0]
        share = 0.5 + 0.5 * erf_of(hidden * 0.7071067811865476)
        density = jnp.exp(hidden * hidden * -0.5) * 0.3989422804014327
        active = (hidden * share).astype(low)
        hidden_grad = active_grad[at, :].astype(jnp.float32) * (share + hidden * density)
        bias_grad = bias_grad + down_sum(hidden_grad)
        hidden_low = hidden_grad.astype(low)
        forward_sum[at, :] = forward_sum[at, :] + mm(active, fc2_weight[...], 1, 0)
        backward_sum[at, :] = backward_sum[at, :] + mm(hidden_low, fc1_weight[...], 1, 1)
        actives.append(active)
        hidden_lows.append(hidden_low)
    hidden_bias_grad[0] = bias_grad
    grad2[slot] = mm(jnp.concatenate(actives, axis=0), out_low[...], 0, 0).astype(low)
    grad1[slot] = mm(normed[...], jnp.concatenate(hidden_lows, axis=0), 0, 0).astype(low).reshape(grad1.shape[1:])
    if paired:
        for copy in swaps(step):
            copy.start()

        @pl.when(step > 0)
        def _():
            settle(step - 1)
    else:
        settle(step)

    @pl.when(step == last)
    def _():
        gain_sum = jnp.zeros((1, width), jnp.float32)
        bias_sum = jnp.zeros((1, width), jnp.float32)
        mid_sum = jnp.zeros((1, width), jnp.float32)
        lows = []
        for at in parts:
            unit, rate = normalised(middle[at, :])
            conv_in[at, :] = (middle[at, :] + forward_sum[at, :] + vectors[7:8]).astype(low)
            incoming = backward_sum[at, :]
            gain_sum = gain_sum + down_sum(incoming * unit)
            bias_sum = bias_sum + down_sum(incoming)
            grad = out_grad[at, :] + norm_back(incoming, unit, rate, vectors[5:6])
            mid_grad[at, :] = grad
            mid_sum = mid_sum + down_sum(grad)
            mid_low = grad.astype(low)
            lows.append(mid_low)
            for k in range(2):
                attended_grad[k] = mm(mid_low, proj_weight[k * width // 2 : (k + 1) * width // 2], 1, 1).astype(low)
        for k in range(2):
            proj_grad[k * width // 2 : (k + 1) * width // 2] = mm(attended[k], lows[0], 0, 0).astype(low)
        vector_grads[4:5] = mid_sum
        vector_grads[5:6] = gain_sum
        vector_grads[6:7] = bias_sum
        if paired:
            settle(step)
        for k in (last - 1, last):
            for copy in stores(k):
                copy.wait()


def middle(attended, stream, out_grad, active_grad, proj_weight, vectors, hidden_bias, fc1_weight, fc2_weight, paired):
    token_count, width = stream.shape
    hidden_width = fc1_weight.shape[1]
    steps, _, block = hidden_bias.shape
    low, wide = jnp.bfloat16, jnp.float32
    cut = 2 if paired else 1
    vmem, anywhere = pl.BlockSpec(memory_space=pltpu.VMEM), pl.BlockSpec(memory_space=pl.ANY)
    scratch = [
        pltpu.VMEM((token_count, width), wide),
        pltpu.VMEM((token_count, width), low),
        pltpu.VMEM((token_count, width), low),
        pltpu.VMEM((token_count, width), wide),
        pltpu.VMEM((token_count, width), wide),
        pltpu.VMEM((2, 4, width // 4, block), low),
        pltpu.VMEM((2, block, width), low),
    ]
    if paired:
        scratch += [
            pltpu.VMEM((steps, 4, width // 4, block // 2), low),
            pltpu.VMEM((steps, block, width // 2), low),
            pltpu.VMEM((2, 4, width // 4, block // 2), low),
            pltpu.VMEM((2, block, width // 2), low),
            pltpu.SemaphoreType.DMA((steps, 2)),
            pltpu.SemaphoreType.DMA((steps, 2)),
        ]
        params = pltpu.CompilerParams(collective_id=4, has_side_effects=True, vmem_limit_bytes=full_vmem)
    else:
        params = pltpu.CompilerParams(vmem_limit_bytes=full_vmem)
    return pl.pallas_call(
        functools.partial(middle_kernel, paired),
        grid=(steps,),
        out_shape=[
            jax.ShapeDtypeStruct((4, width // 4, hidden_width // cut), low),
            jax.ShapeDtypeStruct((hidden_width, width // cut), low),
            jax.ShapeDtypeStruct((steps, 1, block), wide),
            jax.ShapeDtypeStruct((width, width), low),
            jax.ShapeDtypeStruct((2, token_count, width // 2), low),
            jax.ShapeDtypeStruct((token_count, width), wide),
            jax.ShapeDtypeStruct((token_count, width), low),
            jax.ShapeDtypeStruct((8, width), wide),
        ],
        in_specs=[vmem] * 5
        + [
            pl.BlockSpec((1, 1, block), lambda k: (k, 0, 0)),
            pl.BlockSpec((token_count, block), lambda k: (0, k)),
            pl.BlockSpec((width, block), lambda k: (0, k)),
            pl.BlockSpec((block, width), lambda k: (k, 0)),
        ],
        out_specs=[anywhere, anywhere, pl.BlockSpec((1, 1, block), lambda k: (k, 0, 0))] + [vmem] * 5,
        scratch_shapes=scratch + [pltpu.SemaphoreType.DMA((2, 2))],
        compiler_params=params,
        name="middle",
    )(attended, stream, out_grad, proj_weight, vectors, hidden_bias, active_grad, fc1_weight, fc2_weight)


rear_order = (
    "+proj", "+fc2b", "+fc2a", "grad0", "grad1", "grad2", "+qkv0", "+qkv2", "norm", "+qkv0", "+qkv1", "skip",
    "+qkv0", "+qkv2", "+skip", "joined", "+qkv2", "+thin", "+proj", "+qkv1", "+skip", "+thin", "+qkv1", "+fc1",
    "=qkv0", "+fc2b", "+proj", "+skip", "+flat", "+thin", "+fc2a", "=qkv1", "=qkv2", "+qkv0", "+fc1", "+qkv1",
    "+fc2a", "+flat", "+fc2b", "+qkv2", "=skip", "+qkv1", "+fc2a", "+proj", "+fc2b", "+flat", "+qkv0", "+fc1",
    "input", "+qkv0", "=thin", "=flat", "+fc1", "+qkv1", "+qkv2", "+skip", "+fc2a", "+thin", "+flat", "+qkv2",
    "+fc2a", "+flat", "+skip", "+thin",
)


def rear_kernel(
    kinds, reduces, projected_in, qkv_in, normed_in, stream_in, mid_in, embedded_in, skip_in, skip_weight_in,
    latent, vectors, middle_grads, hidden_bias_grad, conv_grad, *refs
):
    count = len(kinds)
    resumed, refs = refs[:count], refs[count:]
    skip_input_grad, refs = refs[0], refs[1:]
    if reduces:
        sums, refs = refs[: count + 6], refs[count + 6 :]
        peers = chip_peers()
    grads, refs = refs[:6], refs[6:]
    skip_grad, thin, flat = grads[3:]
    projected_grad, qkv_weight, normed, stream, mid_grad, embedded, skip, skip_weight, stream_low, load_sem = refs[:10]
    sources = (projected_in, normed_in, qkv_in, stream_in, mid_in, embedded_in, skip_in, skip_weight_in)
    targets = (projected_grad, normed, qkv_weight, stream, mid_grad, embedded, skip, skip_weight)
    loads = [pltpu.make_async_copy(a, b, load_sem.at[k]) for k, (a, b) in enumerate(zip(sources, targets))]
    for load in loads[:3]:
        load.start()
    named = {}
    if reduces:
        items = make_reducers(kinds + (("plane", False),) * 6, resumed + grads, sums, refs[10:], range(count + 3))
        named = dict(zip(("fc1", "fc2a", "fc2b", "proj", "qkv0", "qkv1", "qkv2", "skip", "thin", "flat"), items))
        greet([peers[name] for name in ("core", "x", "y", "xy")] + peers["z"])
        for item in items[:count]:
            item.begin()
    for load in loads[3:]:
        load.start()
    width = stream.shape[1]
    low = jnp.bfloat16
    made = {}

    def open_up(*names):
        for name in names:
            if reduces:
                named[name].begin()

    def weight_grad(k):
        if k == 0:
            loads[0].wait()
            loads[1].wait()
        piece = mm(normed[...], projected_grad[:, k * width : (k + 1) * width], 0, 0)
        grads[k][...] = piece.astype(low).reshape(grads[k].shape)
        open_up(f"qkv{k}")

    def norm():
        for load in loads[2:5]:
            load.wait()
        incoming = mm(projected_grad[...], qkv_weight[...], 1, 1)
        unit, rate = normalised(stream[...])
        grad = mid_grad[...] + norm_back(incoming, unit, rate, vectors[2:3])
        made["rows"] = [down_sum(grad), down_sum(incoming * unit), down_sum(incoming)]
        stream_low[...] = grad.astype(low)

    def skip_weight_grad():
        loads[5].wait()
        loads[6].wait()
        skip_grad[0:2] = mm(embedded[...], stream_low[...], 0, 0).astype(low).reshape(2, width // 2, width)
        skip_grad[2:4] = mm(skip[...], stream_low[...], 0, 0).astype(low).reshape(2, width // 2, width)
        open_up("skip")

    def joined():
        loads[7].wait()
        embed_grad = mm(stream_low[...], skip_weight[:width], 1, 1)
        embed_weight_grad = mm(embed_grad.astype(low), latent[...], 0, 0)
        rest = jnp.zeros((width, 128 - 2 * 16), jnp.float32)
        thin[:, :, :128] = conv_grad[:, :128].astype(low).reshape(4, width // 4, 128)
        edge = jnp.concatenate([conv_grad[:, 128:144], embed_weight_grad, rest], axis=1)
        thin[:, :, 128:] = edge.astype(low).reshape(4, width // 4, 128)
        rows = [down_sum(embed_grad)] + made["rows"] + [middle_grads[k : k + 1] for k in range(4, 8)]
        stack = jnp.concatenate(rows, axis=0)
        share = width // 4
        hidden_line = jnp.concatenate([hidden_bias_grad[k] for k in range(hidden_bias_grad.shape[0])], axis=1)
        for block in range(4):
            own = stack[:, block * share : (block + 1) * share]
            own = jnp.concatenate([own, jnp.zeros((8, 256 - share), jnp.float32)], axis=1)
            line = hidden_line[:, block * width : (block + 1) * width]
            pieces = [line[:, k * 256 : (k + 1) * 256] for k in range(width // 256)]
            body = jnp.concatenate([own] + pieces + [jnp.zeros((8 - len(pieces), 256), jnp.float32)], axis=0)
            flat[block, 0:16] = body.astype(low)
            flat[block, 16:64] = jnp.zeros((48, 256), low)
        open_up("thin", "flat")

    def input_grad():
        skip_input_grad[...] = mm(stream_low[...], skip_weight[width:], 1, 1).astype(low)

    acts = {"norm": norm, "skip": skip_weight_grad, "joined": joined, "input": input_grad}
    for entry in rear_order:
        if entry[0] in "+=":
            if reduces:
                named[entry[1:]].step()
                if entry[0] == "=":
                    named[entry[1:]].step()
        elif entry[:-1] == "grad":
            weight_grad(int(entry[-1]))
        else:
            acts[entry]()
    assert not any(item.stages for item in named.values())


def rear(projected_grad, qkv_weight, normed, stream, mid_grad, embedded, skip, skip_weight, latent, vectors, middle_grads, hidden_bias_grad, conv_grad, resumed, reduces):
    token_count, width = stream.shape
    low = jnp.bfloat16
    kinds = tuple((start, True) for start, _, _ in resumed)
    sizes = [(width // 4, width)] * 3 + [(width // 2, width), (width // 4, 256), (64, 256)]
    totals = [shape for _, _, shape in resumed] + [(r, c // 2) for r, c in sizes]
    vmem, anywhere = pl.BlockSpec(memory_space=pltpu.VMEM), pl.BlockSpec(memory_space=pl.ANY)
    big = [projected_grad, qkv_weight, normed, stream, mid_grad, embedded, skip, skip_weight]
    out_shape = [jax.ShapeDtypeStruct((token_count, width), low)]
    out_specs = [vmem]
    scratch = []
    if reduces:
        out_shape += [jax.ShapeDtypeStruct((2,) + shape, low) for shape in totals]
        out_specs += [anywhere] * len(totals)
        scratch += [pltpu.VMEM((4,) + shape, low) for shape in sizes]
        params = pltpu.CompilerParams(collective_id=3, has_side_effects=True, vmem_limit_bytes=full_vmem)
    else:
        out_shape += [jax.ShapeDtypeStruct((4,) + shape, low) for shape in sizes]
        out_specs += [vmem] * len(sizes)
        params = pltpu.CompilerParams(vmem_limit_bytes=full_vmem)
    scratch += [pltpu.VMEM(entry.shape, entry.dtype) for entry in big]
    scratch += [pltpu.VMEM((token_count, width), low), pltpu.SemaphoreType.DMA((len(big),))]
    if reduces:
        scratch += reducer_scratch(kinds + (("plane", False),) * 6, totals)
    return pl.pallas_call(
        functools.partial(rear_kernel, kinds, reduces),
        out_shape=out_shape,
        in_specs=[anywhere] * len(big) + [vmem] * 5 + [anywhere] * len(kinds),
        out_specs=out_specs,
        scratch_shapes=scratch,
        compiler_params=params,
        name="rear",
    )(*big, latent, vectors, middle_grads, hidden_bias_grad, conv_grad, *[entry for _, entry, _ in resumed])


def finish_kernel(patch, plan, *refs):
    count = len(plan)
    sums, (thin, flat, conv_out) = refs[:count], refs[count : count + 3]
    totals, refs = refs[count + 3 : count + 8], refs[count + 8 :]
    (embed_turned, conv_turned), lines, fc1_line, output, refs = refs[:2], refs[2:10], refs[10], refs[11], refs[12:]
    lows, wides, load_sem, store_sem = refs[:count], refs[count : count + 5], refs[count + 5], refs[count + 6]
    loads = [pltpu.make_async_copy(a, b, load_sem.at[k]) for k, (a, b) in enumerate(zip(sums, lows))]
    for load in loads:
        load.start()
    stores = []
    for k, (low, (which, start, piece, left)) in enumerate(zip(lows, plan)):
        loads[k].wait()
        wide = wides[which]
        half, depth = low.shape[2], low.shape[1]

        def body(i, carry):
            at = pl.ds(pl.multiple_of(i * 16, 16), 16)
            to = pl.ds(pl.multiple_of(start + i * 16, 16), 16)
            for core in range(2):
                for n in range(half // piece):
                    column = left + (2 * n + core) * piece
                    wide[to, column : column + piece] = low[core, at, n * piece : (n + 1) * piece].astype(jnp.float32)
            return carry

        lax.fori_loop(0, depth // 16, body, 0)
        there = (pl.ds(start, depth), pl.ds(left, 2 * half))
        store = pltpu.make_async_copy(wide.at[there], totals[which].at[there], store_sem.at[k])
        store.start()
        stores.append(store)
    share = thin.shape[1]
    turned = jnp.transpose(jnp.concatenate([thin[0], thin[1]], axis=1).astype(jnp.float32))
    taps = 9 * patch
    conv_turned[...] = turned[:taps]
    embed_turned[...] = turned[taps : taps + patch]
    rows = jnp.concatenate([flat[0, 0:16, :], flat[1, 0:16, :]], axis=1).astype(jnp.float32)
    for k, line in enumerate(lines):
        line[...] = rows[k : k + 1, :share].reshape(share)
    fc1_line[...] = jnp.concatenate([rows[k : k + 1] for k in range(8, 11)], axis=1).reshape(fc1_line.shape[0])
    for row in range(output.shape[0]):
        output[row] = jnp.transpose(conv_out[row].astype(jnp.float32)).astype(jnp.bfloat16)
    for store in stores:
        store.wait()


def finish(sums, thin, flat, conv_out):
    row_count, patch, tokens = conv_out.shape
    share = thin.shape[1]
    wide = jnp.float32
    plan = tuple(entry[:4] for entry in sums)
    arrays = [entry[4] for entry in sums]
    whole = [(0, 0)] * 5
    for which, start, _, left, entry in sums:
        rows, columns = whole[which]
        whole[which] = (max(rows, start + entry.shape[1]), max(columns, left + 2 * entry.shape[2]))
    vmem, anywhere = pl.BlockSpec(memory_space=pltpu.VMEM), pl.BlockSpec(memory_space=pl.ANY)
    return pl.pallas_call(
        functools.partial(finish_kernel, patch, plan),
        out_shape=[jax.ShapeDtypeStruct(shape, wide) for shape in whole]
        + [jax.ShapeDtypeStruct((patch, share), wide), jax.ShapeDtypeStruct((9 * patch, share), wide)]
        + [jax.ShapeDtypeStruct((share,), wide)] * 8
        + [jax.ShapeDtypeStruct((4 * share,), wide), jax.ShapeDtypeStruct((row_count, tokens, patch), jnp.bfloat16)],
        in_specs=[anywhere] * len(arrays) + [vmem] * 3,
        out_specs=[anywhere] * 5 + [vmem] * 12,
        scratch_shapes=[pltpu.VMEM(entry.shape, jnp.bfloat16) for entry in arrays]
        + [pltpu.VMEM(shape, wide) for shape in whole]
        + [pltpu.SemaphoreType.DMA((len(arrays),)), pltpu.SemaphoreType.DMA((len(arrays),))],
        compiler_params=pltpu.CompilerParams(vmem_limit_bytes=full_vmem),
        name="finish",
    )(*arrays, thin, flat, conv_out)


def plane_peers():
    z, ty, y = lax.axis_index("rows"), lax.axis_index("ty"), lax.axis_index("tx")
    core, x = lax.rem(ty, 2), ty // 2
    here = x * 2 + core
    across = (1 - x) * 2 + core
    tiles = {
        "own": here * 2 + y,
        "x": across * 2 + y,
        "y": here * 2 + 1 - y,
        "xy": across * 2 + 1 - y,
    }
    peers = {
        "core": (z, x * 2 + 1 - core, y),
        "x": (z, across, y),
        "y": (z, here, 1 - y),
    }
    return tiles, peers


def plane_peer(k):
    z, ty, y = lax.axis_index("rows"), lax.axis_index("ty"), lax.axis_index("tx")
    x, core = ty // 2, lax.rem(ty, 2)
    flip_x, flip_core, flip_y = k // 4, k // 2 % 2, k % 2
    x = x + flip_x - 2 * flip_x * x
    core = core + flip_core - 2 * flip_core * core
    y = y + flip_y - 2 * flip_y * y
    return (z, x * 2 + core, y), (x * 2 + core) * 2 + y


def greet(peers):
    barrier = pltpu.get_barrier_semaphore()
    for peer in peers:
        pl.semaphore_signal(barrier, inc=1, device_id=peer, device_id_type=MESH)
    pl.semaphore_wait(barrier, len(peers))


def fill_mask(mask_ref, cuts_ref, row, tile, tile_height, tile_width):
    columns = lax.axis_size("tx")
    tokens = tile_height * tile_width
    left_width = cuts_ref[row, 0]
    top_height = cuts_ref[row, 1]

    def image_of(down, across):
        return jnp.where(across < left_width, 0, jnp.where(down < top_height, 1, 2))

    lane = lax.broadcasted_iota(jnp.int32, (8, tokens), 1)
    mine = image_of(*cell_of(lane, tile, tile_height, tile_width, columns))[0:1]
    step = lax.broadcasted_iota(jnp.int32, (tokens, tokens), 0)
    down, across = step // tile_width, step % tile_width
    for other in range(mask_ref.shape[0] // tokens):
        theirs = image_of(
            down + other // columns * tile_height, across + other % columns * tile_width
        )
        mask_ref[other * tokens : (other + 1) * tokens, :] = jnp.where(mine == theirs, 0.0, -1e30)


def two_heads(pair, scale):
    lane = lax.broadcasted_iota(jnp.int32, pair.shape, 1)
    wide = pair.astype(jnp.float32) * scale
    first = jnp.where(lane < pair.shape[1] // 2, wide, 0.0)
    return jnp.concatenate([first, wide - first], axis=0).astype(jnp.bfloat16)


def own_blocks(both):
    head, tokens = both.shape[0] // 2, both.shape[1] // 2
    return jnp.concatenate([both[:head, :tokens], both[head:, tokens:]], axis=0)


def attend_kernel(
    tile_height, tile_width, cuts, query, pairs, cot, conv_turned, fc2_in,
    out, lse, query_out, attended_out, all_out, spread, out_grad_out, active_grad_out,
    cot_all, queries, held, results, scores, mask, shift, fc2_weight, out_grad, active_grad,
    local_sem, send_sem, recv_sem, cot_sem, cot_send_sem, cot_recv_sem, side_sem
):
    _, row_count, tokens, half = query.shape
    tile_count = held.shape[1]
    width = 2 * half
    tiles, peers = plane_peers()
    own = tiles["own"]
    x = lax.axis_index("ty") // 2
    fc2_load = pltpu.make_async_copy(fc2_in, fc2_weight, side_sem.at[0])
    fc2_load.start()
    greet([plane_peer(k)[0] for k in range(1, tile_count)])
    cot_copies = [pltpu.make_async_copy(cot, cot_all.at[own], cot_sem.at[0])]
    for k in range(1, tile_count):
        cot_copies.append(
            pltpu.make_async_remote_copy(
                src_ref=cot,
                dst_ref=cot_all.at[own],
                send_sem=cot_send_sem.at[k],
                recv_sem=cot_recv_sem.at[k],
                device_id=plane_peer(k)[0],
                device_id_type=MESH,
            )
        )

    def send(row, slot, source, target, peer):
        copy = pltpu.make_async_remote_copy(
            src_ref=source,
            dst_ref=target,
            send_sem=send_sem.at[row, slot],
            recv_sem=recv_sem.at[row, slot],
            device_id=peer,
            device_id_type=MESH,
        )
        copy.start()
        flights[row][slot] = copy

    def keep(row, slot, source, target):
        copy = pltpu.make_async_copy(source, target, local_sem.at[row, slot])
        copy.start()
        kept[row][slot] = copy

    flights = [{} for _ in range(row_count)]
    kept = [{} for _ in range(row_count)]

    def begin(row):
        here = held.at[row, own]
        send(row, 1, pairs.at[1 - x, row], here, peers["x"])
        send(row, 0, query.at[1 - x, row], queries.at[row, 1], peers["x"])
        send(row, 2, pairs.at[x, row], here, peers["y"])
        send(row, 3, pairs.at[x, row], here, peers["core"])
        keep(row, 0, query.at[x, row], queries.at[row, 0])
        keep(row, 1, pairs.at[x, row], here)

    def forward(row):
        flights[row][1].wait_recv()
        tile = held.at[row, tiles["x"]]
        send(row, 4, tile, tile, peers["y"])
        send(row, 5, tile, tile, peers["core"])
        flights[row][2].wait_recv()
        tile = held.at[row, tiles["y"]]
        send(row, 6, tile, tile, peers["core"])

    def gather_row(row):
        flights[row][4].wait_recv()
        tile = held.at[row, tiles["xy"]]
        send(row, 7, tile, tile, peers["core"])
        for slot in (0, 3, 5, 6, 7):
            flights[row][slot].wait_recv()
        for slot in range(8):
            flights[row][slot].wait_send()
        for slot in range(2):
            kept[row][slot].wait()
        keep(row, 3, held.at[row], all_out.at[row])
        keep(row, 4, queries.at[row], query_out.at[row])

    chunk = 2

    def compute(row):
        def one_pair(p, carry, which=(0, 1)):
            at = pl.ds(pl.multiple_of(p * 128, 128), 128)
            at_value = pl.ds(pl.multiple_of(half + p * 128, 128), 128)
            for t in which:
                both = two_heads(queries[row, t, :, at], 0.125)
                peak = None
                for c in range(tile_count // chunk):
                    span = slice(c * chunk * tokens, (c + 1) * chunk * tokens)
                    keys = held[row, c * chunk : (c + 1) * chunk, :, at].reshape(chunk * tokens, 128)
                    extra = mask[row, t, span, :]
                    part = mm(keys, both, 1, 1) + jnp.concatenate([extra, extra], axis=1)
                    scores[t, span, :] = part
                    top = jnp.max(part, axis=0, keepdims=True)
                    peak = top if peak is None else jnp.maximum(peak, top)
                total = jnp.zeros_like(peak)
                summed = jnp.zeros((128, 2 * tokens), jnp.float32)
                for c in range(tile_count // chunk):
                    span = slice(c * chunk * tokens, (c + 1) * chunk * tokens)
                    values = held[row, c * chunk : (c + 1) * chunk, :, at_value].reshape(chunk * tokens, 128)
                    part = jnp.exp(scores[t, span, :] - peak)
                    total = total + jnp.sum(part, axis=0, keepdims=True)
                    summed = summed + mm(values, part.astype(jnp.bfloat16), 0, 0)
                blocks = own_blocks(summed / total)
                results[row, t, :, at] = jnp.transpose(blocks).astype(jnp.bfloat16)
                lse[row, p, t] = peak + jnp.log(total)
            return carry

        if row < row_count - 1:
            lax.fori_loop(0, half // 128, one_pair, 0)
            hand_back(row)
        else:
            lax.fori_loop(0, half // 128, functools.partial(one_pair, which=(1,)), 0)
            hand_back(row)
            lax.fori_loop(0, half // 128, functools.partial(one_pair, which=(0,)), 0)
        keep(row, 5, results.at[row, 0], out.at[x, row])
        keep(row, 6, results.at[row], attended_out.at[row])

    def hand_back(row):
        send(row, 8, results.at[row, 1], out.at[x, row], peers["x"])

    side_copies = []
    parts = [slice(k * tokens, (k + 1) * tokens) for k in range(row_count)]

    def spread_out():
        patch = cot_all.shape[2]
        turned = jnp.concatenate(
            [cot_all[t].reshape(row_count * patch, tokens) for t in range(tile_count)], axis=1
        )
        moved = mm(turned, shift[...], 1, 0)
        for row in range(row_count):
            for p in range(9):
                piece = moved[row * patch : (row + 1) * patch, p * tokens : (p + 1) * tokens]
                piece = piece * same_image(cuts, row, p, tile_height, tile_width)
                spread[p * patch : (p + 1) * patch, parts[row]] = piece.astype(jnp.bfloat16)
        out_grad[...] = mm(spread[...], conv_turned[...], 0, 0)
        copy = pltpu.make_async_copy(out_grad, out_grad_out, side_sem.at[1])
        copy.start()
        side_copies.append(copy)

    def activate():
        for k in range(fc2_weight.shape[0] // width):
            span = slice(k * width, (k + 1) * width)
            low = out_grad[...].astype(jnp.bfloat16)
            active_grad[:, span] = mm(low, fc2_weight[span, :], 1, 1).astype(jnp.bfloat16)
        copy = pltpu.make_async_copy(active_grad, active_grad_out, side_sem.at[2])
        copy.start()
        side_copies.append(copy)

    for copy in cot_copies:
        copy.start()
    begin(0)
    fill_shift(shift, tile_height, tile_width)
    for copy in cot_copies:
        copy.wait()
    spread_out()
    forward(0)
    for row in range(1, min(row_count, 3)):
        begin(row)
    fc2_load.wait()
    activate()
    for row in range(row_count):
        for t, name in enumerate(("own", "x")):
            fill_mask(mask.at[row, t], cuts, row, tiles[name], tile_height, tile_width)
    for row in range(row_count):
        gather_row(row)
        compute(row)
        for later in range(1 if row == 0 else row + 2, min(row + 3, row_count)):
            if later > 2:
                begin(later)
            forward(later)
    for row in range(row_count):
        flights[row][8].wait()
        for slot in range(3, 7):
            kept[row][slot].wait()
    for copy in side_copies:
        copy.wait()


def attend(cuts, query, pairs, cot, conv_turned, fc2_weight, tile_height, tile_width):
    _, row_count, tokens, half = query.shape
    tile_count = lax.axis_size("ty") * lax.axis_size("tx")
    width = 2 * half
    low, wide = jnp.bfloat16, jnp.float32
    vmem, anywhere = pl.BlockSpec(memory_space=pltpu.VMEM), pl.BlockSpec(memory_space=pl.ANY)
    return pl.pallas_call(
        functools.partial(attend_kernel, tile_height, tile_width),
        out_shape=[
            jax.ShapeDtypeStruct((2, row_count, tokens, half), low),
            jax.ShapeDtypeStruct((row_count, half // 128, 2, 1, 2 * tokens), wide),
            jax.ShapeDtypeStruct((row_count, 2, tokens, half), low),
            jax.ShapeDtypeStruct((row_count, 2, tokens, half), low),
            jax.ShapeDtypeStruct((row_count, tile_count, tokens, width), low),
            jax.ShapeDtypeStruct((conv_turned.shape[0], row_count * tokens), low),
            jax.ShapeDtypeStruct((row_count * tokens, width), wide),
            jax.ShapeDtypeStruct((row_count * tokens, fc2_weight.shape[0]), low),
        ],
        in_specs=[pl.BlockSpec(memory_space=pltpu.SMEM)] + [anywhere] * 3 + [vmem, anywhere],
        out_specs=[anywhere, vmem] + [anywhere] * 3 + [vmem] + [anywhere] * 2,
        scratch_shapes=[
            pltpu.VMEM((tile_count,) + cot.shape, low),
            pltpu.VMEM((row_count, 2, tokens, half), low),
            pltpu.VMEM((row_count, tile_count, tokens, width), low),
            pltpu.VMEM((row_count, 2, tokens, half), low),
            pltpu.VMEM((2, tile_count * tokens, 2 * tokens), wide),
            pltpu.VMEM((row_count, 2, tile_count * tokens, tokens), wide),
            pltpu.VMEM((tile_count * tokens, 9 * tokens), low),
            pltpu.VMEM(fc2_weight.shape, low),
            pltpu.VMEM((row_count * tokens, width), wide),
            pltpu.VMEM((row_count * tokens, fc2_weight.shape[0]), low),
            pltpu.SemaphoreType.DMA((row_count, 7)),
            pltpu.SemaphoreType.DMA((row_count, 9)),
            pltpu.SemaphoreType.DMA((row_count, 9)),
            pltpu.SemaphoreType.DMA((1,)),
            pltpu.SemaphoreType.DMA((tile_count,)),
            pltpu.SemaphoreType.DMA((tile_count,)),
            pltpu.SemaphoreType.DMA((3,)),
        ],
        compiler_params=pltpu.CompilerParams(
            collective_id=1, has_side_effects=True, vmem_limit_bytes=full_vmem
        ),
        name="attend",
    )(cuts, query, pairs, cot, conv_turned, fc2_weight)


back_order = (
    "+fc2b", "+fc1", "compute0", "+fc2a", "begin0", "scatter0", "compute1", "+fc1", "begin1", "+proj", "compute2",
    "+fc2b", "pass0", "+fc1", "+proj", "=fc2a", "begin2", "scatter1", "+fc2b", "scatter2", "convolve", "pass1",
    "+proj", "pass2", "=fc2b", "=fc1", "=proj",
)


def attend_back_kernel(
    tile_height, tile_width, kinds, cuts, query_in, attended_in, grad_in, lse_in, conv_in, conv_turned, spread,
    all_pairs, *refs
):
    count = max([kind[2] for kind in kinds], default=-1) + 1
    sources, refs = refs[:count], refs[count:]
    total_count = len(kinds)
    (out, conv_grad, conv_out), saved, refs = refs[:3], refs[3 : 3 + total_count], refs[3 + total_count :]
    query, attended, grad, lse, row_sem = refs[:5]
    held, terms, core_terms, y_terms, x_terms, x_query, query_grad, mask, shift, taps, part, part_got = refs[5:17]
    send_sem, recv_sem, part_send_sem, part_recv_sem = refs[17:21]
    grads = [
        sources[which] if rows is None else sources[which].at[:, rows[0] : rows[1], :]
        for _, _, which, rows in kinds
    ]
    items = make_reducers([kind[:2] for kind in kinds], grads, saved, refs[21:]) if kinds else []
    row_count, _, tokens, half = query.shape
    tile_count = held.shape[1]
    tiles, peers = plane_peers()
    low = jnp.bfloat16
    x, core = lax.axis_index("ty") // 2, lax.rem(lax.axis_index("ty"), 2)

    def group(which, base=0):
        return pl.ds(pl.multiple_of(base + which * half, 128), half)

    loads = []
    for row in range(row_count):
        loads.append([])
        for k, (source, target) in enumerate((
            (all_pairs.at[row], held.at[row]), (query_in.at[row], query.at[row]), (attended_in.at[row], attended.at[row]),
            (grad_in.at[x, row], grad.at[row, 0]), (lse_in.at[row], lse.at[row]),
        )):
            load = pltpu.make_async_copy(source, target, row_sem.at[row, k])
            load.start()
            loads[-1].append(load)
    greet([plane_peer(k)[0] for k in range(1, tile_count)] + (chip_peers()["z"] if kinds else []))
    chunk = 2
    flights = [{} for _ in range(row_count)]

    def send(row, slot, source, target, peer):
        copy = pltpu.make_async_remote_copy(
            src_ref=source,
            dst_ref=target,
            send_sem=send_sem.at[row, slot],
            recv_sem=recv_sem.at[row, slot],
            device_id=peer,
            device_id_type=MESH,
        )
        copy.start()
        flights[row][slot] = copy

    def compute(row):
        for load in loads[row]:
            load.wait()
        flights[row][8].wait()
        for t, name in enumerate(("own", "x")):
            fill_mask(mask.at[t], cuts, row, tiles[name], tile_height, tile_width)

        def one_pair(p, carry):
            at = pl.ds(pl.multiple_of(p * 128, 128), 128)
            at_value = pl.ds(pl.multiple_of(half + p * 128, 128), 128)
            boths, both_grads, deltas, levels = [], [], [], []
            for t in range(2):
                grad_pair = grad[row, t, :, at]
                boths.append(two_heads(query[row, t, :, at], 0.125))
                both_grads.append(two_heads(grad_pair, 1.0))
                inner = jnp.transpose(grad_pair.astype(jnp.float32) * attended[row, t, :, at].astype(jnp.float32))
                heads = [inner[: inner.shape[0] // 2], inner[inner.shape[0] // 2 :]]
                deltas.append(jnp.concatenate([jnp.sum(head, axis=0, keepdims=True) for head in heads], axis=1))
                levels.append(lse[row, p, t])
            all_both = jnp.concatenate(boths, axis=0)
            all_grads = jnp.concatenate(both_grads, axis=0)
            query_part = jnp.zeros((128, 4 * tokens), jnp.float32)
            for c in range(tile_count // chunk):
                span = slice(c * chunk * tokens, (c + 1) * chunk * tokens)
                some = slice(c * chunk, (c + 1) * chunk)
                keys = held[row, some, :, at].reshape(chunk * tokens, 128)
                values = held[row, some, :, at_value].reshape(chunk * tokens, 128)
                weight_parts, score_parts = [], []
                for t in range(2):
                    extra = mask[t, span, :]
                    raw = mm(keys, boths[t], 1, 1) + jnp.concatenate([extra, extra], axis=1)
                    weights = jnp.exp(raw - levels[t])
                    weight_parts.append(weights.astype(low))
                    score_parts.append((weights * (mm(values, both_grads[t], 1, 1) - deltas[t])).astype(low))
                score_grad = jnp.concatenate(score_parts, axis=1)
                value_part = mm(jnp.concatenate(weight_parts, axis=1), all_grads, 1, 0)
                key_part = mm(score_grad, all_both, 1, 0)
                query_part = query_part + mm(keys, score_grad, 0, 0)
                terms[row, some, :, at] = key_part.astype(low).reshape(chunk, tokens, 128)
                terms[row, some, :, at_value] = value_part.astype(low).reshape(chunk, tokens, 128)
            for t in range(2):
                blocks = own_blocks(query_part[:, 2 * t * tokens : 2 * (t + 1) * tokens]) * 0.125
                query_grad[row, t, :, at] = jnp.transpose(blocks).astype(low)
            return carry

        lax.fori_loop(0, half // 128, one_pair, 0)

    names = ("own", "x", "y", "xy")

    def begin(row):
        other = 2 - 4 * core
        for k in (3, 2, 1, 0):
            send(row, k, terms.at[row, tiles[names[k]] + other], core_terms.at[row, k], peers["core"])
        send(row, 7, query_grad.at[row, 1], x_query.at[row], peers["x"])

    def add(target, source):
        def body(i, carry):
            at = pl.ds(pl.multiple_of(i * 16, 16), 16)
            target[at, :] = target[at, :] + source[at, :]
            return carry

        lax.fori_loop(0, tokens // 16, body, 0)

    def scatter(row):
        for k in (3, 2, 1, 0):
            flights[row][k].wait()
            tile = terms.at[row, tiles[names[k]]]
            add(tile, core_terms.at[row, k])
            if k == 3:
                send(row, 5, tile, y_terms.at[row, 1], peers["y"])
            if k == 2:
                send(row, 4, tile, y_terms.at[row, 0], peers["y"])

    def pass_on(row):
        flights[row][5].wait()
        tile = terms.at[row, tiles["x"]]
        add(tile, y_terms.at[row, 1])
        send(row, 6, tile, x_terms.at[row], peers["x"])

    def close(row):
        for slot in (4, 6, 7):
            flights[row][slot].wait()
        mine = terms.at[row, tiles["own"]]
        width = 2 * half

        def body(i, carry):
            at = pl.ds(pl.multiple_of(i * 16, 16), 16)
            total = mine[at, :].astype(jnp.float32) + y_terms[row, 0, at, :].astype(jnp.float32)
            total = total.astype(low)
            out[row, at, group(x)] = query_grad[row, 0, at, :]
            out[row, at, group(x, width)] = total[:, :half]
            out[row, at, group(x, 2 * width)] = total[:, half:]
            out[row, at, group(1 - x)] = x_query[row, at, :]
            out[row, at, group(1 - x, width)] = x_terms[row, at, :half]
            out[row, at, group(1 - x, 2 * width)] = x_terms[row, at, half : 2 * half]
            return carry

        lax.fori_loop(0, tokens // 16, body, 0)

    part_copies = []

    def convolve():
        fill_shift(shift, tile_height, tile_width)
        patch = part.shape[2]
        taps[...] = mm(conv_turned[...], conv_in[...], 1, 1)
        rows = []
        for row in range(row_count):
            pieces = []
            for p in range(9):
                piece = taps[p * patch : (p + 1) * patch, row * tokens : (row + 1) * tokens]
                pieces.append(piece * same_image(cuts, row, p, tile_height, tile_width))
            rows.append(jnp.concatenate(pieces, axis=1))
        whole = jnp.concatenate(rows, axis=0)
        coarse = whole.astype(low)
        fine = (whole - coarse.astype(jnp.float32)).astype(low)
        moved = mm(coarse, shift[...], 1, 1) + mm(fine, shift[...], 1, 1)
        for tile in range(tile_count):
            part[tile] = moved[:, tile * tokens : (tile + 1) * tokens].reshape(row_count, patch, tokens)
        for k in range(1, tile_count):
            peer, tile = plane_peer(k)
            copy = pltpu.make_async_remote_copy(
                src_ref=part.at[tile],
                dst_ref=part_got.at[k],
                send_sem=part_send_sem.at[k],
                recv_sem=part_recv_sem.at[k],
                device_id=peer,
                device_id_type=MESH,
            )
            copy.start()
            part_copies.append(copy)
        conv_grad[...] = mm(conv_in[...], spread[...], 0, 1)

    def collect():
        total = part[tiles["own"]]
        for k, copy in enumerate(part_copies):
            copy.wait()
            total = total + part_got[k + 1]
        conv_out[...] = total.astype(low)

    def sum_up(item):
        item.step()
        item.save()

    for row in range(row_count):
        send(row, 8, grad_in.at[1 - x, row], grad.at[row, 1], peers["x"])
    for item in items:
        item.begin()
    acts = {"compute": compute, "begin": begin, "scatter": scatter, "pass": pass_on}
    if items and row_count == 3:
        order = list(back_order)
    else:
        rows = range(row_count)
        order = [f"{act}{row}" for row in rows for act in ("compute", "begin")]
        order += [f"scatter{row}" for row in rows] + [f"pass{row}" for row in rows] + ["convolve"]
    named = dict(zip(("fc1", "fc2a", "fc2b", "proj"), items))
    for entry in order:
        if entry == "convolve":
            convolve()
        elif entry[0] == "+":
            named[entry[1:]].step()
        elif entry[0] == "=":
            sum_up(named[entry[1:]])
        else:
            acts[entry[:-1]](int(entry[-1]))
    for row in range(row_count):
        close(row)
    collect()
    for item in items:
        item.land("save")


def attend_back(cuts, query, attended, grad, lse, conv_in, conv_turned, spread, all_pairs, grads, tile_height, tile_width):
    row_count, _, tokens, half = query.shape
    width = 2 * half
    kinds, sources, saves, shapes = [], [], [], []
    for start, paired, entry, rows in grads:
        if not any(entry is source for source in sources):
            sources.append(entry)
        which = [entry is source for source in sources].index(True)
        kinds.append((start, paired, which, rows))
        depth = entry.shape[1] if rows is None else rows[1] - rows[0]
        shapes.append((depth, entry.shape[2] if paired else entry.shape[2] // 2))
        saves.append((depth if start == "z" else depth // 4, shapes[-1][1]))
    kinds = tuple(kinds)
    tile_count = all_pairs.shape[1]
    taps = conv_turned.shape[0]
    low, wide = jnp.bfloat16, jnp.float32
    vmem, anywhere = pl.BlockSpec(memory_space=pltpu.VMEM), pl.BlockSpec(memory_space=pl.ANY)
    return pl.pallas_call(
        functools.partial(attend_back_kernel, tile_height, tile_width, kinds),
        out_shape=[
            jax.ShapeDtypeStruct((row_count, tokens, 3 * width), low),
            jax.ShapeDtypeStruct((width, taps), wide),
            jax.ShapeDtypeStruct((row_count, taps // 9, tokens), low),
        ]
        + [jax.ShapeDtypeStruct(s, low) for s in saves],
        in_specs=[pl.BlockSpec(memory_space=pltpu.SMEM)] + [anywhere] * 4 + [vmem] * 3 + [anywhere] * (1 + len(sources)),
        out_specs=[vmem] * 3 + [anywhere] * len(saves),
        scratch_shapes=[
            pltpu.VMEM(query.shape, low),
            pltpu.VMEM(query.shape, low),
            pltpu.VMEM(query.shape, low),
            pltpu.VMEM(lse.shape, wide),
            pltpu.SemaphoreType.DMA((row_count, 5)),
            pltpu.VMEM((row_count, tile_count, tokens, width), low),
            pltpu.VMEM((row_count, tile_count, tokens, width), low),
            pltpu.VMEM((row_count, 4, tokens, width), low),
            pltpu.VMEM((row_count, 2, tokens, width), low),
            pltpu.VMEM((row_count, tokens, width), low),
            pltpu.VMEM((row_count, tokens, half), low),
            pltpu.VMEM(query.shape, low),
            pltpu.VMEM((2, tile_count * tokens, tokens), wide),
            pltpu.VMEM((tile_count * tokens, 9 * tokens), low),
            pltpu.VMEM((taps, row_count * tokens), wide),
            pltpu.VMEM((tile_count, row_count, taps // 9, tokens), wide),
            pltpu.VMEM((tile_count, row_count, taps // 9, tokens), wide),
            pltpu.SemaphoreType.DMA((row_count, 9)),
            pltpu.SemaphoreType.DMA((row_count, 9)),
            pltpu.SemaphoreType.DMA((tile_count,)),
            pltpu.SemaphoreType.DMA((tile_count,)),
        ]
        + (reducer_scratch([kind[:2] for kind in kinds], shapes) if kinds else []),
        compiler_params=pltpu.CompilerParams(
            collective_id=2, has_side_effects=True, vmem_limit_bytes=full_vmem
        ),
        name="attend_back",
    )(cuts, query, attended, grad, lse, conv_in, conv_turned, spread, all_pairs, *sources)


def add_rows(target, first, second, rows):
    def body(i, carry):
        at = pl.ds(pl.multiple_of(i * 16, 16), 16)
        target[at, :] = first[at, :] + second[at, :]
        return carry

    lax.fori_loop(0, rows // 16, body, 0)


def add_four(target, others, rows):
    def body(i, carry):
        at = pl.ds(pl.multiple_of(i * 16, 16), 16)
        total = target[at, :].astype(jnp.float32) + others[0, at, :].astype(jnp.float32)
        total = total + (others[1, at, :].astype(jnp.float32) + others[2, at, :].astype(jnp.float32))
        target[at, :] = total.astype(jnp.bfloat16)
        return carry

    lax.fori_loop(0, rows // 16, body, 0)


def chip_peers():
    z, ty, y = lax.axis_index("rows"), lax.axis_index("ty"), lax.axis_index("tx")
    core, x = lax.rem(ty, 2), ty // 2
    across = (1 - x) * 2 + core
    return {
        "core": (z, x * 2 + 1 - core, y),
        "x": (z, across, y),
        "y": (z, ty, 1 - y),
        "xy": (z, across, 1 - y),
        "z": [(lax.rem(z + k, 4), ty, y) for k in (1, 2, 3)],
    }


class Reducer:
    def __init__(self, start, paired, relays, grad, out, buffers, sems, w):
        self.relays = relays
        self.start, self.paired, self.grad, self.out, self.w = start, paired, grad, out, w
        self.local_sem, self.send_sem, self.recv_sem = sems
        self.z, ty, self.y = lax.axis_index("rows"), lax.axis_index("ty"), lax.axis_index("tx")
        self.core, self.x = lax.rem(ty, 2), ty // 2
        self.peers = chip_peers()
        self.flying = {}
        self.own = buffers[0]
        if start in ("plane", "z"):
            self.half, self.quarter, self.final = buffers[1:4]
            self.got = None if paired else buffers[4]
            self.depth, self.width = grad.shape[1], grad.shape[2] if paired else grad.shape[2] // 2
        else:
            self.depth, self.width = out.shape[1], out.shape[2]
        if start == "block":
            self.half, self.quarter = buffers[1:]
        share = [self.relay, self.pass_strip] if relays else [self.pass_strip]
        late = [self.begin_late, self.add_half_late, self.add_quarter_late, *share, self.end]
        self.stages = {
            "plane": [self.add_core, self.add_half, self.add_quarter, self.sum_z, self.gather_piece, *share, self.end],
            "z": [self.add_core, self.sum_z_first] + late,
            "block": late,
            "piece": [self.gather_piece, *share, self.end],
        }[start]

    def step(self):
        self.stages.pop(0)()

    def part(self, at):
        if self.start == "block":
            return self.own.at[at]
        return self.own.at[self.z, at]

    def send(self, slot, source, target, peer):
        copy = pltpu.make_async_remote_copy(
            src_ref=source,
            dst_ref=target,
            send_sem=self.send_sem.at[self.w, slot],
            recv_sem=self.recv_sem.at[self.w, slot],
            device_id=peer,
            device_id_type=MESH,
        )
        copy.start()
        return copy

    def keep(self, slot, source, target):
        copy = pltpu.make_async_copy(source, target, self.local_sem.at[self.w, slot])
        copy.start()
        return copy

    def land(self, name):
        for copy in self.flying.pop(name):
            copy.wait()

    def columns(self, which):
        return pl.ds(pl.multiple_of(which * self.width, 128), self.width)

    def rows(self, start, size):
        return pl.ds(pl.multiple_of(start, 16), size)

    def place(self, block, flip_x=False, flip_y=False):
        x = 1 - self.x if flip_x else self.x
        y = 1 - self.y if flip_y else self.y
        later = block // 2
        major = x + later * (y - x)
        minor = y + later * (x - y)
        return self.rows(major * (self.depth // 2) + minor * (self.depth // 4), self.depth // 4)

    def pieces(self, flip_x=False, flip_y=False):
        if self.start in ("plane", "piece"):
            return [self.place(self.z, flip_x, flip_y)]
        x = 1 - self.x if flip_x else self.x
        y = 1 - self.y if flip_y else self.y
        half, less, least = self.depth // 2, self.depth // 4, self.depth // 8
        return [self.rows(x * less + y * least, least), self.rows(half + y * less + x * least, least)]

    def begin(self):
        if self.start in ("block", "piece"):
            self.flying["load"] = [self.keep(0, self.grad, self.own)]
            return
        if self.paired:
            self.flying["core"] = [self.keep(0, self.grad, self.own)]
            return
        swap = self.send(0, self.grad.at[:, :, self.columns(1 - self.core)], self.got, self.peers["core"])
        mine = self.keep(0, self.grad.at[:, :, self.columns(self.core)], self.own)
        self.flying["core"] = [swap, mine]

    def add_core(self):
        self.land("core")
        if not self.paired:
            for block in range(4):
                add_rows(self.own.at[block], self.own.at[block], self.got.at[block], self.depth)
        if self.start == "z":
            self.flying["z"] = [
                self.send(5 + k, self.own.at[peer[0]], self.final.at[k], peer) for k, peer in enumerate(self.peers["z"])
            ]
            return
        part = self.depth // 2
        first = self.send(1, self.own.at[0:2, self.rows((1 - self.x) * part, part)], self.half.at[0:2], self.peers["x"])
        second = self.send(2, self.own.at[2:4, self.rows((1 - self.y) * part, part)], self.half.at[2:4], self.peers["y"])
        self.flying["half"] = [first, second]

    def add_half(self):
        self.land("half")
        part, less = self.depth // 2, self.depth // 4
        for block in range(4):
            side = self.x if block < 2 else self.y
            kept = self.own.at[block, self.rows(side * part, part)]
            add_rows(kept, kept, self.half.at[block], part)
        first = self.own.at[0:2, self.rows(self.x * part + (1 - self.y) * less, less)]
        second = self.own.at[2:4, self.rows(self.y * part + (1 - self.x) * less, less)]
        self.flying["quarter"] = [
            self.send(3, first, self.quarter.at[0:2], self.peers["y"]),
            self.send(4, second, self.quarter.at[2:4], self.peers["x"]),
        ]

    def add_quarter(self):
        self.land("quarter")
        for block in range(4):
            kept = self.own.at[block, self.place(block // 2 * 2)]
            add_rows(kept, kept, self.quarter.at[block], self.depth // 4)
        self.flying["z"] = [
            self.send(5 + k, self.own.at[peer[0], self.place(peer[0])], self.final.at[k], peer)
            for k, peer in enumerate(self.peers["z"])
        ]

    def gather(self, pieces, sources):
        copies = []
        for n, (at, source) in enumerate(zip(pieces, sources)):
            target = self.out.at[self.core, at]
            for k, name in enumerate(("x", "y") if self.relays else ("x", "y", "xy")):
                copies.append(self.send(8 + 3 * n + k, source, target, self.peers[name]))
            copies.append(self.keep(1 + n, source, target))
        self.flying["gather"] = copies

    def relay(self):
        self.land("gather")
        cut = self.width // 256 * 128 + (128 if self.width % 256 and self.w % 2 else 0)
        copies = []
        for n, (from_x, from_y) in enumerate(zip(self.pieces(flip_x=True), self.pieces(flip_y=True))):
            first = self.out.at[self.core, from_x, pl.ds(0, cut)]
            second = self.out.at[self.core, from_y, pl.ds(cut, self.width - cut)]
            copies.append(self.send(14 + 2 * n + 1, first, first, self.peers["y"]))
            copies.append(self.send(14 + 2 * n + 2, second, second, self.peers["x"]))
        self.flying["relay"] = copies

    def sum_z(self):
        self.land("z")
        add_four(self.own.at[self.z, self.place(self.z)], self.final, self.depth // 4)

    def gather_piece(self):
        if self.start == "piece":
            self.land("load")
            self.gather([self.place(self.z)], [self.own])
        else:
            self.gather([self.place(self.z)], [self.own.at[self.z, self.place(self.z)]])

    def sum_z_first(self):
        self.land("z")
        add_four(self.own.at[self.z], self.final, self.depth)

    def save(self):
        source = self.own.at[self.z] if self.start == "z" else self.own.at[self.z, self.place(self.z)]
        self.flying["save"] = [self.keep(1, source, self.out)]

    def begin_late(self):
        if self.start == "block":
            self.land("load")
        half, less = self.depth // 2, self.depth // 4
        self.flying["half"] = [
            self.send(1, self.part(self.rows((1 - self.x) * less, less)), self.half.at[0], self.peers["x"]),
            self.send(2, self.part(self.rows(half + (1 - self.y) * less, less)), self.half.at[1], self.peers["y"]),
        ]

    def add_half_late(self):
        self.land("half")
        half, less, least = self.depth // 2, self.depth // 4, self.depth // 8
        for n, start in enumerate((self.x * less, half + self.y * less)):
            kept = self.part(self.rows(start, less))
            add_rows(kept, kept, self.half.at[n], less)
        first = self.part(self.rows(self.x * less + (1 - self.y) * least, least))
        second = self.part(self.rows(half + self.y * less + (1 - self.x) * least, least))
        self.flying["quarter"] = [
            self.send(3, first, self.quarter.at[0], self.peers["y"]),
            self.send(4, second, self.quarter.at[1], self.peers["x"]),
        ]

    def add_quarter_late(self):
        self.land("quarter")
        least = self.depth // 8
        pieces = self.pieces()
        for n, at in enumerate(pieces):
            add_rows(self.part(at), self.part(at), self.quarter.at[n], least)
        self.gather(pieces, [self.part(at) for at in pieces])

    def pass_strip(self):
        self.land("relay" if self.relays else "gather")
        strip = self.out.at[self.core]
        self.flying["strip"] = [self.send(14, strip, strip, self.peers["core"])]

    def end(self):
        self.land("strip")


def reducer_scratch(kinds, shapes):
    buffers = []
    for (start, paired), (depth, half) in zip(kinds, shapes):
        sizes = {
            "plane": [(4, depth, half), (4, depth // 2, half), (4, depth // 4, half), (3, depth // 4, half)],
            "z": [(4, depth, half), (2, depth // 4, half), (2, depth // 8, half), (3, depth, half)],
            "block": [(depth, half), (2, depth // 4, half), (2, depth // 8, half)],
            "piece": [(depth // 4, half)],
        }[start]
        if not paired:
            sizes.append((4, depth, half))
        buffers += [pltpu.VMEM(size, jnp.bfloat16) for size in sizes]
    count = len(kinds)
    return buffers + [
        pltpu.SemaphoreType.DMA((count, 3)),
        pltpu.SemaphoreType.DMA((count, 19)),
        pltpu.SemaphoreType.DMA((count, 19)),
    ]


def make_reducers(kinds, grads, outs, scratch, relays=()):
    items, at = [], 0
    for w, ((start, paired), grad, out) in enumerate(zip(kinds, grads, outs)):
        size = {"plane": 4, "z": 4, "block": 3, "piece": 1}[start] + (0 if paired else 1)
        items.append(Reducer(start, paired, w in relays, grad, out, scratch[at : at + size], scratch[-3:], w))
        at = at + size
    return items


def sum_by_table(local_grads):
    band_count, column_count = lax.axis_size("ty"), lax.axis_size("tx")
    group_count = lax.axis_size("rows")
    tile_count = band_count * column_count
    table = jnp.concatenate([entry.reshape(group_count, -1) for entry in local_grads], axis=1)
    column_total = table.shape[1]
    padded_columns = -(-column_total // tile_count) * tile_count
    piece_width = padded_columns // tile_count
    table = table.reshape(group_count, tile_count, piece_width)
    shares = lax.psum_scatter(
        table.reshape(group_count * tile_count, piece_width),
        ("rows", "ty", "tx"),
        scatter_dimension=0,
        tiled=True,
    )
    summed = (
        lax.all_gather(shares.astype(jnp.bfloat16), ("ty", "tx"), axis=0, tiled=True)
        .astype(shares.dtype)
        .reshape(-1)
    )
    totals = []
    start_at = 0
    for entry in local_grads:
        length = entry.size // group_count
        shard_shape = (entry.shape[0] // group_count,) + entry.shape[1:]
        totals.append(summed[start_at : start_at + length].reshape(shard_shape))
        start_at = start_at + length
    return tuple(totals)


def shards(
    latent,
    skip_input,
    segment_ids,
    embed_weight,
    embed_bias,
    skip_weight,
    skip_bias,
    norm1_gain,
    norm1_bias,
    qkv_weight,
    proj_weight,
    proj_bias,
    norm2_gain,
    norm2_bias,
    fc1_weight,
    fc1_bias,
    fc2_weight,
    fc2_bias,
    conv_weight,
    cotangent,
):
    row_count, tile_height, tile_width, width = skip_input.shape
    patch = latent.shape[3]
    tokens = tile_height * tile_width
    token_count = row_count * tokens
    low = jnp.bfloat16
    wide = jnp.float32
    conv_turned = conv_weight.T
    flat_latent = latent.reshape(token_count, patch)
    flat_skip = skip_input.reshape(token_count, width)
    biases = (embed_bias, skip_bias, norm1_gain, norm1_bias, proj_bias, norm2_gain, norm2_bias, fc2_bias)
    embedded, stream, normed, query, pairs, cot, vectors, hidden_bias, cuts = front(
        segment_ids, flat_latent, cotangent.reshape(token_count, patch), embed_weight.T, biases, fc1_bias,
        flat_skip, skip_weight, qkv_weight, row_count,
    )
    attended, log_total, held_query, held_attended, held_pairs, spread, out_grad, active_grad = attend(
        cuts, query, pairs, cot, conv_turned, fc2_weight, tile_height, tile_width
    )
    here = (lax.axis_size("rows"), lax.axis_size("ty"), lax.axis_size("tx")) == (4, 4, 2)
    fc1_grad, fc2_grad, hidden_bias_grad, proj_grad, attended_grad, mid_grad, conv_in, middle_grads = middle(
        attended.reshape(2, token_count, width // 2), stream, out_grad, active_grad, proj_weight, vectors, hidden_bias,
        fc1_weight, fc2_weight, here,
    )
    early = []
    if here:
        fc2_blocks = fc2_grad.reshape(4, -1, width // 2)
        middle_row = fc2_blocks.shape[1] // 2
        early = [
            ("plane", True, fc1_grad, None),
            ("z", True, fc2_blocks, (0, middle_row)),
            ("plane", True, fc2_blocks, (middle_row, 2 * middle_row)),
            ("plane", False, proj_grad.reshape(4, -1, width), None),
        ]
    projected_grad, conv_grad, conv_out, *saved = attend_back(
        cuts, held_query, held_attended, attended_grad.reshape(2, row_count, tokens, width // 2), log_total,
        conv_in, conv_turned, spread, held_pairs, early, tile_height, tile_width,
    )
    follow = {"plane": "piece", "z": "block"}
    resumed = [
        (follow[start], entry, (entry.shape[0] if start == "z" else 4 * entry.shape[0], entry.shape[1]))
        for (start, _, _, _), entry in zip(early, saved)
    ]
    skip_input_grad, *rest = rear(
        projected_grad.reshape(token_count, 3 * width), qkv_weight, normed, stream, mid_grad, embedded, flat_skip,
        skip_weight, flat_latent, vectors, middle_grads, hidden_bias_grad, conv_grad, resumed, here,
    )
    skip_input_grad = skip_input_grad.reshape(row_count, tile_height, tile_width, width)
    taps = 9 * patch
    share = width // 4
    if here:
        half = width // 2
        places = [(0, 0, half, 0), (1, 0, half, 0), (1, middle_row, half, 0), (2, 0, half, 0)]
        places += [(3, 0, half, k * width) for k in range(3)] + [(4, 0, half, 0)]
        totals = finish([place + (entry,) for place, entry in zip(places, rest[:8])], rest[8], rest[9], conv_out)
        fc1_total, fc2_total, proj_total, qkv_total, skip_total, embed_turned, conv_grad_turned = totals[:7]
        line, fc1_line = totals[7:15], totals[15]
        output = totals[16].reshape(row_count, tile_height, tile_width, patch)
        return (
            output, skip_input_grad, embed_turned.T, line[0], skip_total, line[1], line[2], line[3], qkv_total,
            proj_total, line[4], line[5], line[6], fc1_total, fc1_line, fc2_total, line[7], conv_grad_turned.T,
        )
    output = conv_out.transpose(0, 2, 1).reshape(row_count, tile_height, tile_width, patch)
    qkv_grad = jnp.concatenate([entry.reshape(-1, width) for entry in rest[:3]], axis=1)
    skip_grad, thin = [entry.reshape(-1, entry.shape[2]) for entry in rest[3:5]]
    flat = rest[5]
    fc1_grad = fc1_grad.reshape(width, -1)
    line = [flat[:, k, :share].reshape(-1) for k in range(8)]
    fc1_line = flat[:, 8:11].reshape(-1)
    local_grads = [
        thin[:, taps : taps + patch], line[0], skip_grad, line[1], line[2], line[3], qkv_grad, proj_grad, line[4],
        line[5], line[6], fc1_grad, fc1_line, fc2_grad, line[7], thin[:, :taps],
    ]
    return (output, skip_input_grad) + sum_by_table([entry.astype(wide) for entry in local_grads])


def solution(mesh):
    return jax.shard_map(
        shards,
        mesh=mesh,
        in_specs=(
            P("rows", "ty", "tx", None),
            P("rows", "ty", "tx", None),
            P("rows", None, None),
            P(),
            P(),
            P(),
            P(),
            P(),
            P(),
            P(),
            P(),
            P(),
            P(),
            P(),
            P(),
            P(),
            P(),
            P(),
            P(),
            P("rows", "ty", "tx", None),
        ),
        out_specs=(
            P("rows", "ty", "tx", None),
            P("rows", "ty", "tx", None),
            P("rows", None),
            P("rows"),
            P("rows", None),
            P("rows"),
            P("rows"),
            P("rows"),
            P("rows", None),
            P("rows", None),
            P("rows"),
            P("rows"),
            P("rows"),
            P("rows", None),
            P("rows"),
            P("rows", None),
            P("rows"),
            P("rows", None),
        ),
        check_vma=False,
    )
```

```python
import functools

import jax
import jax.numpy as jnp
from jax import lax
from jax.experimental import pallas as pl
from jax.experimental.pallas import tpu as pltpu
from jax.sharding import PartitionSpec as P

MESH = pl.DeviceIdType.MESH
norm_eps = 1e-05
full_vmem = 62 * 1024 * 1024


def cell_of(token, tile, tile_height, tile_width, columns):
    down = tile // columns * tile_height + token // tile_width
    across = tile % columns * tile_width + token % tile_width
    return down, across


def fill_shift(shift_ref, tile_height, tile_width):
    tokens = tile_height * tile_width
    bands, columns = lax.axis_size("ty"), lax.axis_size("tx")
    own = lax.axis_index("ty") * columns + lax.axis_index("tx")
    lane = lax.broadcasted_iota(jnp.int32, (8, tokens), 1)
    down, across = cell_of(lane, own, tile_height, tile_width, columns)
    step = lax.broadcasted_iota(jnp.int32, (shift_ref.shape[0], tokens), 0)
    for p in range(9):
        i, j = down - (p // 3 - 1), across - (p % 3 - 1)
        inside = (i >= 0) & (i < bands * tile_height) & (j >= 0) & (j < columns * tile_width)
        tile = i // tile_height * columns + j // tile_width
        place = tile * tokens + i % tile_height * tile_width + j % tile_width
        place = jnp.where(inside, place, -1)[0:1]
        chosen = jnp.where(step == place, 1.0, 0.0)
        shift_ref[:, p * tokens : (p + 1) * tokens] = chosen.astype(jnp.bfloat16)


def same_image(cuts_ref, row, p, tile_height, tile_width):
    tokens = tile_height * tile_width
    columns = lax.axis_size("tx")
    own = lax.axis_index("ty") * columns + lax.axis_index("tx")
    lane = lax.broadcasted_iota(jnp.int32, (8, tokens), 1)
    down, across = cell_of(lane, own, tile_height, tile_width, columns)
    left_width, top_height = cuts_ref[row, 0], cuts_ref[row, 1]

    def image_of(i, j):
        return jnp.where(j < left_width, 0, jnp.where(i < top_height, 1, 2))

    there = image_of(down - (p // 3 - 1), across - (p % 3 - 1))
    return jnp.where(image_of(down, across) == there, 1.0, 0.0)[0:1]


def mm(former, latter, axis_former, axis_latter):
    return lax.dot_general(
        former,
        latter,
        (((axis_former,), (axis_latter,)), ((), ())),
        preferred_element_type=jnp.float32,
    )


def normalised(values):
    average = jnp.mean(values, axis=1, keepdims=True)
    centred = values - average
    rate = lax.rsqrt(jnp.mean(centred * centred, axis=1, keepdims=True) + norm_eps)
    return centred * rate, rate


def norm_back(incoming, unit, rate, gain):
    scaled = incoming * gain
    first = jnp.mean(scaled, axis=1, keepdims=True)
    second = jnp.mean(scaled * unit, axis=1, keepdims=True)
    return (scaled - first - unit * second) * rate


def down_sum(values):
    return jnp.sum(values, axis=0, keepdims=True)


def front_kernel(
    segment_ids, latent, cotangent, embed_turned, *refs
):
    biases, fc1_bias, refs = refs[:8], refs[8], refs[9:]
    skip_in, skip_weight_in, qkv_in, embedded, stream, normed, query, pairs, cot, vectors, hidden_bias, cuts = refs[:12]
    skip, skip_weight, qkv_weight, load_sem = refs[12:]
    sources, targets = (skip_weight_in, skip_in, qkv_in), (skip_weight, skip, qkv_weight)
    loads = [pltpu.make_async_copy(a, b, load_sem.at[k]) for k, (a, b) in enumerate(zip(sources, targets))]
    for load in loads:
        load.start()
    for k, bias in enumerate(biases):
        vectors[k : k + 1] = bias[...].reshape(1, bias.shape[0]).astype(jnp.float32)
    line = fc1_bias[...].reshape(1, fc1_bias.shape[0]).astype(jnp.float32)
    block = hidden_bias.shape[2]
    for k in range(hidden_bias.shape[0]):
        hidden_bias[k] = line[:, k * block : (k + 1) * block]
    width = skip.shape[1]
    row_count, tokens = query.shape[1], query.shape[2]
    side = segment_ids.shape[1]
    for row in range(row_count):

        def count(k, carry):
            left, top = carry
            left = left + jnp.where(segment_ids[row, 0, k] == 0, 1, 0)
            top = top + jnp.where(segment_ids[row, k, side - 1] == 1, 1, 0)
            return left, top

        left, top = lax.fori_loop(0, side, count, (jnp.int32(0), jnp.int32(0)), unroll=8)
        cuts[row, 0] = left
        cuts[row, 1] = top
        at = slice(row * tokens, (row + 1) * tokens)
        cot[row] = jnp.transpose(cotangent[at, :].astype(jnp.float32)).astype(jnp.bfloat16)
        embedded[at, :] = (mm(latent[at, :], embed_turned[...], 1, 0) + vectors[0:1]).astype(jnp.bfloat16)
    loads[0].wait()
    loads[1].wait()
    total = mm(embedded[...], skip_weight[:width], 1, 0) + mm(skip[...], skip_weight[width:], 1, 0) + vectors[1:2]
    stream[...] = total
    unit, rate = normalised(total)
    normed[...] = (unit * vectors[2:3] + vectors[3:4]).astype(jnp.bfloat16)
    loads[2].wait()
    half = width // 2
    for k in range(3):
        piece = mm(normed[...], qkv_weight[:, k * width : (k + 1) * width], 1, 0).astype(jnp.bfloat16)
        for g in range(2):
            part = piece[:, g * half : (g + 1) * half].reshape(row_count, tokens, half)
            if k == 0:
                query[g] = part
            else:
                pairs[g, :, :, (k - 1) * half : k * half] = part


def front(segment_ids, latent, cotangent, embed_turned, biases, fc1_bias, skip, skip_weight, qkv_weight, row_count):
    token_count, width = skip.shape
    tokens = token_count // row_count
    low, wide = jnp.bfloat16, jnp.float32
    smem, vmem = pl.BlockSpec(memory_space=pltpu.SMEM), pl.BlockSpec(memory_space=pltpu.VMEM)
    return pl.pallas_call(
        front_kernel,
        out_shape=[
            jax.ShapeDtypeStruct((token_count, width), low),
            jax.ShapeDtypeStruct((token_count, width), wide),
            jax.ShapeDtypeStruct((token_count, width), low),
            jax.ShapeDtypeStruct((2, row_count, tokens, width // 2), low),
            jax.ShapeDtypeStruct((2, row_count, tokens, width), low),
            jax.ShapeDtypeStruct((row_count, cotangent.shape[1], tokens), low),
            jax.ShapeDtypeStruct((8, width), wide),
            jax.ShapeDtypeStruct((fc1_bias.shape[0] // width, 1, width), wide),
            jax.ShapeDtypeStruct((row_count, 2), jnp.int32),
        ],
        in_specs=[smem] + [vmem] * 12 + [pl.BlockSpec(memory_space=pl.ANY)] * 3,
        out_specs=[vmem] * 8 + [smem],
        scratch_shapes=[pltpu.VMEM(entry.shape, low) for entry in (skip, skip_weight, qkv_weight)]
        + [pltpu.SemaphoreType.DMA((3,))],
        compiler_params=pltpu.CompilerParams(vmem_limit_bytes=full_vmem),
        name="front",
    )(segment_ids, latent, cotangent, embed_turned, *biases, fc1_bias, skip, skip_weight, qkv_weight)


def erf_of(values):
    x = jnp.clip(values, -4.0, 4.0)
    square = x * x
    upper = square * -2.72614225801306e-10 + 2.77068142495902e-08
    for term in (-2.10102402082508e-06, -5.69250639462346e-05, -7.34990630326855e-04, -2.95459980854025e-03, -1.60960333262415e-02):
        upper = upper * square + term
    lower = square * -1.45660718464996e-05 + -2.13374055278905e-04
    for term in (-1.68282697438203e-03, -7.37332916720468e-03, -1.42647390514189e-02):
        lower = lower * square + term
    return x * upper / lower


def middle_kernel(
    paired, attended, stream, out_grad, proj_weight, vectors, hidden_bias, active_grad, fc1_weight, fc2_weight,
    fc1_out, fc2_out, hidden_bias_grad, proj_grad, attended_grad, mid_grad, conv_in, vector_grads,
    middle, normed, out_low, forward_sum, backward_sum, grad1, grad2, *refs
):
    step = pl.program_id(0)
    last = fc2_out.shape[0] // fc2_weight.shape[0] - 1
    token_count, width = stream.shape
    block = fc1_weight.shape[1]
    low = jnp.bfloat16
    parts = [slice(0, token_count)]
    store_sem = refs[-1]
    if paired:
        got1, got2, total1, total2, half_got, send_sem, recv_sem, half_send, half_recv = refs[:9]
        z, ty, y = lax.axis_index("rows"), lax.axis_index("ty"), lax.axis_index("tx")
        core = lax.rem(ty, 2)
        peer = (z, ty + 1 - 2 * core, y)
        x = ty // 2
        sides = (x, x, y, y)
        peer_x, peer_y = (z, (1 - x) * 2 + core, y), (z, ty, 1 - y)

    def store(k, which):
        slot = lax.rem(k, 2)
        if which == 0:
            source = total1 if paired else grad1
            target = fc1_out.at[:, :, pl.ds(pl.multiple_of(k * source.shape[3], 128), source.shape[3])]
        else:
            source = total2 if paired else grad2
            target = fc2_out.at[pl.ds(pl.multiple_of(k * source.shape[1], 16), source.shape[1])]
        return pltpu.make_async_copy(source.at[slot], target, store_sem.at[slot, which])

    def stores(k):
        return [store(k, 0), store(k, 1)]

    def swaps(k):
        slot = lax.rem(k, 2)
        theirs1 = pl.ds(pl.multiple_of((1 - core) * (block // 2), 128), block // 2)
        theirs2 = pl.ds(pl.multiple_of((1 - core) * (width // 2), 128), width // 2)
        pairs = ((grad1.at[slot, :, :, theirs1], got1.at[k]), (grad2.at[slot, :, theirs2], got2.at[k]))
        return [
            pltpu.make_async_remote_copy(
                src_ref=source,
                dst_ref=target,
                send_sem=send_sem.at[k, n],
                recv_sem=recv_sem.at[k, n],
                device_id=peer,
                device_id_type=MESH,
            )
            for n, (source, target) in enumerate(pairs)
        ]

    def halves(k):
        slot = lax.rem(k, 2)
        part = total1.shape[2] // 2
        copies = []
        for n, (side, other) in enumerate(((x, peer_x), (y, peer_y))):
            theirs = pl.ds(pl.multiple_of((1 - side) * part, 16), part)
            copies.append(
                pltpu.make_async_remote_copy(
                    src_ref=total1.at[slot, 2 * n : 2 * n + 2, theirs],
                    dst_ref=half_got.at[k, 2 * n : 2 * n + 2],
                    send_sem=half_send.at[k, n],
                    recv_sem=half_recv.at[k, n],
                    device_id=other,
                    device_id_type=MESH,
                )
            )
        return copies

    def late(k):
        slot = lax.rem(k, 2)
        part = total1.shape[2] // 2
        for copy in halves(k):
            copy.wait()
        for n in range(4):
            kept = pl.ds(pl.multiple_of(sides[n] * part, 16), part)
            total1[slot, n, kept, :] = total1[slot, n, kept, :] + half_got[k, n]
        store(k, 0).start()

    def settle(k):
        slot = lax.rem(k, 2)
        if paired:
            for copy in swaps(k):
                copy.wait()

            @pl.when(k >= 2)
            def _():
                for copy in stores(k - 2):
                    copy.wait()

            mine1 = pl.ds(pl.multiple_of(core * (block // 2), 128), block // 2)
            mine2 = pl.ds(pl.multiple_of(core * (width // 2), 128), width // 2)
            total1[slot] = grad1[slot, :, :, mine1] + got1[k]
            total2[slot] = grad2[slot, :, mine2] + got2[k]
            store(k, 1).start()

            @pl.when(k < last)
            def _():
                for copy in halves(k):
                    copy.start()

            @pl.when(k == last)
            def _():
                store(k, 0).start()
        else:
            for copy in stores(k):
                copy.start()

    @pl.when(step == 0)
    def _():
        if paired:
            greet([peer, peer_x, peer_y])
        total = jnp.zeros((1, width), jnp.float32)
        for at in parts:
            grad = out_grad[at, :]
            out_low[at, :] = grad.astype(low)
            total = total + down_sum(grad)
            value = stream[at, :] + vectors[4:5]
            for k in range(2):
                value = value + mm(attended[k], proj_weight[k * width // 2 : (k + 1) * width // 2], 1, 0)
            middle[at, :] = value
            unit, rate = normalised(value)
            normed[at, :] = (unit * vectors[5:6] + vectors[6:7]).astype(low)
        vector_grads[7:8] = total
        forward_sum[...] = jnp.zeros_like(forward_sum)
        backward_sum[...] = jnp.zeros_like(backward_sum)

    slot = lax.rem(step, 2)
    if not paired:

        @pl.when(step >= 2)
        def _():
            for copy in stores(step - 2):
                copy.wait()

    bias_grad = jnp.zeros((1, block), jnp.float32)
    actives, hidden_lows = [], []
    for at in parts:
        hidden = mm(normed[at, :], fc1_weight[...], 1, 0) + hidden_bias[0]
        share = 0.5 + 0.5 * erf_of(hidden * 0.7071067811865476)
        density = jnp.exp(hidden * hidden * -0.5) * 0.3989422804014327
        active = (hidden * share).astype(low)
        hidden_grad = active_grad[at, :].astype(jnp.float32) * (share + hidden * density)
        bias_grad = bias_grad + down_sum(hidden_grad)
        hidden_low = hidden_grad.astype(low)
        forward_sum[at, :] = forward_sum[at, :] + mm(active, fc2_weight[...], 1, 0)
        backward_sum[at, :] = backward_sum[at, :] + mm(hidden_low, fc1_weight[...], 1, 1)
        actives.append(active)
        hidden_lows.append(hidden_low)
    hidden_bias_grad[0] = bias_grad
    grad2[slot] = mm(jnp.concatenate(actives, axis=0), out_low[...], 0, 0).astype(low)
    grad1[slot] = mm(normed[...], jnp.concatenate(hidden_lows, axis=0), 0, 0).astype(low).reshape(grad1.shape[1:])
    if paired:
        for copy in swaps(step):
            copy.start()

        @pl.when(step > 1)
        def _():
            late(step - 2)

        @pl.when(step > 0)
        def _():
            settle(step - 1)
    else:
        settle(step)

    @pl.when(step == last)
    def _():
        gain_sum = jnp.zeros((1, width), jnp.float32)
        bias_sum = jnp.zeros((1, width), jnp.float32)
        mid_sum = jnp.zeros((1, width), jnp.float32)
        lows = []
        for at in parts:
            unit, rate = normalised(middle[at, :])
            conv_in[at, :] = (middle[at, :] + forward_sum[at, :] + vectors[7:8]).astype(low)
            incoming = backward_sum[at, :]
            gain_sum = gain_sum + down_sum(incoming * unit)
            bias_sum = bias_sum + down_sum(incoming)
            grad = out_grad[at, :] + norm_back(incoming, unit, rate, vectors[5:6])
            mid_grad[at, :] = grad
            mid_sum = mid_sum + down_sum(grad)
            mid_low = grad.astype(low)
            lows.append(mid_low)
            for k in range(2):
                attended_grad[k] = mm(mid_low, proj_weight[k * width // 2 : (k + 1) * width // 2], 1, 1).astype(low)
        for k in range(2):
            proj_grad[k * width // 2 : (k + 1) * width // 2] = mm(attended[k], lows[0], 0, 0).astype(low)
        vector_grads[4:5] = mid_sum
        vector_grads[5:6] = gain_sum
        vector_grads[6:7] = bias_sum
        if paired:
            late(last - 1)
            settle(step)
        for k in (last - 1, last):
            for copy in stores(k):
                copy.wait()


def middle(attended, stream, out_grad, active_grad, proj_weight, vectors, hidden_bias, fc1_weight, fc2_weight, paired):
    token_count, width = stream.shape
    hidden_width = fc1_weight.shape[1]
    steps, _, block = hidden_bias.shape
    low, wide = jnp.bfloat16, jnp.float32
    cut = 2 if paired else 1
    vmem, anywhere = pl.BlockSpec(memory_space=pltpu.VMEM), pl.BlockSpec(memory_space=pl.ANY)
    scratch = [
        pltpu.VMEM((token_count, width), wide),
        pltpu.VMEM((token_count, width), low),
        pltpu.VMEM((token_count, width), low),
        pltpu.VMEM((token_count, width), wide),
        pltpu.VMEM((token_count, width), wide),
        pltpu.VMEM((2, 4, width // 4, block), low),
        pltpu.VMEM((2, block, width), low),
    ]
    if paired:
        scratch += [
            pltpu.VMEM((steps, 4, width // 4, block // 2), low),
            pltpu.VMEM((steps, block, width // 2), low),
            pltpu.VMEM((2, 4, width // 4, block // 2), low),
            pltpu.VMEM((2, block, width // 2), low),
            pltpu.VMEM((steps, 4, width // 8, block // 2), low),
            pltpu.SemaphoreType.DMA((steps, 2)),
            pltpu.SemaphoreType.DMA((steps, 2)),
            pltpu.SemaphoreType.DMA((steps, 2)),
            pltpu.SemaphoreType.DMA((steps, 2)),
        ]
        params = pltpu.CompilerParams(collective_id=4, has_side_effects=True, vmem_limit_bytes=full_vmem)
    else:
        params = pltpu.CompilerParams(vmem_limit_bytes=full_vmem)
    return pl.pallas_call(
        functools.partial(middle_kernel, paired),
        grid=(steps,),
        out_shape=[
            jax.ShapeDtypeStruct((4, width // 4, hidden_width // cut), low),
            jax.ShapeDtypeStruct((hidden_width, width // cut), low),
            jax.ShapeDtypeStruct((steps, 1, block), wide),
            jax.ShapeDtypeStruct((width, width), low),
            jax.ShapeDtypeStruct((2, token_count, width // 2), low),
            jax.ShapeDtypeStruct((token_count, width), wide),
            jax.ShapeDtypeStruct((token_count, width), low),
            jax.ShapeDtypeStruct((8, width), wide),
        ],
        in_specs=[vmem] * 5
        + [
            pl.BlockSpec((1, 1, block), lambda k: (k, 0, 0)),
            pl.BlockSpec((token_count, block), lambda k: (0, k)),
            pl.BlockSpec((width, block), lambda k: (0, k)),
            pl.BlockSpec((block, width), lambda k: (k, 0)),
        ],
        out_specs=[anywhere, anywhere, pl.BlockSpec((1, 1, block), lambda k: (k, 0, 0))] + [vmem] * 5,
        scratch_shapes=scratch + [pltpu.SemaphoreType.DMA((2, 2))],
        compiler_params=params,
        name="middle",
    )(attended, stream, out_grad, proj_weight, vectors, hidden_bias, active_grad, fc1_weight, fc2_weight)


def rear_kernel(
    kinds, reduces, projected_in, qkv_in, normed_in, stream_in, mid_in, embedded_in, skip_in, skip_weight_in,
    latent, vectors, middle_grads, hidden_bias_grad, conv_grad, *refs
):
    count = len(kinds)
    resumed, refs = refs[:count], refs[count:]
    skip_input_grad, refs = refs[0], refs[1:]
    if reduces:
        sums, refs = refs[: count + 6], refs[count + 6 :]
        peers = chip_peers()
    grads, refs = refs[:6], refs[6:]
    skip_grad, thin, flat = grads[3:]
    projected_grad, qkv_weight, normed, stream, mid_grad, embedded, skip, skip_weight, stream_low, load_sem = refs[:10]
    sources = (projected_in, normed_in, qkv_in, stream_in, mid_in, embedded_in, skip_in, skip_weight_in)
    targets = (projected_grad, normed, qkv_weight, stream, mid_grad, embedded, skip, skip_weight)
    loads = [pltpu.make_async_copy(a, b, load_sem.at[k]) for k, (a, b) in enumerate(zip(sources, targets))]
    for load in loads[:3]:
        load.start()
    items = [None] * 10
    if reduces:
        items = make_reducers(kinds + (("plane", False),) * 6, resumed + grads, sums, refs[10:], range(count + 3))
        greet([peers[name] for name in ("core", "x", "y", "xy")] + peers["z"])
        for item in items[:count]:
            item.begin()
    fc1, fc2a, fc2b, proj, qkv0, qkv1, qkv2, skips, thins, flats = items
    for load in loads[3:]:
        load.start()
    width = stream.shape[1]
    low = jnp.bfloat16
    made = {}

    def open_up(*some):
        for item in some:
            if reduces:
                item.begin()

    def weight_grad(k):
        if k == 0:
            loads[0].wait()
            loads[1].wait()
        piece = mm(normed[...], projected_grad[:, k * width : (k + 1) * width], 0, 0)
        grads[k][...] = piece.astype(low).reshape(grads[k].shape)
        open_up((qkv0, qkv1, qkv2)[k])

    def norm():
        for load in loads[2:5]:
            load.wait()
        incoming = mm(projected_grad[...], qkv_weight[...], 1, 1)
        unit, rate = normalised(stream[...])
        grad = mid_grad[...] + norm_back(incoming, unit, rate, vectors[2:3])
        made["rows"] = [down_sum(grad), down_sum(incoming * unit), down_sum(incoming)]
        stream_low[...] = grad.astype(low)

    def skip_weight_grad():
        loads[5].wait()
        loads[6].wait()
        skip_grad[0:2] = mm(embedded[...], stream_low[...], 0, 0).astype(low).reshape(2, width // 2, width)
        skip_grad[2:4] = mm(skip[...], stream_low[...], 0, 0).astype(low).reshape(2, width // 2, width)
        open_up(skips)

    def joined():
        loads[7].wait()
        embed_grad = mm(stream_low[...], skip_weight[:width], 1, 1)
        embed_weight_grad = mm(embed_grad.astype(low), latent[...], 0, 0)
        rest = jnp.zeros((width, 128 - 2 * 16), jnp.float32)
        thin[:, :, :128] = conv_grad[:, :128].astype(low).reshape(4, width // 4, 128)
        edge = jnp.concatenate([conv_grad[:, 128:144], embed_weight_grad, rest], axis=1)
        thin[:, :, 128:] = edge.astype(low).reshape(4, width // 4, 128)
        rows = [down_sum(embed_grad)] + made["rows"] + [middle_grads[k : k + 1] for k in range(4, 8)]
        stack = jnp.concatenate(rows, axis=0)
        share = width // 4
        hidden_line = jnp.concatenate([hidden_bias_grad[k] for k in range(hidden_bias_grad.shape[0])], axis=1)
        for block in range(4):
            own = stack[:, block * share : (block + 1) * share]
            own = jnp.concatenate([own, jnp.zeros((8, 256 - share), jnp.float32)], axis=1)
            line = hidden_line[:, block * width : (block + 1) * width]
            pieces = [line[:, k * 256 : (k + 1) * 256] for k in range(width // 256)]
            body = jnp.concatenate([own] + pieces + [jnp.zeros((8 - len(pieces), 256), jnp.float32)], axis=0)
            flat[block, 0:16] = body.astype(low)
            flat[block, 16:64] = jnp.zeros((48, 256), low)
        open_up(thins, flats)

    def input_grad():
        skip_input_grad[...] = mm(stream_low[...], skip_weight[width:], 1, 1).astype(low)

    def advance(*some):
        for item in some:
            if reduces:
                item.step()

    advance(proj, fc2b, fc2a)
    weight_grad(0)
    weight_grad(1)
    weight_grad(2)
    advance(qkv0, qkv2)
    norm()
    advance(qkv0, qkv1)
    skip_weight_grad()
    advance(qkv0, qkv2, skips)
    joined()
    advance(qkv2, thins, proj, qkv1, skips, thins, qkv1, fc1)
    advance(qkv0, qkv0, fc2b, proj, skips, flats, thins, fc2a)
    advance(qkv1, qkv1, qkv2, qkv2, qkv0, fc1, qkv1, fc2a)
    advance(flats, fc2b, qkv2, skips, skips, qkv1, fc2a, proj)
    advance(fc2b, flats, qkv0, fc1)
    input_grad()
    advance(qkv0, thins, thins, flats, flats, fc1, qkv1, qkv2)
    advance(skips, fc2a, thins, flats, qkv2, fc2a, flats, skips)
    advance(thins)
    assert not reduces or not any(item.stages for item in items)


def rear(projected_grad, qkv_weight, normed, stream, mid_grad, embedded, skip, skip_weight, latent, vectors, middle_grads, hidden_bias_grad, conv_grad, resumed, reduces):
    token_count, width = stream.shape
    low = jnp.bfloat16
    kinds = tuple((start, True) for start, _, _ in resumed)
    sizes = [(width // 4, width)] * 3 + [(width // 2, width), (width // 4, 256), (64, 256)]
    totals = [shape for _, _, shape in resumed] + [(r, c // 2) for r, c in sizes]
    vmem, anywhere = pl.BlockSpec(memory_space=pltpu.VMEM), pl.BlockSpec(memory_space=pl.ANY)
    big = [projected_grad, qkv_weight, normed, stream, mid_grad, embedded, skip, skip_weight]
    out_shape = [jax.ShapeDtypeStruct((token_count, width), low)]
    out_specs = [vmem]
    scratch = []
    if reduces:
        out_shape += [jax.ShapeDtypeStruct((2,) + shape, low) for shape in totals]
        out_specs += [anywhere] * len(totals)
        scratch += [pltpu.VMEM((4,) + shape, low) for shape in sizes]
        params = pltpu.CompilerParams(collective_id=3, has_side_effects=True, vmem_limit_bytes=full_vmem)
    else:
        out_shape += [jax.ShapeDtypeStruct((4,) + shape, low) for shape in sizes]
        out_specs += [vmem] * len(sizes)
        params = pltpu.CompilerParams(vmem_limit_bytes=full_vmem)
    scratch += [pltpu.VMEM(entry.shape, entry.dtype) for entry in big]
    scratch += [pltpu.VMEM((token_count, width), low), pltpu.SemaphoreType.DMA((len(big),))]
    if reduces:
        scratch += reducer_scratch(kinds + (("plane", False),) * 6, totals)
    return pl.pallas_call(
        functools.partial(rear_kernel, kinds, reduces),
        out_shape=out_shape,
        in_specs=[anywhere] * len(big) + [vmem] * 5 + [anywhere] * len(kinds),
        out_specs=out_specs,
        scratch_shapes=scratch,
        compiler_params=params,
        name="rear",
    )(*big, latent, vectors, middle_grads, hidden_bias_grad, conv_grad, *[entry for _, entry, _ in resumed])


def finish_kernel(patch, plan, *refs):
    count = len(plan)
    sums, (thin, flat, conv_out) = refs[:count], refs[count : count + 3]
    totals, refs = refs[count + 3 : count + 8], refs[count + 8 :]
    (embed_turned, conv_turned), lines, fc1_line, output, refs = refs[:2], refs[2:10], refs[10], refs[11], refs[12:]
    lows, wides, load_sem, store_sem = refs[:count], refs[count : count + 5], refs[count + 5], refs[count + 6]
    loads = [pltpu.make_async_copy(a, b, load_sem.at[k]) for k, (a, b) in enumerate(zip(sums, lows))]
    for load in loads:
        load.start()
    stores = []
    for k, (low, (which, start, piece, left)) in enumerate(zip(lows, plan)):
        loads[k].wait()
        wide = wides[which]
        half, depth = low.shape[2], low.shape[1]

        def body(i, carry):
            at = pl.ds(pl.multiple_of(i * 16, 16), 16)
            to = pl.ds(pl.multiple_of(start + i * 16, 16), 16)
            for core in range(2):
                for n in range(half // piece):
                    column = left + (2 * n + core) * piece
                    wide[to, column : column + piece] = low[core, at, n * piece : (n + 1) * piece].astype(jnp.float32)
            return carry

        lax.fori_loop(0, depth // 16, body, 0)
        there = (pl.ds(start, depth), pl.ds(left, 2 * half))
        store = pltpu.make_async_copy(wide.at[there], totals[which].at[there], store_sem.at[k])
        store.start()
        stores.append(store)
    share = thin.shape[1]
    turned = jnp.transpose(jnp.concatenate([thin[0], thin[1]], axis=1).astype(jnp.float32))
    taps = 9 * patch
    conv_turned[...] = turned[:taps]
    embed_turned[...] = turned[taps : taps + patch]
    rows = jnp.concatenate([flat[0, 0:16, :], flat[1, 0:16, :]], axis=1).astype(jnp.float32)
    for k, line in enumerate(lines):
        line[...] = rows[k : k + 1, :share].reshape(share)
    fc1_line[...] = jnp.concatenate([rows[k : k + 1] for k in range(8, 11)], axis=1).reshape(fc1_line.shape[0])
    for row in range(output.shape[0]):
        output[row] = jnp.transpose(conv_out[row].astype(jnp.float32)).astype(jnp.bfloat16)
    for store in stores:
        store.wait()


def finish(sums, thin, flat, conv_out):
    row_count, patch, tokens = conv_out.shape
    share = thin.shape[1]
    wide = jnp.float32
    plan = tuple(entry[:4] for entry in sums)
    arrays = [entry[4] for entry in sums]
    whole = [(0, 0)] * 5
    for which, start, _, left, entry in sums:
        rows, columns = whole[which]
        whole[which] = (max(rows, start + entry.shape[1]), max(columns, left + 2 * entry.shape[2]))
    vmem, anywhere = pl.BlockSpec(memory_space=pltpu.VMEM), pl.BlockSpec(memory_space=pl.ANY)
    return pl.pallas_call(
        functools.partial(finish_kernel, patch, plan),
        out_shape=[jax.ShapeDtypeStruct(shape, wide) for shape in whole]
        + [jax.ShapeDtypeStruct((patch, share), wide), jax.ShapeDtypeStruct((9 * patch, share), wide)]
        + [jax.ShapeDtypeStruct((share,), wide)] * 8
        + [jax.ShapeDtypeStruct((4 * share,), wide), jax.ShapeDtypeStruct((row_count, tokens, patch), jnp.bfloat16)],
        in_specs=[anywhere] * len(arrays) + [vmem] * 3,
        out_specs=[anywhere] * 5 + [vmem] * 12,
        scratch_shapes=[pltpu.VMEM(entry.shape, jnp.bfloat16) for entry in arrays]
        + [pltpu.VMEM(shape, wide) for shape in whole]
        + [pltpu.SemaphoreType.DMA((len(arrays),)), pltpu.SemaphoreType.DMA((len(arrays),))],
        compiler_params=pltpu.CompilerParams(vmem_limit_bytes=full_vmem),
        name="finish",
    )(*arrays, thin, flat, conv_out)


def plane_peers():
    z, ty, y = lax.axis_index("rows"), lax.axis_index("ty"), lax.axis_index("tx")
    core, x = lax.rem(ty, 2), ty // 2
    here = x * 2 + core
    across = (1 - x) * 2 + core
    tiles = {
        "own": here * 2 + y,
        "x": across * 2 + y,
        "y": here * 2 + 1 - y,
        "xy": across * 2 + 1 - y,
    }
    peers = {
        "core": (z, x * 2 + 1 - core, y),
        "x": (z, across, y),
        "y": (z, here, 1 - y),
    }
    return tiles, peers


def plane_peer(k):
    z, ty, y = lax.axis_index("rows"), lax.axis_index("ty"), lax.axis_index("tx")
    x, core = ty // 2, lax.rem(ty, 2)
    flip_x, flip_core, flip_y = k // 4, k // 2 % 2, k % 2
    x = x + flip_x - 2 * flip_x * x
    core = core + flip_core - 2 * flip_core * core
    y = y + flip_y - 2 * flip_y * y
    return (z, x * 2 + core, y), (x * 2 + core) * 2 + y


def greet(peers):
    barrier = pltpu.get_barrier_semaphore()
    for peer in peers:
        pl.semaphore_signal(barrier, inc=1, device_id=peer, device_id_type=MESH)
    pl.semaphore_wait(barrier, len(peers))


def fill_mask(mask_ref, cuts_ref, row, tile, tile_height, tile_width):
    columns = lax.axis_size("tx")
    tokens = tile_height * tile_width
    left_width = cuts_ref[row, 0]
    top_height = cuts_ref[row, 1]

    def image_of(down, across):
        return jnp.where(across < left_width, 0, jnp.where(down < top_height, 1, 2))

    lane = lax.broadcasted_iota(jnp.int32, (8, tokens), 1)
    mine = image_of(*cell_of(lane, tile, tile_height, tile_width, columns))[0:1]
    step = lax.broadcasted_iota(jnp.int32, (tokens, tokens), 0)
    down, across = step // tile_width, step % tile_width
    for other in range(mask_ref.shape[0] // tokens):
        theirs = image_of(
            down + other // columns * tile_height, across + other % columns * tile_width
        )
        mask_ref[other * tokens : (other + 1) * tokens, :] = jnp.where(mine == theirs, 0.0, -1e30)


def two_heads(pair, scale):
    lane = lax.broadcasted_iota(jnp.int32, pair.shape, 1)
    wide = pair.astype(jnp.float32) * scale
    first = jnp.where(lane < pair.shape[1] // 2, wide, 0.0)
    return jnp.concatenate([first, wide - first], axis=0).astype(jnp.bfloat16)


def own_blocks(both):
    head, tokens = both.shape[0] // 2, both.shape[1] // 2
    return jnp.concatenate([both[:head, :tokens], both[head:, tokens:]], axis=0)


def attend_kernel(
    tile_height, tile_width, cuts, query, pairs, cot, conv_turned, fc2_in,
    out, lse, query_out, attended_out, all_out, spread, out_grad_out, active_grad_out,
    cot_all, queries, held, results, scores, mask, shift, fc2_weight, out_grad, active_grad,
    local_sem, send_sem, recv_sem, cot_sem, cot_send_sem, cot_recv_sem, side_sem
):
    _, row_count, tokens, half = query.shape
    tile_count = held.shape[1]
    width = 2 * half
    tiles, peers = plane_peers()
    own = tiles["own"]
    x = lax.axis_index("ty") // 2
    fc2_load = pltpu.make_async_copy(fc2_in, fc2_weight, side_sem.at[0])
    fc2_load.start()
    greet([plane_peer(k)[0] for k in range(1, tile_count)])
    cot_copies = [pltpu.make_async_copy(cot, cot_all.at[own], cot_sem.at[0])]
    for k in range(1, tile_count):
        cot_copies.append(
            pltpu.make_async_remote_copy(
                src_ref=cot,
                dst_ref=cot_all.at[own],
                send_sem=cot_send_sem.at[k],
                recv_sem=cot_recv_sem.at[k],
                device_id=plane_peer(k)[0],
                device_id_type=MESH,
            )
        )

    def send(row, slot, source, target, peer):
        copy = pltpu.make_async_remote_copy(
            src_ref=source,
            dst_ref=target,
            send_sem=send_sem.at[row, slot],
            recv_sem=recv_sem.at[row, slot],
            device_id=peer,
            device_id_type=MESH,
        )
        copy.start()
        flights[row][slot] = copy

    def keep(row, slot, source, target):
        copy = pltpu.make_async_copy(source, target, local_sem.at[row, slot])
        copy.start()
        kept[row][slot] = copy

    flights = [{} for _ in range(row_count)]
    kept = [{} for _ in range(row_count)]

    def begin(row):
        here = held.at[row, own]
        send(row, 1, pairs.at[1 - x, row], here, peers["x"])
        send(row, 0, query.at[1 - x, row], queries.at[row, 1], peers["x"])
        send(row, 2, pairs.at[x, row], here, peers["y"])
        send(row, 3, pairs.at[x, row], here, peers["core"])
        keep(row, 0, query.at[x, row], queries.at[row, 0])
        keep(row, 1, pairs.at[x, row], here)

    def forward(row):
        flights[row][1].wait_recv()
        tile = held.at[row, tiles["x"]]
        send(row, 4, tile, tile, peers["y"])
        send(row, 5, tile, tile, peers["core"])
        flights[row][2].wait_recv()
        tile = held.at[row, tiles["y"]]
        send(row, 6, tile, tile, peers["core"])

    def gather_row(row):
        flights[row][4].wait_recv()
        tile = held.at[row, tiles["xy"]]
        send(row, 7, tile, tile, peers["core"])
        for slot in (0, 3, 5, 6, 7):
            flights[row][slot].wait_recv()
        for slot in range(8):
            flights[row][slot].wait_send()
        for slot in range(2):
            kept[row][slot].wait()
        keep(row, 3, held.at[row], all_out.at[row])
        keep(row, 4, queries.at[row], query_out.at[row])

    chunk = 2

    def compute(row):
        def one_pair(p, carry, which=(0, 1)):
            at = pl.ds(pl.multiple_of(p * 128, 128), 128)
            at_value = pl.ds(pl.multiple_of(half + p * 128, 128), 128)
            for t in which:
                both = two_heads(queries[row, t, :, at], 0.125)
                peak = None
                for c in range(tile_count // chunk):
                    span = slice(c * chunk * tokens, (c + 1) * chunk * tokens)
                    keys = held[row, c * chunk : (c + 1) * chunk, :, at].reshape(chunk * tokens, 128)
                    extra = mask[row, t, span, :]
                    part = mm(keys, both, 1, 1) + jnp.concatenate([extra, extra], axis=1)
                    scores[t, span, :] = part
                    top = jnp.max(part, axis=0, keepdims=True)
                    peak = top if peak is None else jnp.maximum(peak, top)
                total = jnp.zeros_like(peak)
                summed = jnp.zeros((128, 2 * tokens), jnp.float32)
                for c in range(tile_count // chunk):
                    span = slice(c * chunk * tokens, (c + 1) * chunk * tokens)
                    values = held[row, c * chunk : (c + 1) * chunk, :, at_value].reshape(chunk * tokens, 128)
                    part = jnp.exp(scores[t, span, :] - peak)
                    total = total + jnp.sum(part, axis=0, keepdims=True)
                    summed = summed + mm(values, part.astype(jnp.bfloat16), 0, 0)
                blocks = own_blocks(summed / total)
                results[row, t, :, at] = jnp.transpose(blocks).astype(jnp.bfloat16)
                lse[row, p, t] = peak + jnp.log(total)
            return carry

        if row < row_count - 1:
            lax.fori_loop(0, half // 128, one_pair, 0)
            hand_back(row)
        else:
            lax.fori_loop(0, half // 128, functools.partial(one_pair, which=(1,)), 0)
            hand_back(row)
            lax.fori_loop(0, half // 128, functools.partial(one_pair, which=(0,)), 0)
        keep(row, 5, results.at[row, 0], out.at[x, row])
        keep(row, 6, results.at[row], attended_out.at[row])

    def hand_back(row):
        send(row, 8, results.at[row, 1], out.at[x, row], peers["x"])

    side_copies = []
    parts = [slice(k * tokens, (k + 1) * tokens) for k in range(row_count)]

    def spread_out():
        patch = cot_all.shape[2]
        turned = jnp.concatenate(
            [cot_all[t].reshape(row_count * patch, tokens) for t in range(tile_count)], axis=1
        )
        moved = mm(turned, shift[...], 1, 0)
        for row in range(row_count):
            for p in range(9):
                piece = moved[row * patch : (row + 1) * patch, p * tokens : (p + 1) * tokens]
                piece = piece * same_image(cuts, row, p, tile_height, tile_width)
                spread[p * patch : (p + 1) * patch, parts[row]] = piece.astype(jnp.bfloat16)
        out_grad[...] = mm(spread[...], conv_turned[...], 0, 0)
        copy = pltpu.make_async_copy(out_grad, out_grad_out, side_sem.at[1])
        copy.start()
        side_copies.append(copy)

    def activate():
        for k in range(fc2_weight.shape[0] // width):
            span = slice(k * width, (k + 1) * width)
            low = out_grad[...].astype(jnp.bfloat16)
            active_grad[:, span] = mm(low, fc2_weight[span, :], 1, 1).astype(jnp.bfloat16)
        copy = pltpu.make_async_copy(active_grad, active_grad_out, side_sem.at[2])
        copy.start()
        side_copies.append(copy)

    for copy in cot_copies:
        copy.start()
    begin(0)
    fill_shift(shift, tile_height, tile_width)
    for copy in cot_copies:
        copy.wait()
    spread_out()
    forward(0)
    for row in range(1, min(row_count, 3)):
        begin(row)
    fc2_load.wait()
    activate()
    for row in range(row_count):
        for t, name in enumerate(("own", "x")):
            fill_mask(mask.at[row, t], cuts, row, tiles[name], tile_height, tile_width)
    for row in range(row_count):
        gather_row(row)
        compute(row)
        for later in range(1 if row == 0 else row + 2, min(row + 3, row_count)):
            if later > 2:
                begin(later)
            forward(later)
    for row in range(row_count):
        flights[row][8].wait()
        for slot in range(3, 7):
            kept[row][slot].wait()
    for copy in side_copies:
        copy.wait()


def attend(cuts, query, pairs, cot, conv_turned, fc2_weight, tile_height, tile_width):
    _, row_count, tokens, half = query.shape
    tile_count = lax.axis_size("ty") * lax.axis_size("tx")
    width = 2 * half
    low, wide = jnp.bfloat16, jnp.float32
    vmem, anywhere = pl.BlockSpec(memory_space=pltpu.VMEM), pl.BlockSpec(memory_space=pl.ANY)
    return pl.pallas_call(
        functools.partial(attend_kernel, tile_height, tile_width),
        out_shape=[
            jax.ShapeDtypeStruct((2, row_count, tokens, half), low),
            jax.ShapeDtypeStruct((row_count, half // 128, 2, 1, 2 * tokens), wide),
            jax.ShapeDtypeStruct((row_count, 2, tokens, half), low),
            jax.ShapeDtypeStruct((row_count, 2, tokens, half), low),
            jax.ShapeDtypeStruct((row_count, tile_count, tokens, width), low),
            jax.ShapeDtypeStruct((conv_turned.shape[0], row_count * tokens), low),
            jax.ShapeDtypeStruct((row_count * tokens, width), wide),
            jax.ShapeDtypeStruct((row_count * tokens, fc2_weight.shape[0]), low),
        ],
        in_specs=[pl.BlockSpec(memory_space=pltpu.SMEM)] + [anywhere] * 3 + [vmem, anywhere],
        out_specs=[anywhere, vmem] + [anywhere] * 3 + [vmem] + [anywhere] * 2,
        scratch_shapes=[
            pltpu.VMEM((tile_count,) + cot.shape, low),
            pltpu.VMEM((row_count, 2, tokens, half), low),
            pltpu.VMEM((row_count, tile_count, tokens, width), low),
            pltpu.VMEM((row_count, 2, tokens, half), low),
            pltpu.VMEM((2, tile_count * tokens, 2 * tokens), wide),
            pltpu.VMEM((row_count, 2, tile_count * tokens, tokens), wide),
            pltpu.VMEM((tile_count * tokens, 9 * tokens), low),
            pltpu.VMEM(fc2_weight.shape, low),
            pltpu.VMEM((row_count * tokens, width), wide),
            pltpu.VMEM((row_count * tokens, fc2_weight.shape[0]), low),
            pltpu.SemaphoreType.DMA((row_count, 7)),
            pltpu.SemaphoreType.DMA((row_count, 9)),
            pltpu.SemaphoreType.DMA((row_count, 9)),
            pltpu.SemaphoreType.DMA((1,)),
            pltpu.SemaphoreType.DMA((tile_count,)),
            pltpu.SemaphoreType.DMA((tile_count,)),
            pltpu.SemaphoreType.DMA((3,)),
        ],
        compiler_params=pltpu.CompilerParams(
            collective_id=1, has_side_effects=True, vmem_limit_bytes=full_vmem
        ),
        name="attend",
    )(cuts, query, pairs, cot, conv_turned, fc2_weight)


def attend_back_kernel(
    tile_height, tile_width, kinds, done, cuts, query_in, attended_in, grad_in, lse_in, conv_in, conv_turned, spread,
    all_pairs, *refs
):
    count = max([kind[2] for kind in kinds], default=-1) + 1
    sources, refs = refs[:count], refs[count:]
    total_count = len(kinds)
    (out, conv_grad, conv_out), saved, refs = refs[:3], refs[3 : 3 + total_count], refs[3 + total_count :]
    query, attended, grad, lse, row_sem = refs[:5]
    held, terms, core_terms, y_terms, x_terms, x_query, query_grad, mask, shift, taps, part, part_got = refs[5:17]
    send_sem, recv_sem, part_send_sem, part_recv_sem = refs[17:21]
    grads = [
        sources[which] if rows is None else sources[which].at[:, rows[0] : rows[1], :]
        for _, _, which, rows in kinds
    ]
    items = make_reducers([kind[:2] for kind in kinds], grads, saved, refs[21:]) if kinds else []
    for item, columns in zip(items, done):
        item.halved = columns
    row_count, _, tokens, half = query.shape
    tile_count = held.shape[1]
    tiles, peers = plane_peers()
    low = jnp.bfloat16
    x, core = lax.axis_index("ty") // 2, lax.rem(lax.axis_index("ty"), 2)

    def group(which, base=0):
        return pl.ds(pl.multiple_of(base + which * half, 128), half)

    loads = []
    for row in range(row_count):
        loads.append([])
        for k, (source, target) in enumerate((
            (all_pairs.at[row], held.at[row]), (query_in.at[row], query.at[row]), (attended_in.at[row], attended.at[row]),
            (grad_in.at[x, row], grad.at[row, 0]), (lse_in.at[row], lse.at[row]),
        )):
            load = pltpu.make_async_copy(source, target, row_sem.at[row, k])
            load.start()
            loads[-1].append(load)
    greet([plane_peer(k)[0] for k in range(1, tile_count)] + (chip_peers()["z"] if kinds else []))
    chunk = 2
    flights = [{} for _ in range(row_count)]

    def send(row, slot, source, target, peer):
        copy = pltpu.make_async_remote_copy(
            src_ref=source,
            dst_ref=target,
            send_sem=send_sem.at[row, slot],
            recv_sem=recv_sem.at[row, slot],
            device_id=peer,
            device_id_type=MESH,
        )
        copy.start()
        flights[row][slot] = copy

    def compute(row):
        for load in loads[row]:
            load.wait()
        flights[row][8].wait()
        for t, name in enumerate(("own", "x")):
            fill_mask(mask.at[t], cuts, row, tiles[name], tile_height, tile_width)

        def one_pair(p, carry):
            at = pl.ds(pl.multiple_of(p * 128, 128), 128)
            at_value = pl.ds(pl.multiple_of(half + p * 128, 128), 128)
            boths, both_grads, deltas, levels = [], [], [], []
            for t in range(2):
                grad_pair = grad[row, t, :, at]
                boths.append(two_heads(query[row, t, :, at], 0.125))
                both_grads.append(two_heads(grad_pair, 1.0))
                inner = jnp.transpose(grad_pair.astype(jnp.float32) * attended[row, t, :, at].astype(jnp.float32))
                heads = [inner[: inner.shape[0] // 2], inner[inner.shape[0] // 2 :]]
                deltas.append(jnp.concatenate([jnp.sum(head, axis=0, keepdims=True) for head in heads], axis=1))
                levels.append(lse[row, p, t])
            all_both = jnp.concatenate(boths, axis=0)
            all_grads = jnp.concatenate(both_grads, axis=0)
            query_part = jnp.zeros((128, 4 * tokens), jnp.float32)
            for c in range(tile_count // chunk):
                span = slice(c * chunk * tokens, (c + 1) * chunk * tokens)
                some = slice(c * chunk, (c + 1) * chunk)
                keys = held[row, some, :, at].reshape(chunk * tokens, 128)
                values = held[row, some, :, at_value].reshape(chunk * tokens, 128)
                weight_parts, score_parts = [], []
                for t in range(2):
                    extra = mask[t, span, :]
                    raw = mm(keys, boths[t], 1, 1) + jnp.concatenate([extra, extra], axis=1)
                    weights = jnp.exp(raw - levels[t])
                    weight_parts.append(weights.astype(low))
                    score_parts.append((weights * (mm(values, both_grads[t], 1, 1) - deltas[t])).astype(low))
                score_grad = jnp.concatenate(score_parts, axis=1)
                value_part = mm(jnp.concatenate(weight_parts, axis=1), all_grads, 1, 0)
                key_part = mm(score_grad, all_both, 1, 0)
                query_part = query_part + mm(keys, score_grad, 0, 0)
                terms[row, some, :, at] = key_part.astype(low).reshape(chunk, tokens, 128)
                terms[row, some, :, at_value] = value_part.astype(low).reshape(chunk, tokens, 128)
            for t in range(2):
                blocks = own_blocks(query_part[:, 2 * t * tokens : 2 * (t + 1) * tokens]) * 0.125
                query_grad[row, t, :, at] = jnp.transpose(blocks).astype(low)
            return carry

        lax.fori_loop(0, half // 128, one_pair, 0)

    names = ("own", "x", "y", "xy")

    def begin(row):
        other = 2 - 4 * core
        for k in (3, 2, 1, 0):
            send(row, k, terms.at[row, tiles[names[k]] + other], core_terms.at[row, k], peers["core"])
        send(row, 7, query_grad.at[row, 1], x_query.at[row], peers["x"])

    def add(target, source):
        def body(i, carry):
            at = pl.ds(pl.multiple_of(i * 16, 16), 16)
            target[at, :] = target[at, :] + source[at, :]
            return carry

        lax.fori_loop(0, tokens // 16, body, 0)

    def scatter(row):
        for k in (3, 2, 1, 0):
            flights[row][k].wait()
            tile = terms.at[row, tiles[names[k]]]
            add(tile, core_terms.at[row, k])
            if k == 3:
                send(row, 5, tile, y_terms.at[row, 1], peers["y"])
            if k == 2:
                send(row, 4, tile, y_terms.at[row, 0], peers["y"])

    def pass_on(row):
        flights[row][5].wait()
        tile = terms.at[row, tiles["x"]]
        add(tile, y_terms.at[row, 1])
        send(row, 6, tile, x_terms.at[row], peers["x"])

    def close(row):
        for slot in (4, 6, 7):
            flights[row][slot].wait()
        mine = terms.at[row, tiles["own"]]
        width = 2 * half

        def body(i, carry):
            at = pl.ds(pl.multiple_of(i * 16, 16), 16)
            total = mine[at, :].astype(jnp.float32) + y_terms[row, 0, at, :].astype(jnp.float32)
            total = total.astype(low)
            out[row, at, group(x)] = query_grad[row, 0, at, :]
            out[row, at, group(x, width)] = total[:, :half]
            out[row, at, group(x, 2 * width)] = total[:, half:]
            out[row, at, group(1 - x)] = x_query[row, at, :]
            out[row, at, group(1 - x, width)] = x_terms[row, at, :half]
            out[row, at, group(1 - x, 2 * width)] = x_terms[row, at, half : 2 * half]
            return carry

        lax.fori_loop(0, tokens // 16, body, 0)

    part_copies = []

    def convolve():
        fill_shift(shift, tile_height, tile_width)
        patch = part.shape[2]
        taps[...] = mm(conv_turned[...], conv_in[...], 1, 1)
        rows = []
        for row in range(row_count):
            pieces = []
            for p in range(9):
                piece = taps[p * patch : (p + 1) * patch, row * tokens : (row + 1) * tokens]
                pieces.append(piece * same_image(cuts, row, p, tile_height, tile_width))
            rows.append(jnp.concatenate(pieces, axis=1))
        whole = jnp.concatenate(rows, axis=0)
        coarse = whole.astype(low)
        fine = (whole - coarse.astype(jnp.float32)).astype(low)
        moved = mm(coarse, shift[...], 1, 1) + mm(fine, shift[...], 1, 1)
        for tile in range(tile_count):
            part[tile] = moved[:, tile * tokens : (tile + 1) * tokens].reshape(row_count, patch, tokens)
        for k in range(1, tile_count):
            peer, tile = plane_peer(k)
            copy = pltpu.make_async_remote_copy(
                src_ref=part.at[tile],
                dst_ref=part_got.at[k],
                send_sem=part_send_sem.at[k],
                recv_sem=part_recv_sem.at[k],
                device_id=peer,
                device_id_type=MESH,
            )
            copy.start()
            part_copies.append(copy)
        conv_grad[...] = mm(conv_in[...], spread[...], 0, 1)

    def collect():
        total = part[tiles["own"]]
        for k, copy in enumerate(part_copies):
            copy.wait()
            total = total + part_got[k + 1]
        conv_out[...] = total.astype(low)

    def sum_up(item):
        item.step()
        item.save()

    for row in range(row_count):
        send(row, 8, grad_in.at[1 - x, row], grad.at[row, 1], peers["x"])
    for item in items:
        item.begin()
    if items and row_count == 3:
        fc1, fc2a, fc2b, proj = items
        fc1.step()
        fc2a.step()
        proj.step()
        fc2b.step()
        compute(0)
        fc1.step()
        begin(0)
        scatter(0)
        compute(1)
        begin(1)
        fc2b.step()
        proj.step()
        scatter(1)
        fc1.step()
        compute(2)
        pass_on(0)
        proj.step()
        begin(2)
        scatter(2)
        fc2b.step()
        pass_on(1)
        convolve()
        sum_up(proj)
        pass_on(2)
        sum_up(fc1)
        sum_up(fc2a)
        sum_up(fc2b)
        for row in range(row_count):
            close(row)
        collect()
    else:
        for row in range(row_count):
            compute(row)
            begin(row)
        for row in range(row_count):
            scatter(row)
        for row in range(row_count):
            pass_on(row)
        convolve()
        for row in range(row_count):
            close(row)
        collect()
    for item in items:
        item.land("save")


def attend_back(cuts, query, attended, grad, lse, conv_in, conv_turned, spread, all_pairs, grads, tile_height, tile_width):
    row_count, _, tokens, half = query.shape
    width = 2 * half
    kinds, sources, saves, shapes = [], [], [], []
    for start, paired, entry, rows, _ in grads:
        if not any(entry is source for source in sources):
            sources.append(entry)
        which = [entry is source for source in sources].index(True)
        kinds.append((start, paired, which, rows))
        depth = entry.shape[1] if rows is None else rows[1] - rows[0]
        shapes.append((depth, entry.shape[2] if paired else entry.shape[2] // 2))
        saves.append((depth if start == "z" else depth // 4, shapes[-1][1]))
    kinds = tuple(kinds)
    done = tuple(entry[4] for entry in grads)
    tile_count = all_pairs.shape[1]
    taps = conv_turned.shape[0]
    low, wide = jnp.bfloat16, jnp.float32
    vmem, anywhere = pl.BlockSpec(memory_space=pltpu.VMEM), pl.BlockSpec(memory_space=pl.ANY)
    return pl.pallas_call(
        functools.partial(attend_back_kernel, tile_height, tile_width, kinds, done),
        out_shape=[
            jax.ShapeDtypeStruct((row_count, tokens, 3 * width), low),
            jax.ShapeDtypeStruct((width, taps), wide),
            jax.ShapeDtypeStruct((row_count, taps // 9, tokens), low),
        ]
        + [jax.ShapeDtypeStruct(s, low) for s in saves],
        in_specs=[pl.BlockSpec(memory_space=pltpu.SMEM)] + [anywhere] * 4 + [vmem] * 3 + [anywhere] * (1 + len(sources)),
        out_specs=[vmem] * 3 + [anywhere] * len(saves),
        scratch_shapes=[
            pltpu.VMEM(query.shape, low),
            pltpu.VMEM(query.shape, low),
            pltpu.VMEM(query.shape, low),
            pltpu.VMEM(lse.shape, wide),
            pltpu.SemaphoreType.DMA((row_count, 5)),
            pltpu.VMEM((row_count, tile_count, tokens, width), low),
            pltpu.VMEM((row_count, tile_count, tokens, width), low),
            pltpu.VMEM((row_count, 4, tokens, width), low),
            pltpu.VMEM((row_count, 2, tokens, width), low),
            pltpu.VMEM((row_count, tokens, width), low),
            pltpu.VMEM((row_count, tokens, half), low),
            pltpu.VMEM(query.shape, low),
            pltpu.VMEM((2, tile_count * tokens, tokens), wide),
            pltpu.VMEM((tile_count * tokens, 9 * tokens), low),
            pltpu.VMEM((taps, row_count * tokens), wide),
            pltpu.VMEM((tile_count, row_count, taps // 9, tokens), wide),
            pltpu.VMEM((tile_count, row_count, taps // 9, tokens), wide),
            pltpu.SemaphoreType.DMA((row_count, 9)),
            pltpu.SemaphoreType.DMA((row_count, 9)),
            pltpu.SemaphoreType.DMA((tile_count,)),
            pltpu.SemaphoreType.DMA((tile_count,)),
        ]
        + (reducer_scratch([kind[:2] for kind in kinds], shapes) if kinds else []),
        compiler_params=pltpu.CompilerParams(
            collective_id=2, has_side_effects=True, vmem_limit_bytes=full_vmem
        ),
        name="attend_back",
    )(cuts, query, attended, grad, lse, conv_in, conv_turned, spread, all_pairs, *sources)


def add_rows(target, first, second, rows):
    def body(i, carry):
        at = pl.ds(pl.multiple_of(i * 16, 16), 16)
        target[at, :] = first[at, :] + second[at, :]
        return carry

    lax.fori_loop(0, rows // 16, body, 0)


def add_four(target, others, rows):
    def body(i, carry):
        at = pl.ds(pl.multiple_of(i * 16, 16), 16)
        total = target[at, :].astype(jnp.float32) + others[0, at, :].astype(jnp.float32)
        total = total + (others[1, at, :].astype(jnp.float32) + others[2, at, :].astype(jnp.float32))
        target[at, :] = total.astype(jnp.bfloat16)
        return carry

    lax.fori_loop(0, rows // 16, body, 0)


def chip_peers():
    z, ty, y = lax.axis_index("rows"), lax.axis_index("ty"), lax.axis_index("tx")
    core, x = lax.rem(ty, 2), ty // 2
    across = (1 - x) * 2 + core
    return {
        "core": (z, x * 2 + 1 - core, y),
        "x": (z, across, y),
        "y": (z, ty, 1 - y),
        "xy": (z, across, 1 - y),
        "z": [(lax.rem(z + k, 4), ty, y) for k in (1, 2, 3)],
    }


class Reducer:
    def __init__(self, start, paired, relays, grad, out, buffers, sems, w):
        self.relays, self.halved = relays, 0
        self.start, self.paired, self.grad, self.out, self.w = start, paired, grad, out, w
        self.local_sem, self.send_sem, self.recv_sem = sems
        self.z, ty, self.y = lax.axis_index("rows"), lax.axis_index("ty"), lax.axis_index("tx")
        self.core, self.x = lax.rem(ty, 2), ty // 2
        self.peers = chip_peers()
        self.flying = {}
        self.own = buffers[0]
        if start in ("plane", "z"):
            self.half, self.quarter, self.final = buffers[1:4]
            self.got = None if paired else buffers[4]
            self.depth, self.width = grad.shape[1], grad.shape[2] if paired else grad.shape[2] // 2
        else:
            self.depth, self.width = out.shape[1], out.shape[2]
        if start == "block":
            self.half, self.quarter = buffers[1:]
        share = [self.relay, self.pass_strip] if relays else [self.pass_strip]
        late = [self.begin_late, self.add_half_late, self.add_quarter_late, *share, self.end]
        self.stages = {
            "plane": [self.add_core, self.add_half, self.add_quarter, self.sum_z, self.gather_piece, *share, self.end],
            "z": [self.add_core, self.sum_z_first] + late,
            "block": late,
            "piece": [self.gather_piece, *share, self.end],
        }[start]

    def step(self):
        self.stages.pop(0)()

    def part(self, at):
        if self.start == "block":
            return self.own.at[at]
        return self.own.at[self.z, at]

    def send(self, slot, source, target, peer):
        copy = pltpu.make_async_remote_copy(
            src_ref=source,
            dst_ref=target,
            send_sem=self.send_sem.at[self.w, slot],
            recv_sem=self.recv_sem.at[self.w, slot],
            device_id=peer,
            device_id_type=MESH,
        )
        copy.start()
        return copy

    def keep(self, slot, source, target):
        copy = pltpu.make_async_copy(source, target, self.local_sem.at[self.w, slot])
        copy.start()
        return copy

    def land(self, name):
        for copy in self.flying.pop(name):
            copy.wait()

    def columns(self, which):
        return pl.ds(pl.multiple_of(which * self.width, 128), self.width)

    def rows(self, start, size):
        return pl.ds(pl.multiple_of(start, 16), size)

    def place(self, block, flip_x=False, flip_y=False):
        x = 1 - self.x if flip_x else self.x
        y = 1 - self.y if flip_y else self.y
        later = block // 2
        major = x + later * (y - x)
        minor = y + later * (x - y)
        return self.rows(major * (self.depth // 2) + minor * (self.depth // 4), self.depth // 4)

    def pieces(self, flip_x=False, flip_y=False):
        if self.start in ("plane", "piece"):
            return [self.place(self.z, flip_x, flip_y)]
        x = 1 - self.x if flip_x else self.x
        y = 1 - self.y if flip_y else self.y
        half, less, least = self.depth // 2, self.depth // 4, self.depth // 8
        return [self.rows(x * less + y * least, least), self.rows(half + y * less + x * least, least)]

    def begin(self):
        if self.start in ("block", "piece"):
            self.flying["load"] = [self.keep(0, self.grad, self.own)]
            return
        if self.paired:
            self.flying["core"] = [self.keep(0, self.grad, self.own)]
            return
        swap = self.send(0, self.grad.at[:, :, self.columns(1 - self.core)], self.got, self.peers["core"])
        mine = self.keep(0, self.grad.at[:, :, self.columns(self.core)], self.own)
        self.flying["core"] = [swap, mine]

    def add_core(self):
        self.land("core")
        if not self.paired:
            for block in range(4):
                add_rows(self.own.at[block], self.own.at[block], self.got.at[block], self.depth)
        if self.start == "z":
            self.flying["z"] = [
                self.send(5 + k, self.own.at[peer[0]], self.final.at[k], peer) for k, peer in enumerate(self.peers["z"])
            ]
            return
        part = self.depth // 2
        rest = pl.ds(self.halved, self.width - self.halved)
        theirs = [self.rows((1 - side) * part, part) for side in (self.x, self.y)]
        first = self.send(1, self.own.at[0:2, theirs[0], rest], self.half.at[0:2, :, rest], self.peers["x"])
        second = self.send(2, self.own.at[2:4, theirs[1], rest], self.half.at[2:4, :, rest], self.peers["y"])
        self.flying["half"] = [first, second]

    def add_half(self):
        self.land("half")
        part, less = self.depth // 2, self.depth // 4
        for block in range(4):
            side = self.x if block < 2 else self.y
            rest = pl.ds(self.halved, self.width - self.halved)
            kept = self.own.at[block, self.rows(side * part, part), rest]
            add_rows(kept, kept, self.half.at[block, :, rest], part)
        first = self.own.at[0:2, self.rows(self.x * part + (1 - self.y) * less, less)]
        second = self.own.at[2:4, self.rows(self.y * part + (1 - self.x) * less, less)]
        self.flying["quarter"] = [
            self.send(3, first, self.quarter.at[0:2], self.peers["y"]),
            self.send(4, second, self.quarter.at[2:4], self.peers["x"]),
        ]

    def add_quarter(self):
        self.land("quarter")
        for block in range(4):
            kept = self.own.at[block, self.place(block // 2 * 2)]
            add_rows(kept, kept, self.quarter.at[block], self.depth // 4)
        self.flying["z"] = [
            self.send(5 + k, self.own.at[peer[0], self.place(peer[0])], self.final.at[k], peer)
            for k, peer in enumerate(self.peers["z"])
        ]

    def gather(self, pieces, sources):
        copies = []
        for n, (at, source) in enumerate(zip(pieces, sources)):
            target = self.out.at[self.core, at]
            for k, name in enumerate(("x", "y") if self.relays else ("x", "y", "xy")):
                copies.append(self.send(8 + 3 * n + k, source, target, self.peers[name]))
            copies.append(self.keep(1 + n, source, target))
        self.flying["gather"] = copies

    def relay(self):
        self.land("gather")
        cut = self.width // 256 * 128 + (128 if self.width % 256 and self.w % 2 else 0)
        copies = []
        for n, (from_x, from_y) in enumerate(zip(self.pieces(flip_x=True), self.pieces(flip_y=True))):
            first = self.out.at[self.core, from_x, pl.ds(0, cut)]
            second = self.out.at[self.core, from_y, pl.ds(cut, self.width - cut)]
            copies.append(self.send(14 + 2 * n + 1, first, first, self.peers["y"]))
            copies.append(self.send(14 + 2 * n + 2, second, second, self.peers["x"]))
        self.flying["relay"] = copies

    def sum_z(self):
        self.land("z")
        add_four(self.own.at[self.z, self.place(self.z)], self.final, self.depth // 4)

    def gather_piece(self):
        if self.start == "piece":
            self.land("load")
            self.gather([self.place(self.z)], [self.own])
        else:
            self.gather([self.place(self.z)], [self.own.at[self.z, self.place(self.z)]])

    def sum_z_first(self):
        self.land("z")
        add_four(self.own.at[self.z], self.final, self.depth)

    def save(self):
        source = self.own.at[self.z] if self.start == "z" else self.own.at[self.z, self.place(self.z)]
        self.flying["save"] = [self.keep(1, source, self.out)]

    def begin_late(self):
        if self.start == "block":
            self.land("load")
        half, less = self.depth // 2, self.depth // 4
        self.flying["half"] = [
            self.send(1, self.part(self.rows((1 - self.x) * less, less)), self.half.at[0], self.peers["x"]),
            self.send(2, self.part(self.rows(half + (1 - self.y) * less, less)), self.half.at[1], self.peers["y"]),
        ]

    def add_half_late(self):
        self.land("half")
        half, less, least = self.depth // 2, self.depth // 4, self.depth // 8
        for n, start in enumerate((self.x * less, half + self.y * less)):
            kept = self.part(self.rows(start, less))
            add_rows(kept, kept, self.half.at[n], less)
        first = self.part(self.rows(self.x * less + (1 - self.y) * least, least))
        second = self.part(self.rows(half + self.y * less + (1 - self.x) * least, least))
        self.flying["quarter"] = [
            self.send(3, first, self.quarter.at[0], self.peers["y"]),
            self.send(4, second, self.quarter.at[1], self.peers["x"]),
        ]

    def add_quarter_late(self):
        self.land("quarter")
        least = self.depth // 8
        pieces = self.pieces()
        for n, at in enumerate(pieces):
            add_rows(self.part(at), self.part(at), self.quarter.at[n], least)
        self.gather(pieces, [self.part(at) for at in pieces])

    def pass_strip(self):
        self.land("relay" if self.relays else "gather")
        strip = self.out.at[self.core]
        self.flying["strip"] = [self.send(14, strip, strip, self.peers["core"])]

    def end(self):
        self.land("strip")


def reducer_scratch(kinds, shapes):
    buffers = []
    for (start, paired), (depth, half) in zip(kinds, shapes):
        sizes = {
            "plane": [(4, depth, half), (4, depth // 2, half), (4, depth // 4, half), (3, depth // 4, half)],
            "z": [(4, depth, half), (2, depth // 4, half), (2, depth // 8, half), (3, depth, half)],
            "block": [(depth, half), (2, depth // 4, half), (2, depth // 8, half)],
            "piece": [(depth // 4, half)],
        }[start]
        if not paired:
            sizes.append((4, depth, half))
        buffers += [pltpu.VMEM(size, jnp.bfloat16) for size in sizes]
    count = len(kinds)
    return buffers + [
        pltpu.SemaphoreType.DMA((count, 3)),
        pltpu.SemaphoreType.DMA((count, 19)),
        pltpu.SemaphoreType.DMA((count, 19)),
    ]


def make_reducers(kinds, grads, outs, scratch, relays=()):
    items, at = [], 0
    for w, ((start, paired), grad, out) in enumerate(zip(kinds, grads, outs)):
        size = {"plane": 4, "z": 4, "block": 3, "piece": 1}[start] + (0 if paired else 1)
        items.append(Reducer(start, paired, w in relays, grad, out, scratch[at : at + size], scratch[-3:], w))
        at = at + size
    return items


def sum_by_table(local_grads):
    band_count, column_count = lax.axis_size("ty"), lax.axis_size("tx")
    group_count = lax.axis_size("rows")
    tile_count = band_count * column_count
    table = jnp.concatenate([entry.reshape(group_count, -1) for entry in local_grads], axis=1)
    column_total = table.shape[1]
    padded_columns = -(-column_total // tile_count) * tile_count
    piece_width = padded_columns // tile_count
    table = table.reshape(group_count, tile_count, piece_width)
    shares = lax.psum_scatter(
        table.reshape(group_count * tile_count, piece_width),
        ("rows", "ty", "tx"),
        scatter_dimension=0,
        tiled=True,
    )
    summed = (
        lax.all_gather(shares.astype(jnp.bfloat16), ("ty", "tx"), axis=0, tiled=True)
        .astype(shares.dtype)
        .reshape(-1)
    )
    totals = []
    start_at = 0
    for entry in local_grads:
        length = entry.size // group_count
        shard_shape = (entry.shape[0] // group_count,) + entry.shape[1:]
        totals.append(summed[start_at : start_at + length].reshape(shard_shape))
        start_at = start_at + length
    return tuple(totals)


def shards(
    latent,
    skip_input,
    segment_ids,
    embed_weight,
    embed_bias,
    skip_weight,
    skip_bias,
    norm1_gain,
    norm1_bias,
    qkv_weight,
    proj_weight,
    proj_bias,
    norm2_gain,
    norm2_bias,
    fc1_weight,
    fc1_bias,
    fc2_weight,
    fc2_bias,
    conv_weight,
    cotangent,
):
    row_count, tile_height, tile_width, width = skip_input.shape
    patch = latent.shape[3]
    tokens = tile_height * tile_width
    token_count = row_count * tokens
    low = jnp.bfloat16
    wide = jnp.float32
    conv_turned = conv_weight.T
    flat_latent = latent.reshape(token_count, patch)
    flat_skip = skip_input.reshape(token_count, width)
    biases = (embed_bias, skip_bias, norm1_gain, norm1_bias, proj_bias, norm2_gain, norm2_bias, fc2_bias)
    embedded, stream, normed, query, pairs, cot, vectors, hidden_bias, cuts = front(
        segment_ids, flat_latent, cotangent.reshape(token_count, patch), embed_weight.T, biases, fc1_bias,
        flat_skip, skip_weight, qkv_weight, row_count,
    )
    attended, log_total, held_query, held_attended, held_pairs, spread, out_grad, active_grad = attend(
        cuts, query, pairs, cot, conv_turned, fc2_weight, tile_height, tile_width
    )
    here = (lax.axis_size("rows"), lax.axis_size("ty"), lax.axis_size("tx")) == (4, 4, 2)
    fc1_grad, fc2_grad, hidden_bias_grad, proj_grad, attended_grad, mid_grad, conv_in, middle_grads = middle(
        attended.reshape(2, token_count, width // 2), stream, out_grad, active_grad, proj_weight, vectors, hidden_bias,
        fc1_weight, fc2_weight, here,
    )
    early = []
    if here:
        fc2_blocks = fc2_grad.reshape(4, -1, width // 2)
        middle_row = fc2_blocks.shape[1] // 2
        early = [
            ("plane", True, fc1_grad, None, fc1_grad.shape[2] * 3 // 4),
            ("z", True, fc2_blocks, (0, middle_row), 0),
            ("plane", True, fc2_blocks, (middle_row, 2 * middle_row), 0),
            ("plane", False, proj_grad.reshape(4, -1, width), None, 0),
        ]
    projected_grad, conv_grad, conv_out, *saved = attend_back(
        cuts, held_query, held_attended, attended_grad.reshape(2, row_count, tokens, width // 2), log_total,
        conv_in, conv_turned, spread, held_pairs, early, tile_height, tile_width,
    )
    follow = {"plane": "piece", "z": "block"}
    resumed = [
        (follow[start], entry, (entry.shape[0] if start == "z" else 4 * entry.shape[0], entry.shape[1]))
        for (start, *_), entry in zip(early, saved)
    ]
    skip_input_grad, *rest = rear(
        projected_grad.reshape(token_count, 3 * width), qkv_weight, normed, stream, mid_grad, embedded, flat_skip,
        skip_weight, flat_latent, vectors, middle_grads, hidden_bias_grad, conv_grad, resumed, here,
    )
    skip_input_grad = skip_input_grad.reshape(row_count, tile_height, tile_width, width)
    taps = 9 * patch
    share = width // 4
    if here:
        half = width // 2
        places = [(0, 0, half, 0), (1, 0, half, 0), (1, middle_row, half, 0), (2, 0, half, 0)]
        places += [(3, 0, half, k * width) for k in range(3)] + [(4, 0, half, 0)]
        totals = finish([place + (entry,) for place, entry in zip(places, rest[:8])], rest[8], rest[9], conv_out)
        fc1_total, fc2_total, proj_total, qkv_total, skip_total, embed_turned, conv_grad_turned = totals[:7]
        line, fc1_line = totals[7:15], totals[15]
        output = totals[16].reshape(row_count, tile_height, tile_width, patch)
        return (
            output, skip_input_grad, embed_turned.T, line[0], skip_total, line[1], line[2], line[3], qkv_total,
            proj_total, line[4], line[5], line[6], fc1_total, fc1_line, fc2_total, line[7], conv_grad_turned.T,
        )
    output = conv_out.transpose(0, 2, 1).reshape(row_count, tile_height, tile_width, patch)
    qkv_grad = jnp.concatenate([entry.reshape(-1, width) for entry in rest[:3]], axis=1)
    skip_grad, thin = [entry.reshape(-1, entry.shape[2]) for entry in rest[3:5]]
    flat = rest[5]
    fc1_grad = fc1_grad.reshape(width, -1)
    line = [flat[:, k, :share].reshape(-1) for k in range(8)]
    fc1_line = flat[:, 8:11].reshape(-1)
    local_grads = [
        thin[:, taps : taps + patch], line[0], skip_grad, line[1], line[2], line[3], qkv_grad, proj_grad, line[4],
        line[5], line[6], fc1_grad, fc1_line, fc2_grad, line[7], thin[:, :taps],
    ]
    return (output, skip_input_grad) + sum_by_table([entry.astype(wide) for entry in local_grads])


def solution(mesh):
    return jax.shard_map(
        shards,
        mesh=mesh,
        in_specs=(
            P("rows", "ty", "tx", None),
            P("rows", "ty", "tx", None),
            P("rows", None, None),
            P(),
            P(),
            P(),
            P(),
            P(),
            P(),
            P(),
            P(),
            P(),
            P(),
            P(),
            P(),
            P(),
            P(),
            P(),
            P(),
            P("rows", "ty", "tx", None),
        ),
        out_specs=(
            P("rows", "ty", "tx", None),
            P("rows", "ty", "tx", None),
            P("rows", None),
            P("rows"),
            P("rows", None),
            P("rows"),
            P("rows"),
            P("rows"),
            P("rows", None),
            P("rows", None),
            P("rows"),
            P("rows"),
            P("rows"),
            P("rows", None),
            P("rows"),
            P("rows", None),
            P("rows"),
            P("rows", None),
        ),
        check_vma=False,
    )
```

```python
import functools

import jax
import jax.numpy as jnp
from jax import lax
from jax.experimental import pallas as pl
from jax.experimental.pallas import tpu as pltpu
from jax.sharding import PartitionSpec as P

MESH = pl.DeviceIdType.MESH
norm_eps = 1e-05
full_vmem = 62 * 1024 * 1024


def cell_of(token, tile, tile_height, tile_width, columns):
    down = tile // columns * tile_height + token // tile_width
    across = tile % columns * tile_width + token % tile_width
    return down, across


def fill_shift(shift_ref, tile_height, tile_width):
    tokens = tile_height * tile_width
    bands, columns = lax.axis_size("ty"), lax.axis_size("tx")
    own = lax.axis_index("ty") * columns + lax.axis_index("tx")
    lane = lax.broadcasted_iota(jnp.int32, (8, tokens), 1)
    down, across = cell_of(lane, own, tile_height, tile_width, columns)
    step = lax.broadcasted_iota(jnp.int32, (shift_ref.shape[0], tokens), 0)
    for p in range(9):
        i, j = down - (p // 3 - 1), across - (p % 3 - 1)
        inside = (i >= 0) & (i < bands * tile_height) & (j >= 0) & (j < columns * tile_width)
        tile = i // tile_height * columns + j // tile_width
        place = tile * tokens + i % tile_height * tile_width + j % tile_width
        place = jnp.where(inside, place, -1)[0:1]
        chosen = jnp.where(step == place, 1.0, 0.0)
        shift_ref[:, p * tokens : (p + 1) * tokens] = chosen.astype(jnp.bfloat16)


def same_image(cuts_ref, row, p, tile_height, tile_width):
    tokens = tile_height * tile_width
    columns = lax.axis_size("tx")
    own = lax.axis_index("ty") * columns + lax.axis_index("tx")
    lane = lax.broadcasted_iota(jnp.int32, (8, tokens), 1)
    down, across = cell_of(lane, own, tile_height, tile_width, columns)
    left_width, top_height = cuts_ref[row, 0], cuts_ref[row, 1]

    def image_of(i, j):
        return jnp.where(j < left_width, 0, jnp.where(i < top_height, 1, 2))

    there = image_of(down - (p // 3 - 1), across - (p % 3 - 1))
    return jnp.where(image_of(down, across) == there, 1.0, 0.0)[0:1]


def mm(former, latter, axis_former, axis_latter):
    return lax.dot_general(
        former,
        latter,
        (((axis_former,), (axis_latter,)), ((), ())),
        preferred_element_type=jnp.float32,
    )


def normalised(values):
    average = jnp.mean(values, axis=1, keepdims=True)
    centred = values - average
    rate = lax.rsqrt(jnp.mean(centred * centred, axis=1, keepdims=True) + norm_eps)
    return centred * rate, rate


def norm_back(incoming, unit, rate, gain):
    scaled = incoming * gain
    first = jnp.mean(scaled, axis=1, keepdims=True)
    second = jnp.mean(scaled * unit, axis=1, keepdims=True)
    return (scaled - first - unit * second) * rate


def down_sum(values):
    return jnp.sum(values, axis=0, keepdims=True)


def front_kernel(
    segment_ids, latent, cotangent, embed_turned, *refs
):
    biases, fc1_bias, refs = refs[:8], refs[8], refs[9:]
    skip_in, skip_weight_in, qkv_in, embedded, stream, normed, query, pairs, cot, vectors, hidden_bias, cuts = refs[:12]
    skip, skip_weight, qkv_weight, load_sem = refs[12:]
    sources, targets = (skip_weight_in, skip_in, qkv_in), (skip_weight, skip, qkv_weight)
    loads = [pltpu.make_async_copy(a, b, load_sem.at[k]) for k, (a, b) in enumerate(zip(sources, targets))]
    for load in loads:
        load.start()
    for k, bias in enumerate(biases):
        vectors[k : k + 1] = bias[...].reshape(1, bias.shape[0]).astype(jnp.float32)
    line = fc1_bias[...].reshape(1, fc1_bias.shape[0]).astype(jnp.float32)
    block = hidden_bias.shape[2]
    for k in range(hidden_bias.shape[0]):
        hidden_bias[k] = line[:, k * block : (k + 1) * block]
    width = skip.shape[1]
    row_count, tokens = query.shape[1], query.shape[2]
    side = segment_ids.shape[1]
    for row in range(row_count):

        def count(k, carry):
            left, top = carry
            left = left + jnp.where(segment_ids[row, 0, k] == 0, 1, 0)
            top = top + jnp.where(segment_ids[row, k, side - 1] == 1, 1, 0)
            return left, top

        left, top = lax.fori_loop(0, side, count, (jnp.int32(0), jnp.int32(0)), unroll=8)
        cuts[row, 0] = left
        cuts[row, 1] = top
        at = slice(row * tokens, (row + 1) * tokens)
        cot[row] = jnp.transpose(cotangent[at, :].astype(jnp.float32)).astype(jnp.bfloat16)
        embedded[at, :] = (mm(latent[at, :], embed_turned[...], 1, 0) + vectors[0:1]).astype(jnp.bfloat16)
    loads[0].wait()
    loads[1].wait()
    total = mm(embedded[...], skip_weight[:width], 1, 0) + mm(skip[...], skip_weight[width:], 1, 0) + vectors[1:2]
    stream[...] = total
    unit, rate = normalised(total)
    normed[...] = (unit * vectors[2:3] + vectors[3:4]).astype(jnp.bfloat16)
    loads[2].wait()
    half = width // 2
    for k in range(3):
        piece = mm(normed[...], qkv_weight[:, k * width : (k + 1) * width], 1, 0).astype(jnp.bfloat16)
        for g in range(2):
            part = piece[:, g * half : (g + 1) * half].reshape(row_count, tokens, half)
            if k == 0:
                query[g] = part
            else:
                pairs[g, :, :, (k - 1) * half : k * half] = part


def front(segment_ids, latent, cotangent, embed_turned, biases, fc1_bias, skip, skip_weight, qkv_weight, row_count):
    token_count, width = skip.shape
    tokens = token_count // row_count
    low, wide = jnp.bfloat16, jnp.float32
    smem, vmem = pl.BlockSpec(memory_space=pltpu.SMEM), pl.BlockSpec(memory_space=pltpu.VMEM)
    return pl.pallas_call(
        front_kernel,
        out_shape=[
            jax.ShapeDtypeStruct((token_count, width), low),
            jax.ShapeDtypeStruct((token_count, width), wide),
            jax.ShapeDtypeStruct((token_count, width), low),
            jax.ShapeDtypeStruct((2, row_count, tokens, width // 2), low),
            jax.ShapeDtypeStruct((2, row_count, tokens, width), low),
            jax.ShapeDtypeStruct((row_count, cotangent.shape[1], tokens), low),
            jax.ShapeDtypeStruct((8, width), wide),
            jax.ShapeDtypeStruct((fc1_bias.shape[0] // width, 1, width), wide),
            jax.ShapeDtypeStruct((row_count, 2), jnp.int32),
        ],
        in_specs=[smem] + [vmem] * 12 + [pl.BlockSpec(memory_space=pl.ANY)] * 3,
        out_specs=[vmem] * 8 + [smem],
        scratch_shapes=[pltpu.VMEM(entry.shape, low) for entry in (skip, skip_weight, qkv_weight)]
        + [pltpu.SemaphoreType.DMA((3,))],
        compiler_params=pltpu.CompilerParams(vmem_limit_bytes=full_vmem),
        name="front",
    )(segment_ids, latent, cotangent, embed_turned, *biases, fc1_bias, skip, skip_weight, qkv_weight)


def erf_of(values):
    x = jnp.clip(values, -4.0, 4.0)
    square = x * x
    upper = square * -2.72614225801306e-10 + 2.77068142495902e-08
    for term in (-2.10102402082508e-06, -5.69250639462346e-05, -7.34990630326855e-04, -2.95459980854025e-03, -1.60960333262415e-02):
        upper = upper * square + term
    lower = square * -1.45660718464996e-05 + -2.13374055278905e-04
    for term in (-1.68282697438203e-03, -7.37332916720468e-03, -1.42647390514189e-02):
        lower = lower * square + term
    return x * upper / lower


def middle_kernel(
    paired, attended, stream, out_grad, proj_weight, vectors, hidden_bias, active_grad, fc1_weight, fc2_weight,
    fc1_out, fc2_out, hidden_bias_grad, proj_grad, attended_grad, mid_grad, conv_in, vector_grads,
    middle, normed, out_low, forward_sum, backward_sum, grad1, grad2, *refs
):
    step = pl.program_id(0)
    last = fc2_out.shape[0] // fc2_weight.shape[0] - 1
    token_count, width = stream.shape
    block = fc1_weight.shape[1]
    low = jnp.bfloat16
    parts = [slice(0, token_count)]
    store_sem = refs[-1]
    if paired:
        got1, got2, total1, total2, half_got, send_sem, recv_sem, half_send, half_recv = refs[:9]
        z, ty, y = lax.axis_index("rows"), lax.axis_index("ty"), lax.axis_index("tx")
        core = lax.rem(ty, 2)
        peer = (z, ty + 1 - 2 * core, y)
        x = ty // 2
        sides = (x, x, y, y)
        peer_x, peer_y = (z, (1 - x) * 2 + core, y), (z, ty, 1 - y)

    def store(k, which):
        slot = lax.rem(k, 2)
        if which == 0:
            source = total1 if paired else grad1
            target = fc1_out.at[:, :, pl.ds(pl.multiple_of(k * source.shape[3], 128), source.shape[3])]
        else:
            source = total2 if paired else grad2
            target = fc2_out.at[pl.ds(pl.multiple_of(k * source.shape[1], 16), source.shape[1])]
        return pltpu.make_async_copy(source.at[slot], target, store_sem.at[slot, which])

    def stores(k):
        return [store(k, 0), store(k, 1)]

    def swaps(k):
        slot = lax.rem(k, 2)
        theirs1 = pl.ds(pl.multiple_of((1 - core) * (block // 2), 128), block // 2)
        theirs2 = pl.ds(pl.multiple_of((1 - core) * (width // 2), 128), width // 2)
        pairs = ((grad1.at[slot, :, :, theirs1], got1.at[k]), (grad2.at[slot, :, theirs2], got2.at[k]))
        return [
            pltpu.make_async_remote_copy(
                src_ref=source,
                dst_ref=target,
                send_sem=send_sem.at[k, n],
                recv_sem=recv_sem.at[k, n],
                device_id=peer,
                device_id_type=MESH,
            )
            for n, (source, target) in enumerate(pairs)
        ]

    def halves(k):
        slot = lax.rem(k, 2)
        part = total1.shape[2] // 2
        copies = []
        for n, (side, other) in enumerate(((x, peer_x), (y, peer_y))):
            theirs = pl.ds(pl.multiple_of((1 - side) * part, 16), part)
            copies.append(
                pltpu.make_async_remote_copy(
                    src_ref=total1.at[slot, 2 * n : 2 * n + 2, theirs],
                    dst_ref=half_got.at[k, 2 * n : 2 * n + 2],
                    send_sem=half_send.at[k, n],
                    recv_sem=half_recv.at[k, n],
                    device_id=other,
                    device_id_type=MESH,
                )
            )
        return copies

    def late(k):
        slot = lax.rem(k, 2)
        part = total1.shape[2] // 2
        for copy in halves(k):
            copy.wait()
        for n in range(4):
            kept = pl.ds(pl.multiple_of(sides[n] * part, 16), part)
            total1[slot, n, kept, :] = total1[slot, n, kept, :] + half_got[k, n]
        store(k, 0).start()

    def settle(k):
        slot = lax.rem(k, 2)
        if paired:
            for copy in swaps(k):
                copy.wait()

            @pl.when(k >= 2)
            def _():
                for copy in stores(k - 2):
                    copy.wait()

            mine1 = pl.ds(pl.multiple_of(core * (block // 2), 128), block // 2)
            mine2 = pl.ds(pl.multiple_of(core * (width // 2), 128), width // 2)
            total1[slot] = grad1[slot, :, :, mine1] + got1[k]
            total2[slot] = grad2[slot, :, mine2] + got2[k]
            store(k, 1).start()

            @pl.when(k < last)
            def _():
                for copy in halves(k):
                    copy.start()

            @pl.when(k == last)
            def _():
                store(k, 0).start()
        else:
            for copy in stores(k):
                copy.start()

    @pl.when(step == 0)
    def _():
        if paired:
            for other in (peer, peer_x, peer_y):
                pl.semaphore_signal(pltpu.get_barrier_semaphore(), inc=1, device_id=other, device_id_type=MESH)
        total = jnp.zeros((1, width), jnp.float32)
        for at in parts:
            grad = out_grad[at, :]
            out_low[at, :] = grad.astype(low)
            total = total + down_sum(grad)
            value = stream[at, :] + vectors[4:5]
            for k in range(2):
                value = value + mm(attended[k], proj_weight[k * width // 2 : (k + 1) * width // 2], 1, 0)
            middle[at, :] = value
            unit, rate = normalised(value)
            normed[at, :] = (unit * vectors[5:6] + vectors[6:7]).astype(low)
        vector_grads[7:8] = total
        forward_sum[...] = jnp.zeros_like(forward_sum)
        backward_sum[...] = jnp.zeros_like(backward_sum)

    slot = lax.rem(step, 2)
    if not paired:

        @pl.when(step >= 2)
        def _():
            for copy in stores(step - 2):
                copy.wait()

    bias_grad = jnp.zeros((1, block), jnp.float32)
    actives, hidden_lows = [], []
    for at in parts:
        hidden = mm(normed[at, :], fc1_weight[...], 1, 0) + hidden_bias[0]
        share = 0.5 + 0.5 * erf_of(hidden * 0.7071067811865476)
        density = jnp.exp(hidden * hidden * -0.5) * 0.3989422804014327
        active = (hidden * share).astype(low)
        hidden_grad = active_grad[at, :].astype(jnp.float32) * (share + hidden * density)
        bias_grad = bias_grad + down_sum(hidden_grad)
        hidden_low = hidden_grad.astype(low)
        forward_sum[at, :] = forward_sum[at, :] + mm(active, fc2_weight[...], 1, 0)
        backward_sum[at, :] = backward_sum[at, :] + mm(hidden_low, fc1_weight[...], 1, 1)
        actives.append(active)
        hidden_lows.append(hidden_low)
    hidden_bias_grad[0] = bias_grad
    grad2[slot] = mm(jnp.concatenate(actives, axis=0), out_low[...], 0, 0).astype(low)
    grad1[slot] = mm(normed[...], jnp.concatenate(hidden_lows, axis=0), 0, 0).astype(low).reshape(grad1.shape[1:])
    if paired:

        @pl.when(step == 0)
        def _():
            pl.semaphore_wait(pltpu.get_barrier_semaphore(), 3)

        for copy in swaps(step):
            copy.start()

        @pl.when(step > 1)
        def _():
            late(step - 2)

        @pl.when(step > 0)
        def _():
            settle(step - 1)
    else:
        settle(step)

    @pl.when(step == last)
    def _():
        gain_sum = jnp.zeros((1, width), jnp.float32)
        bias_sum = jnp.zeros((1, width), jnp.float32)
        mid_sum = jnp.zeros((1, width), jnp.float32)
        lows = []
        for at in parts:
            unit, rate = normalised(middle[at, :])
            conv_in[at, :] = (middle[at, :] + forward_sum[at, :] + vectors[7:8]).astype(low)
            incoming = backward_sum[at, :]
            gain_sum = gain_sum + down_sum(incoming * unit)
            bias_sum = bias_sum + down_sum(incoming)
            grad = out_grad[at, :] + norm_back(incoming, unit, rate, vectors[5:6])
            mid_grad[at, :] = grad
            mid_sum = mid_sum + down_sum(grad)
            mid_low = grad.astype(low)
            lows.append(mid_low)
            for k in range(2):
                attended_grad[k] = mm(mid_low, proj_weight[k * width // 2 : (k + 1) * width // 2], 1, 1).astype(low)
        for k in range(2):
            proj_grad[k * width // 2 : (k + 1) * width // 2] = mm(attended[k], lows[0], 0, 0).astype(low)
        vector_grads[4:5] = mid_sum
        vector_grads[5:6] = gain_sum
        vector_grads[6:7] = bias_sum
        if paired:
            late(last - 1)
            settle(step)
        for k in (last - 1, last):
            for copy in stores(k):
                copy.wait()


def middle(attended, stream, out_grad, active_grad, proj_weight, vectors, hidden_bias, fc1_weight, fc2_weight, paired):
    token_count, width = stream.shape
    hidden_width = fc1_weight.shape[1]
    steps, _, block = hidden_bias.shape
    low, wide = jnp.bfloat16, jnp.float32
    cut = 2 if paired else 1
    vmem, anywhere = pl.BlockSpec(memory_space=pltpu.VMEM), pl.BlockSpec(memory_space=pl.ANY)
    scratch = [
        pltpu.VMEM((token_count, width), wide),
        pltpu.VMEM((token_count, width), low),
        pltpu.VMEM((token_count, width), low),
        pltpu.VMEM((token_count, width), wide),
        pltpu.VMEM((token_count, width), wide),
        pltpu.VMEM((2, 4, width // 4, block), low),
        pltpu.VMEM((2, block, width), low),
    ]
    if paired:
        scratch += [
            pltpu.VMEM((steps, 4, width // 4, block // 2), low),
            pltpu.VMEM((steps, block, width // 2), low),
            pltpu.VMEM((2, 4, width // 4, block // 2), low),
            pltpu.VMEM((2, block, width // 2), low),
            pltpu.VMEM((steps, 4, width // 8, block // 2), low),
            pltpu.SemaphoreType.DMA((steps, 2)),
            pltpu.SemaphoreType.DMA((steps, 2)),
            pltpu.SemaphoreType.DMA((steps, 2)),
            pltpu.SemaphoreType.DMA((steps, 2)),
        ]
        params = pltpu.CompilerParams(collective_id=4, has_side_effects=True, vmem_limit_bytes=full_vmem)
    else:
        params = pltpu.CompilerParams(vmem_limit_bytes=full_vmem)
    return pl.pallas_call(
        functools.partial(middle_kernel, paired),
        grid=(steps,),
        out_shape=[
            jax.ShapeDtypeStruct((4, width // 4, hidden_width // cut), low),
            jax.ShapeDtypeStruct((hidden_width, width // cut), low),
            jax.ShapeDtypeStruct((steps, 1, block), wide),
            jax.ShapeDtypeStruct((width, width), low),
            jax.ShapeDtypeStruct((2, token_count, width // 2), low),
            jax.ShapeDtypeStruct((token_count, width), wide),
            jax.ShapeDtypeStruct((token_count, width), low),
            jax.ShapeDtypeStruct((8, width), wide),
        ],
        in_specs=[vmem] * 5
        + [
            pl.BlockSpec((1, 1, block), lambda k: (k, 0, 0)),
            pl.BlockSpec((token_count, block), lambda k: (0, k)),
            pl.BlockSpec((width, block), lambda k: (0, k)),
            pl.BlockSpec((block, width), lambda k: (k, 0)),
        ],
        out_specs=[anywhere, anywhere, pl.BlockSpec((1, 1, block), lambda k: (k, 0, 0))] + [vmem] * 5,
        scratch_shapes=scratch + [pltpu.SemaphoreType.DMA((2, 2))],
        compiler_params=params,
        name="middle",
    )(attended, stream, out_grad, proj_weight, vectors, hidden_bias, active_grad, fc1_weight, fc2_weight)


def rear_kernel(
    kinds, reduces, projected_in, qkv_in, normed_in, stream_in, mid_in, embedded_in, skip_in, skip_weight_in,
    latent, vectors, middle_grads, hidden_bias_grad, conv_grad, *refs
):
    count = len(kinds)
    resumed, refs = refs[:count], refs[count:]
    skip_input_grad, refs = refs[0], refs[1:]
    if reduces:
        sums, refs = refs[: count + 6], refs[count + 6 :]
        peers = chip_peers()
    grads, refs = refs[:6], refs[6:]
    skip_grad, thin, flat = grads[3:]
    projected_grad, qkv_weight, normed, stream, mid_grad, embedded, skip, skip_weight, stream_low, load_sem = refs[:10]
    sources = (projected_in, normed_in, qkv_in, stream_in, mid_in, embedded_in, skip_in, skip_weight_in)
    targets = (projected_grad, normed, qkv_weight, stream, mid_grad, embedded, skip, skip_weight)
    loads = [pltpu.make_async_copy(a, b, load_sem.at[k]) for k, (a, b) in enumerate(zip(sources, targets))]
    for load in loads[:3]:
        load.start()
    items = [None] * 10
    if reduces:
        items = make_reducers(kinds + (("plane", False),) * 6, resumed + grads, sums, refs[10:], range(count + 3))
        greet([peers[name] for name in ("core", "x", "y", "xy")] + peers["z"])
        for item in items[:count]:
            item.begin()
    fc1, fc2a, fc2b, proj, qkv0, qkv1, qkv2, skips, thins, flats = items
    for load in loads[3:]:
        load.start()
    width = stream.shape[1]
    low = jnp.bfloat16
    made = {}

    def open_up(*some):
        for item in some:
            if reduces:
                item.begin()

    def weight_grad(k):
        if k == 0:
            loads[0].wait()
            loads[1].wait()
        piece = mm(normed[...], projected_grad[:, k * width : (k + 1) * width], 0, 0)
        grads[k][...] = piece.astype(low).reshape(grads[k].shape)
        open_up((qkv0, qkv1, qkv2)[k])

    def norm():
        for load in loads[2:5]:
            load.wait()
        incoming = mm(projected_grad[...], qkv_weight[...], 1, 1)
        unit, rate = normalised(stream[...])
        grad = mid_grad[...] + norm_back(incoming, unit, rate, vectors[2:3])
        made["rows"] = [down_sum(grad), down_sum(incoming * unit), down_sum(incoming)]
        stream_low[...] = grad.astype(low)

    def skip_weight_grad():
        loads[5].wait()
        loads[6].wait()
        skip_grad[0:2] = mm(embedded[...], stream_low[...], 0, 0).astype(low).reshape(2, width // 2, width)
        skip_grad[2:4] = mm(skip[...], stream_low[...], 0, 0).astype(low).reshape(2, width // 2, width)
        open_up(skips)

    def joined():
        loads[7].wait()
        embed_grad = mm(stream_low[...], skip_weight[:width], 1, 1)
        embed_weight_grad = mm(embed_grad.astype(low), latent[...], 0, 0)
        rest = jnp.zeros((width, 128 - 2 * 16), jnp.float32)
        thin[:, :, :128] = conv_grad[:, :128].astype(low).reshape(4, width // 4, 128)
        edge = jnp.concatenate([conv_grad[:, 128:144], embed_weight_grad, rest], axis=1)
        thin[:, :, 128:] = edge.astype(low).reshape(4, width // 4, 128)
        rows = [down_sum(embed_grad)] + made["rows"] + [middle_grads[k : k + 1] for k in range(4, 8)]
        stack = jnp.concatenate(rows, axis=0)
        share = width // 4
        hidden_line = jnp.concatenate([hidden_bias_grad[k] for k in range(hidden_bias_grad.shape[0])], axis=1)
        for block in range(4):
            own = stack[:, block * share : (block + 1) * share]
            own = jnp.concatenate([own, jnp.zeros((8, 256 - share), jnp.float32)], axis=1)
            line = hidden_line[:, block * width : (block + 1) * width]
            pieces = [line[:, k * 256 : (k + 1) * 256] for k in range(width // 256)]
            body = jnp.concatenate([own] + pieces + [jnp.zeros((8 - len(pieces), 256), jnp.float32)], axis=0)
            flat[block, 0:16] = body.astype(low)
            flat[block, 16:64] = jnp.zeros((48, 256), low)
        open_up(thins, flats)

    def input_grad():
        skip_input_grad[...] = mm(stream_low[...], skip_weight[width:], 1, 1).astype(low)

    def advance(*some):
        for item in some:
            if reduces:
                item.step()

    advance(proj, fc2b, fc2a)
    weight_grad(0)
    weight_grad(1)
    weight_grad(2)
    advance(qkv0, qkv2)
    norm()
    advance(qkv0, qkv1)
    skip_weight_grad()
    advance(qkv0, qkv2, skips)
    joined()
    advance(qkv2, thins, proj, qkv1, skips, thins, qkv1, fc1)
    advance(qkv0, qkv0, fc2b, proj, skips, flats, thins, fc2a)
    advance(qkv1, qkv1, qkv2, qkv2, qkv0, fc1, qkv1, fc2a)
    advance(flats, fc2b, qkv2, skips, skips, qkv1, fc2a, proj)
    advance(fc2b, flats, qkv0, fc1)
    input_grad()
    advance(qkv0, thins, thins, flats, flats, fc1, qkv1, qkv2)
    advance(skips, fc2a, thins, flats, qkv2, fc2a, flats, skips)
    advance(thins)
    assert not reduces or not any(item.stages for item in items)


def rear(projected_grad, qkv_weight, normed, stream, mid_grad, embedded, skip, skip_weight, latent, vectors, middle_grads, hidden_bias_grad, conv_grad, resumed, reduces):
    token_count, width = stream.shape
    low = jnp.bfloat16
    kinds = tuple((start, True) for start, _, _ in resumed)
    sizes = [(width // 4, width)] * 3 + [(width // 2, width), (width // 4, 256), (64, 256)]
    totals = [shape for _, _, shape in resumed] + [(r, c // 2) for r, c in sizes]
    vmem, anywhere = pl.BlockSpec(memory_space=pltpu.VMEM), pl.BlockSpec(memory_space=pl.ANY)
    big = [projected_grad, qkv_weight, normed, stream, mid_grad, embedded, skip, skip_weight]
    out_shape = [jax.ShapeDtypeStruct((token_count, width), low)]
    out_specs = [vmem]
    scratch = []
    if reduces:
        out_shape += [jax.ShapeDtypeStruct((2,) + shape, low) for shape in totals]
        out_specs += [anywhere] * len(totals)
        scratch += [pltpu.VMEM((4,) + shape, low) for shape in sizes]
        params = pltpu.CompilerParams(collective_id=3, has_side_effects=True, vmem_limit_bytes=full_vmem)
    else:
        out_shape += [jax.ShapeDtypeStruct((4,) + shape, low) for shape in sizes]
        out_specs += [vmem] * len(sizes)
        params = pltpu.CompilerParams(vmem_limit_bytes=full_vmem)
    scratch += [pltpu.VMEM(entry.shape, entry.dtype) for entry in big]
    scratch += [pltpu.VMEM((token_count, width), low), pltpu.SemaphoreType.DMA((len(big),))]
    if reduces:
        scratch += reducer_scratch(kinds + (("plane", False),) * 6, totals)
    return pl.pallas_call(
        functools.partial(rear_kernel, kinds, reduces),
        out_shape=out_shape,
        in_specs=[anywhere] * len(big) + [vmem] * 5 + [anywhere] * len(kinds),
        out_specs=out_specs,
        scratch_shapes=scratch,
        compiler_params=params,
        name="rear",
    )(*big, latent, vectors, middle_grads, hidden_bias_grad, conv_grad, *[entry for _, entry, _ in resumed])


def finish_kernel(patch, plan, *refs):
    count = len(plan)
    sums, (thin, flat, conv_out, passed) = refs[:count], refs[count : count + 4]
    totals, refs = refs[count + 4 : count + 9], refs[count + 9 :]
    (embed_turned, conv_turned), lines, fc1_line, output, handed, refs = refs[:2], refs[2:10], refs[10], refs[11], refs[12], refs[13:]
    lows, wides, held, load_sem, store_sem = refs[:count], refs[count : count + 5], *refs[count + 5 :]
    take = pltpu.make_async_copy(passed, held, load_sem.at[count])
    give = pltpu.make_async_copy(held, handed, store_sem.at[count])
    loads = [pltpu.make_async_copy(a, b, load_sem.at[k]) for k, (a, b) in enumerate(zip(sums, lows))]
    for load in loads:
        load.start()
    take.start()
    stores = [give]
    for k, (low, (which, start, piece, left)) in enumerate(zip(lows, plan)):
        loads[k].wait()
        if k == 1:
            take.wait()
            give.start()
        wide = wides[which]
        half, depth = low.shape[2], low.shape[1]

        def body(i, carry):
            at = pl.ds(pl.multiple_of(i * 16, 16), 16)
            to = pl.ds(pl.multiple_of(start + i * 16, 16), 16)
            for core in range(2):
                for n in range(half // piece):
                    column = left + (2 * n + core) * piece
                    wide[to, column : column + piece] = low[core, at, n * piece : (n + 1) * piece].astype(jnp.float32)
            return carry

        lax.fori_loop(0, depth // 16, body, 0)
        there = (pl.ds(start, depth), pl.ds(left, 2 * half))
        store = pltpu.make_async_copy(wide.at[there], totals[which].at[there], store_sem.at[k])
        store.start()
        stores.append(store)
    share = thin.shape[1]
    turned = jnp.transpose(jnp.concatenate([thin[0], thin[1]], axis=1).astype(jnp.float32))
    taps = 9 * patch
    conv_turned[...] = turned[:taps]
    embed_turned[...] = turned[taps : taps + patch]
    rows = jnp.concatenate([flat[0, 0:16, :], flat[1, 0:16, :]], axis=1).astype(jnp.float32)
    for k, line in enumerate(lines):
        line[...] = rows[k : k + 1, :share].reshape(share)
    fc1_line[...] = jnp.concatenate([rows[k : k + 1] for k in range(8, 11)], axis=1).reshape(fc1_line.shape[0])
    for row in range(output.shape[0]):
        output[row] = jnp.transpose(conv_out[row].astype(jnp.float32)).astype(jnp.bfloat16)
    for store in stores:
        store.wait()


def finish(sums, thin, flat, conv_out, passed):
    row_count, patch, tokens = conv_out.shape
    share = thin.shape[1]
    wide = jnp.float32
    plan = tuple(entry[:4] for entry in sums)
    arrays = [entry[4] for entry in sums]
    whole = [(0, 0)] * 5
    for which, start, _, left, entry in sums:
        rows, columns = whole[which]
        whole[which] = (max(rows, start + entry.shape[1]), max(columns, left + 2 * entry.shape[2]))
    vmem, anywhere = pl.BlockSpec(memory_space=pltpu.VMEM), pl.BlockSpec(memory_space=pl.ANY)
    return pl.pallas_call(
        functools.partial(finish_kernel, patch, plan),
        out_shape=[jax.ShapeDtypeStruct(shape, wide) for shape in whole]
        + [jax.ShapeDtypeStruct((patch, share), wide), jax.ShapeDtypeStruct((9 * patch, share), wide)]
        + [jax.ShapeDtypeStruct((share,), wide)] * 8
        + [jax.ShapeDtypeStruct((4 * share,), wide), jax.ShapeDtypeStruct((row_count, tokens, patch), jnp.bfloat16)]
        + [jax.ShapeDtypeStruct(passed.shape, passed.dtype)],
        in_specs=[anywhere] * len(arrays) + [vmem] * 3 + [anywhere],
        out_specs=[anywhere] * 5 + [vmem] * 12 + [anywhere],
        scratch_shapes=[pltpu.VMEM(entry.shape, jnp.bfloat16) for entry in arrays]
        + [pltpu.VMEM(shape, wide) for shape in whole]
        + [pltpu.VMEM(passed.shape, passed.dtype)]
        + [pltpu.SemaphoreType.DMA((len(arrays) + 1,))] * 2,
        compiler_params=pltpu.CompilerParams(vmem_limit_bytes=full_vmem),
        name="finish",
    )(*arrays, thin, flat, conv_out, passed)


def plane_peers():
    z, ty, y = lax.axis_index("rows"), lax.axis_index("ty"), lax.axis_index("tx")
    core, x = lax.rem(ty, 2), ty // 2
    here = x * 2 + core
    across = (1 - x) * 2 + core
    tiles = {
        "own": here * 2 + y,
        "x": across * 2 + y,
        "y": here * 2 + 1 - y,
        "xy": across * 2 + 1 - y,
    }
    peers = {
        "core": (z, x * 2 + 1 - core, y),
        "x": (z, across, y),
        "y": (z, here, 1 - y),
    }
    return tiles, peers


def plane_peer(k):
    z, ty, y = lax.axis_index("rows"), lax.axis_index("ty"), lax.axis_index("tx")
    x, core = ty // 2, lax.rem(ty, 2)
    flip_x, flip_core, flip_y = k // 4, k // 2 % 2, k % 2
    x = x + flip_x - 2 * flip_x * x
    core = core + flip_core - 2 * flip_core * core
    y = y + flip_y - 2 * flip_y * y
    return (z, x * 2 + core, y), (x * 2 + core) * 2 + y


def greet(peers):
    barrier = pltpu.get_barrier_semaphore()
    for peer in peers:
        pl.semaphore_signal(barrier, inc=1, device_id=peer, device_id_type=MESH)
    pl.semaphore_wait(barrier, len(peers))


def fill_mask(mask_ref, cuts_ref, row, tile, tile_height, tile_width):
    columns = lax.axis_size("tx")
    tokens = tile_height * tile_width
    left_width = cuts_ref[row, 0]
    top_height = cuts_ref[row, 1]

    def image_of(down, across):
        return jnp.where(across < left_width, 0, jnp.where(down < top_height, 1, 2))

    lane = lax.broadcasted_iota(jnp.int32, (8, tokens), 1)
    mine = image_of(*cell_of(lane, tile, tile_height, tile_width, columns))[0:1]
    step = lax.broadcasted_iota(jnp.int32, (tokens, tokens), 0)
    down, across = step // tile_width, step % tile_width
    for other in range(mask_ref.shape[0] // tokens):
        theirs = image_of(
            down + other // columns * tile_height, across + other % columns * tile_width
        )
        mask_ref[other * tokens : (other + 1) * tokens, :] = jnp.where(mine == theirs, 0.0, -1e30)


def two_heads(pair, scale):
    lane = lax.broadcasted_iota(jnp.int32, pair.shape, 1)
    wide = pair.astype(jnp.float32) * scale
    first = jnp.where(lane < pair.shape[1] // 2, wide, 0.0)
    return jnp.concatenate([first, wide - first], axis=0).astype(jnp.bfloat16)


def own_blocks(both):
    head, tokens = both.shape[0] // 2, both.shape[1] // 2
    return jnp.concatenate([both[:head, :tokens], both[head:, tokens:]], axis=0)


def attend_kernel(
    tile_height, tile_width, cuts, query, pairs, cot, conv_turned, fc2_in,
    out, lse, query_out, attended_out, all_out, spread, out_grad_out, active_grad_out,
    cot_all, queries, held, results, scores, mask, shift, fc2_weight, out_grad, active_grad,
    local_sem, send_sem, recv_sem, cot_sem, cot_send_sem, cot_recv_sem, side_sem
):
    _, row_count, tokens, half = query.shape
    tile_count = held.shape[1]
    width = 2 * half
    tiles, peers = plane_peers()
    own = tiles["own"]
    x = lax.axis_index("ty") // 2
    fc2_load = pltpu.make_async_copy(fc2_in, fc2_weight, side_sem.at[0])
    fc2_load.start()
    greet([plane_peer(k)[0] for k in range(1, tile_count)])
    cot_copies = [pltpu.make_async_copy(cot, cot_all.at[own], cot_sem.at[0])]
    for k in range(1, tile_count):
        cot_copies.append(
            pltpu.make_async_remote_copy(
                src_ref=cot,
                dst_ref=cot_all.at[own],
                send_sem=cot_send_sem.at[k],
                recv_sem=cot_recv_sem.at[k],
                device_id=plane_peer(k)[0],
                device_id_type=MESH,
            )
        )

    def send(row, slot, source, target, peer):
        copy = pltpu.make_async_remote_copy(
            src_ref=source,
            dst_ref=target,
            send_sem=send_sem.at[row, slot],
            recv_sem=recv_sem.at[row, slot],
            device_id=peer,
            device_id_type=MESH,
        )
        copy.start()
        flights[row][slot] = copy

    def keep(row, slot, source, target):
        copy = pltpu.make_async_copy(source, target, local_sem.at[row, slot])
        copy.start()
        kept[row][slot] = copy

    flights = [{} for _ in range(row_count)]
    kept = [{} for _ in range(row_count)]

    def begin(row):
        here = held.at[row, own]
        send(row, 1, pairs.at[1 - x, row], here, peers["x"])
        send(row, 0, query.at[1 - x, row], queries.at[row, 1], peers["x"])
        send(row, 2, pairs.at[x, row], here, peers["y"])
        send(row, 3, pairs.at[x, row], here, peers["core"])
        keep(row, 0, query.at[x, row], queries.at[row, 0])
        keep(row, 1, pairs.at[x, row], here)

    def forward(row):
        flights[row][1].wait_recv()
        tile = held.at[row, tiles["x"]]
        send(row, 4, tile, tile, peers["y"])
        send(row, 5, tile, tile, peers["core"])
        flights[row][2].wait_recv()
        tile = held.at[row, tiles["y"]]
        send(row, 6, tile, tile, peers["core"])

    def gather_row(row):
        flights[row][4].wait_recv()
        tile = held.at[row, tiles["xy"]]
        send(row, 7, tile, tile, peers["core"])
        for slot in (0, 3, 5, 6, 7):
            flights[row][slot].wait_recv()
        for slot in range(8):
            flights[row][slot].wait_send()
        for slot in range(2):
            kept[row][slot].wait()
        keep(row, 3, held.at[row], all_out.at[row])
        keep(row, 4, queries.at[row], query_out.at[row])

    chunk = 2

    def compute(row):
        def one_pair(p, carry, which=(0, 1)):
            at = pl.ds(pl.multiple_of(p * 128, 128), 128)
            at_value = pl.ds(pl.multiple_of(half + p * 128, 128), 128)
            for t in which:
                both = two_heads(queries[row, t, :, at], 0.125)
                peak = None
                for c in range(tile_count // chunk):
                    span = slice(c * chunk * tokens, (c + 1) * chunk * tokens)
                    keys = held[row, c * chunk : (c + 1) * chunk, :, at].reshape(chunk * tokens, 128)
                    extra = mask[row, t, span, :]
                    part = mm(keys, both, 1, 1) + jnp.concatenate([extra, extra], axis=1)
                    scores[t, span, :] = part
                    top = jnp.max(part, axis=0, keepdims=True)
                    peak = top if peak is None else jnp.maximum(peak, top)
                total = jnp.zeros_like(peak)
                summed = jnp.zeros((128, 2 * tokens), jnp.float32)
                for c in range(tile_count // chunk):
                    span = slice(c * chunk * tokens, (c + 1) * chunk * tokens)
                    values = held[row, c * chunk : (c + 1) * chunk, :, at_value].reshape(chunk * tokens, 128)
                    part = jnp.exp(scores[t, span, :] - peak)
                    total = total + jnp.sum(part, axis=0, keepdims=True)
                    summed = summed + mm(values, part.astype(jnp.bfloat16), 0, 0)
                blocks = own_blocks(summed / total)
                results[row, t, :, at] = jnp.transpose(blocks).astype(jnp.bfloat16)
                lse[row, p, t] = peak + jnp.log(total)
            return carry

        if row < row_count - 1:
            lax.fori_loop(0, half // 128, one_pair, 0)
            hand_back(row)
        else:
            lax.fori_loop(0, half // 128, functools.partial(one_pair, which=(1,)), 0)
            hand_back(row)
            lax.fori_loop(0, half // 128, functools.partial(one_pair, which=(0,)), 0)
        keep(row, 5, results.at[row, 0], out.at[x, row])
        keep(row, 6, results.at[row], attended_out.at[row])

    def hand_back(row):
        send(row, 8, results.at[row, 1], out.at[x, row], peers["x"])

    side_copies = []
    parts = [slice(k * tokens, (k + 1) * tokens) for k in range(row_count)]

    def spread_out():
        patch = cot_all.shape[2]
        turned = jnp.concatenate(
            [cot_all[t].reshape(row_count * patch, tokens) for t in range(tile_count)], axis=1
        )
        moved = mm(turned, shift[...], 1, 0)
        for row in range(row_count):
            for p in range(9):
                piece = moved[row * patch : (row + 1) * patch, p * tokens : (p + 1) * tokens]
                piece = piece * same_image(cuts, row, p, tile_height, tile_width)
                spread[p * patch : (p + 1) * patch, parts[row]] = piece.astype(jnp.bfloat16)
        out_grad[...] = mm(spread[...], conv_turned[...], 0, 0)
        copy = pltpu.make_async_copy(out_grad, out_grad_out, side_sem.at[1])
        copy.start()
        side_copies.append(copy)

    def activate():
        for k in range(fc2_weight.shape[0] // width):
            span = slice(k * width, (k + 1) * width)
            low = out_grad[...].astype(jnp.bfloat16)
            active_grad[:, span] = mm(low, fc2_weight[span, :], 1, 1).astype(jnp.bfloat16)
        copy = pltpu.make_async_copy(active_grad, active_grad_out, side_sem.at[2])
        copy.start()
        side_copies.append(copy)

    for copy in cot_copies:
        copy.start()
    begin(0)
    fill_shift(shift, tile_height, tile_width)
    for copy in cot_copies:
        copy.wait()
    spread_out()
    forward(0)
    for row in range(1, min(row_count, 3)):
        begin(row)
    fc2_load.wait()
    activate()
    for row in range(row_count):
        for t, name in enumerate(("own", "x")):
            fill_mask(mask.at[row, t], cuts, row, tiles[name], tile_height, tile_width)
    for row in range(row_count):
        gather_row(row)
        compute(row)
        for later in range(1 if row == 0 else row + 2, min(row + 3, row_count)):
            if later > 2:
                begin(later)
            forward(later)
    for row in range(row_count):
        flights[row][8].wait()
        for slot in range(3, 7):
            kept[row][slot].wait()
    for copy in side_copies:
        copy.wait()


def attend(cuts, query, pairs, cot, conv_turned, fc2_weight, tile_height, tile_width):
    _, row_count, tokens, half = query.shape
    tile_count = lax.axis_size("ty") * lax.axis_size("tx")
    width = 2 * half
    low, wide = jnp.bfloat16, jnp.float32
    vmem, anywhere = pl.BlockSpec(memory_space=pltpu.VMEM), pl.BlockSpec(memory_space=pl.ANY)
    return pl.pallas_call(
        functools.partial(attend_kernel, tile_height, tile_width),
        out_shape=[
            jax.ShapeDtypeStruct((2, row_count, tokens, half), low),
            jax.ShapeDtypeStruct((row_count, half // 128, 2, 1, 2 * tokens), wide),
            jax.ShapeDtypeStruct((row_count, 2, tokens, half), low),
            jax.ShapeDtypeStruct((row_count, 2, tokens, half), low),
            jax.ShapeDtypeStruct((row_count, tile_count, tokens, width), low),
            jax.ShapeDtypeStruct((conv_turned.shape[0], row_count * tokens), low),
            jax.ShapeDtypeStruct((row_count * tokens, width), wide),
            jax.ShapeDtypeStruct((row_count * tokens, fc2_weight.shape[0]), low),
        ],
        in_specs=[pl.BlockSpec(memory_space=pltpu.SMEM)] + [anywhere] * 3 + [vmem, anywhere],
        out_specs=[anywhere, vmem] + [anywhere] * 3 + [vmem] + [anywhere] * 2,
        scratch_shapes=[
            pltpu.VMEM((tile_count,) + cot.shape, low),
            pltpu.VMEM((row_count, 2, tokens, half), low),
            pltpu.VMEM((row_count, tile_count, tokens, width), low),
            pltpu.VMEM((row_count, 2, tokens, half), low),
            pltpu.VMEM((2, tile_count * tokens, 2 * tokens), wide),
            pltpu.VMEM((row_count, 2, tile_count * tokens, tokens), wide),
            pltpu.VMEM((tile_count * tokens, 9 * tokens), low),
            pltpu.VMEM(fc2_weight.shape, low),
            pltpu.VMEM((row_count * tokens, width), wide),
            pltpu.VMEM((row_count * tokens, fc2_weight.shape[0]), low),
            pltpu.SemaphoreType.DMA((row_count, 7)),
            pltpu.SemaphoreType.DMA((row_count, 9)),
            pltpu.SemaphoreType.DMA((row_count, 9)),
            pltpu.SemaphoreType.DMA((1,)),
            pltpu.SemaphoreType.DMA((tile_count,)),
            pltpu.SemaphoreType.DMA((tile_count,)),
            pltpu.SemaphoreType.DMA((3,)),
        ],
        compiler_params=pltpu.CompilerParams(
            collective_id=1, has_side_effects=True, vmem_limit_bytes=full_vmem
        ),
        name="attend",
    )(cuts, query, pairs, cot, conv_turned, fc2_weight)


def attend_back_kernel(
    tile_height, tile_width, kinds, done, cuts, query_in, attended_in, grad_in, lse_in, conv_in, conv_turned, spread,
    all_pairs, *refs
):
    count = max([kind[2] for kind in kinds], default=-1) + 1
    sources, refs = refs[:count], refs[count:]
    total_count = len(kinds)
    (out, conv_grad, conv_out), saved, refs = refs[:3], refs[3 : 3 + total_count], refs[3 + total_count :]
    query, attended, grad, lse, row_sem = refs[:5]
    held, terms, core_terms, y_terms, x_terms, x_query, query_grad, mask, shift, taps, part, part_got = refs[5:17]
    send_sem, recv_sem, part_send_sem, part_recv_sem = refs[17:21]
    grads = [
        sources[which] if rows is None else sources[which].at[:, rows[0] : rows[1], :]
        for _, _, which, rows in kinds
    ]
    items = make_reducers([kind[:2] for kind in kinds], grads, saved, refs[21:]) if kinds else []
    for item, columns in zip(items, done):
        item.halved = columns
    row_count, _, tokens, half = query.shape
    tile_count = held.shape[1]
    tiles, peers = plane_peers()
    low = jnp.bfloat16
    x, core = lax.axis_index("ty") // 2, lax.rem(lax.axis_index("ty"), 2)

    def group(which, base=0):
        return pl.ds(pl.multiple_of(base + which * half, 128), half)

    loads = []
    for row in range(row_count):
        loads.append([])
        for k, (source, target) in enumerate((
            (all_pairs.at[row], held.at[row]), (query_in.at[row], query.at[row]), (attended_in.at[row], attended.at[row]),
            (grad_in.at[x, row], grad.at[row, 0]), (lse_in.at[row], lse.at[row]),
        )):
            load = pltpu.make_async_copy(source, target, row_sem.at[row, k])
            load.start()
            loads[-1].append(load)
    greet([plane_peer(k)[0] for k in range(1, tile_count)] + (chip_peers()["z"] if kinds else []))
    chunk = 2
    flights = [{} for _ in range(row_count)]

    def send(row, slot, source, target, peer):
        copy = pltpu.make_async_remote_copy(
            src_ref=source,
            dst_ref=target,
            send_sem=send_sem.at[row, slot],
            recv_sem=recv_sem.at[row, slot],
            device_id=peer,
            device_id_type=MESH,
        )
        copy.start()
        flights[row][slot] = copy

    def compute(row):
        for load in loads[row]:
            load.wait()
        flights[row][8].wait()
        for t, name in enumerate(("own", "x")):
            fill_mask(mask.at[t], cuts, row, tiles[name], tile_height, tile_width)

        def one_pair(p, carry):
            at = pl.ds(pl.multiple_of(p * 128, 128), 128)
            at_value = pl.ds(pl.multiple_of(half + p * 128, 128), 128)
            boths, both_grads, deltas, levels = [], [], [], []
            for t in range(2):
                grad_pair = grad[row, t, :, at]
                boths.append(two_heads(query[row, t, :, at], 0.125))
                both_grads.append(two_heads(grad_pair, 1.0))
                inner = jnp.transpose(grad_pair.astype(jnp.float32) * attended[row, t, :, at].astype(jnp.float32))
                heads = [inner[: inner.shape[0] // 2], inner[inner.shape[0] // 2 :]]
                deltas.append(jnp.concatenate([jnp.sum(head, axis=0, keepdims=True) for head in heads], axis=1))
                levels.append(lse[row, p, t])
            all_both = jnp.concatenate(boths, axis=0)
            all_grads = jnp.concatenate(both_grads, axis=0)
            query_part = jnp.zeros((128, 4 * tokens), jnp.float32)
            for c in range(tile_count // chunk):
                span = slice(c * chunk * tokens, (c + 1) * chunk * tokens)
                some = slice(c * chunk, (c + 1) * chunk)
                keys = held[row, some, :, at].reshape(chunk * tokens, 128)
                values = held[row, some, :, at_value].reshape(chunk * tokens, 128)
                weight_parts, score_parts = [], []
                for t in range(2):
                    extra = mask[t, span, :]
                    raw = mm(keys, boths[t], 1, 1) + jnp.concatenate([extra, extra], axis=1)
                    weights = jnp.exp(raw - levels[t])
                    weight_parts.append(weights.astype(low))
                    score_parts.append((weights * (mm(values, both_grads[t], 1, 1) - deltas[t])).astype(low))
                score_grad = jnp.concatenate(score_parts, axis=1)
                value_part = mm(jnp.concatenate(weight_parts, axis=1), all_grads, 1, 0)
                key_part = mm(score_grad, all_both, 1, 0)
                query_part = query_part + mm(keys, score_grad, 0, 0)
                terms[row, some, :, at] = key_part.astype(low).reshape(chunk, tokens, 128)
                terms[row, some, :, at_value] = value_part.astype(low).reshape(chunk, tokens, 128)
            for t in range(2):
                blocks = own_blocks(query_part[:, 2 * t * tokens : 2 * (t + 1) * tokens]) * 0.125
                query_grad[row, t, :, at] = jnp.transpose(blocks).astype(low)
            return carry

        lax.fori_loop(0, half // 128, one_pair, 0)

    names = ("own", "x", "y", "xy")

    def begin(row):
        other = 2 - 4 * core
        for k in (3, 2, 1, 0):
            send(row, k, terms.at[row, tiles[names[k]] + other], core_terms.at[row, k], peers["core"])
        send(row, 7, query_grad.at[row, 1], x_query.at[row], peers["x"])

    def add(target, source):
        def body(i, carry):
            at = pl.ds(pl.multiple_of(i * 16, 16), 16)
            target[at, :] = target[at, :] + source[at, :]
            return carry

        lax.fori_loop(0, tokens // 16, body, 0)

    def scatter(row):
        for k in (3, 2, 1, 0):
            flights[row][k].wait()
            tile = terms.at[row, tiles[names[k]]]
            add(tile, core_terms.at[row, k])
            if k == 3:
                send(row, 5, tile, y_terms.at[row, 1], peers["y"])
            if k == 2:
                send(row, 4, tile, y_terms.at[row, 0], peers["y"])

    def pass_on(row):
        flights[row][5].wait()
        tile = terms.at[row, tiles["x"]]
        add(tile, y_terms.at[row, 1])
        send(row, 6, tile, x_terms.at[row], peers["x"])

    def close(row):
        for slot in (4, 6, 7):
            flights[row][slot].wait()
        mine = terms.at[row, tiles["own"]]
        width = 2 * half

        def body(i, carry):
            at = pl.ds(pl.multiple_of(i * 16, 16), 16)
            total = mine[at, :].astype(jnp.float32) + y_terms[row, 0, at, :].astype(jnp.float32)
            total = total.astype(low)
            out[row, at, group(x)] = query_grad[row, 0, at, :]
            out[row, at, group(x, width)] = total[:, :half]
            out[row, at, group(x, 2 * width)] = total[:, half:]
            out[row, at, group(1 - x)] = x_query[row, at, :]
            out[row, at, group(1 - x, width)] = x_terms[row, at, :half]
            out[row, at, group(1 - x, 2 * width)] = x_terms[row, at, half : 2 * half]
            return carry

        lax.fori_loop(0, tokens // 16, body, 0)

    part_copies = []

    def convolve():
        fill_shift(shift, tile_height, tile_width)
        patch = part.shape[2]
        taps[...] = mm(conv_turned[...], conv_in[...], 1, 1)
        rows = []
        for row in range(row_count):
            pieces = []
            for p in range(9):
                piece = taps[p * patch : (p + 1) * patch, row * tokens : (row + 1) * tokens]
                pieces.append(piece * same_image(cuts, row, p, tile_height, tile_width))
            rows.append(jnp.concatenate(pieces, axis=1))
        whole = jnp.concatenate(rows, axis=0)
        coarse = whole.astype(low)
        fine = (whole - coarse.astype(jnp.float32)).astype(low)
        moved = mm(coarse, shift[...], 1, 1) + mm(fine, shift[...], 1, 1)
        for tile in range(tile_count):
            part[tile] = moved[:, tile * tokens : (tile + 1) * tokens].reshape(row_count, patch, tokens)
        for k in range(1, tile_count):
            peer, tile = plane_peer(k)
            copy = pltpu.make_async_remote_copy(
                src_ref=part.at[tile],
                dst_ref=part_got.at[k],
                send_sem=part_send_sem.at[k],
                recv_sem=part_recv_sem.at[k],
                device_id=peer,
                device_id_type=MESH,
            )
            copy.start()
            part_copies.append(copy)
        conv_grad[...] = mm(conv_in[...], spread[...], 0, 1)

    def collect():
        total = part[tiles["own"]]
        for k, copy in enumerate(part_copies):
            copy.wait()
            total = total + part_got[k + 1]
        conv_out[...] = total.astype(low)

    def sum_up(item):
        item.step()
        item.save()

    for row in range(row_count):
        send(row, 8, grad_in.at[1 - x, row], grad.at[row, 1], peers["x"])
    for item in items:
        item.begin()
    if items and row_count == 3:
        fc1, fc2a, fc2b, proj = items
        fc1.step()
        fc2a.step()
        proj.step()
        fc2b.step()
        compute(0)
        fc1.step()
        begin(0)
        scatter(0)
        compute(1)
        begin(1)
        fc2b.step()
        proj.step()
        scatter(1)
        fc1.step()
        compute(2)
        pass_on(0)
        proj.step()
        begin(2)
        scatter(2)
        fc2b.step()
        pass_on(1)
        convolve()
        sum_up(proj)
        pass_on(2)
        sum_up(fc1)
        sum_up(fc2a)
        sum_up(fc2b)
        for row in range(row_count):
            close(row)
        collect()
    else:
        for row in range(row_count):
            compute(row)
            begin(row)
        for row in range(row_count):
            scatter(row)
        for row in range(row_count):
            pass_on(row)
        convolve()
        for row in range(row_count):
            close(row)
        collect()
    for item in items:
        item.land("save")


def attend_back(cuts, query, attended, grad, lse, conv_in, conv_turned, spread, all_pairs, grads, tile_height, tile_width):
    row_count, _, tokens, half = query.shape
    width = 2 * half
    kinds, sources, saves, shapes = [], [], [], []
    for start, paired, entry, rows, _ in grads:
        if not any(entry is source for source in sources):
            sources.append(entry)
        which = [entry is source for source in sources].index(True)
        kinds.append((start, paired, which, rows))
        depth = entry.shape[1] if rows is None else rows[1] - rows[0]
        shapes.append((depth, entry.shape[2] if paired else entry.shape[2] // 2))
        saves.append((depth if start == "z" else depth // 4, shapes[-1][1]))
    kinds = tuple(kinds)
    done = tuple(entry[4] for entry in grads)
    tile_count = all_pairs.shape[1]
    taps = conv_turned.shape[0]
    low, wide = jnp.bfloat16, jnp.float32
    vmem, anywhere = pl.BlockSpec(memory_space=pltpu.VMEM), pl.BlockSpec(memory_space=pl.ANY)
    return pl.pallas_call(
        functools.partial(attend_back_kernel, tile_height, tile_width, kinds, done),
        out_shape=[
            jax.ShapeDtypeStruct((row_count, tokens, 3 * width), low),
            jax.ShapeDtypeStruct((width, taps), wide),
            jax.ShapeDtypeStruct((row_count, taps // 9, tokens), low),
        ]
        + [jax.ShapeDtypeStruct(s, low) for s in saves],
        in_specs=[pl.BlockSpec(memory_space=pltpu.SMEM)] + [anywhere] * 4 + [vmem] * 3 + [anywhere] * (1 + len(sources)),
        out_specs=[vmem] * 3 + [anywhere] * len(saves),
        scratch_shapes=[
            pltpu.VMEM(query.shape, low),
            pltpu.VMEM(query.shape, low),
            pltpu.VMEM(query.shape, low),
            pltpu.VMEM(lse.shape, wide),
            pltpu.SemaphoreType.DMA((row_count, 5)),
            pltpu.VMEM((row_count, tile_count, tokens, width), low),
            pltpu.VMEM((row_count, tile_count, tokens, width), low),
            pltpu.VMEM((row_count, 4, tokens, width), low),
            pltpu.VMEM((row_count, 2, tokens, width), low),
            pltpu.VMEM((row_count, tokens, width), low),
            pltpu.VMEM((row_count, tokens, half), low),
            pltpu.VMEM(query.shape, low),
            pltpu.VMEM((2, tile_count * tokens, tokens), wide),
            pltpu.VMEM((tile_count * tokens, 9 * tokens), low),
            pltpu.VMEM((taps, row_count * tokens), wide),
            pltpu.VMEM((tile_count, row_count, taps // 9, tokens), wide),
            pltpu.VMEM((tile_count, row_count, taps // 9, tokens), wide),
            pltpu.SemaphoreType.DMA((row_count, 9)),
            pltpu.SemaphoreType.DMA((row_count, 9)),
            pltpu.SemaphoreType.DMA((tile_count,)),
            pltpu.SemaphoreType.DMA((tile_count,)),
        ]
        + (reducer_scratch([kind[:2] for kind in kinds], shapes) if kinds else []),
        compiler_params=pltpu.CompilerParams(
            collective_id=2, has_side_effects=True, vmem_limit_bytes=full_vmem
        ),
        name="attend_back",
    )(cuts, query, attended, grad, lse, conv_in, conv_turned, spread, all_pairs, *sources)


def add_rows(target, first, second, rows):
    def body(i, carry):
        at = pl.ds(pl.multiple_of(i * 16, 16), 16)
        target[at, :] = first[at, :] + second[at, :]
        return carry

    lax.fori_loop(0, rows // 16, body, 0)


def add_four(target, others, rows):
    def body(i, carry):
        at = pl.ds(pl.multiple_of(i * 16, 16), 16)
        total = target[at, :].astype(jnp.float32) + others[0, at, :].astype(jnp.float32)
        total = total + (others[1, at, :].astype(jnp.float32) + others[2, at, :].astype(jnp.float32))
        target[at, :] = total.astype(jnp.bfloat16)
        return carry

    lax.fori_loop(0, rows // 16, body, 0)


def chip_peers():
    z, ty, y = lax.axis_index("rows"), lax.axis_index("ty"), lax.axis_index("tx")
    core, x = lax.rem(ty, 2), ty // 2
    across = (1 - x) * 2 + core
    return {
        "core": (z, x * 2 + 1 - core, y),
        "x": (z, across, y),
        "y": (z, ty, 1 - y),
        "xy": (z, across, 1 - y),
        "z": [(lax.rem(z + k, 4), ty, y) for k in (1, 2, 3)],
    }


class Reducer:
    def __init__(self, start, paired, relays, grad, out, buffers, sems, w):
        self.relays, self.halved = relays, 0
        self.start, self.paired, self.grad, self.out, self.w = start, paired, grad, out, w
        self.local_sem, self.send_sem, self.recv_sem = sems
        self.z, ty, self.y = lax.axis_index("rows"), lax.axis_index("ty"), lax.axis_index("tx")
        self.core, self.x = lax.rem(ty, 2), ty // 2
        self.peers = chip_peers()
        self.flying = {}
        self.own = buffers[0]
        if start in ("plane", "z"):
            self.half, self.quarter, self.final = buffers[1:4]
            self.got = None if paired else buffers[4]
            self.depth, self.width = grad.shape[1], grad.shape[2] if paired else grad.shape[2] // 2
        else:
            self.depth, self.width = out.shape[1], out.shape[2]
        if start == "block":
            self.half, self.quarter = buffers[1:]
        share = [self.relay, self.pass_strip] if relays else [self.pass_strip]
        late = [self.begin_late, self.add_half_late, self.add_quarter_late, *share, self.end]
        self.stages = {
            "plane": [self.add_core, self.add_half, self.add_quarter, self.sum_z, self.gather_piece, *share, self.end],
            "z": [self.add_core, self.sum_z_first] + late,
            "block": late,
            "piece": [self.gather_piece, *share, self.end],
        }[start]

    def step(self):
        self.stages.pop(0)()

    def part(self, at):
        if self.start == "block":
            return self.own.at[at]
        return self.own.at[self.z, at]

    def send(self, slot, source, target, peer):
        copy = pltpu.make_async_remote_copy(
            src_ref=source,
            dst_ref=target,
            send_sem=self.send_sem.at[self.w, slot],
            recv_sem=self.recv_sem.at[self.w, slot],
            device_id=peer,
            device_id_type=MESH,
        )
        copy.start()
        return copy

    def keep(self, slot, source, target):
        copy = pltpu.make_async_copy(source, target, self.local_sem.at[self.w, slot])
        copy.start()
        return copy

    def land(self, name):
        for copy in self.flying.pop(name):
            copy.wait()

    def columns(self, which):
        return pl.ds(pl.multiple_of(which * self.width, 128), self.width)

    def rows(self, start, size):
        return pl.ds(pl.multiple_of(start, 16), size)

    def place(self, block, flip_x=False, flip_y=False):
        x = 1 - self.x if flip_x else self.x
        y = 1 - self.y if flip_y else self.y
        later = block // 2
        major = x + later * (y - x)
        minor = y + later * (x - y)
        return self.rows(major * (self.depth // 2) + minor * (self.depth // 4), self.depth // 4)

    def pieces(self, flip_x=False, flip_y=False):
        if self.start in ("plane", "piece"):
            return [self.place(self.z, flip_x, flip_y)]
        x = 1 - self.x if flip_x else self.x
        y = 1 - self.y if flip_y else self.y
        half, less, least = self.depth // 2, self.depth // 4, self.depth // 8
        return [self.rows(x * less + y * least, least), self.rows(half + y * less + x * least, least)]

    def begin(self):
        if self.start in ("block", "piece"):
            self.flying["load"] = [self.keep(0, self.grad, self.own)]
            return
        if self.paired:
            self.flying["core"] = [self.keep(0, self.grad, self.own)]
            return
        swap = self.send(0, self.grad.at[:, :, self.columns(1 - self.core)], self.got, self.peers["core"])
        mine = self.keep(0, self.grad.at[:, :, self.columns(self.core)], self.own)
        self.flying["core"] = [swap, mine]

    def add_core(self):
        self.land("core")
        if not self.paired:
            for block in range(4):
                add_rows(self.own.at[block], self.own.at[block], self.got.at[block], self.depth)
        if self.start == "z":
            self.flying["z"] = [
                self.send(5 + k, self.own.at[peer[0]], self.final.at[k], peer) for k, peer in enumerate(self.peers["z"])
            ]
            return
        part = self.depth // 2
        rest = pl.ds(self.halved, self.width - self.halved)
        theirs = [self.rows((1 - side) * part, part) for side in (self.x, self.y)]
        first = self.send(1, self.own.at[0:2, theirs[0], rest], self.half.at[0:2, :, rest], self.peers["x"])
        second = self.send(2, self.own.at[2:4, theirs[1], rest], self.half.at[2:4, :, rest], self.peers["y"])
        self.flying["half"] = [first, second]

    def add_half(self):
        self.land("half")
        part, less = self.depth // 2, self.depth // 4
        for block in range(4):
            side = self.x if block < 2 else self.y
            rest = pl.ds(self.halved, self.width - self.halved)
            kept = self.own.at[block, self.rows(side * part, part), rest]
            add_rows(kept, kept, self.half.at[block, :, rest], part)
        first = self.own.at[0:2, self.rows(self.x * part + (1 - self.y) * less, less)]
        second = self.own.at[2:4, self.rows(self.y * part + (1 - self.x) * less, less)]
        self.flying["quarter"] = [
            self.send(3, first, self.quarter.at[0:2], self.peers["y"]),
            self.send(4, second, self.quarter.at[2:4], self.peers["x"]),
        ]

    def add_quarter(self):
        self.land("quarter")
        for block in range(4):
            kept = self.own.at[block, self.place(block // 2 * 2)]
            add_rows(kept, kept, self.quarter.at[block], self.depth // 4)
        self.flying["z"] = [
            self.send(5 + k, self.own.at[peer[0], self.place(peer[0])], self.final.at[k], peer)
            for k, peer in enumerate(self.peers["z"])
        ]

    def gather(self, pieces, sources):
        copies = []
        for n, (at, source) in enumerate(zip(pieces, sources)):
            target = self.out.at[self.core, at]
            for k, name in enumerate(("x", "y") if self.relays else ("x", "y", "xy")):
                copies.append(self.send(8 + 3 * n + k, source, target, self.peers[name]))
            copies.append(self.keep(1 + n, source, target))
        self.flying["gather"] = copies

    def relay(self):
        self.land("gather")
        cut = self.width // 256 * 128 + (128 if self.width % 256 and self.w % 2 else 0)
        copies = []
        for n, (from_x, from_y) in enumerate(zip(self.pieces(flip_x=True), self.pieces(flip_y=True))):
            first = self.out.at[self.core, from_x, pl.ds(0, cut)]
            second = self.out.at[self.core, from_y, pl.ds(cut, self.width - cut)]
            copies.append(self.send(14 + 2 * n + 1, first, first, self.peers["y"]))
            copies.append(self.send(14 + 2 * n + 2, second, second, self.peers["x"]))
        self.flying["relay"] = copies

    def sum_z(self):
        self.land("z")
        add_four(self.own.at[self.z, self.place(self.z)], self.final, self.depth // 4)

    def gather_piece(self):
        if self.start == "piece":
            self.land("load")
            self.gather([self.place(self.z)], [self.own])
        else:
            self.gather([self.place(self.z)], [self.own.at[self.z, self.place(self.z)]])

    def sum_z_first(self):
        self.land("z")
        add_four(self.own.at[self.z], self.final, self.depth)

    def save(self):
        source = self.own.at[self.z] if self.start == "z" else self.own.at[self.z, self.place(self.z)]
        self.flying["save"] = [self.keep(1, source, self.out)]

    def begin_late(self):
        if self.start == "block":
            self.land("load")
        half, less = self.depth // 2, self.depth // 4
        self.flying["half"] = [
            self.send(1, self.part(self.rows((1 - self.x) * less, less)), self.half.at[0], self.peers["x"]),
            self.send(2, self.part(self.rows(half + (1 - self.y) * less, less)), self.half.at[1], self.peers["y"]),
        ]

    def add_half_late(self):
        self.land("half")
        half, less, least = self.depth // 2, self.depth // 4, self.depth // 8
        for n, start in enumerate((self.x * less, half + self.y * less)):
            kept = self.part(self.rows(start, less))
            add_rows(kept, kept, self.half.at[n], less)
        first = self.part(self.rows(self.x * less + (1 - self.y) * least, least))
        second = self.part(self.rows(half + self.y * less + (1 - self.x) * least, least))
        self.flying["quarter"] = [
            self.send(3, first, self.quarter.at[0], self.peers["y"]),
            self.send(4, second, self.quarter.at[1], self.peers["x"]),
        ]

    def add_quarter_late(self):
        self.land("quarter")
        least = self.depth // 8
        pieces = self.pieces()
        for n, at in enumerate(pieces):
            add_rows(self.part(at), self.part(at), self.quarter.at[n], least)
        self.gather(pieces, [self.part(at) for at in pieces])

    def pass_strip(self):
        self.land("relay" if self.relays else "gather")
        strip = self.out.at[self.core]
        self.flying["strip"] = [self.send(14, strip, strip, self.peers["core"])]

    def end(self):
        self.land("strip")


def reducer_scratch(kinds, shapes):
    buffers = []
    for (start, paired), (depth, half) in zip(kinds, shapes):
        sizes = {
            "plane": [(4, depth, half), (4, depth // 2, half), (4, depth // 4, half), (3, depth // 4, half)],
            "z": [(4, depth, half), (2, depth // 4, half), (2, depth // 8, half), (3, depth, half)],
            "block": [(depth, half), (2, depth // 4, half), (2, depth // 8, half)],
            "piece": [(depth // 4, half)],
        }[start]
        if not paired:
            sizes.append((4, depth, half))
        buffers += [pltpu.VMEM(size, jnp.bfloat16) for size in sizes]
    count = len(kinds)
    return buffers + [
        pltpu.SemaphoreType.DMA((count, 3)),
        pltpu.SemaphoreType.DMA((count, 19)),
        pltpu.SemaphoreType.DMA((count, 19)),
    ]


def make_reducers(kinds, grads, outs, scratch, relays=()):
    items, at = [], 0
    for w, ((start, paired), grad, out) in enumerate(zip(kinds, grads, outs)):
        size = {"plane": 4, "z": 4, "block": 3, "piece": 1}[start] + (0 if paired else 1)
        items.append(Reducer(start, paired, w in relays, grad, out, scratch[at : at + size], scratch[-3:], w))
        at = at + size
    return items


def sum_by_table(local_grads):
    band_count, column_count = lax.axis_size("ty"), lax.axis_size("tx")
    group_count = lax.axis_size("rows")
    tile_count = band_count * column_count
    table = jnp.concatenate([entry.reshape(group_count, -1) for entry in local_grads], axis=1)
    column_total = table.shape[1]
    padded_columns = -(-column_total // tile_count) * tile_count
    piece_width = padded_columns // tile_count
    table = table.reshape(group_count, tile_count, piece_width)
    shares = lax.psum_scatter(
        table.reshape(group_count * tile_count, piece_width),
        ("rows", "ty", "tx"),
        scatter_dimension=0,
        tiled=True,
    )
    summed = (
        lax.all_gather(shares.astype(jnp.bfloat16), ("ty", "tx"), axis=0, tiled=True)
        .astype(shares.dtype)
        .reshape(-1)
    )
    totals = []
    start_at = 0
    for entry in local_grads:
        length = entry.size // group_count
        shard_shape = (entry.shape[0] // group_count,) + entry.shape[1:]
        totals.append(summed[start_at : start_at + length].reshape(shard_shape))
        start_at = start_at + length
    return tuple(totals)


def shards(
    latent,
    skip_input,
    segment_ids,
    embed_weight,
    embed_bias,
    skip_weight,
    skip_bias,
    norm1_gain,
    norm1_bias,
    qkv_weight,
    proj_weight,
    proj_bias,
    norm2_gain,
    norm2_bias,
    fc1_weight,
    fc1_bias,
    fc2_weight,
    fc2_bias,
    conv_weight,
    cotangent,
):
    row_count, tile_height, tile_width, width = skip_input.shape
    patch = latent.shape[3]
    tokens = tile_height * tile_width
    token_count = row_count * tokens
    low = jnp.bfloat16
    wide = jnp.float32
    conv_turned = conv_weight.T
    flat_latent = latent.reshape(token_count, patch)
    flat_skip = skip_input.reshape(token_count, width)
    biases = (embed_bias, skip_bias, norm1_gain, norm1_bias, proj_bias, norm2_gain, norm2_bias, fc2_bias)
    embedded, stream, normed, query, pairs, cot, vectors, hidden_bias, cuts = front(
        segment_ids, flat_latent, cotangent.reshape(token_count, patch), embed_weight.T, biases, fc1_bias,
        flat_skip, skip_weight, qkv_weight, row_count,
    )
    attended, log_total, held_query, held_attended, held_pairs, spread, out_grad, active_grad = attend(
        cuts, query, pairs, cot, conv_turned, fc2_weight, tile_height, tile_width
    )
    here = (lax.axis_size("rows"), lax.axis_size("ty"), lax.axis_size("tx")) == (4, 4, 2)
    fc1_grad, fc2_grad, hidden_bias_grad, proj_grad, attended_grad, mid_grad, conv_in, middle_grads = middle(
        attended.reshape(2, token_count, width // 2), stream, out_grad, active_grad, proj_weight, vectors, hidden_bias,
        fc1_weight, fc2_weight, here,
    )
    early = []
    if here:
        fc2_blocks = fc2_grad.reshape(4, -1, width // 2)
        middle_row = fc2_blocks.shape[1] // 2
        early = [
            ("plane", True, fc1_grad, None, fc1_grad.shape[2] * 3 // 4),
            ("z", True, fc2_blocks, (0, middle_row), 0),
            ("plane", True, fc2_blocks, (middle_row, 2 * middle_row), 0),
            ("plane", False, proj_grad.reshape(4, -1, width), None, 0),
        ]
    projected_grad, conv_grad, conv_out, *saved = attend_back(
        cuts, held_query, held_attended, attended_grad.reshape(2, row_count, tokens, width // 2), log_total,
        conv_in, conv_turned, spread, held_pairs, early, tile_height, tile_width,
    )
    follow = {"plane": "piece", "z": "block"}
    resumed = [
        (follow[start], entry, (entry.shape[0] if start == "z" else 4 * entry.shape[0], entry.shape[1]))
        for (start, *_), entry in zip(early, saved)
    ]
    skip_input_grad, *rest = rear(
        projected_grad.reshape(token_count, 3 * width), qkv_weight, normed, stream, mid_grad, embedded, flat_skip,
        skip_weight, flat_latent, vectors, middle_grads, hidden_bias_grad, conv_grad, resumed, here,
    )
    taps = 9 * patch
    share = width // 4
    if here:
        half = width // 2
        places = [(0, 0, half, 0), (1, 0, half, 0), (1, middle_row, half, 0), (2, 0, half, 0)]
        places += [(3, 0, half, k * width) for k in range(3)] + [(4, 0, half, 0)]
        totals = finish([place + (entry,) for place, entry in zip(places, rest[:8])], rest[8], rest[9], conv_out, skip_input_grad)
        fc1_total, fc2_total, proj_total, qkv_total, skip_total, embed_turned, conv_grad_turned = totals[:7]
        line, fc1_line = totals[7:15], totals[15]
        output = totals[16].reshape(row_count, tile_height, tile_width, patch)
        skip_input_grad = totals[17].reshape(skip_input.shape)
        return (
            output, skip_input_grad, embed_turned.T, line[0], skip_total, line[1], line[2], line[3], qkv_total,
            proj_total, line[4], line[5], line[6], fc1_total, fc1_line, fc2_total, line[7], conv_grad_turned.T,
        )
    output = conv_out.transpose(0, 2, 1).reshape(row_count, tile_height, tile_width, patch)
    skip_input_grad = skip_input_grad.reshape(skip_input.shape)
    qkv_grad = jnp.concatenate([entry.reshape(-1, width) for entry in rest[:3]], axis=1)
    skip_grad, thin = [entry.reshape(-1, entry.shape[2]) for entry in rest[3:5]]
    flat = rest[5]
    fc1_grad = fc1_grad.reshape(width, -1)
    line = [flat[:, k, :share].reshape(-1) for k in range(8)]
    fc1_line = flat[:, 8:11].reshape(-1)
    local_grads = [
        thin[:, taps : taps + patch], line[0], skip_grad, line[1], line[2], line[3], qkv_grad, proj_grad, line[4],
        line[5], line[6], fc1_grad, fc1_line, fc2_grad, line[7], thin[:, :taps],
    ]
    return (output, skip_input_grad) + sum_by_table([entry.astype(wide) for entry in local_grads])


def solution(mesh):
    return jax.shard_map(
        shards,
        mesh=mesh,
        in_specs=(
            P("rows", "ty", "tx", None),
            P("rows", "ty", "tx", None),
            P("rows", None, None),
            P(),
            P(),
            P(),
            P(),
            P(),
            P(),
            P(),
            P(),
            P(),
            P(),
            P(),
            P(),
            P(),
            P(),
            P(),
            P(),
            P("rows", "ty", "tx", None),
        ),
        out_specs=(
            P("rows", "ty", "tx", None),
            P("rows", "ty", "tx", None),
            P("rows", None),
            P("rows"),
            P("rows", None),
            P("rows"),
            P("rows"),
            P("rows"),
            P("rows", None),
            P("rows", None),
            P("rows"),
            P("rows"),
            P("rows"),
            P("rows", None),
            P("rows"),
            P("rows", None),
            P("rows"),
            P("rows", None),
        ),
        check_vma=False,
    )
```

```python
import functools

import jax
import jax.numpy as jnp
from jax import lax
from jax.experimental import pallas as pl
from jax.experimental.pallas import tpu as pltpu
from jax.sharding import PartitionSpec as P

MESH = pl.DeviceIdType.MESH
norm_eps = 1e-05
full_vmem = 62 * 1024 * 1024


def cell_of(token, tile, tile_height, tile_width, columns):
    down = tile // columns * tile_height + token // tile_width
    across = tile % columns * tile_width + token % tile_width
    return down, across


def fill_shift(shift_ref, tile_height, tile_width):
    tokens = tile_height * tile_width
    bands, columns = lax.axis_size("ty"), lax.axis_size("tx")
    own = lax.axis_index("ty") * columns + lax.axis_index("tx")
    lane = lax.broadcasted_iota(jnp.int32, (8, tokens), 1)
    down, across = cell_of(lane, own, tile_height, tile_width, columns)
    step = lax.broadcasted_iota(jnp.int32, (shift_ref.shape[0], tokens), 0)
    for p in range(9):
        i, j = down - (p // 3 - 1), across - (p % 3 - 1)
        inside = (i >= 0) & (i < bands * tile_height) & (j >= 0) & (j < columns * tile_width)
        tile = i // tile_height * columns + j // tile_width
        place = tile * tokens + i % tile_height * tile_width + j % tile_width
        place = jnp.where(inside, place, -1)[0:1]
        chosen = jnp.where(step == place, 1.0, 0.0)
        shift_ref[:, p * tokens : (p + 1) * tokens] = chosen.astype(jnp.bfloat16)


def same_image(cuts_ref, row, p, tile_height, tile_width):
    tokens = tile_height * tile_width
    columns = lax.axis_size("tx")
    own = lax.axis_index("ty") * columns + lax.axis_index("tx")
    lane = lax.broadcasted_iota(jnp.int32, (8, tokens), 1)
    down, across = cell_of(lane, own, tile_height, tile_width, columns)
    left_width, top_height = cuts_ref[row, 0], cuts_ref[row, 1]

    def image_of(i, j):
        return jnp.where(j < left_width, 0, jnp.where(i < top_height, 1, 2))

    there = image_of(down - (p // 3 - 1), across - (p % 3 - 1))
    return jnp.where(image_of(down, across) == there, 1.0, 0.0)[0:1]


def mm(former, latter, axis_former, axis_latter):
    return lax.dot_general(
        former,
        latter,
        (((axis_former,), (axis_latter,)), ((), ())),
        preferred_element_type=jnp.float32,
    )


def normalised(values):
    average = jnp.mean(values, axis=1, keepdims=True)
    centred = values - average
    rate = lax.rsqrt(jnp.mean(centred * centred, axis=1, keepdims=True) + norm_eps)
    return centred * rate, rate


def norm_back(incoming, unit, rate, gain):
    scaled = incoming * gain
    first = jnp.mean(scaled, axis=1, keepdims=True)
    second = jnp.mean(scaled * unit, axis=1, keepdims=True)
    return (scaled - first - unit * second) * rate


def down_sum(values):
    return jnp.sum(values, axis=0, keepdims=True)


def front_kernel(
    segment_ids, latent, cotangent, embed_turned, *refs
):
    biases, fc1_bias, refs = refs[:8], refs[8], refs[9:]
    skip_in, skip_weight_in, qkv_in, embedded, stream, normed, query, pairs, cot, vectors, hidden_bias, cuts = refs[:12]
    skip, skip_weight, qkv_weight, load_sem = refs[12:]
    sources, targets = (skip_weight_in, skip_in, qkv_in), (skip_weight, skip, qkv_weight)
    loads = [pltpu.make_async_copy(a, b, load_sem.at[k]) for k, (a, b) in enumerate(zip(sources, targets))]
    for load in loads:
        load.start()
    for k, bias in enumerate(biases):
        vectors[k : k + 1] = bias[...].reshape(1, bias.shape[0]).astype(jnp.float32)
    line = fc1_bias[...].reshape(1, fc1_bias.shape[0]).astype(jnp.float32)
    block = hidden_bias.shape[2]
    for k in range(hidden_bias.shape[0]):
        hidden_bias[k] = line[:, k * block : (k + 1) * block]
    width = skip.shape[1]
    row_count, tokens = query.shape[1], query.shape[2]
    side = segment_ids.shape[1]
    for row in range(row_count):

        def count(k, carry):
            left, top = carry
            left = left + jnp.where(segment_ids[row, 0, k] == 0, 1, 0)
            top = top + jnp.where(segment_ids[row, k, side - 1] == 1, 1, 0)
            return left, top

        left, top = lax.fori_loop(0, side, count, (jnp.int32(0), jnp.int32(0)), unroll=8)
        cuts[row, 0] = left
        cuts[row, 1] = top
        at = slice(row * tokens, (row + 1) * tokens)
        cot[row] = jnp.transpose(cotangent[at, :].astype(jnp.float32)).astype(jnp.bfloat16)
        embedded[at, :] = (mm(latent[at, :], embed_turned[...], 1, 0) + vectors[0:1]).astype(jnp.bfloat16)
    loads[0].wait()
    loads[1].wait()
    total = mm(embedded[...], skip_weight[:width], 1, 0) + mm(skip[...], skip_weight[width:], 1, 0) + vectors[1:2]
    stream[...] = total
    unit, rate = normalised(total)
    normed[...] = (unit * vectors[2:3] + vectors[3:4]).astype(jnp.bfloat16)
    loads[2].wait()
    half = width // 2
    for k in range(3):
        piece = mm(normed[...], qkv_weight[:, k * width : (k + 1) * width], 1, 0).astype(jnp.bfloat16)
        for g in range(2):
            part = piece[:, g * half : (g + 1) * half].reshape(row_count, tokens, half)
            if k == 0:
                query[g] = part
            else:
                pairs[g, :, :, (k - 1) * half : k * half] = part


def front(segment_ids, latent, cotangent, embed_turned, biases, fc1_bias, skip, skip_weight, qkv_weight, row_count):
    token_count, width = skip.shape
    tokens = token_count // row_count
    low, wide = jnp.bfloat16, jnp.float32
    smem, vmem = pl.BlockSpec(memory_space=pltpu.SMEM), pl.BlockSpec(memory_space=pltpu.VMEM)
    return pl.pallas_call(
        front_kernel,
        out_shape=[
            jax.ShapeDtypeStruct((token_count, width), low),
            jax.ShapeDtypeStruct((token_count, width), wide),
            jax.ShapeDtypeStruct((token_count, width), low),
            jax.ShapeDtypeStruct((2, row_count, tokens, width // 2), low),
            jax.ShapeDtypeStruct((2, row_count, tokens, width), low),
            jax.ShapeDtypeStruct((row_count, cotangent.shape[1], tokens), low),
            jax.ShapeDtypeStruct((8, width), wide),
            jax.ShapeDtypeStruct((fc1_bias.shape[0] // width, 1, width), wide),
            jax.ShapeDtypeStruct((row_count, 2), jnp.int32),
        ],
        in_specs=[smem] + [vmem] * 12 + [pl.BlockSpec(memory_space=pl.ANY)] * 3,
        out_specs=[vmem] * 8 + [smem],
        scratch_shapes=[pltpu.VMEM(entry.shape, low) for entry in (skip, skip_weight, qkv_weight)]
        + [pltpu.SemaphoreType.DMA((3,))],
        compiler_params=pltpu.CompilerParams(vmem_limit_bytes=full_vmem),
        name="front",
    )(segment_ids, latent, cotangent, embed_turned, *biases, fc1_bias, skip, skip_weight, qkv_weight)


def erf_of(values):
    x = jnp.clip(values, -4.0, 4.0)
    square = x * x
    upper = square * -2.72614225801306e-10 + 2.77068142495902e-08
    for term in (-2.10102402082508e-06, -5.69250639462346e-05, -7.34990630326855e-04, -2.95459980854025e-03, -1.60960333262415e-02):
        upper = upper * square + term
    lower = square * -1.45660718464996e-05 + -2.13374055278905e-04
    for term in (-1.68282697438203e-03, -7.37332916720468e-03, -1.42647390514189e-02):
        lower = lower * square + term
    return x * upper / lower


def middle_kernel(
    paired, attended, stream, out_grad, proj_weight, vectors, hidden_bias, active_grad, fc1_weight, fc2_weight,
    fc1_out, fc2_out, hidden_bias_grad, proj_grad, attended_grad, mid_grad, conv_in, vector_grads,
    middle, normed, out_low, forward_sum, backward_sum, grad1, grad2, *refs
):
    step = pl.program_id(0)
    last = fc2_out.shape[0] // fc2_weight.shape[0] - 1
    token_count, width = stream.shape
    block = fc1_weight.shape[1]
    low = jnp.bfloat16
    parts = [slice(0, token_count)]
    store_sem = refs[-1]
    if paired:
        got1, got2, total1, total2, half_got, send_sem, recv_sem, half_send, half_recv = refs[:9]
        z, ty, y = lax.axis_index("rows"), lax.axis_index("ty"), lax.axis_index("tx")
        core = lax.rem(ty, 2)
        peer = (z, ty + 1 - 2 * core, y)
        x = ty // 2
        sides = (x, x, y, y)
        peer_x, peer_y = (z, (1 - x) * 2 + core, y), (z, ty, 1 - y)

    def store(k, which):
        slot = lax.rem(k, 2)
        if which == 0:
            source = total1 if paired else grad1
            target = fc1_out.at[:, :, pl.ds(pl.multiple_of(k * source.shape[3], 128), source.shape[3])]
        else:
            source = total2 if paired else grad2
            target = fc2_out.at[pl.ds(pl.multiple_of(k * source.shape[1], 16), source.shape[1])]
        return pltpu.make_async_copy(source.at[slot], target, store_sem.at[slot, which])

    def stores(k):
        return [store(k, 0), store(k, 1)]

    def swaps(k):
        slot = lax.rem(k, 2)
        theirs1 = pl.ds(pl.multiple_of((1 - core) * (block // 2), 128), block // 2)
        theirs2 = pl.ds(pl.multiple_of((1 - core) * (width // 2), 128), width // 2)
        pairs = ((grad1.at[slot, :, :, theirs1], got1.at[k]), (grad2.at[slot, :, theirs2], got2.at[k]))
        return [
            pltpu.make_async_remote_copy(
                src_ref=source,
                dst_ref=target,
                send_sem=send_sem.at[k, n],
                recv_sem=recv_sem.at[k, n],
                device_id=peer,
                device_id_type=MESH,
            )
            for n, (source, target) in enumerate(pairs)
        ]

    def halves(k):
        slot = lax.rem(k, 2)
        part = total1.shape[2] // 2
        copies = []
        for n, (side, other) in enumerate(((x, peer_x), (y, peer_y))):
            theirs = pl.ds(pl.multiple_of((1 - side) * part, 16), part)
            copies.append(
                pltpu.make_async_remote_copy(
                    src_ref=total1.at[slot, 2 * n : 2 * n + 2, theirs],
                    dst_ref=half_got.at[k, 2 * n : 2 * n + 2],
                    send_sem=half_send.at[k, n],
                    recv_sem=half_recv.at[k, n],
                    device_id=other,
                    device_id_type=MESH,
                )
            )
        return copies

    def late(k):
        slot = lax.rem(k, 2)
        part = total1.shape[2] // 2
        for copy in halves(k):
            copy.wait()
        for n in range(4):
            kept = pl.ds(pl.multiple_of(sides[n] * part, 16), part)
            total1[slot, n, kept, :] = total1[slot, n, kept, :] + half_got[k, n]
        store(k, 0).start()

    def settle(k):
        slot = lax.rem(k, 2)
        if paired:
            for copy in swaps(k):
                copy.wait()

            @pl.when(k >= 2)
            def _():
                for copy in stores(k - 2):
                    copy.wait()

            mine1 = pl.ds(pl.multiple_of(core * (block // 2), 128), block // 2)
            mine2 = pl.ds(pl.multiple_of(core * (width // 2), 128), width // 2)
            total1[slot] = grad1[slot, :, :, mine1] + got1[k]
            total2[slot] = grad2[slot, :, mine2] + got2[k]
            store(k, 1).start()

            @pl.when(k < last)
            def _():
                for copy in halves(k):
                    copy.start()

            @pl.when(k == last)
            def _():
                store(k, 0).start()
        else:
            for copy in stores(k):
                copy.start()

    @pl.when(step == 0)
    def _():
        if paired:
            for other in (peer, peer_x, peer_y):
                pl.semaphore_signal(pltpu.get_barrier_semaphore(), inc=1, device_id=other, device_id_type=MESH)
        total = jnp.zeros((1, width), jnp.float32)
        for at in parts:
            grad = out_grad[at, :]
            out_low[at, :] = grad.astype(low)
            total = total + down_sum(grad)
            value = stream[at, :] + vectors[4:5]
            for k in range(2):
                value = value + mm(attended[k], proj_weight[k * width // 2 : (k + 1) * width // 2], 1, 0)
            middle[at, :] = value
            unit, rate = normalised(value)
            normed[at, :] = (unit * vectors[5:6] + vectors[6:7]).astype(low)
        vector_grads[7:8] = total
        forward_sum[...] = jnp.zeros_like(forward_sum)
        backward_sum[...] = jnp.zeros_like(backward_sum)

    slot = lax.rem(step, 2)
    if not paired:

        @pl.when(step >= 2)
        def _():
            for copy in stores(step - 2):
                copy.wait()

    bias_grad = jnp.zeros((1, block), jnp.float32)
    actives, hidden_lows = [], []
    for at in parts:
        hidden = mm(normed[at, :], fc1_weight[...], 1, 0) + hidden_bias[0]
        share = 0.5 + 0.5 * erf_of(hidden * 0.7071067811865476)
        density = jnp.exp(hidden * hidden * -0.5) * 0.3989422804014327
        active = (hidden * share).astype(low)
        hidden_grad = active_grad[at, :].astype(jnp.float32) * (share + hidden * density)
        bias_grad = bias_grad + down_sum(hidden_grad)
        hidden_low = hidden_grad.astype(low)
        forward_sum[at, :] = forward_sum[at, :] + mm(active, fc2_weight[...], 1, 0)
        backward_sum[at, :] = backward_sum[at, :] + mm(hidden_low, fc1_weight[...], 1, 1)
        actives.append(active)
        hidden_lows.append(hidden_low)
    hidden_bias_grad[0] = bias_grad
    grad2[slot] = mm(jnp.concatenate(actives, axis=0), out_low[...], 0, 0).astype(low)
    grad1[slot] = mm(normed[...], jnp.concatenate(hidden_lows, axis=0), 0, 0).astype(low).reshape(grad1.shape[1:])
    if paired:

        @pl.when(step == 0)
        def _():
            pl.semaphore_wait(pltpu.get_barrier_semaphore(), 3)

        for copy in swaps(step):
            copy.start()

        @pl.when(step > 1)
        def _():
            late(step - 2)

        @pl.when(step > 0)
        def _():
            settle(step - 1)
    else:
        settle(step)

    @pl.when(step == last)
    def _():
        gain_sum = jnp.zeros((1, width), jnp.float32)
        bias_sum = jnp.zeros((1, width), jnp.float32)
        mid_sum = jnp.zeros((1, width), jnp.float32)
        lows = []
        for at in parts:
            unit, rate = normalised(middle[at, :])
            conv_in[at, :] = (middle[at, :] + forward_sum[at, :] + vectors[7:8]).astype(low)
            incoming = backward_sum[at, :]
            gain_sum = gain_sum + down_sum(incoming * unit)
            bias_sum = bias_sum + down_sum(incoming)
            grad = out_grad[at, :] + norm_back(incoming, unit, rate, vectors[5:6])
            mid_grad[at, :] = grad
            mid_sum = mid_sum + down_sum(grad)
            mid_low = grad.astype(low)
            lows.append(mid_low)
            for k in range(2):
                attended_grad[k] = mm(mid_low, proj_weight[k * width // 2 : (k + 1) * width // 2], 1, 1).astype(low)
        for k in range(2):
            proj_grad[k * width // 2 : (k + 1) * width // 2] = mm(attended[k], lows[0], 0, 0).astype(low)
        vector_grads[4:5] = mid_sum
        vector_grads[5:6] = gain_sum
        vector_grads[6:7] = bias_sum
        if paired:
            late(last - 1)
            settle(step)
        for k in (last - 1, last):
            for copy in stores(k):
                copy.wait()


def middle(attended, stream, out_grad, active_grad, proj_weight, vectors, hidden_bias, fc1_weight, fc2_weight, paired):
    token_count, width = stream.shape
    hidden_width = fc1_weight.shape[1]
    steps, _, block = hidden_bias.shape
    low, wide = jnp.bfloat16, jnp.float32
    cut = 2 if paired else 1
    vmem, anywhere = pl.BlockSpec(memory_space=pltpu.VMEM), pl.BlockSpec(memory_space=pl.ANY)
    scratch = [
        pltpu.VMEM((token_count, width), wide),
        pltpu.VMEM((token_count, width), low),
        pltpu.VMEM((token_count, width), low),
        pltpu.VMEM((token_count, width), wide),
        pltpu.VMEM((token_count, width), wide),
        pltpu.VMEM((2, 4, width // 4, block), low),
        pltpu.VMEM((2, block, width), low),
    ]
    if paired:
        scratch += [
            pltpu.VMEM((steps, 4, width // 4, block // 2), low),
            pltpu.VMEM((steps, block, width // 2), low),
            pltpu.VMEM((2, 4, width // 4, block // 2), low),
            pltpu.VMEM((2, block, width // 2), low),
            pltpu.VMEM((steps, 4, width // 8, block // 2), low),
            pltpu.SemaphoreType.DMA((steps, 2)),
            pltpu.SemaphoreType.DMA((steps, 2)),
            pltpu.SemaphoreType.DMA((steps, 2)),
            pltpu.SemaphoreType.DMA((steps, 2)),
        ]
        params = pltpu.CompilerParams(collective_id=4, has_side_effects=True, vmem_limit_bytes=full_vmem)
    else:
        params = pltpu.CompilerParams(vmem_limit_bytes=full_vmem)
    return pl.pallas_call(
        functools.partial(middle_kernel, paired),
        grid=(steps,),
        out_shape=[
            jax.ShapeDtypeStruct((4, width // 4, hidden_width // cut), low),
            jax.ShapeDtypeStruct((hidden_width, width // cut), low),
            jax.ShapeDtypeStruct((steps, 1, block), wide),
            jax.ShapeDtypeStruct((width, width), low),
            jax.ShapeDtypeStruct((2, token_count, width // 2), low),
            jax.ShapeDtypeStruct((token_count, width), wide),
            jax.ShapeDtypeStruct((token_count, width), low),
            jax.ShapeDtypeStruct((8, width), wide),
        ],
        in_specs=[vmem] * 5
        + [
            pl.BlockSpec((1, 1, block), lambda k: (k, 0, 0)),
            pl.BlockSpec((token_count, block), lambda k: (0, k)),
            pl.BlockSpec((width, block), lambda k: (0, k)),
            pl.BlockSpec((block, width), lambda k: (k, 0)),
        ],
        out_specs=[anywhere, anywhere, pl.BlockSpec((1, 1, block), lambda k: (k, 0, 0))] + [vmem] * 5,
        scratch_shapes=scratch + [pltpu.SemaphoreType.DMA((2, 2))],
        compiler_params=params,
        name="middle",
    )(attended, stream, out_grad, proj_weight, vectors, hidden_bias, active_grad, fc1_weight, fc2_weight)


def rear_kernel(
    kinds, reduces, projected_in, qkv_in, normed_in, stream_in, mid_in, embedded_in, skip_in, skip_weight_in,
    latent, vectors, middle_grads, hidden_bias_grad, conv_grad, *refs
):
    count = len(kinds)
    resumed, refs = refs[:count], refs[count:]
    skip_input_grad, refs = refs[0], refs[1:]
    if reduces:
        sums, refs = refs[: count + 6], refs[count + 6 :]
        peers = chip_peers()
    grads, refs = refs[:6], refs[6:]
    skip_grad, thin, flat = grads[3:]
    projected_grad, qkv_weight, normed, stream, mid_grad, embedded, skip, skip_weight, stream_low, load_sem = refs[:10]
    sources = (projected_in, normed_in, qkv_in, stream_in, mid_in, embedded_in, skip_in, skip_weight_in)
    targets = (projected_grad, normed, qkv_weight, stream, mid_grad, embedded, skip, skip_weight)
    loads = [pltpu.make_async_copy(a, b, load_sem.at[k]) for k, (a, b) in enumerate(zip(sources, targets))]
    for load in loads[:3]:
        load.start()
    items = [None] * 10
    if reduces:
        items = make_reducers(kinds + (("plane", False),) * 6, resumed + grads, sums, refs[10:], range(count + 3))
        greet([peers[name] for name in ("core", "x", "y", "xy")] + peers["z"])
        for item in items[:count]:
            item.begin()
    fc1, fc2a, fc2b, proj, qkv0, qkv1, qkv2, skips, thins, flats = items
    for load in loads[3:]:
        load.start()
    width = stream.shape[1]
    low = jnp.bfloat16
    made = {}

    def open_up(*some):
        for item in some:
            if reduces:
                item.begin()

    def weight_grad(k):
        if k == 0:
            loads[0].wait()
            loads[1].wait()
        piece = mm(normed[...], projected_grad[:, k * width : (k + 1) * width], 0, 0)
        grads[k][...] = piece.astype(low).reshape(grads[k].shape)
        open_up((qkv0, qkv1, qkv2)[k])

    def norm():
        for load in loads[2:5]:
            load.wait()
        incoming = mm(projected_grad[...], qkv_weight[...], 1, 1)
        unit, rate = normalised(stream[...])
        grad = mid_grad[...] + norm_back(incoming, unit, rate, vectors[2:3])
        made["rows"] = [down_sum(grad), down_sum(incoming * unit), down_sum(incoming)]
        stream_low[...] = grad.astype(low)

    def skip_weight_grad():
        loads[5].wait()
        loads[6].wait()
        skip_grad[0:2] = mm(embedded[...], stream_low[...], 0, 0).astype(low).reshape(2, width // 2, width)
        skip_grad[2:4] = mm(skip[...], stream_low[...], 0, 0).astype(low).reshape(2, width // 2, width)
        open_up(skips)

    def joined():
        loads[7].wait()
        embed_grad = mm(stream_low[...], skip_weight[:width], 1, 1)
        embed_weight_grad = mm(embed_grad.astype(low), latent[...], 0, 0)
        rest = jnp.zeros((width, 128 - 2 * 16), jnp.float32)
        thin[:, :, :128] = conv_grad[:, :128].astype(low).reshape(4, width // 4, 128)
        edge = jnp.concatenate([conv_grad[:, 128:144], embed_weight_grad, rest], axis=1)
        thin[:, :, 128:] = edge.astype(low).reshape(4, width // 4, 128)
        rows = [down_sum(embed_grad)] + made["rows"] + [middle_grads[k : k + 1] for k in range(4, 8)]
        stack = jnp.concatenate(rows, axis=0)
        share = width // 4
        hidden_line = jnp.concatenate([hidden_bias_grad[k] for k in range(hidden_bias_grad.shape[0])], axis=1)
        for block in range(4):
            own = stack[:, block * share : (block + 1) * share]
            own = jnp.concatenate([own, jnp.zeros((8, 256 - share), jnp.float32)], axis=1)
            line = hidden_line[:, block * width : (block + 1) * width]
            pieces = [line[:, k * 256 : (k + 1) * 256] for k in range(width // 256)]
            body = jnp.concatenate([own] + pieces + [jnp.zeros((8 - len(pieces), 256), jnp.float32)], axis=0)
            flat[block, 0:16] = body.astype(low)
            flat[block, 16:64] = jnp.zeros((48, 256), low)
        open_up(thins, flats)

    def input_grad():
        skip_input_grad[...] = mm(stream_low[...], skip_weight[width:], 1, 1).astype(low)

    def advance(*some):
        for item in some:
            if reduces:
                item.step()

    advance(proj, fc2b, fc2a)
    weight_grad(0)
    weight_grad(1)
    weight_grad(2)
    advance(qkv0, qkv2)
    norm()
    advance(qkv0, qkv1)
    skip_weight_grad()
    advance(qkv0, qkv2, skips)
    joined()
    advance(qkv2, thins, proj, qkv1, skips, thins, qkv1, fc1)
    advance(qkv0, qkv0, fc2b, proj, skips, flats, thins, fc2a)
    advance(qkv1, qkv1, qkv2, qkv2, qkv0, fc1, qkv1, fc2a)
    advance(flats, fc2b, qkv2, skips, skips, qkv1, fc2a, proj)
    advance(fc2b, flats, qkv0, fc1)
    input_grad()
    advance(qkv0, thins, thins, flats, flats, fc1, qkv1, qkv2)
    advance(skips, fc2a, thins, flats, qkv2, fc2a, flats, skips)
    advance(thins)
    assert not reduces or not any(item.stages for item in items)


def rear(projected_grad, qkv_weight, normed, stream, mid_grad, embedded, skip, skip_weight, latent, vectors, middle_grads, hidden_bias_grad, conv_grad, resumed, reduces):
    token_count, width = stream.shape
    low = jnp.bfloat16
    kinds = tuple((start, True) for start, _, _ in resumed)
    sizes = [(width // 4, width)] * 3 + [(width // 2, width), (width // 4, 256), (64, 256)]
    totals = [shape for _, _, shape in resumed] + [(r, c // 2) for r, c in sizes]
    vmem, anywhere = pl.BlockSpec(memory_space=pltpu.VMEM), pl.BlockSpec(memory_space=pl.ANY)
    big = [projected_grad, qkv_weight, normed, stream, mid_grad, embedded, skip, skip_weight]
    out_shape = [jax.ShapeDtypeStruct((token_count, width), low)]
    out_specs = [vmem]
    scratch = []
    if reduces:
        out_shape += [jax.ShapeDtypeStruct((2,) + shape, low) for shape in totals]
        out_specs += [anywhere] * len(totals)
        scratch += [pltpu.VMEM((4,) + shape, low) for shape in sizes]
        params = pltpu.CompilerParams(collective_id=3, has_side_effects=True, vmem_limit_bytes=full_vmem)
    else:
        out_shape += [jax.ShapeDtypeStruct((4,) + shape, low) for shape in sizes]
        out_specs += [vmem] * len(sizes)
        params = pltpu.CompilerParams(vmem_limit_bytes=full_vmem)
    scratch += [pltpu.VMEM(entry.shape, entry.dtype) for entry in big]
    scratch += [pltpu.VMEM((token_count, width), low), pltpu.SemaphoreType.DMA((len(big),))]
    if reduces:
        scratch += reducer_scratch(kinds + (("plane", False),) * 6, totals)
    return pl.pallas_call(
        functools.partial(rear_kernel, kinds, reduces),
        out_shape=out_shape,
        in_specs=[anywhere] * len(big) + [vmem] * 5 + [anywhere] * len(kinds),
        out_specs=out_specs,
        scratch_shapes=scratch,
        compiler_params=params,
        name="rear",
    )(*big, latent, vectors, middle_grads, hidden_bias_grad, conv_grad, *[entry for _, entry, _ in resumed])


def finish_kernel(patch, plan, *refs):
    count = len(plan)
    sums, (thin, flat, conv_out, passed) = refs[:count], refs[count : count + 4]
    totals, refs = refs[count + 4 : count + 9], refs[count + 9 :]
    (embed_turned, conv_turned), lines, fc1_line, output, handed, refs = refs[:2], refs[2:10], refs[10], refs[11], refs[12], refs[13:]
    lows, wides, held, load_sem, store_sem = refs[:count], refs[count : count + 5], *refs[count + 5 :]
    take = pltpu.make_async_copy(passed, held, load_sem.at[count])
    give = pltpu.make_async_copy(held, handed, store_sem.at[count])
    loads = [pltpu.make_async_copy(a, b, load_sem.at[k]) for k, (a, b) in enumerate(zip(sums, lows))]
    for load in loads:
        load.start()
    take.start()
    stores = [give]
    for k, (low, (which, start, piece, left)) in enumerate(zip(lows, plan)):
        loads[k].wait()
        if k == 1:
            take.wait()
            give.start()
        wide = wides[which]
        half, depth = low.shape[2], low.shape[1]

        def body(i, carry):
            at = pl.ds(pl.multiple_of(i * 16, 16), 16)
            to = pl.ds(pl.multiple_of(start + i * 16, 16), 16)
            for core in range(2):
                for n in range(half // piece):
                    column = left + (2 * n + core) * piece
                    wide[to, column : column + piece] = low[core, at, n * piece : (n + 1) * piece].astype(jnp.float32)
            return carry

        lax.fori_loop(0, depth // 16, body, 0)
        there = (pl.ds(start, depth), pl.ds(left, 2 * half))
        store = pltpu.make_async_copy(wide.at[there], totals[which].at[there], store_sem.at[k])
        store.start()
        stores.append(store)
    share = thin.shape[1]
    turned = jnp.transpose(jnp.concatenate([thin[0], thin[1]], axis=1).astype(jnp.float32))
    taps = 9 * patch
    conv_turned[...] = turned[:taps]
    embed_turned[...] = turned[taps : taps + patch]
    rows = jnp.concatenate([flat[0, 0:16, :], flat[1, 0:16, :]], axis=1).astype(jnp.float32)
    for k, line in enumerate(lines):
        line[...] = rows[k : k + 1, :share].reshape(share)
    fc1_line[...] = jnp.concatenate([rows[k : k + 1] for k in range(8, 11)], axis=1).reshape(fc1_line.shape[0])
    for row in range(output.shape[0]):
        output[row] = jnp.transpose(conv_out[row].astype(jnp.float32)).astype(jnp.bfloat16)
    for store in stores:
        store.wait()


def finish(sums, thin, flat, conv_out, passed):
    row_count, patch, tokens = conv_out.shape
    share = thin.shape[1]
    wide = jnp.float32
    plan = tuple(entry[:4] for entry in sums)
    arrays = [entry[4] for entry in sums]
    whole = [(0, 0)] * 5
    for which, start, _, left, entry in sums:
        rows, columns = whole[which]
        whole[which] = (max(rows, start + entry.shape[1]), max(columns, left + 2 * entry.shape[2]))
    vmem, anywhere = pl.BlockSpec(memory_space=pltpu.VMEM), pl.BlockSpec(memory_space=pl.ANY)
    return pl.pallas_call(
        functools.partial(finish_kernel, patch, plan),
        out_shape=[jax.ShapeDtypeStruct(shape, wide) for shape in whole]
        + [jax.ShapeDtypeStruct((patch, share), wide), jax.ShapeDtypeStruct((9 * patch, share), wide)]
        + [jax.ShapeDtypeStruct((share,), wide)] * 8
        + [jax.ShapeDtypeStruct((4 * share,), wide), jax.ShapeDtypeStruct((row_count, tokens, patch), jnp.bfloat16)]
        + [jax.ShapeDtypeStruct(passed.shape, passed.dtype)],
        in_specs=[anywhere] * len(arrays) + [vmem] * 3 + [anywhere],
        out_specs=[anywhere] * 5 + [vmem] * 12 + [anywhere],
        scratch_shapes=[pltpu.VMEM(entry.shape, jnp.bfloat16) for entry in arrays]
        + [pltpu.VMEM(shape, wide) for shape in whole]
        + [pltpu.VMEM(passed.shape, passed.dtype)]
        + [pltpu.SemaphoreType.DMA((len(arrays) + 1,))] * 2,
        compiler_params=pltpu.CompilerParams(vmem_limit_bytes=full_vmem),
        name="finish",
    )(*arrays, thin, flat, conv_out, passed)


def plane_peers():
    z, ty, y = lax.axis_index("rows"), lax.axis_index("ty"), lax.axis_index("tx")
    core, x = lax.rem(ty, 2), ty // 2
    here = x * 2 + core
    across = (1 - x) * 2 + core
    tiles = {
        "own": here * 2 + y,
        "x": across * 2 + y,
        "y": here * 2 + 1 - y,
        "xy": across * 2 + 1 - y,
    }
    peers = {
        "core": (z, x * 2 + 1 - core, y),
        "x": (z, across, y),
        "y": (z, here, 1 - y),
    }
    return tiles, peers


def plane_peer(k):
    z, ty, y = lax.axis_index("rows"), lax.axis_index("ty"), lax.axis_index("tx")
    x, core = ty // 2, lax.rem(ty, 2)
    flip_x, flip_core, flip_y = k // 4, k // 2 % 2, k % 2
    x = x + flip_x - 2 * flip_x * x
    core = core + flip_core - 2 * flip_core * core
    y = y + flip_y - 2 * flip_y * y
    return (z, x * 2 + core, y), (x * 2 + core) * 2 + y


def greet(peers):
    barrier = pltpu.get_barrier_semaphore()
    for peer in peers:
        pl.semaphore_signal(barrier, inc=1, device_id=peer, device_id_type=MESH)
    pl.semaphore_wait(barrier, len(peers))


def fill_mask(mask_ref, cuts_ref, row, tile, tile_height, tile_width):
    columns = lax.axis_size("tx")
    tokens = tile_height * tile_width
    left_width = cuts_ref[row, 0]
    top_height = cuts_ref[row, 1]

    def image_of(down, across):
        return jnp.where(across < left_width, 0, jnp.where(down < top_height, 1, 2))

    lane = lax.broadcasted_iota(jnp.int32, (8, tokens), 1)
    mine = image_of(*cell_of(lane, tile, tile_height, tile_width, columns))[0:1]
    step = lax.broadcasted_iota(jnp.int32, (tokens, tokens), 0)
    down, across = step // tile_width, step % tile_width
    for other in range(mask_ref.shape[0] // tokens):
        theirs = image_of(
            down + other // columns * tile_height, across + other % columns * tile_width
        )
        mask_ref[other * tokens : (other + 1) * tokens, :] = jnp.where(mine == theirs, 0.0, -1e30)


def two_heads(pair, scale):
    lane = lax.broadcasted_iota(jnp.int32, pair.shape, 1)
    wide = pair.astype(jnp.float32) * scale
    first = jnp.where(lane < pair.shape[1] // 2, wide, 0.0)
    return jnp.concatenate([first, wide - first], axis=0).astype(jnp.bfloat16)


def own_blocks(both):
    head, tokens = both.shape[0] // 2, both.shape[1] // 2
    return jnp.concatenate([both[:head, :tokens], both[head:, tokens:]], axis=0)


def attend_kernel(
    tile_height, tile_width, cuts, query, pairs, cot, conv_turned, fc2_in,
    out, lse, query_out, attended_out, all_out, spread, out_grad_out, active_grad_out,
    cot_all, queries, held, results, scores, mask, shift, fc2_weight, out_grad, active_grad,
    local_sem, send_sem, recv_sem, cot_sem, cot_send_sem, cot_recv_sem, side_sem
):
    _, row_count, tokens, half = query.shape
    tile_count = held.shape[1]
    width = 2 * half
    tiles, peers = plane_peers()
    own = tiles["own"]
    x = lax.axis_index("ty") // 2
    fc2_load = pltpu.make_async_copy(fc2_in, fc2_weight, side_sem.at[0])
    fc2_load.start()
    greet([plane_peer(k)[0] for k in range(1, tile_count)])
    cot_copies = [pltpu.make_async_copy(cot, cot_all.at[own], cot_sem.at[0])]
    for k in range(1, tile_count):
        cot_copies.append(
            pltpu.make_async_remote_copy(
                src_ref=cot,
                dst_ref=cot_all.at[own],
                send_sem=cot_send_sem.at[k],
                recv_sem=cot_recv_sem.at[k],
                device_id=plane_peer(k)[0],
                device_id_type=MESH,
            )
        )

    def send(row, slot, source, target, peer):
        copy = pltpu.make_async_remote_copy(
            src_ref=source,
            dst_ref=target,
            send_sem=send_sem.at[row, slot],
            recv_sem=recv_sem.at[row, slot],
            device_id=peer,
            device_id_type=MESH,
        )
        copy.start()
        flights[row][slot] = copy

    def keep(row, slot, source, target):
        copy = pltpu.make_async_copy(source, target, local_sem.at[row, slot])
        copy.start()
        kept[row][slot] = copy

    flights = [{} for _ in range(row_count)]
    kept = [{} for _ in range(row_count)]

    def begin(row):
        here = held.at[row, own]
        send(row, 1, pairs.at[1 - x, row], here, peers["x"])
        send(row, 0, query.at[1 - x, row], queries.at[row, 1], peers["x"])
        send(row, 2, pairs.at[x, row], here, peers["y"])
        send(row, 3, pairs.at[x, row], here, peers["core"])
        keep(row, 0, query.at[x, row], queries.at[row, 0])
        keep(row, 1, pairs.at[x, row], here)

    def forward_x(row):
        flights[row][1].wait_recv()
        tile = held.at[row, tiles["x"]]
        send(row, 4, tile, tile, peers["y"])
        send(row, 5, tile, tile, peers["core"])

    def forward_y(row):
        flights[row][2].wait_recv()
        tile = held.at[row, tiles["y"]]
        send(row, 6, tile, tile, peers["core"])

    def gather_row(row):
        flights[row][4].wait_recv()
        tile = held.at[row, tiles["xy"]]
        send(row, 7, tile, tile, peers["core"])
        for slot in (0, 3, 5, 6, 7):
            flights[row][slot].wait_recv()
        for slot in range(8):
            flights[row][slot].wait_send()
        for slot in range(2):
            kept[row][slot].wait()
        keep(row, 3, held.at[row], all_out.at[row])
        keep(row, 4, queries.at[row], query_out.at[row])

    chunk = 2

    def compute(row):
        def one_pair(p, carry, which=(0, 1)):
            at = pl.ds(pl.multiple_of(p * 128, 128), 128)
            at_value = pl.ds(pl.multiple_of(half + p * 128, 128), 128)
            for t in which:
                both = two_heads(queries[row, t, :, at], 0.125)
                peak = None
                for c in range(tile_count // chunk):
                    span = slice(c * chunk * tokens, (c + 1) * chunk * tokens)
                    keys = held[row, c * chunk : (c + 1) * chunk, :, at].reshape(chunk * tokens, 128)
                    extra = mask[row, t, span, :]
                    part = mm(keys, both, 1, 1) + jnp.concatenate([extra, extra], axis=1)
                    scores[t, span, :] = part
                    top = jnp.max(part, axis=0, keepdims=True)
                    peak = top if peak is None else jnp.maximum(peak, top)
                total = jnp.zeros_like(peak)
                summed = jnp.zeros((128, 2 * tokens), jnp.float32)
                for c in range(tile_count // chunk):
                    span = slice(c * chunk * tokens, (c + 1) * chunk * tokens)
                    values = held[row, c * chunk : (c + 1) * chunk, :, at_value].reshape(chunk * tokens, 128)
                    part = jnp.exp(scores[t, span, :] - peak)
                    total = total + jnp.sum(part, axis=0, keepdims=True)
                    summed = summed + mm(values, part.astype(jnp.bfloat16), 0, 0)
                blocks = own_blocks(summed / total)
                results[row, t, :, at] = jnp.transpose(blocks).astype(jnp.bfloat16)
                lse[row, p, t] = peak + jnp.log(total)
            return carry

        if row < row_count - 1:
            lax.fori_loop(0, half // 128, one_pair, 0)
            hand_back(row)
        else:
            lax.fori_loop(0, half // 128, functools.partial(one_pair, which=(1,)), 0)
            hand_back(row)
            lax.fori_loop(0, half // 128, functools.partial(one_pair, which=(0,)), 0)
        keep(row, 5, results.at[row, 0], out.at[x, row])
        keep(row, 6, results.at[row], attended_out.at[row])

    def hand_back(row):
        send(row, 8, results.at[row, 1], out.at[x, row], peers["x"])

    side_copies = []
    parts = [slice(k * tokens, (k + 1) * tokens) for k in range(row_count)]

    def spread_out():
        patch = cot_all.shape[2]
        turned = jnp.concatenate(
            [cot_all[t].reshape(row_count * patch, tokens) for t in range(tile_count)], axis=1
        )
        moved = mm(turned, shift[...], 1, 0)
        for row in range(row_count):
            for p in range(9):
                piece = moved[row * patch : (row + 1) * patch, p * tokens : (p + 1) * tokens]
                piece = piece * same_image(cuts, row, p, tile_height, tile_width)
                spread[p * patch : (p + 1) * patch, parts[row]] = piece.astype(jnp.bfloat16)
        out_grad[...] = mm(spread[...], conv_turned[...], 0, 0)
        copy = pltpu.make_async_copy(out_grad, out_grad_out, side_sem.at[1])
        copy.start()
        side_copies.append(copy)

    def activate():
        for k in range(fc2_weight.shape[0] // width):
            span = slice(k * width, (k + 1) * width)
            low = out_grad[...].astype(jnp.bfloat16)
            active_grad[:, span] = mm(low, fc2_weight[span, :], 1, 1).astype(jnp.bfloat16)
        copy = pltpu.make_async_copy(active_grad, active_grad_out, side_sem.at[2])
        copy.start()
        side_copies.append(copy)

    begin(0)
    for copy in cot_copies:
        copy.start()
    if row_count > 1:
        begin(1)
    forward_x(0)
    for row in range(row_count):
        for t, name in enumerate(("own", "x")):
            fill_mask(mask.at[row, t], cuts, row, tiles[name], tile_height, tile_width)
    fill_shift(shift, tile_height, tile_width)
    forward_y(0)
    for copy in cot_copies:
        copy.wait()
    spread_out()
    fc2_load.wait()
    activate()
    if row_count > 1:
        forward_x(1)
        if row_count > 2:
            begin(2)
        forward_y(1)
    for row in range(row_count):
        gather_row(row)
        compute(row)
        if row + 3 < row_count:
            begin(row + 3)
        if row + 2 < row_count:
            forward_x(row + 2)
        if 0 < row < row_count - 1:
            forward_y(row + 1)
    for row in range(row_count):
        flights[row][8].wait()
        for slot in range(3, 7):
            kept[row][slot].wait()
    for copy in side_copies:
        copy.wait()


def attend(cuts, query, pairs, cot, conv_turned, fc2_weight, tile_height, tile_width):
    _, row_count, tokens, half = query.shape
    tile_count = lax.axis_size("ty") * lax.axis_size("tx")
    width = 2 * half
    low, wide = jnp.bfloat16, jnp.float32
    vmem, anywhere = pl.BlockSpec(memory_space=pltpu.VMEM), pl.BlockSpec(memory_space=pl.ANY)
    return pl.pallas_call(
        functools.partial(attend_kernel, tile_height, tile_width),
        out_shape=[
            jax.ShapeDtypeStruct((2, row_count, tokens, half), low),
            jax.ShapeDtypeStruct((row_count, half // 128, 2, 1, 2 * tokens), wide),
            jax.ShapeDtypeStruct((row_count, 2, tokens, half), low),
            jax.ShapeDtypeStruct((row_count, 2, tokens, half), low),
            jax.ShapeDtypeStruct((row_count, tile_count, tokens, width), low),
            jax.ShapeDtypeStruct((conv_turned.shape[0], row_count * tokens), low),
            jax.ShapeDtypeStruct((row_count * tokens, width), wide),
            jax.ShapeDtypeStruct((row_count * tokens, fc2_weight.shape[0]), low),
        ],
        in_specs=[pl.BlockSpec(memory_space=pltpu.SMEM)] + [anywhere] * 3 + [vmem, anywhere],
        out_specs=[anywhere, vmem] + [anywhere] * 3 + [vmem] + [anywhere] * 2,
        scratch_shapes=[
            pltpu.VMEM((tile_count,) + cot.shape, low),
            pltpu.VMEM((row_count, 2, tokens, half), low),
            pltpu.VMEM((row_count, tile_count, tokens, width), low),
            pltpu.VMEM((row_count, 2, tokens, half), low),
            pltpu.VMEM((2, tile_count * tokens, 2 * tokens), wide),
            pltpu.VMEM((row_count, 2, tile_count * tokens, tokens), wide),
            pltpu.VMEM((tile_count * tokens, 9 * tokens), low),
            pltpu.VMEM(fc2_weight.shape, low),
            pltpu.VMEM((row_count * tokens, width), wide),
            pltpu.VMEM((row_count * tokens, fc2_weight.shape[0]), low),
            pltpu.SemaphoreType.DMA((row_count, 7)),
            pltpu.SemaphoreType.DMA((row_count, 9)),
            pltpu.SemaphoreType.DMA((row_count, 9)),
            pltpu.SemaphoreType.DMA((1,)),
            pltpu.SemaphoreType.DMA((tile_count,)),
            pltpu.SemaphoreType.DMA((tile_count,)),
            pltpu.SemaphoreType.DMA((3,)),
        ],
        compiler_params=pltpu.CompilerParams(
            collective_id=1, has_side_effects=True, vmem_limit_bytes=full_vmem
        ),
        name="attend",
    )(cuts, query, pairs, cot, conv_turned, fc2_weight)


def attend_back_kernel(
    tile_height, tile_width, kinds, done, cuts, query_in, attended_in, grad_in, lse_in, conv_in, conv_turned, spread,
    all_pairs, *refs
):
    count = max([kind[2] for kind in kinds], default=-1) + 1
    sources, refs = refs[:count], refs[count:]
    total_count = len(kinds)
    (out, conv_grad, conv_out), saved, refs = refs[:3], refs[3 : 3 + total_count], refs[3 + total_count :]
    query, attended, grad, lse, row_sem = refs[:5]
    held, terms, core_terms, y_terms, x_terms, x_query, query_grad, mask, shift, taps, part, part_got = refs[5:17]
    send_sem, recv_sem, part_send_sem, part_recv_sem = refs[17:21]
    grads = [
        sources[which] if rows is None else sources[which].at[:, rows[0] : rows[1], :]
        for _, _, which, rows in kinds
    ]
    items = make_reducers([kind[:2] for kind in kinds], grads, saved, refs[21:]) if kinds else []
    for item, columns in zip(items, done):
        item.halved = columns
    row_count, _, tokens, half = query.shape
    tile_count = held.shape[1]
    tiles, peers = plane_peers()
    low = jnp.bfloat16
    x, core = lax.axis_index("ty") // 2, lax.rem(lax.axis_index("ty"), 2)

    def group(which, base=0):
        return pl.ds(pl.multiple_of(base + which * half, 128), half)

    loads = []
    for row in range(row_count):
        loads.append([])
        for k, (source, target) in enumerate((
            (all_pairs.at[row], held.at[row]), (query_in.at[row], query.at[row]), (attended_in.at[row], attended.at[row]),
            (grad_in.at[x, row], grad.at[row, 0]), (lse_in.at[row], lse.at[row]),
        )):
            load = pltpu.make_async_copy(source, target, row_sem.at[row, k])
            load.start()
            loads[-1].append(load)
    greet([plane_peer(k)[0] for k in range(1, tile_count)] + (chip_peers()["z"] if kinds else []))
    chunk = 2
    flights = [{} for _ in range(row_count)]

    def send(row, slot, source, target, peer):
        copy = pltpu.make_async_remote_copy(
            src_ref=source,
            dst_ref=target,
            send_sem=send_sem.at[row, slot],
            recv_sem=recv_sem.at[row, slot],
            device_id=peer,
            device_id_type=MESH,
        )
        copy.start()
        flights[row][slot] = copy

    def compute(row):
        for load in loads[row]:
            load.wait()
        flights[row][8].wait()
        for t, name in enumerate(("own", "x")):
            fill_mask(mask.at[t], cuts, row, tiles[name], tile_height, tile_width)

        def one_pair(p, carry):
            at = pl.ds(pl.multiple_of(p * 128, 128), 128)
            at_value = pl.ds(pl.multiple_of(half + p * 128, 128), 128)
            boths, both_grads, deltas, levels = [], [], [], []
            for t in range(2):
                grad_pair = grad[row, t, :, at]
                boths.append(two_heads(query[row, t, :, at], 0.125))
                both_grads.append(two_heads(grad_pair, 1.0))
                inner = jnp.transpose(grad_pair.astype(jnp.float32) * attended[row, t, :, at].astype(jnp.float32))
                heads = [inner[: inner.shape[0] // 2], inner[inner.shape[0] // 2 :]]
                deltas.append(jnp.concatenate([jnp.sum(head, axis=0, keepdims=True) for head in heads], axis=1))
                levels.append(lse[row, p, t])
            all_both = jnp.concatenate(boths, axis=0)
            all_grads = jnp.concatenate(both_grads, axis=0)
            query_part = jnp.zeros((128, 4 * tokens), jnp.float32)
            for c in range(tile_count // chunk):
                span = slice(c * chunk * tokens, (c + 1) * chunk * tokens)
                some = slice(c * chunk, (c + 1) * chunk)
                keys = held[row, some, :, at].reshape(chunk * tokens, 128)
                values = held[row, some, :, at_value].reshape(chunk * tokens, 128)
                weight_parts, score_parts = [], []
                for t in range(2):
                    extra = mask[t, span, :]
                    raw = mm(keys, boths[t], 1, 1) + jnp.concatenate([extra, extra], axis=1)
                    weights = jnp.exp(raw - levels[t])
                    weight_parts.append(weights.astype(low))
                    score_parts.append((weights * (mm(values, both_grads[t], 1, 1) - deltas[t])).astype(low))
                score_grad = jnp.concatenate(score_parts, axis=1)
                value_part = mm(jnp.concatenate(weight_parts, axis=1), all_grads, 1, 0)
                key_part = mm(score_grad, all_both, 1, 0)
                query_part = query_part + mm(keys, score_grad, 0, 0)
                terms[row, some, :, at] = key_part.astype(low).reshape(chunk, tokens, 128)
                terms[row, some, :, at_value] = value_part.astype(low).reshape(chunk, tokens, 128)
            for t in range(2):
                blocks = own_blocks(query_part[:, 2 * t * tokens : 2 * (t + 1) * tokens]) * 0.125
                query_grad[row, t, :, at] = jnp.transpose(blocks).astype(low)
            return carry

        lax.fori_loop(0, half // 128, one_pair, 0)

    names = ("own", "x", "y", "xy")

    def begin(row):
        other = 2 - 4 * core
        for k in (3, 2, 1, 0):
            send(row, k, terms.at[row, tiles[names[k]] + other], core_terms.at[row, k], peers["core"])
        send(row, 7, query_grad.at[row, 1], x_query.at[row], peers["x"])

    def add(target, source):
        def body(i, carry):
            at = pl.ds(pl.multiple_of(i * 16, 16), 16)
            target[at, :] = target[at, :] + source[at, :]
            return carry

        lax.fori_loop(0, tokens // 16, body, 0)

    def scatter(row):
        for k in (3, 2, 1, 0):
            flights[row][k].wait()
            tile = terms.at[row, tiles[names[k]]]
            add(tile, core_terms.at[row, k])
            if k == 3:
                send(row, 5, tile, y_terms.at[row, 1], peers["y"])
            if k == 2:
                send(row, 4, tile, y_terms.at[row, 0], peers["y"])

    def pass_on(row):
        flights[row][5].wait()
        tile = terms.at[row, tiles["x"]]
        add(tile, y_terms.at[row, 1])
        send(row, 6, tile, x_terms.at[row], peers["x"])

    def close(row):
        for slot in (4, 6, 7):
            flights[row][slot].wait()
        mine = terms.at[row, tiles["own"]]
        width = 2 * half

        def body(i, carry):
            at = pl.ds(pl.multiple_of(i * 16, 16), 16)
            total = mine[at, :].astype(jnp.float32) + y_terms[row, 0, at, :].astype(jnp.float32)
            total = total.astype(low)
            out[row, at, group(x)] = query_grad[row, 0, at, :]
            out[row, at, group(x, width)] = total[:, :half]
            out[row, at, group(x, 2 * width)] = total[:, half:]
            out[row, at, group(1 - x)] = x_query[row, at, :]
            out[row, at, group(1 - x, width)] = x_terms[row, at, :half]
            out[row, at, group(1 - x, 2 * width)] = x_terms[row, at, half : 2 * half]
            return carry

        lax.fori_loop(0, tokens // 16, body, 0)

    part_copies = []

    def convolve():
        fill_shift(shift, tile_height, tile_width)
        patch = part.shape[2]
        taps[...] = mm(conv_turned[...], conv_in[...], 1, 1)
        rows = []
        for row in range(row_count):
            pieces = []
            for p in range(9):
                piece = taps[p * patch : (p + 1) * patch, row * tokens : (row + 1) * tokens]
                pieces.append(piece * same_image(cuts, row, p, tile_height, tile_width))
            rows.append(jnp.concatenate(pieces, axis=1))
        whole = jnp.concatenate(rows, axis=0)
        coarse = whole.astype(low)
        fine = (whole - coarse.astype(jnp.float32)).astype(low)
        moved = mm(coarse, shift[...], 1, 1) + mm(fine, shift[...], 1, 1)
        for tile in range(tile_count):
            part[tile] = moved[:, tile * tokens : (tile + 1) * tokens].reshape(row_count, patch, tokens)
        for k in range(1, tile_count):
            peer, tile = plane_peer(k)
            copy = pltpu.make_async_remote_copy(
                src_ref=part.at[tile],
                dst_ref=part_got.at[k],
                send_sem=part_send_sem.at[k],
                recv_sem=part_recv_sem.at[k],
                device_id=peer,
                device_id_type=MESH,
            )
            copy.start()
            part_copies.append(copy)
        conv_grad[...] = mm(conv_in[...], spread[...], 0, 1)

    def collect():
        total = part[tiles["own"]]
        for k, copy in enumerate(part_copies):
            copy.wait()
            total = total + part_got[k + 1]
        conv_out[...] = total.astype(low)

    def sum_up(item):
        item.step()
        item.save()

    for row in range(row_count):
        send(row, 8, grad_in.at[1 - x, row], grad.at[row, 1], peers["x"])
    for item in items:
        item.begin()
    if items and row_count == 3:
        fc1, fc2a, fc2b, proj = items
        fc1.step()
        fc2a.step()
        proj.step()
        fc2b.step()
        compute(0)
        fc1.step()
        begin(0)
        scatter(0)
        compute(1)
        begin(1)
        fc2b.step()
        proj.step()
        scatter(1)
        fc1.step()
        compute(2)
        pass_on(0)
        proj.step()
        begin(2)
        scatter(2)
        fc2b.step()
        pass_on(1)
        convolve()
        sum_up(proj)
        pass_on(2)
        sum_up(fc1)
        sum_up(fc2a)
        sum_up(fc2b)
        for row in range(row_count):
            close(row)
        collect()
    else:
        for row in range(row_count):
            compute(row)
            begin(row)
        for row in range(row_count):
            scatter(row)
        for row in range(row_count):
            pass_on(row)
        convolve()
        for row in range(row_count):
            close(row)
        collect()
    for item in items:
        item.land("save")


def attend_back(cuts, query, attended, grad, lse, conv_in, conv_turned, spread, all_pairs, grads, tile_height, tile_width):
    row_count, _, tokens, half = query.shape
    width = 2 * half
    kinds, sources, saves, shapes = [], [], [], []
    for start, paired, entry, rows, _ in grads:
        if not any(entry is source for source in sources):
            sources.append(entry)
        which = [entry is source for source in sources].index(True)
        kinds.append((start, paired, which, rows))
        depth = entry.shape[1] if rows is None else rows[1] - rows[0]
        shapes.append((depth, entry.shape[2] if paired else entry.shape[2] // 2))
        saves.append((depth if start == "z" else depth // 4, shapes[-1][1]))
    kinds = tuple(kinds)
    done = tuple(entry[4] for entry in grads)
    tile_count = all_pairs.shape[1]
    taps = conv_turned.shape[0]
    low, wide = jnp.bfloat16, jnp.float32
    vmem, anywhere = pl.BlockSpec(memory_space=pltpu.VMEM), pl.BlockSpec(memory_space=pl.ANY)
    return pl.pallas_call(
        functools.partial(attend_back_kernel, tile_height, tile_width, kinds, done),
        out_shape=[
            jax.ShapeDtypeStruct((row_count, tokens, 3 * width), low),
            jax.ShapeDtypeStruct((width, taps), wide),
            jax.ShapeDtypeStruct((row_count, taps // 9, tokens), low),
        ]
        + [jax.ShapeDtypeStruct(s, low) for s in saves],
        in_specs=[pl.BlockSpec(memory_space=pltpu.SMEM)] + [anywhere] * 4 + [vmem] * 3 + [anywhere] * (1 + len(sources)),
        out_specs=[vmem] * 3 + [anywhere] * len(saves),
        scratch_shapes=[
            pltpu.VMEM(query.shape, low),
            pltpu.VMEM(query.shape, low),
            pltpu.VMEM(query.shape, low),
            pltpu.VMEM(lse.shape, wide),
            pltpu.SemaphoreType.DMA((row_count, 5)),
            pltpu.VMEM((row_count, tile_count, tokens, width), low),
            pltpu.VMEM((row_count, tile_count, tokens, width), low),
            pltpu.VMEM((row_count, 4, tokens, width), low),
            pltpu.VMEM((row_count, 2, tokens, width), low),
            pltpu.VMEM((row_count, tokens, width), low),
            pltpu.VMEM((row_count, tokens, half), low),
            pltpu.VMEM(query.shape, low),
            pltpu.VMEM((2, tile_count * tokens, tokens), wide),
            pltpu.VMEM((tile_count * tokens, 9 * tokens), low),
            pltpu.VMEM((taps, row_count * tokens), wide),
            pltpu.VMEM((tile_count, row_count, taps // 9, tokens), wide),
            pltpu.VMEM((tile_count, row_count, taps // 9, tokens), wide),
            pltpu.SemaphoreType.DMA((row_count, 9)),
            pltpu.SemaphoreType.DMA((row_count, 9)),
            pltpu.SemaphoreType.DMA((tile_count,)),
            pltpu.SemaphoreType.DMA((tile_count,)),
        ]
        + (reducer_scratch([kind[:2] for kind in kinds], shapes) if kinds else []),
        compiler_params=pltpu.CompilerParams(
            collective_id=2, has_side_effects=True, vmem_limit_bytes=full_vmem
        ),
        name="attend_back",
    )(cuts, query, attended, grad, lse, conv_in, conv_turned, spread, all_pairs, *sources)


def add_rows(target, first, second, rows):
    def body(i, carry):
        at = pl.ds(pl.multiple_of(i * 16, 16), 16)
        target[at, :] = first[at, :] + second[at, :]
        return carry

    lax.fori_loop(0, rows // 16, body, 0)


def add_four(target, others, rows):
    def body(i, carry):
        at = pl.ds(pl.multiple_of(i * 16, 16), 16)
        total = target[at, :].astype(jnp.float32) + others[0, at, :].astype(jnp.float32)
        total = total + (others[1, at, :].astype(jnp.float32) + others[2, at, :].astype(jnp.float32))
        target[at, :] = total.astype(jnp.bfloat16)
        return carry

    lax.fori_loop(0, rows // 16, body, 0)


def chip_peers():
    z, ty, y = lax.axis_index("rows"), lax.axis_index("ty"), lax.axis_index("tx")
    core, x = lax.rem(ty, 2), ty // 2
    across = (1 - x) * 2 + core
    return {
        "core": (z, x * 2 + 1 - core, y),
        "x": (z, across, y),
        "y": (z, ty, 1 - y),
        "xy": (z, across, 1 - y),
        "z": [(lax.rem(z + k, 4), ty, y) for k in (1, 2, 3)],
    }


class Reducer:
    def __init__(self, start, paired, relays, grad, out, buffers, sems, w):
        self.relays, self.halved = relays, 0
        self.start, self.paired, self.grad, self.out, self.w = start, paired, grad, out, w
        self.local_sem, self.send_sem, self.recv_sem = sems
        self.z, ty, self.y = lax.axis_index("rows"), lax.axis_index("ty"), lax.axis_index("tx")
        self.core, self.x = lax.rem(ty, 2), ty // 2
        self.peers = chip_peers()
        self.flying = {}
        self.own = buffers[0]
        if start in ("plane", "z"):
            self.half, self.quarter, self.final = buffers[1:4]
            self.got = None if paired else buffers[4]
            self.depth, self.width = grad.shape[1], grad.shape[2] if paired else grad.shape[2] // 2
        else:
            self.depth, self.width = out.shape[1], out.shape[2]
        if start == "block":
            self.half, self.quarter = buffers[1:]
        share = [self.relay, self.pass_strip] if relays else [self.pass_strip]
        late = [self.begin_late, self.add_half_late, self.add_quarter_late, *share, self.end]
        self.stages = {
            "plane": [self.add_core, self.add_half, self.add_quarter, self.sum_z, self.gather_piece, *share, self.end],
            "z": [self.add_core, self.sum_z_first] + late,
            "block": late,
            "piece": [self.gather_piece, *share, self.end],
        }[start]

    def step(self):
        self.stages.pop(0)()

    def part(self, at):
        if self.start == "block":
            return self.own.at[at]
        return self.own.at[self.z, at]

    def send(self, slot, source, target, peer):
        copy = pltpu.make_async_remote_copy(
            src_ref=source,
            dst_ref=target,
            send_sem=self.send_sem.at[self.w, slot],
            recv_sem=self.recv_sem.at[self.w, slot],
            device_id=peer,
            device_id_type=MESH,
        )
        copy.start()
        return copy

    def keep(self, slot, source, target):
        copy = pltpu.make_async_copy(source, target, self.local_sem.at[self.w, slot])
        copy.start()
        return copy

    def land(self, name):
        for copy in self.flying.pop(name):
            copy.wait()

    def columns(self, which):
        return pl.ds(pl.multiple_of(which * self.width, 128), self.width)

    def rows(self, start, size):
        return pl.ds(pl.multiple_of(start, 16), size)

    def place(self, block, flip_x=False, flip_y=False):
        x = 1 - self.x if flip_x else self.x
        y = 1 - self.y if flip_y else self.y
        later = block // 2
        major = x + later * (y - x)
        minor = y + later * (x - y)
        return self.rows(major * (self.depth // 2) + minor * (self.depth // 4), self.depth // 4)

    def pieces(self, flip_x=False, flip_y=False):
        if self.start in ("plane", "piece"):
            return [self.place(self.z, flip_x, flip_y)]
        x = 1 - self.x if flip_x else self.x
        y = 1 - self.y if flip_y else self.y
        half, less, least = self.depth // 2, self.depth // 4, self.depth // 8
        return [self.rows(x * less + y * least, least), self.rows(half + y * less + x * least, least)]

    def begin(self):
        if self.start in ("block", "piece"):
            self.flying["load"] = [self.keep(0, self.grad, self.own)]
            return
        if self.paired:
            self.flying["core"] = [self.keep(0, self.grad, self.own)]
            return
        swap = self.send(0, self.grad.at[:, :, self.columns(1 - self.core)], self.got, self.peers["core"])
        mine = self.keep(0, self.grad.at[:, :, self.columns(self.core)], self.own)
        self.flying["core"] = [swap, mine]

    def add_core(self):
        self.land("core")
        if not self.paired:
            for block in range(4):
                add_rows(self.own.at[block], self.own.at[block], self.got.at[block], self.depth)
        if self.start == "z":
            self.flying["z"] = [
                self.send(5 + k, self.own.at[peer[0]], self.final.at[k], peer) for k, peer in enumerate(self.peers["z"])
            ]
            return
        part = self.depth // 2
        rest = pl.ds(self.halved, self.width - self.halved)
        theirs = [self.rows((1 - side) * part, part) for side in (self.x, self.y)]
        first = self.send(1, self.own.at[0:2, theirs[0], rest], self.half.at[0:2, :, rest], self.peers["x"])
        second = self.send(2, self.own.at[2:4, theirs[1], rest], self.half.at[2:4, :, rest], self.peers["y"])
        self.flying["half"] = [first, second]

    def add_half(self):
        self.land("half")
        part, less = self.depth // 2, self.depth // 4
        for block in range(4):
            side = self.x if block < 2 else self.y
            rest = pl.ds(self.halved, self.width - self.halved)
            kept = self.own.at[block, self.rows(side * part, part), rest]
            add_rows(kept, kept, self.half.at[block, :, rest], part)
        first = self.own.at[0:2, self.rows(self.x * part + (1 - self.y) * less, less)]
        second = self.own.at[2:4, self.rows(self.y * part + (1 - self.x) * less, less)]
        self.flying["quarter"] = [
            self.send(3, first, self.quarter.at[0:2], self.peers["y"]),
            self.send(4, second, self.quarter.at[2:4], self.peers["x"]),
        ]

    def add_quarter(self):
        self.land("quarter")
        for block in range(4):
            kept = self.own.at[block, self.place(block // 2 * 2)]
            add_rows(kept, kept, self.quarter.at[block], self.depth // 4)
        self.flying["z"] = [
            self.send(5 + k, self.own.at[peer[0], self.place(peer[0])], self.final.at[k], peer)
            for k, peer in enumerate(self.peers["z"])
        ]

    def gather(self, pieces, sources):
        copies = []
        for n, (at, source) in enumerate(zip(pieces, sources)):
            target = self.out.at[self.core, at]
            for k, name in enumerate(("x", "y") if self.relays else ("x", "y", "xy")):
                copies.append(self.send(8 + 3 * n + k, source, target, self.peers[name]))
            copies.append(self.keep(1 + n, source, target))
        self.flying["gather"] = copies

    def relay(self):
        self.land("gather")
        cut = self.width // 256 * 128 + (128 if self.width % 256 and self.w % 2 else 0)
        copies = []
        for n, (from_x, from_y) in enumerate(zip(self.pieces(flip_x=True), self.pieces(flip_y=True))):
            first = self.out.at[self.core, from_x, pl.ds(0, cut)]
            second = self.out.at[self.core, from_y, pl.ds(cut, self.width - cut)]
            copies.append(self.send(14 + 2 * n + 1, first, first, self.peers["y"]))
            copies.append(self.send(14 + 2 * n + 2, second, second, self.peers["x"]))
        self.flying["relay"] = copies

    def sum_z(self):
        self.land("z")
        add_four(self.own.at[self.z, self.place(self.z)], self.final, self.depth // 4)

    def gather_piece(self):
        if self.start == "piece":
            self.land("load")
            self.gather([self.place(self.z)], [self.own])
        else:
            self.gather([self.place(self.z)], [self.own.at[self.z, self.place(self.z)]])

    def sum_z_first(self):
        self.land("z")
        add_four(self.own.at[self.z], self.final, self.depth)

    def save(self):
        source = self.own.at[self.z] if self.start == "z" else self.own.at[self.z, self.place(self.z)]
        self.flying["save"] = [self.keep(1, source, self.out)]

    def begin_late(self):
        if self.start == "block":
            self.land("load")
        half, less = self.depth // 2, self.depth // 4
        self.flying["half"] = [
            self.send(1, self.part(self.rows((1 - self.x) * less, less)), self.half.at[0], self.peers["x"]),
            self.send(2, self.part(self.rows(half + (1 - self.y) * less, less)), self.half.at[1], self.peers["y"]),
        ]

    def add_half_late(self):
        self.land("half")
        half, less, least = self.depth // 2, self.depth // 4, self.depth // 8
        for n, start in enumerate((self.x * less, half + self.y * less)):
            kept = self.part(self.rows(start, less))
            add_rows(kept, kept, self.half.at[n], less)
        first = self.part(self.rows(self.x * less + (1 - self.y) * least, least))
        second = self.part(self.rows(half + self.y * less + (1 - self.x) * least, least))
        self.flying["quarter"] = [
            self.send(3, first, self.quarter.at[0], self.peers["y"]),
            self.send(4, second, self.quarter.at[1], self.peers["x"]),
        ]

    def add_quarter_late(self):
        self.land("quarter")
        least = self.depth // 8
        pieces = self.pieces()
        for n, at in enumerate(pieces):
            add_rows(self.part(at), self.part(at), self.quarter.at[n], least)
        self.gather(pieces, [self.part(at) for at in pieces])

    def pass_strip(self):
        self.land("relay" if self.relays else "gather")
        strip = self.out.at[self.core]
        self.flying["strip"] = [self.send(14, strip, strip, self.peers["core"])]

    def end(self):
        self.land("strip")


def reducer_scratch(kinds, shapes):
    buffers = []
    for (start, paired), (depth, half) in zip(kinds, shapes):
        sizes = {
            "plane": [(4, depth, half), (4, depth // 2, half), (4, depth // 4, half), (3, depth // 4, half)],
            "z": [(4, depth, half), (2, depth // 4, half), (2, depth // 8, half), (3, depth, half)],
            "block": [(depth, half), (2, depth // 4, half), (2, depth // 8, half)],
            "piece": [(depth // 4, half)],
        }[start]
        if not paired:
            sizes.append((4, depth, half))
        buffers += [pltpu.VMEM(size, jnp.bfloat16) for size in sizes]
    count = len(kinds)
    return buffers + [
        pltpu.SemaphoreType.DMA((count, 3)),
        pltpu.SemaphoreType.DMA((count, 19)),
        pltpu.SemaphoreType.DMA((count, 19)),
    ]


def make_reducers(kinds, grads, outs, scratch, relays=()):
    items, at = [], 0
    for w, ((start, paired), grad, out) in enumerate(zip(kinds, grads, outs)):
        size = {"plane": 4, "z": 4, "block": 3, "piece": 1}[start] + (0 if paired else 1)
        items.append(Reducer(start, paired, w in relays, grad, out, scratch[at : at + size], scratch[-3:], w))
        at = at + size
    return items


def sum_by_table(local_grads):
    band_count, column_count = lax.axis_size("ty"), lax.axis_size("tx")
    group_count = lax.axis_size("rows")
    tile_count = band_count * column_count
    table = jnp.concatenate([entry.reshape(group_count, -1) for entry in local_grads], axis=1)
    column_total = table.shape[1]
    padded_columns = -(-column_total // tile_count) * tile_count
    piece_width = padded_columns // tile_count
    table = table.reshape(group_count, tile_count, piece_width)
    shares = lax.psum_scatter(
        table.reshape(group_count * tile_count, piece_width),
        ("rows", "ty", "tx"),
        scatter_dimension=0,
        tiled=True,
    )
    summed = (
        lax.all_gather(shares.astype(jnp.bfloat16), ("ty", "tx"), axis=0, tiled=True)
        .astype(shares.dtype)
        .reshape(-1)
    )
    totals = []
    start_at = 0
    for entry in local_grads:
        length = entry.size // group_count
        shard_shape = (entry.shape[0] // group_count,) + entry.shape[1:]
        totals.append(summed[start_at : start_at + length].reshape(shard_shape))
        start_at = start_at + length
    return tuple(totals)


def shards(
    latent,
    skip_input,
    segment_ids,
    embed_weight,
    embed_bias,
    skip_weight,
    skip_bias,
    norm1_gain,
    norm1_bias,
    qkv_weight,
    proj_weight,
    proj_bias,
    norm2_gain,
    norm2_bias,
    fc1_weight,
    fc1_bias,
    fc2_weight,
    fc2_bias,
    conv_weight,
    cotangent,
):
    row_count, tile_height, tile_width, width = skip_input.shape
    patch = latent.shape[3]
    tokens = tile_height * tile_width
    token_count = row_count * tokens
    low = jnp.bfloat16
    wide = jnp.float32
    conv_turned = conv_weight.T
    flat_latent = latent.reshape(token_count, patch)
    flat_skip = skip_input.reshape(token_count, width)
    biases = (embed_bias, skip_bias, norm1_gain, norm1_bias, proj_bias, norm2_gain, norm2_bias, fc2_bias)
    embedded, stream, normed, query, pairs, cot, vectors, hidden_bias, cuts = front(
        segment_ids, flat_latent, cotangent.reshape(token_count, patch), embed_weight.T, biases, fc1_bias,
        flat_skip, skip_weight, qkv_weight, row_count,
    )
    attended, log_total, held_query, held_attended, held_pairs, spread, out_grad, active_grad = attend(
        cuts, query, pairs, cot, conv_turned, fc2_weight, tile_height, tile_width
    )
    here = (lax.axis_size("rows"), lax.axis_size("ty"), lax.axis_size("tx")) == (4, 4, 2)
    fc1_grad, fc2_grad, hidden_bias_grad, proj_grad, attended_grad, mid_grad, conv_in, middle_grads = middle(
        attended.reshape(2, token_count, width // 2), stream, out_grad, active_grad, proj_weight, vectors, hidden_bias,
        fc1_weight, fc2_weight, here,
    )
    early = []
    if here:
        fc2_blocks = fc2_grad.reshape(4, -1, width // 2)
        middle_row = fc2_blocks.shape[1] // 2
        early = [
            ("plane", True, fc1_grad, None, fc1_grad.shape[2] * 3 // 4),
            ("z", True, fc2_blocks, (0, middle_row), 0),
            ("plane", True, fc2_blocks, (middle_row, 2 * middle_row), 0),
            ("plane", False, proj_grad.reshape(4, -1, width), None, 0),
        ]
    projected_grad, conv_grad, conv_out, *saved = attend_back(
        cuts, held_query, held_attended, attended_grad.reshape(2, row_count, tokens, width // 2), log_total,
        conv_in, conv_turned, spread, held_pairs, early, tile_height, tile_width,
    )
    follow = {"plane": "piece", "z": "block"}
    resumed = [
        (follow[start], entry, (entry.shape[0] if start == "z" else 4 * entry.shape[0], entry.shape[1]))
        for (start, *_), entry in zip(early, saved)
    ]
    skip_input_grad, *rest = rear(
        projected_grad.reshape(token_count, 3 * width), qkv_weight, normed, stream, mid_grad, embedded, flat_skip,
        skip_weight, flat_latent, vectors, middle_grads, hidden_bias_grad, conv_grad, resumed, here,
    )
    taps = 9 * patch
    share = width // 4
    if here:
        half = width // 2
        places = [(0, 0, half, 0), (1, 0, half, 0), (1, middle_row, half, 0), (2, 0, half, 0)]
        places += [(3, 0, half, k * width) for k in range(3)] + [(4, 0, half, 0)]
        totals = finish([place + (entry,) for place, entry in zip(places, rest[:8])], rest[8], rest[9], conv_out, skip_input_grad)
        fc1_total, fc2_total, proj_total, qkv_total, skip_total, embed_turned, conv_grad_turned = totals[:7]
        line, fc1_line = totals[7:15], totals[15]
        output = totals[16].reshape(row_count, tile_height, tile_width, patch)
        skip_input_grad = totals[17].reshape(skip_input.shape)
        return (
            output, skip_input_grad, embed_turned.T, line[0], skip_total, line[1], line[2], line[3], qkv_total,
            proj_total, line[4], line[5], line[6], fc1_total, fc1_line, fc2_total, line[7], conv_grad_turned.T,
        )
    output = conv_out.transpose(0, 2, 1).reshape(row_count, tile_height, tile_width, patch)
    skip_input_grad = skip_input_grad.reshape(skip_input.shape)
    qkv_grad = jnp.concatenate([entry.reshape(-1, width) for entry in rest[:3]], axis=1)
    skip_grad, thin = [entry.reshape(-1, entry.shape[2]) for entry in rest[3:5]]
    flat = rest[5]
    fc1_grad = fc1_grad.reshape(width, -1)
    line = [flat[:, k, :share].reshape(-1) for k in range(8)]
    fc1_line = flat[:, 8:11].reshape(-1)
    local_grads = [
        thin[:, taps : taps + patch], line[0], skip_grad, line[1], line[2], line[3], qkv_grad, proj_grad, line[4],
        line[5], line[6], fc1_grad, fc1_line, fc2_grad, line[7], thin[:, :taps],
    ]
    return (output, skip_input_grad) + sum_by_table([entry.astype(wide) for entry in local_grads])


def solution(mesh):
    return jax.shard_map(
        shards,
        mesh=mesh,
        in_specs=(
            P("rows", "ty", "tx", None),
            P("rows", "ty", "tx", None),
            P("rows", None, None),
            P(),
            P(),
            P(),
            P(),
            P(),
            P(),
            P(),
            P(),
            P(),
            P(),
            P(),
            P(),
            P(),
            P(),
            P(),
            P(),
            P("rows", "ty", "tx", None),
        ),
        out_specs=(
            P("rows", "ty", "tx", None),
            P("rows", "ty", "tx", None),
            P("rows", None),
            P("rows"),
            P("rows", None),
            P("rows"),
            P("rows"),
            P("rows"),
            P("rows", None),
            P("rows", None),
            P("rows"),
            P("rows"),
            P("rows"),
            P("rows", None),
            P("rows"),
            P("rows", None),
            P("rows"),
            P("rows", None),
        ),
        check_vma=False,
    )
```
